32 devices in a mesh: dp: 8 (over y, x, core), tensor: 4 (over z).
Axes of the slice: x: 2, y: 2, z: 4, core: 2. Of those that a mesh axis runs over, the one named last changes fastest.
Arguments:
- block_in: bfloat16 [12288, 1536], P(('dp', 'tensor')), may hold values from -6 to 6
- cotangent: bfloat16 [12288, 1536], P(('dp', 'tensor')), may hold values from -6 to 6
- segment_ids: int32 [24, 512], P('dp'), may hold values from 0 to 3, never falling along the last dimension, each value on 1 to 256 neighbouring positions
- attn_gain: bfloat16 [1536], P('dp'), may hold values from 0.5 to 1.5
- qkv_weight: bfloat16 [1536, 3072], P('dp', 'tensor'), may hold values from -4 to 4
- out_weight: bfloat16 [1536, 1536], P('tensor', 'dp'), may hold values from -1.25 to 1.25
- mlp_gain: bfloat16 [1536], P('dp'), may hold values from 0.5 to 1.5
- gate_weight: bfloat16 [1536, 4096], P('dp', 'tensor'), may hold values from -0.15625 to 0.15625
- up_weight: bfloat16 [1536, 4096], P('dp', 'tensor'), may hold values from -0.15625 to 0.15625
- down_weight: bfloat16 [4096, 1536], P('tensor', 'dp'), may hold values from -0.09375 to 0.09375
Outputs:
- block_out: bfloat16 [12288, 1536], P(('dp', 'tensor'))
- input_grad: bfloat16 [12288, 1536], P(('dp', 'tensor'))
- attn_gain_grad: float32 [1536], P('dp')
- qkv_grad: float32 [1536, 3072], P('dp', 'tensor')
- out_grad: float32 [1536, 1536], P('tensor', 'dp')
- mlp_gain_grad: float32 [1536], P('dp')
- gate_grad: float32 [1536, 4096], P('dp', 'tensor')
- up_grad: float32 [1536, 4096], P('dp', 'tensor')
- down_grad: float32 [4096, 1536], P('tensor', 'dp')
The draws below stay inside these ranges and needn't reach their ends.
Inputs may be any that keep to these rules, and one draw needn't show every extreme that they name: `segment_ids`: segment numbers never fall along a sequence; a segment holds at most 256 tokens of its sequence, and some segment of every sequence holds exactly that many.
All inputs are finite; a program needn't handle non-finite values.
Results may differ from the reference program's by a relative error of at most 0.025.
The reference program's roundings to bfloat16 on the way count: a program that leaves them out, or rounds other values in their place, can miss the bound.
Values may be sent and summed in bfloat16 or wider, within the bound.
A program may use at most 192 MiB of HBM per device.

```python
import math
import jax
import jax.numpy as jnp
import numpy as np
from jax import lax

MODEL_WIDTH = 1536
QUERY_HEADS = 16
KEY_VALUE_HEADS = 8
HEAD_SIZE = 96
FF = 4096
SEQ = 512
SEQS = 24
TOKENS = 12288


def draw_qkv_weight(key, part):
    repeat_factor = QUERY_HEADS // KEY_VALUE_HEADS
    complete_shape = (MODEL_WIDTH, KEY_VALUE_HEADS, repeat_factor + 2, HEAD_SIZE)
    rotary_base = jnp.clip(jax.random.normal(key, complete_shape, jnp.float32), -6.0, 6.0) * MODEL_WIDTH ** (-0.5)
    return rotary_base.reshape(MODEL_WIDTH, KEY_VALUE_HEADS * (repeat_factor + 2) * HEAD_SIZE).astype(jnp.bfloat16)


def levels(stream_key, extent, shards, least, top_value):
    def one(axis_at, parts):
        steps = jax.random.uniform(jax.random.fold_in(jax.random.fold_in(stream_key, 6), axis_at), (parts,), jnp.float32, least / len(shards), top_value / len(shards))
        return jnp.repeat(jnp.exp(steps), extent[axis_at] // parts).reshape((-1,) + (1,) * (len(extent) - axis_at - 1))

    gain = one(*shards[0])
    for cut in shards[1:]:
        gain = gain * one(*cut)
    return gain


def split_up(amount, total, bound, skew):
    weights = [(1 << 20) // math.isqrt(rank ** skew) + 1 for rank in range(2, amount + 1)]
    rest, holding = total - bound - (amount - 1), [1] * (amount - 1)
    while rest > 0:
        movable = [i for i in range(amount - 1) if holding[i] < bound]
        whole, left = sum([weights[i] for i in movable]), rest
        for i in movable:
            addition = min(bound - holding[i], max(1, left * weights[i] // whole), rest)
            holding[i] = holding[i] + addition
            rest = rest - addition
    return np.array([bound] + holding)


def ragged(own_key, number_of, total, limit, skew):
    if number_of == 2:
        one = jax.random.randint(own_key, (), max(1, total - limit), min(limit, total - 1) + 1)
        return jnp.stack([one, total - one])
    tallies = jnp.asarray(split_up(number_of, total, limit, skew), jnp.int32)
    couples = (number_of - 1) // 2
    giver, sink = tallies[1:1 + 2 * couples:2], tallies[2:2 + 2 * couples:2]
    margin = jnp.minimum(giver - 1, limit - sink)
    moved = jax.random.randint(jax.random.fold_in(own_key, 1), (couples,), 0, 1 << 20) % (margin + 1)
    tallies = tallies.at[1:1 + 2 * couples:2].set(giver - moved).at[2:2 + 2 * couples:2].set(sink + moved)
    return tallies[jax.random.permutation(jax.random.fold_in(own_key, 2), number_of)]


def noise(key, shape, width, most, shards=(), held_as=jnp.bfloat16):
    array = width * jax.random.normal(key, shape, jnp.float32)
    if shards:
        array = array * levels(key, shape, shards, -0.22, 0.18)
    return jnp.clip(array, -most, most).astype(held_as)


def setup_inputs(seed: int = 0) -> dict:
    key_list = jax.random.split(jax.random.key(seed), 11)
    return {
        "block_in": noise(key_list[0], (TOKENS, MODEL_WIDTH), 1.0, 6.0, ((0, 32),)),
        "cotangent": noise(key_list[1], (TOKENS, MODEL_WIDTH), 1.0, 6.0, ((0, 32),)),
        "segment_ids": jax.vmap(lambda own: jnp.searchsorted(jnp.cumsum(ragged(own, 4, SEQ, SEQ // 2, 0)), jnp.arange(SEQ), side="right"))(jax.random.split(key_list[2], SEQS)).reshape((SEQS, SEQ)).astype(jnp.int32),
        "attn_gain": jnp.clip(1.0 + 0.1 * jax.random.normal(key_list[3], (MODEL_WIDTH,), jnp.float32), 0.5, 1.5).astype(jnp.bfloat16),
        "qkv_weight": draw_qkv_weight(jax.random.fold_in(key_list[10], 71), 0),
        "out_weight": noise(key_list[5], (QUERY_HEADS * HEAD_SIZE, MODEL_WIDTH), (QUERY_HEADS * HEAD_SIZE // 64) ** -0.5, 1.25, ((0, 4), (1, 8))),
        "mlp_gain": jnp.clip(1.0 + 0.1 * jax.random.normal(key_list[6], (MODEL_WIDTH,), jnp.float32), 0.5, 1.5).astype(jnp.bfloat16),
        "gate_weight": noise(key_list[7], (MODEL_WIDTH, FF), MODEL_WIDTH ** -0.5, 0.15625, ((0, 8), (1, 4))),
        "up_weight": noise(key_list[8], (MODEL_WIDTH, FF), MODEL_WIDTH ** -0.5, 0.15625, ((0, 8), (1, 4))),
        "down_weight": noise(key_list[9], (FF, MODEL_WIDTH), FF ** -0.5, 0.09375, ((0, 4), (1, 8))),
    }


EPS = 1e-05
ROPE_BASE = 100000.0
NEG_FILL = -1e+30

def doc_positions(segments):
    length = segments.shape[1]
    position_index = jnp.broadcast_to(jnp.arange(length, dtype=jnp.int32)[None, :], segments.shape)
    change = jnp.concatenate([jnp.ones((segments.shape[0], 1), dtype=bool), segments[:, 1:] != segments[:, :-1]], axis=1)
    starts = lax.cummax(jnp.where(change, position_index, jnp.zeros_like(position_index)), axis=1)
    return position_index - starts

def rotary_tables(segments):
    half_dim = HEAD_SIZE // 2
    frequency = jnp.power(ROPE_BASE, -(2.0 * jnp.arange(half_dim, dtype=jnp.float32)) / HEAD_SIZE)
    angles = doc_positions(segments).astype(jnp.float32)[..., None] * frequency
    cosine_table = jnp.concatenate([jnp.cos(angles), jnp.cos(angles)], axis=-1)
    sine_table = jnp.concatenate([jnp.sin(angles), jnp.sin(angles)], axis=-1)
    return (cosine_table, sine_table)

def rotate(vector, cosine_table, sine_table):
    half_dim = vector.shape[-1] // 2
    turned = jnp.concatenate([-vector[..., half_dim:], vector[..., :half_dim]], axis=-1)
    return vector * cosine_table + turned * sine_table

def unrotate(vector, cosine_table, sine_table):
    half_dim = vector.shape[-1] // 2
    shifted = vector * sine_table
    returned = jnp.concatenate([shifted[..., half_dim:], -shifted[..., :half_dim]], axis=-1)
    return vector * cosine_table + returned

def allowed_pairs(segments):
    length = segments.shape[1]
    offsets = jnp.arange(length)
    causal = offsets[None, :] <= offsets[:, None]
    same_doc = segments[:, :, None] == segments[:, None, :]
    return (causal[None] & same_doc)[:, None, None]

def score_block(queries, key_heads, segments):
    scores = jnp.einsum('sqgrd,skgd->sgrqk', queries.astype(jnp.float32), key_heads.astype(jnp.float32)) * HEAD_SIZE ** (-0.5)
    return jnp.where(allowed_pairs(segments), scores, NEG_FILL)

def rms_scale(features):
    return lax.rsqrt(lax.optimization_barrier(jnp.mean(features * features, axis=-1, keepdims=True)) + EPS)

def norm_back(features, inverse, gain_vector, upstream):
    scaled = gain_vector * upstream
    return inverse * scaled - features * (inverse * inverse * inverse) * lax.optimization_barrier(jnp.mean(scaled * features, axis=-1, keepdims=True))

def layer(rows_in, cot_in, segments, attn_gain, qkv_weight, out_weight, mlp_gain, gate_weight, up_weight, down_weight):
    seq_count, length = segments.shape
    repeat_factor = QUERY_HEADS // KEY_VALUE_HEADS
    groups = qkv_weight.shape[1] // ((repeat_factor + 2) * HEAD_SIZE)
    gain_attn = attn_gain.astype(jnp.float32)
    gain_mlp = mlp_gain.astype(jnp.float32)
    residual = rows_in.astype(jnp.float32)
    scale_attn = rms_scale(residual)
    normed1 = (residual * scale_attn * gain_attn).astype(jnp.bfloat16)
    projected = jnp.dot(normed1, qkv_weight, preferred_element_type=jnp.float32).reshape(seq_count, length, groups, repeat_factor + 2, HEAD_SIZE)
    cosine_table, sine_table = rotary_tables(segments)
    cos_query = cosine_table[:, :, None, None, :]
    sin_query = sine_table[:, :, None, None, :]
    cos_key = cosine_table[:, :, None, :]
    sin_key = sine_table[:, :, None, :]
    queries = rotate(projected[:, :, :, :repeat_factor], cos_query, sin_query).astype(jnp.bfloat16)
    key_heads = rotate(projected[:, :, :, repeat_factor], cos_key, sin_key).astype(jnp.bfloat16)
    values = projected[:, :, :, repeat_factor + 1].astype(jnp.bfloat16)
    scores = score_block(queries, key_heads, segments)
    highest = lax.optimization_barrier(jnp.max(scores, axis=-1, keepdims=True))
    log_total = highest + jnp.log(lax.optimization_barrier(jnp.sum(jnp.exp(scores - highest), axis=-1, keepdims=True)))
    probability = jnp.exp(scores - log_total).astype(jnp.bfloat16)
    attended = jnp.einsum('sgrqk,skgd->sqgrd', probability.astype(jnp.float32), values.astype(jnp.float32)).astype(jnp.bfloat16)
    attn_flat = attended.reshape(seq_count * length, groups * repeat_factor * HEAD_SIZE)
    hidden1 = residual + jnp.dot(attn_flat, out_weight, preferred_element_type=jnp.float32)
    scale_mlp = rms_scale(hidden1)
    normed2 = (hidden1 * scale_mlp * gain_mlp).astype(jnp.bfloat16)
    gate = jnp.dot(normed2, gate_weight, preferred_element_type=jnp.float32)
    up_value = jnp.dot(normed2, up_weight, preferred_element_type=jnp.float32)
    sigmoid_gate = jax.nn.sigmoid(gate)
    activated = (gate * sigmoid_gate * up_value).astype(jnp.bfloat16)
    block_out = (hidden1 + jnp.dot(activated, down_weight, preferred_element_type=jnp.float32)).astype(jnp.bfloat16)
    down_grad = jnp.dot(activated.T, cot_in, preferred_element_type=jnp.float32)
    act_grad = jnp.dot(cot_in, down_weight.T, preferred_element_type=jnp.float32)
    gate_delta = (act_grad * up_value * sigmoid_gate * (1.0 + gate * (1.0 - sigmoid_gate))).astype(jnp.bfloat16)
    up_delta = (act_grad * gate * sigmoid_gate).astype(jnp.bfloat16)
    gate_grad = jnp.dot(normed2.T, gate_delta, preferred_element_type=jnp.float32)
    up_grad = jnp.dot(normed2.T, up_delta, preferred_element_type=jnp.float32)
    normed2_grad = jnp.dot(gate_delta, gate_weight.T, preferred_element_type=jnp.float32) + jnp.dot(up_delta, up_weight.T, preferred_element_type=jnp.float32)
    mlp_gain_grad = lax.optimization_barrier(jnp.sum(normed2_grad * hidden1 * scale_mlp, axis=0))
    hidden1_grad = cot_in.astype(jnp.float32) + norm_back(hidden1, scale_mlp, gain_mlp, normed2_grad)
    hidden1_rounded = hidden1_grad.astype(jnp.bfloat16)
    out_grad = jnp.dot(attn_flat.T, hidden1_rounded, preferred_element_type=jnp.float32)
    attended_grad = jnp.dot(hidden1_rounded, out_weight.T, preferred_element_type=jnp.float32).astype(jnp.bfloat16)
    attended_grad = attended_grad.reshape(seq_count, length, groups, repeat_factor, HEAD_SIZE)
    prob_full = jnp.exp(score_block(queries, key_heads, segments) - log_total)
    prob_grad = jnp.einsum('sqgrd,skgd->sgrqk', attended_grad.astype(jnp.float32), values.astype(jnp.float32))
    inner_sum = lax.optimization_barrier(jnp.sum(prob_full * prob_grad, axis=-1, keepdims=True))
    score_grad = (prob_full * (prob_grad - inner_sum) * HEAD_SIZE ** (-0.5)).astype(jnp.bfloat16)
    query_grad = jnp.einsum('sgrqk,skgd->sqgrd', score_grad.astype(jnp.float32), key_heads.astype(jnp.float32))
    key_grad = jnp.einsum('sgrqk,sqgrd->skgd', score_grad.astype(jnp.float32), queries.astype(jnp.float32))
    value_grad = jnp.einsum('sgrqk,sqgrd->skgd', prob_full.astype(jnp.bfloat16).astype(jnp.float32), attended_grad.astype(jnp.float32))
    projected_grad = jnp.concatenate([unrotate(query_grad, cos_query, sin_query), unrotate(key_grad, cos_key, sin_key)[:, :, :, None], value_grad[:, :, :, None]], axis=3)
    projected_grad = projected_grad.astype(jnp.bfloat16).reshape(seq_count * length, groups * (repeat_factor + 2) * HEAD_SIZE)
    qkv_grad = jnp.dot(normed1.T, projected_grad, preferred_element_type=jnp.float32)
    normed1_grad = jnp.dot(projected_grad, qkv_weight.T, preferred_element_type=jnp.float32)
    attn_gain_grad = lax.optimization_barrier(jnp.sum(normed1_grad * residual * scale_attn, axis=0))
    input_grad = (hidden1_grad + norm_back(residual, scale_attn, gain_attn, normed1_grad)).astype(jnp.bfloat16)
    return (block_out, input_grad, (attn_gain_grad, qkv_grad, out_grad, mlp_gain_grad, gate_grad, up_grad, down_grad))

def reference(block_in, cotangent, segment_ids, attn_gain, qkv_weight, out_weight, mlp_gain, gate_weight, up_weight, down_weight):
    per_block = math.gcd(SEQS, max(1, 4096 // SEQ))
    blocks = SEQS // per_block
    row_block = per_block * SEQ
    inputs_all = (block_in.reshape(blocks, row_block, MODEL_WIDTH), cotangent.reshape(blocks, row_block, MODEL_WIDTH), segment_ids.reshape(blocks, per_block, SEQ))
    initial = (jnp.zeros((MODEL_WIDTH,), jnp.float32), jnp.zeros(qkv_weight.shape, jnp.float32), jnp.zeros(out_weight.shape, jnp.float32), jnp.zeros((MODEL_WIDTH,), jnp.float32), jnp.zeros(gate_weight.shape, jnp.float32), jnp.zeros(up_weight.shape, jnp.float32), jnp.zeros(down_weight.shape, jnp.float32))

    def step(totals, inputs_block):
        rows_in, cot_in, seg_in = inputs_block
        result_out, result_grad, grads = layer(rows_in, cot_in, seg_in, attn_gain, qkv_weight, out_weight, mlp_gain, gate_weight, up_weight, down_weight)
        summed = tuple((left_sum + right_sum for left_sum, right_sum in zip(totals, grads)))
        return (summed, (result_out, result_grad))
    totals, (outputs_all, grads_all) = lax.scan(step, initial, inputs_all)
    return (outputs_all.reshape(TOKENS, MODEL_WIDTH), grads_all.reshape(TOKENS, MODEL_WIDTH), totals[0], totals[1], totals[2], totals[3], totals[4], totals[5], totals[6])
```

```python
import jax
import jax.numpy as jnp
from jax import lax
from jax.experimental import pallas as pl
from jax.experimental.pallas import tpu as pltpu
from jax.sharding import PartitionSpec as P

QUERY_HEADS = 16
KEY_VALUE_HEADS = 8
HEAD_SIZE = 96


EPS = 1e-05
ROPE_BASE = 100000.0
NEG_FILL = -1e30


def doc_positions(segments):
    length = segments.shape[1]
    position_index = jnp.broadcast_to(jnp.arange(length, dtype=jnp.int32)[None, :], segments.shape)
    change = jnp.concatenate(
        [jnp.ones((segments.shape[0], 1), dtype=bool), segments[:, 1:] != segments[:, :-1]], axis=1
    )
    starts = lax.cummax(jnp.where(change, position_index, jnp.zeros_like(position_index)), axis=1)
    return position_index - starts


def rotary_tables(segments):
    half_dim = HEAD_SIZE // 2
    frequency = jnp.power(ROPE_BASE, -(2.0 * jnp.arange(half_dim, dtype=jnp.float32)) / HEAD_SIZE)
    angles = doc_positions(segments).astype(jnp.float32)[..., None] * frequency
    cosine_table = jnp.concatenate([jnp.cos(angles), jnp.cos(angles)], axis=-1)
    sine_table = jnp.concatenate([jnp.sin(angles), jnp.sin(angles)], axis=-1)
    return (cosine_table, sine_table)


def rotate(vector, cosine_table, sine_table):
    half_dim = vector.shape[-1] // 2
    turned = jnp.concatenate([-vector[..., half_dim:], vector[..., :half_dim]], axis=-1)
    return vector * cosine_table + turned * sine_table


def unrotate(vector, cosine_table, sine_table):
    half_dim = vector.shape[-1] // 2
    shifted = vector * sine_table
    returned = jnp.concatenate([shifted[..., half_dim:], -shifted[..., :half_dim]], axis=-1)
    return vector * cosine_table + returned


def allowed_pairs(segments):
    length = segments.shape[1]
    offsets = jnp.arange(length)
    causal = offsets[None, :] <= offsets[:, None]
    same_doc = segments[:, :, None] == segments[:, None, :]
    return (causal[None] & same_doc)[:, None, None]


def score_block(queries, key_heads, segments):
    scores = jnp.einsum(
        "sqgrd,skgd->sgrqk", queries, key_heads, preferred_element_type=jnp.float32
    ) * HEAD_SIZE ** (-0.5)
    return jnp.where(allowed_pairs(segments), scores, NEG_FILL)


def rms_scale(features):
    return lax.rsqrt(jnp.mean(features * features, axis=-1, keepdims=True) + EPS)


def norm_back(features, inverse, gain_vector, upstream):
    scaled = gain_vector * upstream
    return inverse * scaled - features * (inverse * inverse * inverse) * jnp.mean(
        scaled * features, axis=-1, keepdims=True
    )


def widen(shard_rows):
    return lax.all_gather(shard_rows, "tensor", axis=0, tiled=True)


def narrow(partial_value):
    return lax.psum_scatter(
        partial_value.astype(jnp.bfloat16), "tensor", scatter_dimension=0, tiled=True
    ).astype(jnp.float32)


def local(
    block_in,
    cotangent,
    segment_ids,
    attn_gain,
    qkv_weight,
    out_weight,
    mlp_gain,
    gate_weight,
    up_weight,
    down_weight,
):
    qkv_full, gate_full, up_full, gain_attn_raw, gain_mlp_raw = (
        lax.all_gather(qkv_weight, "dp", axis=0, tiled=True),
        lax.all_gather(gate_weight, "dp", axis=0, tiled=True),
        lax.all_gather(up_weight, "dp", axis=0, tiled=True),
        lax.all_gather(attn_gain, "dp", axis=0, tiled=True),
        lax.all_gather(mlp_gain, "dp", axis=0, tiled=True),
    )
    out_cols, down_cols = (
        lax.all_gather(out_weight, "dp", axis=1, tiled=True),
        lax.all_gather(down_weight, "dp", axis=1, tiled=True),
    )
    seq_count, length = segment_ids.shape
    repeat_factor = QUERY_HEADS // KEY_VALUE_HEADS
    groups = qkv_full.shape[1] // ((repeat_factor + 2) * HEAD_SIZE)
    gain_attn = gain_attn_raw.astype(jnp.float32)
    gain_mlp = gain_mlp_raw.astype(jnp.float32)
    residual = block_in.astype(jnp.float32)
    scale_attn = rms_scale(residual)
    normed1 = widen((residual * scale_attn * gain_attn).astype(jnp.bfloat16))
    projected = jnp.dot(normed1, qkv_full, preferred_element_type=jnp.float32).reshape(
        seq_count, length, groups, repeat_factor + 2, HEAD_SIZE
    )
    cosine_table, sine_table = rotary_tables(segment_ids)
    cos_query = cosine_table[:, :, None, None, :]
    sin_query = sine_table[:, :, None, None, :]
    cos_key = cosine_table[:, :, None, :]
    sin_key = sine_table[:, :, None, :]
    queries = rotate(projected[:, :, :, :repeat_factor], cos_query, sin_query).astype(jnp.bfloat16)
    key_heads = rotate(projected[:, :, :, repeat_factor], cos_key, sin_key).astype(jnp.bfloat16)
    values = projected[:, :, :, repeat_factor + 1].astype(jnp.bfloat16)
    scores = score_block(queries, key_heads, segment_ids)
    highest = jnp.max(scores, axis=-1, keepdims=True)
    log_total = highest + jnp.log(jnp.sum(jnp.exp(scores - highest), axis=-1, keepdims=True))
    probability = jnp.exp(scores - log_total).astype(jnp.bfloat16)
    attended = jnp.einsum(
        "sgrqk,skgd->sqgrd", probability, values, preferred_element_type=jnp.float32
    ).astype(jnp.bfloat16)
    attn_flat = attended.reshape(seq_count * length, groups * repeat_factor * HEAD_SIZE)
    attn_delta = lax.psum_scatter(
        jnp.dot(attn_flat, out_cols, preferred_element_type=jnp.float32).astype(jnp.bfloat16),
        "tensor",
        scatter_dimension=0,
        tiled=True,
    ).astype(jnp.float32)
    hidden1 = residual + attn_delta
    scale_mlp = rms_scale(hidden1)
    normed2 = widen((hidden1 * scale_mlp * gain_mlp).astype(jnp.bfloat16))
    gate = jnp.dot(normed2, gate_full, preferred_element_type=jnp.float32)
    up_value = jnp.dot(normed2, up_full, preferred_element_type=jnp.float32)
    sigmoid_gate = jax.nn.sigmoid(gate)
    activated = (gate * sigmoid_gate * up_value).astype(jnp.bfloat16)
    mlp_delta = narrow(jnp.dot(activated, down_cols, preferred_element_type=jnp.float32))
    block_out = (hidden1 + mlp_delta).astype(jnp.bfloat16)
    grad_rows = widen(cotangent)
    down_part = jnp.einsum("tf,td->fd", activated, grad_rows, preferred_element_type=jnp.float32)
    act_grad = jnp.einsum("td,fd->tf", grad_rows, down_cols, preferred_element_type=jnp.float32)
    gate_delta = (act_grad * up_value * sigmoid_gate * (1.0 + gate * (1.0 - sigmoid_gate))).astype(
        jnp.bfloat16
    )
    up_delta = (act_grad * gate * sigmoid_gate).astype(jnp.bfloat16)
    gate_part = jnp.einsum("td,tf->df", normed2, gate_delta, preferred_element_type=jnp.float32)
    up_part = jnp.einsum("td,tf->df", normed2, up_delta, preferred_element_type=jnp.float32)
    normed2_term = jnp.einsum(
        "tf,df->td", gate_delta, gate_full, preferred_element_type=jnp.float32
    ) + jnp.einsum("tf,df->td", up_delta, up_full, preferred_element_type=jnp.float32)
    normed2_grad = narrow(normed2_term)
    mlp_gain_part = jnp.sum(normed2_grad * hidden1 * scale_mlp, axis=0)
    hidden1_grad = cotangent.astype(jnp.float32) + norm_back(
        hidden1, scale_mlp, gain_mlp, normed2_grad
    )
    hidden1_rounded = hidden1_grad.astype(jnp.bfloat16)
    grad_full = lax.all_gather(hidden1_rounded, "tensor", axis=0, tiled=True)
    attended_grad = jnp.einsum(
        "td,hd->th", grad_full, out_cols, preferred_element_type=jnp.float32
    ).astype(jnp.bfloat16)
    out_part = jnp.einsum("th,td->hd", attn_flat, grad_full, preferred_element_type=jnp.float32)
    attended_grad = attended_grad.reshape(seq_count, length, groups, repeat_factor, HEAD_SIZE)
    prob_full = jnp.exp(score_block(queries, key_heads, segment_ids) - log_total)
    prob_grad = jnp.einsum(
        "sqgrd,skgd->sgrqk", attended_grad, values, preferred_element_type=jnp.float32
    )
    inner_sum = jnp.sum(prob_full * prob_grad, axis=-1, keepdims=True)
    score_grad = (prob_full * (prob_grad - inner_sum) * HEAD_SIZE ** (-0.5)).astype(jnp.bfloat16)
    query_grad = jnp.einsum(
        "sgrqk,skgd->sqgrd", score_grad, key_heads, preferred_element_type=jnp.float32
    )
    key_grad = jnp.einsum(
        "sgrqk,sqgrd->skgd", score_grad, queries, preferred_element_type=jnp.float32
    )
    value_grad = jnp.einsum(
        "sgrqk,sqgrd->skgd",
        prob_full.astype(jnp.bfloat16),
        attended_grad,
        preferred_element_type=jnp.float32,
    )
    projected_grad = jnp.concatenate(
        [
            unrotate(query_grad, cos_query, sin_query),
            unrotate(key_grad, cos_key, sin_key)[:, :, :, None],
            value_grad[:, :, :, None],
        ],
        axis=3,
    )
    projected_grad = projected_grad.astype(jnp.bfloat16).reshape(
        seq_count * length, groups * (repeat_factor + 2) * HEAD_SIZE
    )
    qkv_part = jnp.einsum("td,tc->dc", normed1, projected_grad, preferred_element_type=jnp.float32)
    normed1_grad = narrow(
        jnp.einsum("tc,dc->td", projected_grad, qkv_full, preferred_element_type=jnp.float32)
    )
    attn_gain_part = jnp.sum(normed1_grad * residual * scale_attn, axis=0)
    input_grad = (hidden1_grad + norm_back(residual, scale_attn, gain_attn, normed1_grad)).astype(
        jnp.bfloat16
    )
    attn_gain_total, mlp_gain_total = lax.psum((attn_gain_part, mlp_gain_part), "tensor")
    attn_gain_grad, qkv_grad, gate_grad, up_grad, mlp_gain_grad = (
        lax.psum_scatter(
            attn_gain_total.astype(jnp.bfloat16), "dp", scatter_dimension=0, tiled=True
        ).astype(jnp.float32),
        lax.psum_scatter(
            qkv_part.astype(jnp.bfloat16), "dp", scatter_dimension=0, tiled=True
        ).astype(jnp.float32),
        lax.psum_scatter(
            gate_part.astype(jnp.bfloat16), "dp", scatter_dimension=0, tiled=True
        ).astype(jnp.float32),
        lax.psum_scatter(
            up_part.astype(jnp.bfloat16), "dp", scatter_dimension=0, tiled=True
        ).astype(jnp.float32),
        lax.psum_scatter(
            mlp_gain_total.astype(jnp.bfloat16), "dp", scatter_dimension=0, tiled=True
        ).astype(jnp.float32),
    )
    out_grad, down_grad = (
        lax.psum_scatter(
            out_part.astype(jnp.bfloat16), "dp", scatter_dimension=1, tiled=True
        ).astype(jnp.float32),
        lax.psum_scatter(
            down_part.astype(jnp.bfloat16), "dp", scatter_dimension=1, tiled=True
        ).astype(jnp.float32),
    )
    return (
        block_out,
        input_grad,
        attn_gain_grad,
        qkv_grad,
        out_grad,
        mlp_gain_grad,
        gate_grad,
        up_grad,
        down_grad,
    )


GROUP = 4
WINDOW = 256
LANES = 384
TILE = 128


def kernel_qkv(tokens, weight, cos, sin_up, sin_down, out):
    product = lax.dot_general(
        tokens[0], weight[...], (((1,), (1,)), ((), ())), preferred_element_type=jnp.float32
    )
    repeat = product.shape[1] // LANES
    half = HEAD_SIZE // 2
    c = jnp.concatenate([cos[0]] * repeat, axis=1)
    u = jnp.concatenate([sin_up[0]] * repeat, axis=1)
    d = jnp.concatenate([sin_down[0]] * repeat, axis=1)
    width = product.shape[1]
    turned = pltpu.roll(product, half, 1) * u + pltpu.roll(product, width - half, 1) * d
    out[0] = (product * c + turned).astype(out.dtype)


def project(tokens, weight, tables):
    blocks, rows, width = tokens.shape
    units = weight.shape[0]
    table_spec = pl.BlockSpec((1, rows, LANES), lambda i: (i, 0, 0))
    return pl.pallas_call(
        kernel_qkv,
        grid=(blocks,),
        in_specs=[
            pl.BlockSpec((1, rows, width), lambda i: (i, 0, 0)),
            pl.BlockSpec((units, width), lambda i: (0, 0)),
            table_spec,
            table_spec,
            table_spec,
        ],
        out_specs=pl.BlockSpec((1, rows, units), lambda i: (i, 0, 0)),
        out_shape=jax.ShapeDtypeStruct((blocks, rows, units), jnp.bfloat16),
        name="project",
    )(tokens, weight, *tables)


def load_group(core, keep, recv, halo, queries, keyvals):
    mine, other = keep[0], recv[0]
    first = core == 0
    queries[...] = jnp.where(first, mine, other)
    keyvals[:WINDOW] = halo[0]
    keyvals[WINDOW:] = jnp.where(first, other, mine)


def allowed_tile(lowest, start):
    low = lowest[0, pl.ds(start, TILE), :]
    key = lax.broadcasted_iota(jnp.int32, (TILE, TILE + WINDOW), 1)
    query = lax.broadcasted_iota(jnp.int32, (TILE, TILE + WINDOW), 0)
    return (key >= low) & (key <= query + WINDOW)


def kernel_attend(core_ref, keep, recv, halo, lowest, out, log_out, queries, keyvals):
    core = core_ref[0]
    load_group(core, keep, recv, halo, queries, keyvals)
    heads = queries.shape[1] // HEAD_SIZE
    repeat = QUERY_HEADS // KEY_VALUE_HEADS

    def body(tile, carry):
        start = pl.multiple_of(tile * TILE, TILE)
        allowed = allowed_tile(lowest, start)
        for head in range(heads):
            group, r = head // repeat, head % repeat
            base = group * 2 * HEAD_SIZE
            q = queries[pl.ds(start, TILE), head * HEAD_SIZE : (head + 1) * HEAD_SIZE]
            k = keyvals[pl.ds(start, TILE + WINDOW), base : base + HEAD_SIZE]
            v = keyvals[pl.ds(start, TILE + WINDOW), base + HEAD_SIZE : base + 2 * HEAD_SIZE]
            s = lax.dot_general(
                q, k, (((1,), (1,)), ((), ())), preferred_element_type=jnp.float32
            ) * HEAD_SIZE ** (-0.5)
            s = jnp.where(allowed, s, NEG_FILL)
            highest = jnp.max(s, axis=1, keepdims=True)
            total = highest + jnp.log(jnp.sum(jnp.exp(s - highest), axis=1, keepdims=True))
            p = jnp.exp(s - total).astype(jnp.bfloat16)
            o = jnp.dot(p, v, preferred_element_type=jnp.float32).astype(jnp.bfloat16)
            slot = jnp.where(core == r, 0, 1)
            out[slot, 0, pl.ds(start, TILE), group * HEAD_SIZE : (group + 1) * HEAD_SIZE] = o
            log_out[0, pl.ds(start, TILE), head : head + 1] = total
        return carry

    lax.fori_loop(0, queries.shape[0] // TILE, body, 0)


def attend(core, keep, recv, halo, lowest):
    pairs, rows, units = keep.shape
    heads = units // HEAD_SIZE
    spec = pl.BlockSpec((1, rows, units), lambda i: (i, 0, 0))
    return pl.pallas_call(
        kernel_attend,
        grid=(pairs,),
        in_specs=[
            pl.BlockSpec(memory_space=pltpu.SMEM),
            spec,
            spec,
            pl.BlockSpec((1, WINDOW, units), lambda i: (i, 0, 0)),
            pl.BlockSpec((1, rows, 1), lambda i: (i, 0, 0)),
        ],
        out_specs=[
            pl.BlockSpec((2, 1, rows, units // 2), lambda i: (0, i, 0, 0)),
            pl.BlockSpec((1, rows, heads), lambda i: (i, 0, 0)),
        ],
        out_shape=[
            jax.ShapeDtypeStruct((2, pairs, rows, units // 2), jnp.bfloat16),
            jax.ShapeDtypeStruct((pairs, rows, heads), jnp.float32),
        ],
        scratch_shapes=[
            pltpu.VMEM((rows, units), jnp.bfloat16),
            pltpu.VMEM((rows + WINDOW, units), jnp.bfloat16),
        ],
        name="attend",
    )(core, keep, recv, halo, lowest)


def turn_back(gradient, cos, sin_up, sin_down):
    repeat = gradient.shape[1] // LANES
    half = HEAD_SIZE // 2
    c = jnp.concatenate([cos] * repeat, axis=1)
    u = jnp.concatenate([sin_up] * repeat, axis=1)
    d = jnp.concatenate([sin_down] * repeat, axis=1)
    width = gradient.shape[1]
    turned = pltpu.roll(gradient, half, 1) * u + pltpu.roll(gradient, width - half, 1) * d
    return gradient * c - turned


def kernel_attend_back(
    core_ref, keep, recv, halo, lowest, log_total, grads, grads_other, cos, sin_up, sin_down,
    query_out, key_out, halo_out, queries, keyvals, totals, query_total,
):
    core = core_ref[0]
    load_group(core, keep, recv, halo, queries, keyvals)
    totals[...] = jnp.zeros_like(totals)
    heads = queries.shape[1] // HEAD_SIZE
    repeat = QUERY_HEADS // KEY_VALUE_HEADS
    scale = HEAD_SIZE ** (-0.5)

    def body(tile, carry):
        start = pl.multiple_of(tile * TILE, TILE)
        allowed = allowed_tile(lowest, start)
        mine = grads[0, pl.ds(start, TILE), :]
        other = grads_other[0, pl.ds(start, TILE), :]
        first = core == 0
        by_repeat = (jnp.where(first, mine, other), jnp.where(first, other, mine))
        for group in range(heads // repeat):
            base = group * 2 * HEAD_SIZE
            k = keyvals[pl.ds(start, TILE + WINDOW), base : base + HEAD_SIZE]
            v = keyvals[pl.ds(start, TILE + WINDOW), base + HEAD_SIZE : base + 2 * HEAD_SIZE]
            key_sum = None
            for r in range(repeat):
                head = group * repeat + r
                q = queries[pl.ds(start, TILE), head * HEAD_SIZE : (head + 1) * HEAD_SIZE]
                g = by_repeat[r][:, group * HEAD_SIZE : (group + 1) * HEAD_SIZE]
                s = lax.dot_general(
                    q, k, (((1,), (1,)), ((), ())), preferred_element_type=jnp.float32
                ) * scale
                total = log_total[0, pl.ds(start, TILE), head : head + 1]
                p = jnp.exp(jnp.where(allowed, s, NEG_FILL) - total)
                pg = lax.dot_general(
                    g, v, (((1,), (1,)), ((), ())), preferred_element_type=jnp.float32
                )
                inner = jnp.sum(p * pg, axis=1, keepdims=True)
                sg = (p * (pg - inner) * scale).astype(jnp.bfloat16)
                query_total[:, head * HEAD_SIZE : (head + 1) * HEAD_SIZE] = jnp.dot(
                    sg, k, preferred_element_type=jnp.float32
                )
                dk = lax.dot_general(
                    sg, q, (((0,), (0,)), ((), ())), preferred_element_type=jnp.float32
                )
                dv = lax.dot_general(
                    p.astype(jnp.bfloat16), g, (((0,), (0,)), ((), ())),
                    preferred_element_type=jnp.float32,
                )
                both = jnp.concatenate([dk, dv], axis=1)
                key_sum = both if key_sum is None else key_sum + both
            totals[pl.ds(start, TILE + WINDOW), base : base + 2 * HEAD_SIZE] += key_sum
        rows = pl.ds(start, TILE)
        query_out[0, rows, :] = turn_back(
            query_total[...], cos[0, rows, :], sin_up[0, rows, :], sin_down[0, rows, :]
        ).astype(jnp.bfloat16)
        return carry

    lax.fori_loop(0, queries.shape[0] // TILE, body, 0)
    key_out[0] = totals[WINDOW:]
    halo_out[0] = totals[:WINDOW].astype(jnp.bfloat16)


def attend_back(core, keep, recv, halo, lowest, log_total, grads, grads_other, tables):
    pairs, rows, units = keep.shape
    heads = units // HEAD_SIZE
    spec = pl.BlockSpec((1, rows, units), lambda i: (i, 0, 0))
    half_spec = pl.BlockSpec((1, rows, units // 2), lambda i: (i, 0, 0))
    halo_spec = pl.BlockSpec((1, WINDOW, units), lambda i: (i, 0, 0))
    table_spec = pl.BlockSpec((1, rows, LANES), lambda i: (i, 0, 0))
    return pl.pallas_call(
        kernel_attend_back,
        grid=(pairs,),
        in_specs=[
            pl.BlockSpec(memory_space=pltpu.SMEM),
            spec,
            spec,
            halo_spec,
            pl.BlockSpec((1, rows, 1), lambda i: (i, 0, 0)),
            pl.BlockSpec((1, rows, heads), lambda i: (i, 0, 0)),
            half_spec,
            half_spec,
            table_spec,
            table_spec,
            table_spec,
        ],
        out_specs=[spec, spec, halo_spec],
        out_shape=[
            jax.ShapeDtypeStruct((pairs, rows, units), jnp.bfloat16),
            jax.ShapeDtypeStruct((pairs, rows, units), jnp.float32),
            jax.ShapeDtypeStruct((pairs, WINDOW, units), jnp.bfloat16),
        ],
        scratch_shapes=[
            pltpu.VMEM((rows, units), jnp.bfloat16),
            pltpu.VMEM((rows + WINDOW, units), jnp.bfloat16),
            pltpu.VMEM((rows + WINDOW, units), jnp.float32),
            pltpu.VMEM((TILE, units), jnp.float32),
        ],
        name="attend_back",
    )(core, keep, recv, halo, lowest, log_total, grads, grads_other, *tables)


def kernel_finish_keys(key_sum, halo, cos, sin_up, sin_down, out):
    rows = key_sum.shape[1]
    full = key_sum[0]
    tail = full[rows - WINDOW :] + halo[0].astype(jnp.float32)
    full = jnp.concatenate([full[: rows - WINDOW], tail], axis=0)
    out[0] = turn_back(full, cos[0], sin_up[0], sin_down[0]).astype(jnp.bfloat16)


def finish_keys(key_sum, halo, tables):
    pairs, rows, units = key_sum.shape
    spec = pl.BlockSpec((1, rows, units), lambda i: (i, 0, 0))
    table_spec = pl.BlockSpec((1, rows, LANES), lambda i: (i, 0, 0))
    return pl.pallas_call(
        kernel_finish_keys,
        grid=(pairs,),
        in_specs=[
            spec,
            pl.BlockSpec((1, WINDOW, units), lambda i: (i, 0, 0)),
            table_spec,
            table_spec,
            table_spec,
        ],
        out_specs=spec,
        out_shape=jax.ShapeDtypeStruct((pairs, rows, units), jnp.bfloat16),
        name="finish_keys",
    )(key_sum, halo, *tables)


def fast_local(
    n_dp,
    n_tensor,
    block_in,
    cotangent,
    segment_ids,
    attn_gain,
    qkv_weight,
    out_weight,
    mlp_gain,
    gate_weight,
    up_weight,
    down_weight,
):
    bf16, f32 = jnp.bfloat16, jnp.float32
    d_at = lax.axis_index("dp")
    z_at = lax.axis_index("tensor")
    core = d_at % 2
    member = d_at % GROUP
    upper = d_at // GROUP
    rows, width = block_in.shape
    seqs, length = segment_ids.shape
    half = width // 2

    def swap(value, bit):
        return lax.ppermute(value, "dp", [(i, i ^ bit) for i in range(n_dp)])

    def own_order(value):
        turned = jnp.concatenate([value[..., half:], value[..., :half]], axis=-1)
        return jnp.where(upper == 0, value, turned)

    shards = [qkv_weight.T, out_weight, gate_weight.T, up_weight.T, down_weight]
    quarters = [s.reshape(GROUP, s.shape[0] // GROUP, s.shape[1]) for s in shards]
    sizes = [q.shape[1] for q in quarters]

    def deal(parcel):
        pieces = [lax.dynamic_index_in_dim(parcel, member, 0, keepdims=False)]
        for k in range(1, GROUP):
            sent = lax.dynamic_index_in_dim(parcel, member ^ k, 0, keepdims=False)
            pieces.append(swap(sent, k))
        stacked = jnp.stack(pieces)
        ordered = [
            lax.dynamic_index_in_dim(stacked, member ^ i, 0, keepdims=False) for i in range(GROUP)
        ]
        return jnp.concatenate(ordered, axis=-1)

    def spread(piece):
        mine = lax.all_gather(piece, "tensor", axis=0, tiled=True)
        return jnp.concatenate([mine, swap(mine, GROUP)], axis=1)

    first_deal = deal(quarters[0])
    rest_deal = deal(jnp.concatenate(quarters[1:], axis=1))
    offsets = [0]
    for size in sizes[1:]:
        offsets.append(offsets[-1] + size)
    dealt = [first_deal] + [
        rest_deal[offsets[i] : offsets[i + 1]] for i in range(len(sizes) - 1)
    ]
    qkv_full, out_full, gate_full, up_full, down_full = [spread(piece) for piece in dealt]

    def gather_pair(value):
        return jnp.stack([value, swap(value, 2)])

    def gather(value):
        pair = gather_pair(value)
        return jnp.concatenate([pair, swap(pair, 1)], axis=0)

    def scatter(partial_value):
        blocks = partial_value.reshape(GROUP, rows, partial_value.shape[-1])
        got = swap(blocks[2:].astype(bf16), 1)
        pair = blocks[:2].astype(f32) + got.astype(f32)
        return pair[0] + swap(pair[1].astype(bf16), 2).astype(f32)

    starts_row = jnp.arange(length, dtype=jnp.int32)[None, :] - doc_positions(segment_ids)
    stream = starts_row + jnp.arange(seqs, dtype=jnp.int32)[:, None] * length
    stream = stream.reshape(n_tensor, rows)
    first_key = lax.dynamic_index_in_dim(stream, z_at, 0, keepdims=False)
    own_position = z_at * rows + jnp.arange(rows, dtype=jnp.int32) - first_key
    small = jnp.concatenate(
        [attn_gain.astype(f32), mlp_gain.astype(f32), own_position.astype(f32), first_key.astype(f32)]
    )
    smalls = lax.all_gather(small, "dp", axis=0)
    part = attn_gain.shape[0]
    gain_attn = own_order(smalls[:, :part].reshape(width))
    gain_mlp = own_order(smalls[:, part : 2 * part].reshape(width))
    block_order = jnp.stack([d_at, d_at ^ 2, d_at ^ 1, d_at ^ 3])
    token_info = smalls[:, 2 * part :][block_order]
    positions = token_info[:, :rows]
    lowest = token_info[:2, rows:].astype(jnp.int32) - z_at * rows + WINDOW
    tile_at = jnp.arange(rows, dtype=jnp.int32) // TILE * TILE
    lowest = (lowest - tile_at[None, :])[:, :, None]

    lane = jnp.arange(LANES, dtype=jnp.int32)
    within = lane % HEAD_SIZE
    frequency = jnp.power(
        ROPE_BASE, -(2.0 * (within % (HEAD_SIZE // 2)).astype(f32)) / HEAD_SIZE
    )
    angles = positions[:, :, None] * frequency
    cosine, sine = jnp.cos(angles), jnp.sin(angles)
    is_key = (lane % (2 * HEAD_SIZE)) < HEAD_SIZE
    is_second = within >= HEAD_SIZE // 2

    def tables_for(turns, count):
        return (
            jnp.where(turns, cosine[:count], 1.0),
            jnp.where(turns & is_second, sine[:count], 0.0),
            jnp.where(turns & ~is_second, -sine[:count], 0.0),
        )

    whole_lane = jnp.full((LANES,), True)
    query_tables = tables_for(whole_lane, 2)
    key_tables = tables_for(is_key, 2)
    own_tables = tables_for(is_key | (core == 0), GROUP)

    residual = own_order(block_in).astype(f32)
    cot_own = own_order(cotangent)
    scale_attn = rms_scale(residual)
    normed1 = gather((residual * scale_attn * gain_attn).astype(bf16))
    grad_rows = gather(cot_own)

    projected = project(normed1, qkv_full, own_tables)
    keep, send = projected[:2], projected[2:]
    recv = swap(send, 1)
    tail = jnp.where(core == 0, recv[:, rows - WINDOW :], keep[:, rows - WINDOW :])
    halo = lax.ppermute(tail, "tensor", [(i, i + 1) for i in range(n_tensor - 1)])
    core_arg = core.astype(jnp.int32).reshape(1)
    outs, log_total = attend(core_arg, keep, recv, halo, lowest)
    attended = jnp.concatenate([outs[0], swap(outs[1], 1)], axis=0)
    attn_flat = attended.reshape(GROUP * rows, attended.shape[-1])
    hidden1 = residual + scatter(
        jnp.dot(attn_flat, out_full, preferred_element_type=f32).astype(bf16)
    )
    scale_mlp = rms_scale(hidden1)
    normed2 = gather((hidden1 * scale_mlp * gain_mlp).astype(bf16)).reshape(GROUP * rows, width)
    grad_rows = grad_rows.reshape(GROUP * rows, width)

    def to_units(tokens, weight):
        return jnp.einsum("td,ud->tu", tokens, weight, preferred_element_type=f32)

    def grad_of(left, right):
        return jnp.einsum("tu,td->ud", left, right, preferred_element_type=f32).astype(bf16)

    gate = to_units(normed2, gate_full)
    up_value = to_units(normed2, up_full)
    sigmoid_gate = jax.nn.sigmoid(gate)
    activated = (gate * sigmoid_gate * up_value).astype(bf16)
    act_grad = to_units(grad_rows, down_full)
    gate_delta = (act_grad * up_value * sigmoid_gate * (1.0 + gate * (1.0 - sigmoid_gate))).astype(
        bf16
    )
    up_delta = (act_grad * gate * sigmoid_gate).astype(bf16)
    normed2_term = jnp.dot(gate_delta, gate_full, preferred_element_type=f32) + jnp.dot(
        up_delta, up_full, preferred_element_type=f32
    )
    normed2_grad = scatter(normed2_term.astype(bf16))
    mlp_delta = scatter(jnp.dot(activated, down_full, preferred_element_type=f32).astype(bf16))
    block_out = own_order((hidden1 + mlp_delta).astype(bf16))
    down_part = grad_of(activated, grad_rows)
    gate_part = grad_of(gate_delta, normed2)
    up_part = grad_of(up_delta, normed2)
    mlp_gain_part = jnp.sum(normed2_grad * hidden1 * scale_mlp, axis=0)
    hidden1_grad = cot_own.astype(f32) + norm_back(hidden1, scale_mlp, gain_mlp, normed2_grad)
    grad_full = gather(hidden1_grad.astype(bf16)).reshape(GROUP * rows, width)
    attended_grad = to_units(grad_full, out_full).astype(bf16)
    out_part = grad_of(attn_flat, grad_full)
    attended_grad = attended_grad.reshape(GROUP, rows, attended_grad.shape[-1])
    grads_other = swap(attended_grad[2:], 1)
    query_grad, key_sum, halo_grad = attend_back(
        core_arg, keep, recv, halo, lowest, log_total, attended_grad[:2], grads_other, query_tables
    )
    halo_back = lax.ppermute(halo_grad, "tensor", [(i + 1, i) for i in range(n_tensor - 1)])
    key_grad = finish_keys(key_sum, halo_back, key_tables)
    kept = jnp.where(core == 0, query_grad, key_grad)
    passed = jnp.where(core == 0, key_grad, query_grad)
    projected_grad = jnp.concatenate([kept, swap(passed, 1)], axis=0)
    projected_grad = projected_grad.reshape(GROUP * rows, projected_grad.shape[-1])
    normed1_flat = normed1.reshape(GROUP * rows, width)
    normed1_grad = scatter(
        jnp.dot(projected_grad, qkv_full, preferred_element_type=f32).astype(bf16)
    )
    qkv_part = grad_of(projected_grad, normed1_flat)
    attn_gain_part = jnp.sum(normed1_grad * residual * scale_attn, axis=0)
    input_grad = own_order(
        (hidden1_grad + norm_back(residual, scale_attn, gain_attn, normed1_grad)).astype(bf16)
    )

    def collect(part_grad):
        summed = part_grad[:, :half].astype(f32) + swap(part_grad[:, half:], GROUP).astype(f32)
        piece = lax.psum_scatter(
            summed.astype(bf16), "tensor", scatter_dimension=0, tiled=True
        )
        units = piece.shape[0]
        columns = piece.reshape(units, GROUP, half // GROUP).transpose(1, 0, 2)
        pieces = [lax.dynamic_index_in_dim(columns, member, 0, keepdims=False)]
        for k in range(1, GROUP):
            sent = lax.dynamic_index_in_dim(columns, member ^ k, 0, keepdims=False)
            pieces.append(swap(sent, k))
        stacked = jnp.stack(pieces)
        ordered = [
            lax.dynamic_index_in_dim(stacked, member ^ i, 0, keepdims=False) for i in range(GROUP)
        ]
        return jnp.concatenate(ordered, axis=0)

    down_grad = collect(down_part).astype(f32)
    gate_grad = collect(gate_part).T.astype(f32)
    up_grad = collect(up_part).T.astype(f32)
    out_grad = collect(out_part).astype(f32)
    qkv_grad = collect(qkv_part).T.astype(f32)
    gains = own_order(jnp.stack([attn_gain_part, mlp_gain_part]))
    gains = lax.psum(gains, ("dp", "tensor"))
    gains = lax.dynamic_slice_in_dim(gains, d_at * part, part, axis=1)
    return (
        block_out,
        input_grad,
        gains[0],
        qkv_grad,
        out_grad,
        gains[1],
        gate_grad,
        up_grad,
        down_grad,
    )


def solution(mesh):
    in_specs = (
        P(("dp", "tensor"), None),
        P(("dp", "tensor"), None),
        P("dp", None),
        P("dp"),
        P("dp", "tensor"),
        P("tensor", "dp"),
        P("dp"),
        P("dp", "tensor"),
        P("dp", "tensor"),
        P("tensor", "dp"),
    )
    out_specs = (
        P(("dp", "tensor"), None),
        P(("dp", "tensor"), None),
        P("dp"),
        P("dp", "tensor"),
        P("tensor", "dp"),
        P("dp"),
        P("dp", "tensor"),
        P("dp", "tensor"),
        P("tensor", "dp"),
    )
    n_dp, n_tensor = mesh.shape["dp"], mesh.shape["tensor"]

    def body(*arrays):
        rows = arrays[0].shape[0]
        groups = arrays[4].shape[1] // (4 * HEAD_SIZE)
        if n_dp == 2 * GROUP and groups == 2 and rows >= WINDOW and rows % TILE == 0:
            return fast_local(n_dp, n_tensor, *arrays)
        return local(*arrays)

    return jax.shard_map(body, mesh=mesh, in_specs=in_specs, out_specs=out_specs, check_vma=False)
```

```python
import functools

import jax
import jax.numpy as jnp
from jax import lax
from jax.experimental import pallas as pl
from jax.experimental.pallas import tpu as pltpu
from jax.sharding import PartitionSpec as P

QUERY_HEADS = 16
KEY_VALUE_HEADS = 8
HEAD_SIZE = 96


EPS = 1e-05
ROPE_BASE = 100000.0
NEG_FILL = -1e30


def doc_positions(segments):
    length = segments.shape[1]
    position_index = jnp.broadcast_to(jnp.arange(length, dtype=jnp.int32)[None, :], segments.shape)
    change = jnp.concatenate(
        [jnp.ones((segments.shape[0], 1), dtype=bool), segments[:, 1:] != segments[:, :-1]], axis=1
    )
    starts = lax.cummax(jnp.where(change, position_index, jnp.zeros_like(position_index)), axis=1)
    return position_index - starts


def rotary_tables(segments):
    half_dim = HEAD_SIZE // 2
    frequency = jnp.power(ROPE_BASE, -(2.0 * jnp.arange(half_dim, dtype=jnp.float32)) / HEAD_SIZE)
    angles = doc_positions(segments).astype(jnp.float32)[..., None] * frequency
    cosine_table = jnp.concatenate([jnp.cos(angles), jnp.cos(angles)], axis=-1)
    sine_table = jnp.concatenate([jnp.sin(angles), jnp.sin(angles)], axis=-1)
    return (cosine_table, sine_table)


def rotate(vector, cosine_table, sine_table):
    half_dim = vector.shape[-1] // 2
    turned = jnp.concatenate([-vector[..., half_dim:], vector[..., :half_dim]], axis=-1)
    return vector * cosine_table + turned * sine_table


def unrotate(vector, cosine_table, sine_table):
    half_dim = vector.shape[-1] // 2
    shifted = vector * sine_table
    returned = jnp.concatenate([shifted[..., half_dim:], -shifted[..., :half_dim]], axis=-1)
    return vector * cosine_table + returned


def allowed_pairs(segments):
    length = segments.shape[1]
    offsets = jnp.arange(length)
    causal = offsets[None, :] <= offsets[:, None]
    same_doc = segments[:, :, None] == segments[:, None, :]
    return (causal[None] & same_doc)[:, None, None]


def score_block(queries, key_heads, segments):
    scores = jnp.einsum(
        "sqgrd,skgd->sgrqk", queries, key_heads, preferred_element_type=jnp.float32
    ) * HEAD_SIZE ** (-0.5)
    return jnp.where(allowed_pairs(segments), scores, NEG_FILL)


def rms_scale(features):
    return lax.rsqrt(jnp.mean(features * features, axis=-1, keepdims=True) + EPS)


def norm_back(features, inverse, gain_vector, upstream):
    scaled = gain_vector * upstream
    return inverse * scaled - features * (inverse * inverse * inverse) * jnp.mean(
        scaled * features, axis=-1, keepdims=True
    )


def widen(shard_rows):
    return lax.all_gather(shard_rows, "tensor", axis=0, tiled=True)


def narrow(partial_value):
    return lax.psum_scatter(
        partial_value.astype(jnp.bfloat16), "tensor", scatter_dimension=0, tiled=True
    ).astype(jnp.float32)


def local(
    block_in,
    cotangent,
    segment_ids,
    attn_gain,
    qkv_weight,
    out_weight,
    mlp_gain,
    gate_weight,
    up_weight,
    down_weight,
):
    qkv_full, gate_full, up_full, gain_attn_raw, gain_mlp_raw = (
        lax.all_gather(qkv_weight, "dp", axis=0, tiled=True),
        lax.all_gather(gate_weight, "dp", axis=0, tiled=True),
        lax.all_gather(up_weight, "dp", axis=0, tiled=True),
        lax.all_gather(attn_gain, "dp", axis=0, tiled=True),
        lax.all_gather(mlp_gain, "dp", axis=0, tiled=True),
    )
    out_cols, down_cols = (
        lax.all_gather(out_weight, "dp", axis=1, tiled=True),
        lax.all_gather(down_weight, "dp", axis=1, tiled=True),
    )
    seq_count, length = segment_ids.shape
    repeat_factor = QUERY_HEADS // KEY_VALUE_HEADS
    groups = qkv_full.shape[1] // ((repeat_factor + 2) * HEAD_SIZE)
    gain_attn = gain_attn_raw.astype(jnp.float32)
    gain_mlp = gain_mlp_raw.astype(jnp.float32)
    residual = block_in.astype(jnp.float32)
    scale_attn = rms_scale(residual)
    normed1 = widen((residual * scale_attn * gain_attn).astype(jnp.bfloat16))
    projected = jnp.dot(normed1, qkv_full, preferred_element_type=jnp.float32).reshape(
        seq_count, length, groups, repeat_factor + 2, HEAD_SIZE
    )
    cosine_table, sine_table = rotary_tables(segment_ids)
    cos_query = cosine_table[:, :, None, None, :]
    sin_query = sine_table[:, :, None, None, :]
    cos_key = cosine_table[:, :, None, :]
    sin_key = sine_table[:, :, None, :]
    queries = rotate(projected[:, :, :, :repeat_factor], cos_query, sin_query).astype(jnp.bfloat16)
    key_heads = rotate(projected[:, :, :, repeat_factor], cos_key, sin_key).astype(jnp.bfloat16)
    values = projected[:, :, :, repeat_factor + 1].astype(jnp.bfloat16)
    scores = score_block(queries, key_heads, segment_ids)
    highest = jnp.max(scores, axis=-1, keepdims=True)
    log_total = highest + jnp.log(jnp.sum(jnp.exp(scores - highest), axis=-1, keepdims=True))
    probability = jnp.exp(scores - log_total).astype(jnp.bfloat16)
    attended = jnp.einsum(
        "sgrqk,skgd->sqgrd", probability, values, preferred_element_type=jnp.float32
    ).astype(jnp.bfloat16)
    attn_flat = attended.reshape(seq_count * length, groups * repeat_factor * HEAD_SIZE)
    attn_delta = lax.psum_scatter(
        jnp.dot(attn_flat, out_cols, preferred_element_type=jnp.float32).astype(jnp.bfloat16),
        "tensor",
        scatter_dimension=0,
        tiled=True,
    ).astype(jnp.float32)
    hidden1 = residual + attn_delta
    scale_mlp = rms_scale(hidden1)
    normed2 = widen((hidden1 * scale_mlp * gain_mlp).astype(jnp.bfloat16))
    gate = jnp.dot(normed2, gate_full, preferred_element_type=jnp.float32)
    up_value = jnp.dot(normed2, up_full, preferred_element_type=jnp.float32)
    sigmoid_gate = jax.nn.sigmoid(gate)
    activated = (gate * sigmoid_gate * up_value).astype(jnp.bfloat16)
    mlp_delta = narrow(jnp.dot(activated, down_cols, preferred_element_type=jnp.float32))
    block_out = (hidden1 + mlp_delta).astype(jnp.bfloat16)
    grad_rows = widen(cotangent)
    down_part = jnp.einsum("tf,td->fd", activated, grad_rows, preferred_element_type=jnp.float32)
    act_grad = jnp.einsum("td,fd->tf", grad_rows, down_cols, preferred_element_type=jnp.float32)
    gate_delta = (act_grad * up_value * sigmoid_gate * (1.0 + gate * (1.0 - sigmoid_gate))).astype(
        jnp.bfloat16
    )
    up_delta = (act_grad * gate * sigmoid_gate).astype(jnp.bfloat16)
    gate_part = jnp.einsum("td,tf->df", normed2, gate_delta, preferred_element_type=jnp.float32)
    up_part = jnp.einsum("td,tf->df", normed2, up_delta, preferred_element_type=jnp.float32)
    normed2_term = jnp.einsum(
        "tf,df->td", gate_delta, gate_full, preferred_element_type=jnp.float32
    ) + jnp.einsum("tf,df->td", up_delta, up_full, preferred_element_type=jnp.float32)
    normed2_grad = narrow(normed2_term)
    mlp_gain_part = jnp.sum(normed2_grad * hidden1 * scale_mlp, axis=0)
    hidden1_grad = cotangent.astype(jnp.float32) + norm_back(
        hidden1, scale_mlp, gain_mlp, normed2_grad
    )
    hidden1_rounded = hidden1_grad.astype(jnp.bfloat16)
    grad_full = lax.all_gather(hidden1_rounded, "tensor", axis=0, tiled=True)
    attended_grad = jnp.einsum(
        "td,hd->th", grad_full, out_cols, preferred_element_type=jnp.float32
    ).astype(jnp.bfloat16)
    out_part = jnp.einsum("th,td->hd", attn_flat, grad_full, preferred_element_type=jnp.float32)
    attended_grad = attended_grad.reshape(seq_count, length, groups, repeat_factor, HEAD_SIZE)
    prob_full = jnp.exp(score_block(queries, key_heads, segment_ids) - log_total)
    prob_grad = jnp.einsum(
        "sqgrd,skgd->sgrqk", attended_grad, values, preferred_element_type=jnp.float32
    )
    inner_sum = jnp.sum(prob_full * prob_grad, axis=-1, keepdims=True)
    score_grad = (prob_full * (prob_grad - inner_sum) * HEAD_SIZE ** (-0.5)).astype(jnp.bfloat16)
    query_grad = jnp.einsum(
        "sgrqk,skgd->sqgrd", score_grad, key_heads, preferred_element_type=jnp.float32
    )
    key_grad = jnp.einsum(
        "sgrqk,sqgrd->skgd", score_grad, queries, preferred_element_type=jnp.float32
    )
    value_grad = jnp.einsum(
        "sgrqk,sqgrd->skgd",
        prob_full.astype(jnp.bfloat16),
        attended_grad,
        preferred_element_type=jnp.float32,
    )
    projected_grad = jnp.concatenate(
        [
            unrotate(query_grad, cos_query, sin_query),
            unrotate(key_grad, cos_key, sin_key)[:, :, :, None],
            value_grad[:, :, :, None],
        ],
        axis=3,
    )
    projected_grad = projected_grad.astype(jnp.bfloat16).reshape(
        seq_count * length, groups * (repeat_factor + 2) * HEAD_SIZE
    )
    qkv_part = jnp.einsum("td,tc->dc", normed1, projected_grad, preferred_element_type=jnp.float32)
    normed1_grad = narrow(
        jnp.einsum("tc,dc->td", projected_grad, qkv_full, preferred_element_type=jnp.float32)
    )
    attn_gain_part = jnp.sum(normed1_grad * residual * scale_attn, axis=0)
    input_grad = (hidden1_grad + norm_back(residual, scale_attn, gain_attn, normed1_grad)).astype(
        jnp.bfloat16
    )
    attn_gain_total, mlp_gain_total = lax.psum((attn_gain_part, mlp_gain_part), "tensor")
    attn_gain_grad, qkv_grad, gate_grad, up_grad, mlp_gain_grad = (
        lax.psum_scatter(
            attn_gain_total.astype(jnp.bfloat16), "dp", scatter_dimension=0, tiled=True
        ).astype(jnp.float32),
        lax.psum_scatter(
            qkv_part.astype(jnp.bfloat16), "dp", scatter_dimension=0, tiled=True
        ).astype(jnp.float32),
        lax.psum_scatter(
            gate_part.astype(jnp.bfloat16), "dp", scatter_dimension=0, tiled=True
        ).astype(jnp.float32),
        lax.psum_scatter(
            up_part.astype(jnp.bfloat16), "dp", scatter_dimension=0, tiled=True
        ).astype(jnp.float32),
        lax.psum_scatter(
            mlp_gain_total.astype(jnp.bfloat16), "dp", scatter_dimension=0, tiled=True
        ).astype(jnp.float32),
    )
    out_grad, down_grad = (
        lax.psum_scatter(
            out_part.astype(jnp.bfloat16), "dp", scatter_dimension=1, tiled=True
        ).astype(jnp.float32),
        lax.psum_scatter(
            down_part.astype(jnp.bfloat16), "dp", scatter_dimension=1, tiled=True
        ).astype(jnp.float32),
    )
    return (
        block_out,
        input_grad,
        attn_gain_grad,
        qkv_grad,
        out_grad,
        mlp_gain_grad,
        gate_grad,
        up_grad,
        down_grad,
    )


GROUP = 4
WINDOW = 256
LANES = 384
TILE = 128


MESH = pl.DeviceIdType.MESH


def kernel_front(
    n_dp, n_tensor, tokens, first, rest, small, tokens_all, mine, theirs, rest_all, small_all,
    dealt, out_sems, in_sems,
):
    d_at = lax.axis_index("dp")
    z_at = lax.axis_index("tensor")
    member = d_at % GROUP
    chunk = first.shape[2]
    barrier = pltpu.get_barrier_semaphore()
    for k in range(1, n_dp):
        pl.semaphore_signal(
            barrier, inc=1, device_id={"dp": d_at ^ k, "tensor": z_at}, device_id_type=MESH
        )
    for s in range(1, n_tensor):
        pl.semaphore_signal(
            barrier,
            inc=1,
            device_id={"dp": d_at, "tensor": lax.rem(z_at + s, n_tensor)},
            device_id_type=MESH,
        )
    pl.semaphore_wait(barrier, n_dp - 1 + n_tensor - 1)

    used = [0]

    def send(source, target, bit=0, shift=0):
        slot = used[0]
        used[0] += 1
        copy = pltpu.make_async_remote_copy(
            src_ref=source,
            dst_ref=target,
            send_sem=out_sems.at[slot],
            recv_sem=in_sems.at[slot],
            device_id={"dp": d_at ^ bit, "tensor": lax.rem(z_at + shift, n_tensor)},
            device_id_type=MESH,
        )
        copy.start()
        return copy

    deals = [send(first.at[member ^ k], dealt.at[member], bit=k) for k in range(1, GROUP)]
    smalls = [send(small, small_all.at[d_at], bit=k) for k in range(1, n_dp)]
    across = send(tokens, tokens_all.at[1], bit=2)
    beside = send(tokens, tokens_all.at[2], bit=1)
    small_all[d_at] = small[...]
    dealt[member] = first[member]
    for copy in deals:
        copy.wait_recv()
    for i in range(GROUP):
        mine[z_at, :, i * chunk : (i + 1) * chunk] = dealt[i]
    spreads = [
        send(mine.at[z_at], mine.at[z_at], shift=s) for s in range(1, n_tensor)
    ]
    swaps = [send(mine.at[z_at], theirs.at[z_at], bit=GROUP)]
    rests = [send(rest.at[member ^ k], rest_all.at[member], bit=k) for k in range(1, GROUP)]
    tokens_all[0] = tokens[...]
    rest_all[member] = rest[member]
    for s, copy in enumerate(spreads, 1):
        copy.wait_recv()
        origin = lax.rem(z_at + n_tensor - s, n_tensor)
        swaps.append(send(mine.at[origin], theirs.at[origin], bit=GROUP))
    across.wait_recv()
    both = send(tokens_all.at[1], tokens_all.at[3], bit=1)
    for copy in smalls + swaps + rests + [beside, both]:
        copy.wait_recv()
    for copy in deals + smalls + spreads + swaps + rests + [across, beside, both]:
        copy.wait_send()


def front(n_dp, n_tensor, tokens, first, rest, small):
    rows, width = tokens.shape
    units, chunk = first.shape[1:]
    vmem = pl.BlockSpec(memory_space=pltpu.VMEM)
    copies = 3 * (GROUP - 1) - 3 + (n_dp - 1) + 3 + (n_tensor - 1) + n_tensor
    half = jax.ShapeDtypeStruct((n_tensor, units, GROUP * chunk), jnp.bfloat16)
    return pl.pallas_call(
        functools.partial(kernel_front, n_dp, n_tensor),
        in_specs=[vmem] * 4,
        out_specs=[vmem] * 5,
        out_shape=[
            jax.ShapeDtypeStruct((GROUP, rows, width), jnp.bfloat16),
            half,
            half,
            jax.ShapeDtypeStruct(rest.shape, jnp.bfloat16),
            jax.ShapeDtypeStruct((n_dp,) + small.shape, jnp.float32),
        ],
        scratch_shapes=[
            pltpu.VMEM(first.shape, jnp.bfloat16),
            pltpu.SemaphoreType.DMA((copies,)),
            pltpu.SemaphoreType.DMA((copies,)),
        ],
        compiler_params=pltpu.CompilerParams(collective_id=0, has_side_effects=True),
        name="front",
    )(tokens, first, rest, small)


def kernel_project(
    tokens, position, mine, theirs, gain, cos_parts, sin_parts, lanes, out, normed, cos_out, sin_out
):
    features = tokens[0].astype(jnp.float32)
    scale = lax.rsqrt(jnp.mean(features * features, axis=1, keepdims=True) + EPS)
    normal = (features * scale * gain[...]).astype(jnp.bfloat16)
    normed[0] = normal
    half = mine.shape[1]
    contract = (((1,), (1,)), ((), ()))
    product = lax.dot_general(
        normal[:, :half], mine[...], contract, preferred_element_type=jnp.float32
    ) + lax.dot_general(
        normal[:, half:], theirs[...], contract, preferred_element_type=jnp.float32
    )
    entries = cos_parts.shape[1]
    key = lax.broadcasted_iota(jnp.int32, (features.shape[0], entries), 1)
    chosen = (position[0] == key).astype(jnp.bfloat16)

    def pick(parts):
        total = jnp.dot(chosen, parts[0], preferred_element_type=jnp.float32)
        for i in range(1, parts.shape[0]):
            total += jnp.dot(chosen, parts[i], preferred_element_type=jnp.float32)
        return total

    cosine, sine = pick(cos_parts), pick(sin_parts)
    cos_out[0] = cosine
    sin_out[0] = sine
    out[0] = turn(product, cosine, sine, lanes[0:1], lanes[1:2], 1.0).astype(out.dtype)


def turn(value, cosine, sine, second, turns, sign):
    width = value.shape[1]
    half = HEAD_SIZE // 2
    c = turns * cosine + (1.0 - turns)
    u = (sign * turns * second) * sine
    d = (sign * turns * (second - 1.0)) * sine
    pieces = []
    up = pltpu.roll(value, half, 1)
    down = pltpu.roll(value, width - half, 1)
    for i in range(width // LANES):
        at = slice(i * LANES, (i + 1) * LANES)
        pieces.append(value[:, at] * c + up[:, at] * u + down[:, at] * d)
    return jnp.concatenate(pieces, axis=1)


def project(tokens, position, mine, theirs, gain, cos_parts, sin_parts, lanes):
    blocks, rows, width = tokens.shape
    units, half = mine.shape
    table_spec = pl.BlockSpec((1, rows, LANES), lambda i: (i, 0, 0))

    def whole(array):
        return pl.BlockSpec(array.shape, lambda i: (0,) * array.ndim)

    return pl.pallas_call(
        kernel_project,
        grid=(blocks,),
        in_specs=[
            pl.BlockSpec((1, rows, width), lambda i: (i, 0, 0)),
            pl.BlockSpec((1, rows, 1), lambda i: (i, 0, 0)),
            whole(mine),
            whole(theirs),
            whole(gain),
            whole(cos_parts),
            whole(sin_parts),
            whole(lanes),
        ],
        out_specs=[
            pl.BlockSpec((1, rows, units), lambda i: (i, 0, 0)),
            pl.BlockSpec((1, rows, width), lambda i: (i, 0, 0)),
            table_spec,
            table_spec,
        ],
        out_shape=[
            jax.ShapeDtypeStruct((blocks, rows, units), jnp.bfloat16),
            jax.ShapeDtypeStruct((blocks, rows, width), jnp.bfloat16),
            jax.ShapeDtypeStruct((blocks, rows, LANES), jnp.float32),
            jax.ShapeDtypeStruct((blocks, rows, LANES), jnp.float32),
        ],
        name="project",
    )(tokens, position, mine, theirs, gain, cos_parts, sin_parts, lanes)


def load_group(core, keep, recv, halo, queries, keyvals):
    mine, other = keep[0], recv[0]
    first = core == 0
    queries[...] = jnp.where(first, mine, other)
    keyvals[:WINDOW] = halo[0]
    keyvals[WINDOW:] = jnp.where(first, other, mine)


def allowed_tile(lowest, start):
    low = lowest[0, pl.ds(start, TILE), :]
    key = lax.broadcasted_iota(jnp.int32, (TILE, TILE + WINDOW), 1)
    query = lax.broadcasted_iota(jnp.int32, (TILE, TILE + WINDOW), 0)
    return (key >= low) & (key <= query + WINDOW)


def kernel_attend(core_ref, keep, recv, halo, lowest, out, log_out, queries, keyvals):
    core = core_ref[0]
    load_group(core, keep, recv, halo, queries, keyvals)
    heads = queries.shape[1] // HEAD_SIZE
    repeat = QUERY_HEADS // KEY_VALUE_HEADS

    def body(tile, carry):
        start = pl.multiple_of(tile * TILE, TILE)
        allowed = allowed_tile(lowest, start)
        for head in range(heads):
            group, r = head // repeat, head % repeat
            base = group * 2 * HEAD_SIZE
            q = queries[pl.ds(start, TILE), head * HEAD_SIZE : (head + 1) * HEAD_SIZE]
            k = keyvals[pl.ds(start, TILE + WINDOW), base : base + HEAD_SIZE]
            v = keyvals[pl.ds(start, TILE + WINDOW), base + HEAD_SIZE : base + 2 * HEAD_SIZE]
            s = lax.dot_general(
                q, k, (((1,), (1,)), ((), ())), preferred_element_type=jnp.float32
            ) * HEAD_SIZE ** (-0.5)
            s = jnp.where(allowed, s, NEG_FILL)
            highest = jnp.max(s, axis=1, keepdims=True)
            e = jnp.exp(s - highest)
            whole = jnp.sum(e, axis=1, keepdims=True)
            total = highest + jnp.log(whole)
            p = (e * (1.0 / whole)).astype(jnp.bfloat16)
            o = jnp.dot(p, v, preferred_element_type=jnp.float32).astype(jnp.bfloat16)
            slot = jnp.where(core == r, 0, 1)
            out[slot, 0, pl.ds(start, TILE), group * HEAD_SIZE : (group + 1) * HEAD_SIZE] = o
            log_out[0, pl.ds(start, TILE), head : head + 1] = total
        return carry

    lax.fori_loop(0, queries.shape[0] // TILE, body, 0)


def attend(core, keep, recv, halo, lowest):
    pairs, rows, units = keep.shape
    heads = units // HEAD_SIZE
    spec = pl.BlockSpec((1, rows, units), lambda i: (i, 0, 0))
    return pl.pallas_call(
        kernel_attend,
        grid=(pairs,),
        in_specs=[
            pl.BlockSpec(memory_space=pltpu.SMEM),
            spec,
            spec,
            pl.BlockSpec((1, WINDOW, units), lambda i: (i, 0, 0)),
            pl.BlockSpec((1, rows, 1), lambda i: (i, 0, 0)),
        ],
        out_specs=[
            pl.BlockSpec((2, 1, rows, units // 2), lambda i: (0, i, 0, 0)),
            pl.BlockSpec((1, rows, heads), lambda i: (i, 0, 0)),
        ],
        out_shape=[
            jax.ShapeDtypeStruct((2, pairs, rows, units // 2), jnp.bfloat16),
            jax.ShapeDtypeStruct((pairs, rows, heads), jnp.float32),
        ],
        scratch_shapes=[
            pltpu.VMEM((rows, units), jnp.bfloat16),
            pltpu.VMEM((rows + WINDOW, units), jnp.bfloat16),
        ],
        name="attend",
    )(core, keep, recv, halo, lowest)


def kernel_attend_back(
    core_ref, keep, recv, halo, lowest, log_total, grads, grads_other, cosine, sine, lanes,
    query_out, key_out, halo_out, queries, keyvals, totals, query_total,
):
    core = core_ref[0]
    load_group(core, keep, recv, halo, queries, keyvals)
    totals[...] = jnp.zeros_like(totals)
    heads = queries.shape[1] // HEAD_SIZE
    repeat = QUERY_HEADS // KEY_VALUE_HEADS
    scale = HEAD_SIZE ** (-0.5)

    def body(tile, carry):
        start = pl.multiple_of(tile * TILE, TILE)
        allowed = allowed_tile(lowest, start)
        mine = grads[0, pl.ds(start, TILE), :]
        other = grads_other[0, pl.ds(start, TILE), :]
        first = core == 0
        by_repeat = (jnp.where(first, mine, other), jnp.where(first, other, mine))
        for group in range(heads // repeat):
            base = group * 2 * HEAD_SIZE
            k = keyvals[pl.ds(start, TILE + WINDOW), base : base + HEAD_SIZE]
            v = keyvals[pl.ds(start, TILE + WINDOW), base + HEAD_SIZE : base + 2 * HEAD_SIZE]
            key_sum = None
            for r in range(repeat):
                head = group * repeat + r
                q = queries[pl.ds(start, TILE), head * HEAD_SIZE : (head + 1) * HEAD_SIZE]
                g = by_repeat[r][:, group * HEAD_SIZE : (group + 1) * HEAD_SIZE]
                s = lax.dot_general(
                    q, k, (((1,), (1,)), ((), ())), preferred_element_type=jnp.float32
                ) * scale
                total = log_total[0, pl.ds(start, TILE), head : head + 1]
                p = jnp.exp(jnp.where(allowed, s, NEG_FILL) - total)
                pg = lax.dot_general(
                    g, v, (((1,), (1,)), ((), ())), preferred_element_type=jnp.float32
                )
                inner = jnp.sum(p * pg, axis=1, keepdims=True)
                sg = (p * (pg - inner) * scale).astype(jnp.bfloat16)
                query_total[:, head * HEAD_SIZE : (head + 1) * HEAD_SIZE] = jnp.dot(
                    sg, k, preferred_element_type=jnp.float32
                )
                dk = lax.dot_general(
                    sg, q, (((0,), (0,)), ((), ())), preferred_element_type=jnp.float32
                )
                dv = lax.dot_general(
                    p.astype(jnp.bfloat16), g, (((0,), (0,)), ((), ())),
                    preferred_element_type=jnp.float32,
                )
                both = jnp.concatenate([dk, dv], axis=1)
                key_sum = both if key_sum is None else key_sum + both
            totals[pl.ds(start, TILE + WINDOW), base : base + 2 * HEAD_SIZE] += key_sum
        rows = pl.ds(start, TILE)
        query_out[0, rows, :] = turn(
            query_total[...], cosine[0, rows, :], sine[0, rows, :], lanes[0:1], lanes[3:4], -1.0
        ).astype(jnp.bfloat16)
        return carry

    lax.fori_loop(0, queries.shape[0] // TILE, body, 0)
    key_out[0] = totals[WINDOW:]
    halo_out[0] = totals[:WINDOW].astype(jnp.bfloat16)


def attend_back(
    core, keep, recv, halo, lowest, log_total, grads, grads_other, cosine, sine, lanes
):
    pairs, rows, units = keep.shape
    heads = units // HEAD_SIZE
    spec = pl.BlockSpec((1, rows, units), lambda i: (i, 0, 0))
    half_spec = pl.BlockSpec((1, rows, units // 2), lambda i: (i, 0, 0))
    halo_spec = pl.BlockSpec((1, WINDOW, units), lambda i: (i, 0, 0))
    table_spec = pl.BlockSpec((1, rows, LANES), lambda i: (i, 0, 0))
    return pl.pallas_call(
        kernel_attend_back,
        grid=(pairs,),
        in_specs=[
            pl.BlockSpec(memory_space=pltpu.SMEM),
            spec,
            spec,
            halo_spec,
            pl.BlockSpec((1, rows, 1), lambda i: (i, 0, 0)),
            pl.BlockSpec((1, rows, heads), lambda i: (i, 0, 0)),
            half_spec,
            half_spec,
            table_spec,
            table_spec,
            pl.BlockSpec(lanes.shape, lambda i: (0, 0)),
        ],
        out_specs=[spec, spec, halo_spec],
        out_shape=[
            jax.ShapeDtypeStruct((pairs, rows, units), jnp.bfloat16),
            jax.ShapeDtypeStruct((pairs, rows, units), jnp.float32),
            jax.ShapeDtypeStruct((pairs, WINDOW, units), jnp.bfloat16),
        ],
        scratch_shapes=[
            pltpu.VMEM((rows, units), jnp.bfloat16),
            pltpu.VMEM((rows + WINDOW, units), jnp.bfloat16),
            pltpu.VMEM((rows + WINDOW, units), jnp.float32),
            pltpu.VMEM((TILE, units), jnp.float32),
        ],
        name="attend_back",
    )(core, keep, recv, halo, lowest, log_total, grads, grads_other, cosine, sine, lanes)


def kernel_finish_keys(key_sum, halo, cosine, sine, lanes, out):
    rows = key_sum.shape[1]
    full = key_sum[0]
    tail = full[rows - WINDOW :] + halo[0].astype(jnp.float32)
    full = jnp.concatenate([full[: rows - WINDOW], tail], axis=0)
    out[0] = turn(full, cosine[0], sine[0], lanes[0:1], lanes[2:3], -1.0).astype(jnp.bfloat16)


def finish_keys(key_sum, halo, cosine, sine, lanes):
    pairs, rows, units = key_sum.shape
    spec = pl.BlockSpec((1, rows, units), lambda i: (i, 0, 0))
    table_spec = pl.BlockSpec((1, rows, LANES), lambda i: (i, 0, 0))
    return pl.pallas_call(
        kernel_finish_keys,
        grid=(pairs,),
        in_specs=[
            spec,
            pl.BlockSpec((1, WINDOW, units), lambda i: (i, 0, 0)),
            table_spec,
            table_spec,
            pl.BlockSpec(lanes.shape, lambda i: (0, 0)),
        ],
        out_specs=spec,
        out_shape=jax.ShapeDtypeStruct((pairs, rows, units), jnp.bfloat16),
        name="finish_keys",
    )(key_sum, halo, cosine, sine, lanes)


def fast_local(
    n_dp,
    n_tensor,
    block_in,
    cotangent,
    segment_ids,
    attn_gain,
    qkv_weight,
    out_weight,
    mlp_gain,
    gate_weight,
    up_weight,
    down_weight,
):
    bf16, f32 = jnp.bfloat16, jnp.float32
    d_at = lax.axis_index("dp")
    z_at = lax.axis_index("tensor")
    core = d_at % 2
    member = d_at % GROUP
    upper = d_at // GROUP
    rows, width = block_in.shape
    seqs, length = segment_ids.shape
    half = width // 2

    def swap(value, bit):
        return lax.ppermute(value, "dp", [(i, i ^ bit) for i in range(n_dp)])

    def own_order(value):
        turned = jnp.concatenate([value[..., half:], value[..., :half]], axis=-1)
        return jnp.where(upper == 0, value, turned)

    first = qkv_weight.T.reshape(GROUP, qkv_weight.shape[1] // GROUP, qkv_weight.shape[0])
    shards = [out_weight.T, gate_weight, up_weight, down_weight.T]
    sizes = [s.shape[1] // GROUP for s in shards]
    rest = jnp.concatenate(
        [s.reshape(s.shape[0], GROUP, s.shape[1] // GROUP).transpose(1, 0, 2) for s in shards],
        axis=2,
    )

    def gather_pair(value):
        return jnp.stack([value, swap(value, 2)])

    def gather(value):
        pair = gather_pair(value)
        return jnp.concatenate([pair, swap(pair, 1)], axis=0)

    def scatter(partial_value):
        blocks = partial_value.reshape(GROUP, rows, partial_value.shape[-1])
        got = swap(blocks[2:].astype(bf16), 1)
        pair = blocks[:2].astype(f32) + got.astype(f32)
        return pair[0] + swap(pair[1].astype(bf16), 2).astype(f32)

    starts_row = jnp.arange(length, dtype=jnp.int32)[None, :] - doc_positions(segment_ids)
    stream = starts_row + jnp.arange(seqs, dtype=jnp.int32)[:, None] * length
    stream = stream.reshape(n_tensor, rows)
    first_key = lax.dynamic_index_in_dim(stream, z_at, 0, keepdims=False)
    own_position = z_at * rows + jnp.arange(rows, dtype=jnp.int32) - first_key
    part = attn_gain.shape[0]
    gains_row = jnp.zeros((rows,), f32)
    small = jnp.stack(
        [
            own_position.astype(f32),
            first_key.astype(f32),
            gains_row.at[:part].set(attn_gain.astype(f32)),
            gains_row.at[:part].set(mlp_gain.astype(f32)),
        ]
    )
    lane = jnp.arange(LANES, dtype=jnp.int32)
    within = lane % HEAD_SIZE
    frequency = jnp.power(
        ROPE_BASE, -(2.0 * (within % (HEAD_SIZE // 2)).astype(f32)) / HEAD_SIZE
    )
    angles = jnp.arange(WINDOW, dtype=f32)[:, None] * frequency

    def split(table):
        parts = []
        for _ in range(3):
            parts.append(table.astype(bf16))
            table = table - lax.reduce_precision(table, 8, 7)
        return jnp.stack(parts)

    cos_parts, sin_parts = split(jnp.cos(angles)), split(jnp.sin(angles))
    is_key = (lane % (2 * HEAD_SIZE)) < HEAD_SIZE
    lanes = jnp.stack(
        [within >= HEAD_SIZE // 2, is_key | (core == 0), is_key, lane >= 0]
    ).astype(f32)

    residual = own_order(block_in)
    cot_own = own_order(cotangent)
    tokens_all, qkv_mine, qkv_theirs, rest_all, smalls = front(
        n_dp, n_tensor, residual, first, rest, small
    )
    gain_attn = own_order(smalls[:, 2, :part].reshape(width))
    gain_mlp = own_order(smalls[:, 3, :part].reshape(width))
    block_order = [d_at, d_at ^ 2, d_at ^ 1, d_at ^ 3]
    token_info = jnp.stack(
        [lax.dynamic_index_in_dim(smalls, i, 0, keepdims=False)[:2] for i in block_order]
    )
    positions = token_info[:, 0].astype(jnp.int32)[:, :, None]
    lowest = token_info[:2, 1].astype(jnp.int32) - z_at * rows + WINDOW
    tile_at = jnp.arange(rows, dtype=jnp.int32) // TILE * TILE
    lowest = (lowest - tile_at[None, :])[:, :, None]

    def spread(piece):
        mine = lax.all_gather(piece, "tensor", axis=0, tiled=True)
        return jnp.concatenate([mine, swap(mine, GROUP)], axis=1)

    rest_units = rest_all.reshape(half, rest_all.shape[2]).T
    at = sizes[0] + sizes[1]
    early = lax.all_gather(rest_units[:at], "tensor", axis=0, tiled=True)
    early = jnp.concatenate([early, swap(early, GROUP)], axis=1)
    early = early.reshape(n_tensor, at, width)
    out_full = early[:, : sizes[0]].reshape(n_tensor * sizes[0], width)
    gate_full = early[:, sizes[0] :].reshape(n_tensor * sizes[1], width)
    up_full = spread(rest_units[at : at + sizes[2]])
    down_full = spread(rest_units[at + sizes[2] :])
    qkv_mine = qkv_mine.reshape(-1, half)
    qkv_theirs = qkv_theirs.reshape(-1, half)
    qkv_full = jnp.concatenate([qkv_mine, qkv_theirs], axis=1)

    residual = residual.astype(f32)
    scale_attn = rms_scale(residual)
    grad_rows = gather(cot_own)
    projected, normed1, cosine, sine = project(
        tokens_all, positions, qkv_mine, qkv_theirs, gain_attn[None], cos_parts, sin_parts, lanes
    )
    keep, send = projected[:2], projected[2:]
    recv = swap(send, 1)
    tail = jnp.where(core == 0, recv[:, rows - WINDOW :], keep[:, rows - WINDOW :])
    halo = lax.ppermute(tail, "tensor", [(i, i + 1) for i in range(n_tensor - 1)])
    core_arg = core.astype(jnp.int32).reshape(1)
    outs, log_total = attend(core_arg, keep, recv, halo, lowest)
    attended = jnp.concatenate([outs[0], swap(outs[1], 1)], axis=0)
    attn_flat = attended.reshape(GROUP * rows, attended.shape[-1])
    hidden1 = residual + scatter(
        jnp.dot(attn_flat, out_full, preferred_element_type=f32).astype(bf16)
    )
    scale_mlp = rms_scale(hidden1)
    normed2 = gather((hidden1 * scale_mlp * gain_mlp).astype(bf16)).reshape(GROUP * rows, width)
    grad_rows = grad_rows.reshape(GROUP * rows, width)

    def to_units(tokens, weight):
        return jnp.einsum("td,ud->tu", tokens, weight, preferred_element_type=f32)

    def grad_of(left, right):
        return jnp.einsum("tu,td->ud", left, right, preferred_element_type=f32).astype(bf16)

    gate = to_units(normed2, gate_full)
    up_value = to_units(normed2, up_full)
    sigmoid_gate = jax.nn.sigmoid(gate)
    activated = (gate * sigmoid_gate * up_value).astype(bf16)
    act_grad = to_units(grad_rows, down_full)
    gate_delta = (act_grad * up_value * sigmoid_gate * (1.0 + gate * (1.0 - sigmoid_gate))).astype(
        bf16
    )
    up_delta = (act_grad * gate * sigmoid_gate).astype(bf16)
    normed2_term = jnp.dot(gate_delta, gate_full, preferred_element_type=f32) + jnp.dot(
        up_delta, up_full, preferred_element_type=f32
    )
    normed2_grad = scatter(normed2_term.astype(bf16))
    mlp_delta = scatter(jnp.dot(activated, down_full, preferred_element_type=f32).astype(bf16))
    block_out = own_order((hidden1 + mlp_delta).astype(bf16))
    down_part = grad_of(activated, grad_rows)
    gate_part = grad_of(gate_delta, normed2)
    up_part = grad_of(up_delta, normed2)
    hidden1_grad = cot_own.astype(f32) + norm_back(hidden1, scale_mlp, gain_mlp, normed2_grad)
    grad_full = gather(hidden1_grad.astype(bf16)).reshape(GROUP * rows, width)
    attended_grad = to_units(grad_full, out_full).astype(bf16)
    out_part = grad_of(attn_flat, grad_full)
    attended_grad = attended_grad.reshape(GROUP, rows, attended_grad.shape[-1])
    grads_other = swap(attended_grad[2:], 1)
    query_grad, key_sum, halo_grad = attend_back(
        core_arg, keep, recv, halo, lowest, log_total, attended_grad[:2], grads_other, cosine, sine, lanes
    )
    halo_back = lax.ppermute(halo_grad, "tensor", [(i + 1, i) for i in range(n_tensor - 1)])
    key_grad = finish_keys(key_sum, halo_back, cosine, sine, lanes)
    kept = jnp.where(core == 0, query_grad, key_grad)
    passed = jnp.where(core == 0, key_grad, query_grad)
    projected_grad = jnp.concatenate([kept, swap(passed, 1)], axis=0)
    projected_grad = projected_grad.reshape(GROUP * rows, projected_grad.shape[-1])
    normed1_flat = normed1.reshape(GROUP * rows, width)
    normed1_grad = scatter(
        jnp.dot(projected_grad, qkv_full, preferred_element_type=f32).astype(bf16)
    )
    qkv_part = grad_of(projected_grad, normed1_flat)
    input_grad = own_order(
        (hidden1_grad + norm_back(residual, scale_attn, gain_attn, normed1_grad)).astype(bf16)
    )

    def overlap(weight, grad):
        return jnp.sum(weight.astype(f32) * grad.astype(f32), axis=0)

    def with_row(part_grad, row):
        blocks = part_grad.reshape(n_tensor, -1, width)
        extra = jnp.zeros((n_tensor, 16, width), bf16).at[:, 0].set(row.astype(bf16))
        return jnp.concatenate([blocks, extra], axis=1).reshape(-1, width)

    def collect(part_grad):
        summed = part_grad[:, :half].astype(f32) + swap(part_grad[:, half:], GROUP).astype(f32)
        piece = lax.psum_scatter(
            summed.astype(bf16), "tensor", scatter_dimension=0, tiled=True
        )
        units = piece.shape[0]
        columns = piece.reshape(units, GROUP, half // GROUP).transpose(1, 0, 2)
        pieces = [lax.dynamic_index_in_dim(columns, member, 0, keepdims=False)]
        for k in range(1, GROUP):
            sent = lax.dynamic_index_in_dim(columns, member ^ k, 0, keepdims=False)
            pieces.append(swap(sent, k))
        stacked = jnp.stack(pieces)
        return jnp.stack(
            [lax.dynamic_index_in_dim(stacked, member ^ i, 0, keepdims=False) for i in range(GROUP)]
        )

    def flat(blocks):
        return blocks.reshape(-1, blocks.shape[2])

    def row_of(blocks, gain):
        return jnp.sum(blocks[:, -16].astype(f32), axis=0) / gain.astype(f32)

    mlp_row = overlap(gate_full, gate_part) + overlap(up_full, up_part)
    down_grad = flat(collect(down_part)).astype(f32)
    gate_grad = flat(collect(gate_part)).T.astype(f32)
    up_blocks = collect(with_row(up_part, mlp_row))
    up_grad = flat(up_blocks[:, :-16]).T.astype(f32)
    out_grad = flat(collect(out_part)).astype(f32)
    qkv_blocks = collect(with_row(qkv_part, overlap(qkv_full, qkv_part)))
    qkv_grad = flat(qkv_blocks[:, :-16]).T.astype(f32)
    gains = [row_of(qkv_blocks, attn_gain), row_of(up_blocks, mlp_gain)]
    return (
        block_out,
        input_grad,
        gains[0],
        qkv_grad,
        out_grad,
        gains[1],
        gate_grad,
        up_grad,
        down_grad,
    )


def solution(mesh):
    in_specs = (
        P(("dp", "tensor"), None),
        P(("dp", "tensor"), None),
        P("dp", None),
        P("dp"),
        P("dp", "tensor"),
        P("tensor", "dp"),
        P("dp"),
        P("dp", "tensor"),
        P("dp", "tensor"),
        P("tensor", "dp"),
    )
    out_specs = (
        P(("dp", "tensor"), None),
        P(("dp", "tensor"), None),
        P("dp"),
        P("dp", "tensor"),
        P("tensor", "dp"),
        P("dp"),
        P("dp", "tensor"),
        P("dp", "tensor"),
        P("tensor", "dp"),
    )
    n_dp, n_tensor = mesh.shape["dp"], mesh.shape["tensor"]

    def body(*arrays):
        rows = arrays[0].shape[0]
        groups = arrays[4].shape[1] // (4 * HEAD_SIZE)
        if n_dp == 2 * GROUP and groups == 2 and rows >= WINDOW and rows % TILE == 0:
            return fast_local(n_dp, n_tensor, *arrays)
        return local(*arrays)

    return jax.shard_map(body, mesh=mesh, in_specs=in_specs, out_specs=out_specs, check_vma=False)
```

```python
import functools

import jax
import jax.numpy as jnp
from jax import lax
from jax.experimental import pallas as pl
from jax.experimental.pallas import tpu as pltpu
from jax.sharding import PartitionSpec as P

QUERY_HEADS = 16
KEY_VALUE_HEADS = 8
HEAD_SIZE = 96


EPS = 1e-05
ROPE_BASE = 100000.0
NEG_FILL = -1e30


def doc_positions(segments):
    length = segments.shape[1]
    position_index = jnp.broadcast_to(jnp.arange(length, dtype=jnp.int32)[None, :], segments.shape)
    change = jnp.concatenate(
        [jnp.ones((segments.shape[0], 1), dtype=bool), segments[:, 1:] != segments[:, :-1]], axis=1
    )
    starts = lax.cummax(jnp.where(change, position_index, jnp.zeros_like(position_index)), axis=1)
    return position_index - starts


def rotary_tables(segments):
    half_dim = HEAD_SIZE // 2
    frequency = jnp.power(ROPE_BASE, -(2.0 * jnp.arange(half_dim, dtype=jnp.float32)) / HEAD_SIZE)
    angles = doc_positions(segments).astype(jnp.float32)[..., None] * frequency
    cosine_table = jnp.concatenate([jnp.cos(angles), jnp.cos(angles)], axis=-1)
    sine_table = jnp.concatenate([jnp.sin(angles), jnp.sin(angles)], axis=-1)
    return (cosine_table, sine_table)


def rotate(vector, cosine_table, sine_table):
    half_dim = vector.shape[-1] // 2
    turned = jnp.concatenate([-vector[..., half_dim:], vector[..., :half_dim]], axis=-1)
    return vector * cosine_table + turned * sine_table


def unrotate(vector, cosine_table, sine_table):
    half_dim = vector.shape[-1] // 2
    shifted = vector * sine_table
    returned = jnp.concatenate([shifted[..., half_dim:], -shifted[..., :half_dim]], axis=-1)
    return vector * cosine_table + returned


def allowed_pairs(segments):
    length = segments.shape[1]
    offsets = jnp.arange(length)
    causal = offsets[None, :] <= offsets[:, None]
    same_doc = segments[:, :, None] == segments[:, None, :]
    return (causal[None] & same_doc)[:, None, None]


def score_block(queries, key_heads, segments):
    scores = jnp.einsum(
        "sqgrd,skgd->sgrqk", queries, key_heads, preferred_element_type=jnp.float32
    ) * HEAD_SIZE ** (-0.5)
    return jnp.where(allowed_pairs(segments), scores, NEG_FILL)


def rms_scale(features):
    return lax.rsqrt(jnp.mean(features * features, axis=-1, keepdims=True) + EPS)


def norm_back(features, inverse, gain_vector, upstream):
    scaled = gain_vector * upstream
    return inverse * scaled - features * (inverse * inverse * inverse) * jnp.mean(
        scaled * features, axis=-1, keepdims=True
    )


def widen(shard_rows):
    return lax.all_gather(shard_rows, "tensor", axis=0, tiled=True)


def narrow(partial_value):
    return lax.psum_scatter(
        partial_value.astype(jnp.bfloat16), "tensor", scatter_dimension=0, tiled=True
    ).astype(jnp.float32)


def local(
    block_in,
    cotangent,
    segment_ids,
    attn_gain,
    qkv_weight,
    out_weight,
    mlp_gain,
    gate_weight,
    up_weight,
    down_weight,
):
    qkv_full, gate_full, up_full, gain_attn_raw, gain_mlp_raw = (
        lax.all_gather(qkv_weight, "dp", axis=0, tiled=True),
        lax.all_gather(gate_weight, "dp", axis=0, tiled=True),
        lax.all_gather(up_weight, "dp", axis=0, tiled=True),
        lax.all_gather(attn_gain, "dp", axis=0, tiled=True),
        lax.all_gather(mlp_gain, "dp", axis=0, tiled=True),
    )
    out_cols, down_cols = (
        lax.all_gather(out_weight, "dp", axis=1, tiled=True),
        lax.all_gather(down_weight, "dp", axis=1, tiled=True),
    )
    seq_count, length = segment_ids.shape
    repeat_factor = QUERY_HEADS // KEY_VALUE_HEADS
    groups = qkv_full.shape[1] // ((repeat_factor + 2) * HEAD_SIZE)
    gain_attn = gain_attn_raw.astype(jnp.float32)
    gain_mlp = gain_mlp_raw.astype(jnp.float32)
    residual = block_in.astype(jnp.float32)
    scale_attn = rms_scale(residual)
    normed1 = widen((residual * scale_attn * gain_attn).astype(jnp.bfloat16))
    projected = jnp.dot(normed1, qkv_full, preferred_element_type=jnp.float32).reshape(
        seq_count, length, groups, repeat_factor + 2, HEAD_SIZE
    )
    cosine_table, sine_table = rotary_tables(segment_ids)
    cos_query = cosine_table[:, :, None, None, :]
    sin_query = sine_table[:, :, None, None, :]
    cos_key = cosine_table[:, :, None, :]
    sin_key = sine_table[:, :, None, :]
    queries = rotate(projected[:, :, :, :repeat_factor], cos_query, sin_query).astype(jnp.bfloat16)
    key_heads = rotate(projected[:, :, :, repeat_factor], cos_key, sin_key).astype(jnp.bfloat16)
    values = projected[:, :, :, repeat_factor + 1].astype(jnp.bfloat16)
    scores = score_block(queries, key_heads, segment_ids)
    highest = jnp.max(scores, axis=-1, keepdims=True)
    log_total = highest + jnp.log(jnp.sum(jnp.exp(scores - highest), axis=-1, keepdims=True))
    probability = jnp.exp(scores - log_total).astype(jnp.bfloat16)
    attended = jnp.einsum(
        "sgrqk,skgd->sqgrd", probability, values, preferred_element_type=jnp.float32
    ).astype(jnp.bfloat16)
    attn_flat = attended.reshape(seq_count * length, groups * repeat_factor * HEAD_SIZE)
    attn_delta = lax.psum_scatter(
        jnp.dot(attn_flat, out_cols, preferred_element_type=jnp.float32).astype(jnp.bfloat16),
        "tensor",
        scatter_dimension=0,
        tiled=True,
    ).astype(jnp.float32)
    hidden1 = residual + attn_delta
    scale_mlp = rms_scale(hidden1)
    normed2 = widen((hidden1 * scale_mlp * gain_mlp).astype(jnp.bfloat16))
    gate = jnp.dot(normed2, gate_full, preferred_element_type=jnp.float32)
    up_value = jnp.dot(normed2, up_full, preferred_element_type=jnp.float32)
    sigmoid_gate = jax.nn.sigmoid(gate)
    activated = (gate * sigmoid_gate * up_value).astype(jnp.bfloat16)
    mlp_delta = narrow(jnp.dot(activated, down_cols, preferred_element_type=jnp.float32))
    block_out = (hidden1 + mlp_delta).astype(jnp.bfloat16)
    grad_rows = widen(cotangent)
    down_part = jnp.einsum("tf,td->fd", activated, grad_rows, preferred_element_type=jnp.float32)
    act_grad = jnp.einsum("td,fd->tf", grad_rows, down_cols, preferred_element_type=jnp.float32)
    gate_delta = (act_grad * up_value * sigmoid_gate * (1.0 + gate * (1.0 - sigmoid_gate))).astype(
        jnp.bfloat16
    )
    up_delta = (act_grad * gate * sigmoid_gate).astype(jnp.bfloat16)
    gate_part = jnp.einsum("td,tf->df", normed2, gate_delta, preferred_element_type=jnp.float32)
    up_part = jnp.einsum("td,tf->df", normed2, up_delta, preferred_element_type=jnp.float32)
    normed2_term = jnp.einsum(
        "tf,df->td", gate_delta, gate_full, preferred_element_type=jnp.float32
    ) + jnp.einsum("tf,df->td", up_delta, up_full, preferred_element_type=jnp.float32)
    normed2_grad = narrow(normed2_term)
    mlp_gain_part = jnp.sum(normed2_grad * hidden1 * scale_mlp, axis=0)
    hidden1_grad = cotangent.astype(jnp.float32) + norm_back(
        hidden1, scale_mlp, gain_mlp, normed2_grad
    )
    hidden1_rounded = hidden1_grad.astype(jnp.bfloat16)
    grad_full = lax.all_gather(hidden1_rounded, "tensor", axis=0, tiled=True)
    attended_grad = jnp.einsum(
        "td,hd->th", grad_full, out_cols, preferred_element_type=jnp.float32
    ).astype(jnp.bfloat16)
    out_part = jnp.einsum("th,td->hd", attn_flat, grad_full, preferred_element_type=jnp.float32)
    attended_grad = attended_grad.reshape(seq_count, length, groups, repeat_factor, HEAD_SIZE)
    prob_full = jnp.exp(score_block(queries, key_heads, segment_ids) - log_total)
    prob_grad = jnp.einsum(
        "sqgrd,skgd->sgrqk", attended_grad, values, preferred_element_type=jnp.float32
    )
    inner_sum = jnp.sum(prob_full * prob_grad, axis=-1, keepdims=True)
    score_grad = (prob_full * (prob_grad - inner_sum) * HEAD_SIZE ** (-0.5)).astype(jnp.bfloat16)
    query_grad = jnp.einsum(
        "sgrqk,skgd->sqgrd", score_grad, key_heads, preferred_element_type=jnp.float32
    )
    key_grad = jnp.einsum(
        "sgrqk,sqgrd->skgd", score_grad, queries, preferred_element_type=jnp.float32
    )
    value_grad = jnp.einsum(
        "sgrqk,sqgrd->skgd",
        prob_full.astype(jnp.bfloat16),
        attended_grad,
        preferred_element_type=jnp.float32,
    )
    projected_grad = jnp.concatenate(
        [
            unrotate(query_grad, cos_query, sin_query),
            unrotate(key_grad, cos_key, sin_key)[:, :, :, None],
            value_grad[:, :, :, None],
        ],
        axis=3,
    )
    projected_grad = projected_grad.astype(jnp.bfloat16).reshape(
        seq_count * length, groups * (repeat_factor + 2) * HEAD_SIZE
    )
    qkv_part = jnp.einsum("td,tc->dc", normed1, projected_grad, preferred_element_type=jnp.float32)
    normed1_grad = narrow(
        jnp.einsum("tc,dc->td", projected_grad, qkv_full, preferred_element_type=jnp.float32)
    )
    attn_gain_part = jnp.sum(normed1_grad * residual * scale_attn, axis=0)
    input_grad = (hidden1_grad + norm_back(residual, scale_attn, gain_attn, normed1_grad)).astype(
        jnp.bfloat16
    )
    attn_gain_total, mlp_gain_total = lax.psum((attn_gain_part, mlp_gain_part), "tensor")
    attn_gain_grad, qkv_grad, gate_grad, up_grad, mlp_gain_grad = (
        lax.psum_scatter(
            attn_gain_total.astype(jnp.bfloat16), "dp", scatter_dimension=0, tiled=True
        ).astype(jnp.float32),
        lax.psum_scatter(
            qkv_part.astype(jnp.bfloat16), "dp", scatter_dimension=0, tiled=True
        ).astype(jnp.float32),
        lax.psum_scatter(
            gate_part.astype(jnp.bfloat16), "dp", scatter_dimension=0, tiled=True
        ).astype(jnp.float32),
        lax.psum_scatter(
            up_part.astype(jnp.bfloat16), "dp", scatter_dimension=0, tiled=True
        ).astype(jnp.float32),
        lax.psum_scatter(
            mlp_gain_total.astype(jnp.bfloat16), "dp", scatter_dimension=0, tiled=True
        ).astype(jnp.float32),
    )
    out_grad, down_grad = (
        lax.psum_scatter(
            out_part.astype(jnp.bfloat16), "dp", scatter_dimension=1, tiled=True
        ).astype(jnp.float32),
        lax.psum_scatter(
            down_part.astype(jnp.bfloat16), "dp", scatter_dimension=1, tiled=True
        ).astype(jnp.float32),
    )
    return (
        block_out,
        input_grad,
        attn_gain_grad,
        qkv_grad,
        out_grad,
        mlp_gain_grad,
        gate_grad,
        up_grad,
        down_grad,
    )


GROUP = 4
WINDOW = 256
LANES = 384
TILE = 128


MESH = pl.DeviceIdType.MESH


def kernel_forward(
    n_dp, n_tensor, sizes,
    tokens, cot, first, rest, small, cos_parts, sin_parts, lanes,
    normed1_out, normed2_out, hidden_out, query_out, keyval_out, log_out, att_out,
    cos_out, sin_out, qkv_out, out_out, small_out, cot_out, *refs,
):
    weights = refs[: len(sizes) - 1]
    (
        x_all, n1_all, dealt, qkv, rbuf, piece, outw, small_all, parts, recv, queries, keyvals,
        att, att_send, logs, cosine, sine, low_col, to_core, from_core, to_across, from_across,
        hidden, n2_all, stage, out_sems, in_sems, local_sems,
    ) = refs[len(sizes) - 1 :]
    f32, bf16 = jnp.float32, jnp.bfloat16
    d_at = lax.axis_index("dp")
    z_at = lax.axis_index("tensor")
    member = d_at % GROUP
    core = d_at % 2
    upper = d_at // GROUP
    rows, width = tokens.shape
    half = width // 2
    chunk = first.shape[2]
    contract = (((1,), (1,)), ((), ()))
    barrier = pltpu.get_barrier_semaphore()
    for k in range(1, n_dp):
        pl.semaphore_signal(
            barrier, inc=1, device_id={"dp": d_at ^ k, "tensor": z_at}, device_id_type=MESH
        )
    for s in range(1, n_tensor):
        pl.semaphore_signal(
            barrier,
            inc=1,
            device_id={"dp": d_at, "tensor": lax.rem(z_at + s, n_tensor)},
            device_id_type=MESH,
        )
    pl.semaphore_wait(barrier, n_dp - 1 + n_tensor - 1)

    used = [0, 0]
    sent = []
    saved = []

    def describe(source, target, bit=0, shift=0):
        slot = used[0]
        used[0] += 1
        return pltpu.make_async_remote_copy(
            src_ref=source,
            dst_ref=target,
            send_sem=out_sems.at[slot],
            recv_sem=in_sems.at[slot],
            device_id={"dp": d_at ^ bit, "tensor": lax.rem(z_at + shift, n_tensor)},
            device_id_type=MESH,
        )

    def send(source, target, bit=0, shift=0):
        copy = describe(source, target, bit, shift)
        copy.start()
        sent.append(copy)
        return copy

    def move(source, target):
        copy = pltpu.make_async_copy(source, target, local_sems.at[used[1]])
        used[1] += 1
        copy.start()
        return copy

    def save(source, target):
        saved.append(move(source, target))

    deals = [send(first.at[member ^ k], dealt.at[member], bit=k) for k in range(1, GROUP)]
    smalls = [send(small, small_all.at[d_at], bit=k) for k in range(1, n_dp)]
    across = send(tokens, x_all.at[1], bit=2)
    beside = send(tokens, x_all.at[2], bit=1)
    rests = [send(rest.at[member ^ k], rbuf.at[member], bit=k) for k in range(1, GROUP)]
    own = [
        move(tokens, x_all.at[0]),
        move(first.at[member], dealt.at[member]),
        move(rest.at[member], rbuf.at[member]),
    ]
    cot_stage = move(cot, stage)
    small_all[d_at] = small[...]

    @pl.when(z_at == 0)
    def _():
        keyvals[:, :WINDOW, :] = jnp.zeros_like(keyvals[:, :WINDOW, :])

    for copy in own:
        copy.wait()
    for copy in deals:
        copy.wait_recv()
    for i in range(GROUP):
        qkv[z_at, :, i * chunk : (i + 1) * chunk] = dealt[i]
    low, high = pl.ds(0, half), pl.ds(half, half)

    def spread(target):
        return [
            send(target.at[z_at, :, low], target.at[z_at, :, low], shift=s)
            for s in range(1, n_tensor)
        ]

    def forward(target, s):
        origin = lax.rem(z_at + n_tensor - s, n_tensor)
        return send(target.at[origin, :, low], target.at[origin, :, high], bit=GROUP)

    first_spread = spread(qkv)
    first_swaps = [forward(qkv, 0)]
    cot_stage.wait()
    save(stage, cot_out.at[0])

    for copy in smalls:
        copy.wait_recv()
    for copy in rests:
        copy.wait_recv()
    for i in range(GROUP):
        piece[:, i * chunk : (i + 1) * chunk] = rbuf[i].T

    swaps = []
    forwards = [[] for _ in sizes]

    targets = [outw] + list(weights)
    starts = [sum(sizes[:i]) for i in range(len(sizes))]

    def issue(index):
        own_piece = piece.at[pl.ds(starts[index], sizes[index])]
        target = targets[index]
        spreads = [send(own_piece, target.at[z_at, :, low], shift=s) for s in range(1, n_tensor)]
        if index == 0:
            outw[z_at, :, :half] = piece[: sizes[0]]
        else:
            save(own_piece, target.at[z_at, :, low])
        swaps.append(send(own_piece, target.at[z_at, :, high], bit=GROUP))
        return spreads

    def background():
        count = len(targets)
        spreads = [issue(0)]
        yield
        for index in range(count):
            if index + 1 < count:
                spreads.append(issue(index + 1))
                yield
            for s, copy in enumerate(spreads[index], 1):
                copy.wait_recv()
                forwards[index].append(forward(targets[index], s))
                yield
        while True:
            yield

    stages = background()

    def advance(count=1):
        for _ in range(count):
            next(stages)

    for s, copy in enumerate(first_spread, 1):
        copy.wait_recv()
        first_swaps.append(forward(qkv, s))
    advance(2)
    gains = []
    for row in (2, 3):
        pieces = []
        for i in range(n_dp):
            at = lax.rem(GROUP * upper + i, n_dp)
            pieces.append(small_all[at, row : row + 1, :chunk])
        gains.append(jnp.concatenate(pieces, axis=1))
    beside.wait_recv()
    for copy in first_swaps:
        copy.wait_recv()
    wait_cot = []

    def project_block(m, k):
        features = x_all[m].astype(f32)
        scale = lax.rsqrt(jnp.mean(features * features, axis=1, keepdims=True) + EPS)
        normal = (features * scale * gains[0]).astype(bf16)
        n1_all[m] = normal
        units = qkv.shape[0] * qkv.shape[1]
        product = lax.dot_general(
            normal, qkv[...].reshape(units, width), contract, preferred_element_type=f32
        )
        info = small_all[d_at ^ k].T
        key = lax.broadcasted_iota(jnp.int32, (rows, cos_parts.shape[1]), 1)
        chosen = (info[:, 0:1].astype(jnp.int32) == key).astype(bf16)

        def pick(table):
            total = jnp.dot(chosen, table[0], preferred_element_type=f32)
            for i in range(1, table.shape[0]):
                total += jnp.dot(chosen, table[i], preferred_element_type=f32)
            return total

        cos_here, sin_here = pick(cos_parts), pick(sin_parts)
        parts[m] = turn(product, cos_here, sin_here, lanes[0:1], lanes[1:2], 1.0).astype(bf16)
        if m < 2:
            cosine[m] = cos_here
            sine[m] = sin_here
            low_col[m] = info[:, 1:2].astype(jnp.int32) - z_at * rows + WINDOW

    project_block(2, 1)
    part_swaps = [send(parts.at[2], recv.at[0], bit=1)]
    project_block(0, 0)
    advance()
    across.wait_recv()
    both = send(x_all.at[1], x_all.at[3], bit=1)
    cot_across = send(cot, cot_out.at[1], bit=2)
    cot_beside = send(cot, cot_out.at[2], bit=1)
    project_block(1, 2)
    advance()
    both.wait_recv()
    project_block(3, 3)
    part_swaps.append(send(parts.at[3], recv.at[1], bit=1))
    advance(2)
    save(n1_all, normed1_out)
    save(cosine, cos_out)
    save(sine, sin_out)

    is_first = core == 0
    halos = []
    for m in range(2):
        part_swaps[m].wait_recv()
        mine, other = parts[m], recv[m]
        queries[m] = jnp.where(is_first, mine, other)
        keyvals[m, WINDOW:, :] = jnp.where(is_first, other, mine)
        halos.append(
            describe(keyvals.at[m, pl.ds(rows, WINDOW)], keyvals.at[m, pl.ds(0, WINDOW)], shift=1)
        )

        @pl.when(z_at < n_tensor - 1)
        def _(m=m):
            halos[m].start()

    save(queries, query_out)
    heads = queries.shape[2] // HEAD_SIZE
    repeat = QUERY_HEADS // KEY_VALUE_HEADS
    span = TILE + WINDOW

    def attend_tile(m, start):
        key = lax.broadcasted_iota(jnp.int32, (TILE, span), 1)
        query = lax.broadcasted_iota(jnp.int32, (TILE, span), 0)
        lowest = low_col[m, pl.ds(start, TILE), :] - start
        allowed = (key >= lowest) & (key <= query + WINDOW)
        for head in range(heads):
            group, r = head // repeat, head % repeat
            base = group * 2 * HEAD_SIZE
            q = queries[m, pl.ds(start, TILE), head * HEAD_SIZE : (head + 1) * HEAD_SIZE]
            k = keyvals[m, pl.ds(start, span), base : base + HEAD_SIZE]
            v = keyvals[m, pl.ds(start, span), base + HEAD_SIZE : base + 2 * HEAD_SIZE]
            s = lax.dot_general(q, k, contract, preferred_element_type=f32) * HEAD_SIZE ** (-0.5)
            s = jnp.where(allowed, s, NEG_FILL)
            highest = jnp.max(s, axis=1, keepdims=True)
            e = jnp.exp(s - highest)
            whole = jnp.sum(e, axis=1, keepdims=True)
            p = (e * (1.0 / whole)).astype(bf16)
            o = jnp.dot(p, v, preferred_element_type=f32).astype(bf16)
            logs[m, pl.ds(start, TILE), head : head + 1] = highest + jnp.log(whole)
            lanes_at = slice(group * HEAD_SIZE, (group + 1) * HEAD_SIZE)

            @pl.when(core == r)
            def _():
                att[m, pl.ds(start, TILE), lanes_at] = o

            @pl.when(core != r)
            def _():
                att_send[m, pl.ds(start, TILE), lanes_at] = o

    tiles = rows // TILE

    def loop(first_tile, last_tile, m_list):
        for m in m_list:

            def body(i, carry, m=m):
                attend_tile(m, pl.multiple_of(i * TILE, TILE))
                return carry

            lax.fori_loop(first_tile, last_tile, body, 0)

    free = -(-WINDOW // TILE)
    loop(free, tiles, (1, 0))
    cot_across.wait_recv()
    cot_both = send(cot_out.at[1], cot_out.at[3], bit=1)
    for m in range(2):

        @pl.when(z_at > 0)
        def _(m=m):
            halos[m].wait_recv()

    loop(0, free, (1,))
    att_swaps = [send(att_send.at[1], att.at[3], bit=1)]
    advance()
    loop(0, free, (0,))
    att_swaps.append(send(att_send.at[0], att.at[2], bit=1))
    advance(1)
    save(keyvals, keyval_out)
    save(logs, log_out)

    for copy in swaps[:1] + forwards[0]:
        copy.wait_recv()

    def project_out(b):
        units = outw.shape[0] * outw.shape[1]
        return jnp.dot(att[b], outw[...].reshape(units, width), preferred_element_type=f32)

    att_swaps[0].wait_recv()
    to_core[1] = project_out(3).astype(bf16)
    core_sends = [send(to_core.at[1], from_core.at[1], bit=1)]
    hidden[...] = project_out(1)
    att_swaps[1].wait_recv()
    to_core[0] = project_out(2).astype(bf16)
    core_sends.append(send(to_core.at[0], from_core.at[0], bit=1))
    core_sends[0].wait_recv()
    across_sends = []
    for i in range(rows // TILE):
        at = pl.ds(i * TILE, TILE)
        to_across[at] = (hidden[at, :] + from_core[1, at, :].astype(f32)).astype(bf16)
        across_sends.append(send(to_across.at[at], from_across.at[at], bit=2))
    hidden[...] = project_out(0) + x_all[0].astype(f32)
    core_sends[1].wait_recv()
    hidden[...] += from_core[0].astype(f32)
    save(att, att_out)
    advance(2)
    last = []
    for i in range(rows // TILE):
        at = pl.ds(i * TILE, TILE)
        across_sends[i].wait_recv()
        value = hidden[at, :] + from_across[at, :].astype(f32)
        hidden[at, :] = value
        scale = lax.rsqrt(jnp.mean(value * value, axis=1, keepdims=True) + EPS)
        n2_all[0, at, :] = (value * scale * gains[1]).astype(bf16)
        last.append(send(n2_all.at[0, at], n2_all.at[1, at], bit=2))
        last.append(send(n2_all.at[0, at], n2_all.at[2, at], bit=1))
        advance(1)
    save(hidden, hidden_out)
    save(qkv, qkv_out)
    save(outw, out_out)
    save(small_all, small_out)
    ends = []
    for i in range(rows // TILE):
        at = pl.ds(i * TILE, TILE)
        last[2 * i].wait_recv()
        ends.append(send(n2_all.at[1, at], n2_all.at[3, at], bit=1))
        advance(1)
    for copy in ends + last[1::2]:
        copy.wait_recv()
    save(n2_all, normed2_out)
    advance(len(sizes) * (n_tensor + 1))
    for copy in swaps[1:] + sum(forwards[1:], []) + [cot_beside, cot_both]:
        copy.wait_recv()
    for copy in sent:
        copy.wait_send()
    for m in range(2):

        @pl.when(z_at < n_tensor - 1)
        def _(m=m):
            halos[m].wait_send()

    for copy in saved:
        copy.wait()


def forward(n_dp, n_tensor, sizes, tokens, cot, first, rest, small, cos_parts, sin_parts, lanes):
    rows, width = tokens.shape
    units = first.shape[1] * n_tensor
    heads = units // HEAD_SIZE
    f32, bf16 = jnp.float32, jnp.bfloat16
    vmem = pl.BlockSpec(memory_space=pltpu.VMEM)
    hbm = pl.BlockSpec(memory_space=pl.ANY)

    def shape(dims, dtype=bf16):
        return jax.ShapeDtypeStruct(tuple(dims), dtype)

    full = (GROUP, rows, width)
    qkv_shape = (n_tensor, first.shape[1], width)
    out_shape = (n_tensor, sizes[0], width)
    att_shape = (GROUP, rows, units // 2)
    small_shape = (n_dp,) + small.shape
    table = (2, rows, LANES)
    outs = [
        shape(full),
        shape(full),
        shape((rows, width), f32),
        shape((2, rows, units)),
        shape((2, rows + WINDOW, units)),
        shape((2, rows, heads), f32),
        shape(att_shape),
        shape(table, f32),
        shape(table, f32),
        shape(qkv_shape),
        shape(out_shape),
        shape(small_shape, f32),
        shape(full),
    ] + [shape((n_tensor, size, width)) for size in sizes[1:]]
    copies = 96
    scratch = [
        pltpu.VMEM(full, bf16),
        pltpu.VMEM(full, bf16),
        pltpu.VMEM(first.shape, bf16),
        pltpu.VMEM(qkv_shape, bf16),
        pltpu.VMEM(rest.shape, bf16),
        pltpu.VMEM((rest.shape[2], width // 2), bf16),
        pltpu.VMEM(out_shape, bf16),
        pltpu.VMEM(small_shape, f32),
        pltpu.VMEM((GROUP, rows, units), bf16),
        pltpu.VMEM((2, rows, units), bf16),
        pltpu.VMEM((2, rows, units), bf16),
        pltpu.VMEM((2, rows + WINDOW, units), bf16),
        pltpu.VMEM(att_shape, bf16),
        pltpu.VMEM((2, rows, units // 2), bf16),
        pltpu.VMEM((2, rows, heads), f32),
        pltpu.VMEM(table, f32),
        pltpu.VMEM(table, f32),
        pltpu.VMEM((2, rows, 1), jnp.int32),
        pltpu.VMEM((2, rows, width), bf16),
        pltpu.VMEM((2, rows, width), bf16),
        pltpu.VMEM((rows, width), bf16),
        pltpu.VMEM((rows, width), bf16),
        pltpu.VMEM((rows, width), f32),
        pltpu.VMEM(full, bf16),
        pltpu.VMEM((rows, width), bf16),
        pltpu.SemaphoreType.DMA((copies,)),
        pltpu.SemaphoreType.DMA((copies,)),
        pltpu.SemaphoreType.DMA((32,)),
    ]
    return pl.pallas_call(
        functools.partial(kernel_forward, n_dp, n_tensor, sizes),
        in_specs=[hbm] * 4 + [vmem] * 4,
        out_specs=[hbm] * len(outs),
        out_shape=outs,
        scratch_shapes=scratch,
        compiler_params=pltpu.CompilerParams(
            collective_id=0, has_side_effects=True, vmem_limit_bytes=60 * 1024 * 1024
        ),
        name="forward",
    )(tokens, cot, first, rest, small, cos_parts, sin_parts, lanes)


def turn(value, cosine, sine, second, turns, sign):
    width = value.shape[1]
    half = HEAD_SIZE // 2
    c = turns * cosine + (1.0 - turns)
    u = (sign * turns * second) * sine
    d = (sign * turns * (second - 1.0)) * sine
    pieces = []
    up = pltpu.roll(value, half, 1)
    down = pltpu.roll(value, width - half, 1)
    for i in range(width // LANES):
        at = slice(i * LANES, (i + 1) * LANES)
        pieces.append(value[:, at] * c + up[:, at] * u + down[:, at] * d)
    return jnp.concatenate(pieces, axis=1)


def allowed_tile(lowest, start):
    low = lowest[0, pl.ds(start, TILE), :]
    key = lax.broadcasted_iota(jnp.int32, (TILE, TILE + WINDOW), 1)
    query = lax.broadcasted_iota(jnp.int32, (TILE, TILE + WINDOW), 0)
    return (key >= low) & (key <= query + WINDOW)


def kernel_attend_back(
    core_ref, queries_ref, keyvals_ref, lowest, log_total, grads, grads_other, cosine, sine, lanes,
    query_out, key_out, halo_out, totals, query_total,
):
    core = core_ref[0]
    queries, keyvals = queries_ref.at[0], keyvals_ref.at[0]
    totals[...] = jnp.zeros_like(totals)
    heads = queries.shape[1] // HEAD_SIZE
    repeat = QUERY_HEADS // KEY_VALUE_HEADS
    scale = HEAD_SIZE ** (-0.5)

    def body(tile, carry):
        start = pl.multiple_of(tile * TILE, TILE)
        allowed = allowed_tile(lowest, start)
        mine = grads[0, pl.ds(start, TILE), :]
        other = grads_other[0, pl.ds(start, TILE), :]
        first = core == 0
        by_repeat = (jnp.where(first, mine, other), jnp.where(first, other, mine))
        for group in range(heads // repeat):
            base = group * 2 * HEAD_SIZE
            k = keyvals[pl.ds(start, TILE + WINDOW), base : base + HEAD_SIZE]
            v = keyvals[pl.ds(start, TILE + WINDOW), base + HEAD_SIZE : base + 2 * HEAD_SIZE]
            key_sum = None
            for r in range(repeat):
                head = group * repeat + r
                q = queries[pl.ds(start, TILE), head * HEAD_SIZE : (head + 1) * HEAD_SIZE]
                g = by_repeat[r][:, group * HEAD_SIZE : (group + 1) * HEAD_SIZE]
                s = lax.dot_general(
                    q, k, (((1,), (1,)), ((), ())), preferred_element_type=jnp.float32
                ) * scale
                total = log_total[0, pl.ds(start, TILE), head : head + 1]
                p = jnp.exp(jnp.where(allowed, s, NEG_FILL) - total)
                pg = lax.dot_general(
                    g, v, (((1,), (1,)), ((), ())), preferred_element_type=jnp.float32
                )
                inner = jnp.sum(p * pg, axis=1, keepdims=True)
                sg = (p * (pg - inner) * scale).astype(jnp.bfloat16)
                query_total[:, head * HEAD_SIZE : (head + 1) * HEAD_SIZE] = jnp.dot(
                    sg, k, preferred_element_type=jnp.float32
                )
                dk = lax.dot_general(
                    sg, q, (((0,), (0,)), ((), ())), preferred_element_type=jnp.float32
                )
                dv = lax.dot_general(
                    p.astype(jnp.bfloat16), g, (((0,), (0,)), ((), ())),
                    preferred_element_type=jnp.float32,
                )
                both = jnp.concatenate([dk, dv], axis=1)
                key_sum = both if key_sum is None else key_sum + both
            totals[pl.ds(start, TILE + WINDOW), base : base + 2 * HEAD_SIZE] += key_sum
        rows = pl.ds(start, TILE)
        query_out[0, rows, :] = turn(
            query_total[...], cosine[0, rows, :], sine[0, rows, :], lanes[0:1], lanes[3:4], -1.0
        ).astype(jnp.bfloat16)
        return carry

    lax.fori_loop(0, queries.shape[0] // TILE, body, 0)
    key_out[0] = totals[WINDOW:]
    halo_out[0] = totals[:WINDOW].astype(jnp.bfloat16)


def attend_back(
    core, queries, keyvals, lowest, log_total, grads, grads_other, cosine, sine, lanes
):
    pairs, rows, units = queries.shape
    heads = units // HEAD_SIZE
    spec = pl.BlockSpec((1, rows, units), lambda i: (i, 0, 0))
    half_spec = pl.BlockSpec((1, rows, units // 2), lambda i: (i, 0, 0))
    halo_spec = pl.BlockSpec((1, WINDOW, units), lambda i: (i, 0, 0))
    table_spec = pl.BlockSpec((1, rows, LANES), lambda i: (i, 0, 0))
    return pl.pallas_call(
        kernel_attend_back,
        grid=(pairs,),
        in_specs=[
            pl.BlockSpec(memory_space=pltpu.SMEM),
            spec,
            pl.BlockSpec((1, rows + WINDOW, units), lambda i: (i, 0, 0)),
            pl.BlockSpec((1, rows, 1), lambda i: (i, 0, 0)),
            pl.BlockSpec((1, rows, heads), lambda i: (i, 0, 0)),
            half_spec,
            half_spec,
            table_spec,
            table_spec,
            pl.BlockSpec(lanes.shape, lambda i: (0, 0)),
        ],
        out_specs=[spec, spec, halo_spec],
        out_shape=[
            jax.ShapeDtypeStruct((pairs, rows, units), jnp.bfloat16),
            jax.ShapeDtypeStruct((pairs, rows, units), jnp.float32),
            jax.ShapeDtypeStruct((pairs, WINDOW, units), jnp.bfloat16),
        ],
        scratch_shapes=[
            pltpu.VMEM((rows + WINDOW, units), jnp.float32),
            pltpu.VMEM((TILE, units), jnp.float32),
        ],
        name="attend_back",
    )(core, queries, keyvals, lowest, log_total, grads, grads_other, cosine, sine, lanes)


def kernel_finish_keys(key_sum, halo, cosine, sine, lanes, out):
    rows = key_sum.shape[1]
    full = key_sum[0]
    tail = full[rows - WINDOW :] + halo[0].astype(jnp.float32)
    full = jnp.concatenate([full[: rows - WINDOW], tail], axis=0)
    out[0] = turn(full, cosine[0], sine[0], lanes[0:1], lanes[2:3], -1.0).astype(jnp.bfloat16)


def finish_keys(key_sum, halo, cosine, sine, lanes):
    pairs, rows, units = key_sum.shape
    spec = pl.BlockSpec((1, rows, units), lambda i: (i, 0, 0))
    table_spec = pl.BlockSpec((1, rows, LANES), lambda i: (i, 0, 0))
    return pl.pallas_call(
        kernel_finish_keys,
        grid=(pairs,),
        in_specs=[
            spec,
            pl.BlockSpec((1, WINDOW, units), lambda i: (i, 0, 0)),
            table_spec,
            table_spec,
            pl.BlockSpec(lanes.shape, lambda i: (0, 0)),
        ],
        out_specs=spec,
        out_shape=jax.ShapeDtypeStruct((pairs, rows, units), jnp.bfloat16),
        name="finish_keys",
    )(key_sum, halo, cosine, sine, lanes)


def fast_local(
    n_dp,
    n_tensor,
    block_in,
    cotangent,
    segment_ids,
    attn_gain,
    qkv_weight,
    out_weight,
    mlp_gain,
    gate_weight,
    up_weight,
    down_weight,
):
    bf16, f32 = jnp.bfloat16, jnp.float32
    d_at = lax.axis_index("dp")
    z_at = lax.axis_index("tensor")
    core = d_at % 2
    member = d_at % GROUP
    upper = d_at // GROUP
    rows, width = block_in.shape
    seqs, length = segment_ids.shape
    half = width // 2

    def swap(value, bit):
        return lax.ppermute(value, "dp", [(i, i ^ bit) for i in range(n_dp)])

    def own_order(value):
        turned = jnp.concatenate([value[..., half:], value[..., :half]], axis=-1)
        return jnp.where(upper == 0, value, turned)

    first = qkv_weight.T.reshape(GROUP, qkv_weight.shape[1] // GROUP, qkv_weight.shape[0])
    shards = [out_weight.T, gate_weight, up_weight, down_weight.T]
    sizes = [s.shape[1] // GROUP for s in shards]
    rest = jnp.concatenate(
        [s.reshape(s.shape[0], GROUP, s.shape[1] // GROUP).transpose(1, 0, 2) for s in shards],
        axis=2,
    )

    def gather_pair(value):
        return jnp.stack([value, swap(value, 2)])

    def gather(value):
        pair = gather_pair(value)
        return jnp.concatenate([pair, swap(pair, 1)], axis=0)

    def scatter(partial_value):
        blocks = partial_value.reshape(GROUP, rows, partial_value.shape[-1])
        got = swap(blocks[2:].astype(bf16), 1)
        pair = blocks[:2].astype(f32) + got.astype(f32)
        return pair[0] + swap(pair[1].astype(bf16), 2).astype(f32)

    starts_row = jnp.arange(length, dtype=jnp.int32)[None, :] - doc_positions(segment_ids)
    stream = starts_row + jnp.arange(seqs, dtype=jnp.int32)[:, None] * length
    stream = stream.reshape(n_tensor, rows)
    first_key = lax.dynamic_index_in_dim(stream, z_at, 0, keepdims=False)
    own_position = z_at * rows + jnp.arange(rows, dtype=jnp.int32) - first_key
    part = attn_gain.shape[0]
    gains_row = jnp.zeros((rows,), f32)
    small = jnp.stack(
        [
            own_position.astype(f32),
            first_key.astype(f32),
            gains_row.at[:part].set(attn_gain.astype(f32)),
            gains_row.at[:part].set(mlp_gain.astype(f32)),
        ]
        + [gains_row] * 4
    )
    lane = jnp.arange(LANES, dtype=jnp.int32)
    within = lane % HEAD_SIZE
    frequency = jnp.power(
        ROPE_BASE, -(2.0 * (within % (HEAD_SIZE // 2)).astype(f32)) / HEAD_SIZE
    )
    angles = jnp.arange(WINDOW, dtype=f32)[:, None] * frequency

    def split(table):
        parts = []
        for _ in range(3):
            parts.append(table.astype(bf16))
            table = table - lax.reduce_precision(table, 8, 7)
        return jnp.stack(parts)

    cos_parts, sin_parts = split(jnp.cos(angles)), split(jnp.sin(angles))
    is_key = (lane % (2 * HEAD_SIZE)) < HEAD_SIZE
    lanes = jnp.stack(
        [within >= HEAD_SIZE // 2, is_key | (core == 0), is_key, lane >= 0]
    ).astype(f32)

    residual = own_order(block_in)
    cot_own = own_order(cotangent)
    (
        normed1, normed2, hidden1, queries, keyvals, log_total, attended, cosine, sine, qkv_full,
        out_full, smalls, grad_rows, gate_full, up_full, down_full,
    ) = forward(
        n_dp, n_tensor, sizes, residual, cot_own, first, rest, small, cos_parts, sin_parts, lanes
    )
    qkv_full, out_full, gate_full, up_full, down_full = [
        w.reshape(-1, width) for w in (qkv_full, out_full, gate_full, up_full, down_full)
    ]
    gain_attn = own_order(smalls[:, 2, :part].reshape(width))
    gain_mlp = own_order(smalls[:, 3, :part].reshape(width))
    lowest = jnp.stack(
        [lax.dynamic_index_in_dim(smalls, i, 0, keepdims=False)[1] for i in (d_at, d_at ^ 2)]
    ).astype(jnp.int32)
    tile_at = jnp.arange(rows, dtype=jnp.int32) // TILE * TILE
    lowest = (lowest - z_at * rows + WINDOW - tile_at[None, :])[:, :, None]
    core_arg = core.astype(jnp.int32).reshape(1)
    residual = residual.astype(f32)
    scale_attn = rms_scale(residual)
    scale_mlp = rms_scale(hidden1)
    attn_flat = attended.reshape(GROUP * rows, attended.shape[-1])
    normed2 = normed2.reshape(GROUP * rows, width)
    grad_rows = grad_rows.reshape(GROUP * rows, width)

    def to_units(tokens, weight):
        return jnp.einsum("td,ud->tu", tokens, weight, preferred_element_type=f32)

    def grad_of(left, right):
        return jnp.einsum("tu,td->ud", left, right, preferred_element_type=f32).astype(bf16)

    gate = to_units(normed2, gate_full)
    up_value = to_units(normed2, up_full)
    sigmoid_gate = jax.nn.sigmoid(gate)
    activated = (gate * sigmoid_gate * up_value).astype(bf16)
    act_grad = to_units(grad_rows, down_full)
    gate_delta = (act_grad * up_value * sigmoid_gate * (1.0 + gate * (1.0 - sigmoid_gate))).astype(
        bf16
    )
    up_delta = (act_grad * gate * sigmoid_gate).astype(bf16)
    normed2_term = jnp.dot(gate_delta, gate_full, preferred_element_type=f32) + jnp.dot(
        up_delta, up_full, preferred_element_type=f32
    )
    normed2_grad = scatter(normed2_term.astype(bf16))
    mlp_delta = scatter(jnp.dot(activated, down_full, preferred_element_type=f32).astype(bf16))
    block_out = own_order((hidden1 + mlp_delta).astype(bf16))
    down_part = grad_of(activated, grad_rows)
    gate_part = grad_of(gate_delta, normed2)
    up_part = grad_of(up_delta, normed2)
    hidden1_grad = cot_own.astype(f32) + norm_back(hidden1, scale_mlp, gain_mlp, normed2_grad)
    grad_full = gather(hidden1_grad.astype(bf16)).reshape(GROUP * rows, width)
    attended_grad = to_units(grad_full, out_full).astype(bf16)
    out_part = grad_of(attn_flat, grad_full)
    attended_grad = attended_grad.reshape(GROUP, rows, attended_grad.shape[-1])
    grads_other = swap(attended_grad[2:], 1)
    query_grad, key_sum, halo_grad = attend_back(
        core_arg, queries, keyvals, lowest, log_total, attended_grad[:2], grads_other, cosine, sine, lanes
    )
    halo_back = lax.ppermute(halo_grad, "tensor", [(i + 1, i) for i in range(n_tensor - 1)])
    key_grad = finish_keys(key_sum, halo_back, cosine, sine, lanes)
    kept = jnp.where(core == 0, query_grad, key_grad)
    passed = jnp.where(core == 0, key_grad, query_grad)
    projected_grad = jnp.concatenate([kept, swap(passed, 1)], axis=0)
    projected_grad = projected_grad.reshape(GROUP * rows, projected_grad.shape[-1])
    normed1_flat = normed1.reshape(GROUP * rows, width)
    normed1_grad = scatter(
        jnp.dot(projected_grad, qkv_full, preferred_element_type=f32).astype(bf16)
    )
    qkv_part = grad_of(projected_grad, normed1_flat)
    input_grad = own_order(
        (hidden1_grad + norm_back(residual, scale_attn, gain_attn, normed1_grad)).astype(bf16)
    )

    def overlap(weight, grad):
        return jnp.sum(weight.astype(f32) * grad.astype(f32), axis=0)

    def with_row(part_grad, row):
        blocks = part_grad.reshape(n_tensor, -1, width)
        extra = jnp.zeros((n_tensor, 16, width), bf16).at[:, 0].set(row.astype(bf16))
        return jnp.concatenate([blocks, extra], axis=1).reshape(-1, width)

    def collect(part_grad):
        summed = part_grad[:, :half].astype(f32) + swap(part_grad[:, half:], GROUP).astype(f32)
        piece = lax.psum_scatter(
            summed.astype(bf16), "tensor", scatter_dimension=0, tiled=True
        )
        units = piece.shape[0]
        columns = piece.reshape(units, GROUP, half // GROUP).transpose(1, 0, 2)
        pieces = [lax.dynamic_index_in_dim(columns, member, 0, keepdims=False)]
        for k in range(1, GROUP):
            sent = lax.dynamic_index_in_dim(columns, member ^ k, 0, keepdims=False)
            pieces.append(swap(sent, k))
        stacked = jnp.stack(pieces)
        return jnp.stack(
            [lax.dynamic_index_in_dim(stacked, member ^ i, 0, keepdims=False) for i in range(GROUP)]
        )

    def flat(blocks):
        return blocks.reshape(-1, blocks.shape[2])

    def row_of(blocks, gain):
        return jnp.sum(blocks[:, -16].astype(f32), axis=0) / gain.astype(f32)

    mlp_row = overlap(gate_full, gate_part) + overlap(up_full, up_part)
    down_grad = flat(collect(down_part)).astype(f32)
    gate_grad = flat(collect(gate_part)).T.astype(f32)
    up_blocks = collect(with_row(up_part, mlp_row))
    up_grad = flat(up_blocks[:, :-16]).T.astype(f32)
    out_grad = flat(collect(out_part)).astype(f32)
    qkv_blocks = collect(with_row(qkv_part, overlap(qkv_full, qkv_part)))
    qkv_grad = flat(qkv_blocks[:, :-16]).T.astype(f32)
    gains = [row_of(qkv_blocks, attn_gain), row_of(up_blocks, mlp_gain)]
    return (
        block_out,
        input_grad,
        gains[0],
        qkv_grad,
        out_grad,
        gains[1],
        gate_grad,
        up_grad,
        down_grad,
    )


def solution(mesh):
    in_specs = (
        P(("dp", "tensor"), None),
        P(("dp", "tensor"), None),
        P("dp", None),
        P("dp"),
        P("dp", "tensor"),
        P("tensor", "dp"),
        P("dp"),
        P("dp", "tensor"),
        P("dp", "tensor"),
        P("tensor", "dp"),
    )
    out_specs = (
        P(("dp", "tensor"), None),
        P(("dp", "tensor"), None),
        P("dp"),
        P("dp", "tensor"),
        P("tensor", "dp"),
        P("dp"),
        P("dp", "tensor"),
        P("dp", "tensor"),
        P("tensor", "dp"),
    )
    n_dp, n_tensor = mesh.shape["dp"], mesh.shape["tensor"]

    def body(*arrays):
        rows = arrays[0].shape[0]
        groups = arrays[4].shape[1] // (4 * HEAD_SIZE)
        if n_dp == 2 * GROUP and groups == 2 and rows >= WINDOW and rows % TILE == 0:
            return fast_local(n_dp, n_tensor, *arrays)
        return local(*arrays)

    return jax.shard_map(body, mesh=mesh, in_specs=in_specs, out_specs=out_specs, check_vma=False)
```

```python
import functools

import jax
import jax.numpy as jnp
import numpy as np
from jax import lax
from jax.experimental import pallas as pl
from jax.experimental.pallas import tpu as pltpu
from jax.sharding import PartitionSpec as P

QUERY_HEADS = 16
KEY_VALUE_HEADS = 8
HEAD_SIZE = 96


EPS = 1e-05
ROPE_BASE = 100000.0
NEG_FILL = -1e30


def doc_positions(segments):
    length = segments.shape[1]
    position_index = jnp.broadcast_to(jnp.arange(length, dtype=jnp.int32)[None, :], segments.shape)
    change = jnp.concatenate(
        [jnp.ones((segments.shape[0], 1), dtype=bool), segments[:, 1:] != segments[:, :-1]], axis=1
    )
    starts = lax.cummax(jnp.where(change, position_index, jnp.zeros_like(position_index)), axis=1)
    return position_index - starts


def rotary_tables(segments):
    half_dim = HEAD_SIZE // 2
    frequency = jnp.power(ROPE_BASE, -(2.0 * jnp.arange(half_dim, dtype=jnp.float32)) / HEAD_SIZE)
    angles = doc_positions(segments).astype(jnp.float32)[..., None] * frequency
    cosine_table = jnp.concatenate([jnp.cos(angles), jnp.cos(angles)], axis=-1)
    sine_table = jnp.concatenate([jnp.sin(angles), jnp.sin(angles)], axis=-1)
    return (cosine_table, sine_table)


def rotate(vector, cosine_table, sine_table):
    half_dim = vector.shape[-1] // 2
    turned = jnp.concatenate([-vector[..., half_dim:], vector[..., :half_dim]], axis=-1)
    return vector * cosine_table + turned * sine_table


def unrotate(vector, cosine_table, sine_table):
    half_dim = vector.shape[-1] // 2
    shifted = vector * sine_table
    returned = jnp.concatenate([shifted[..., half_dim:], -shifted[..., :half_dim]], axis=-1)
    return vector * cosine_table + returned


def allowed_pairs(segments):
    length = segments.shape[1]
    offsets = jnp.arange(length)
    causal = offsets[None, :] <= offsets[:, None]
    same_doc = segments[:, :, None] == segments[:, None, :]
    return (causal[None] & same_doc)[:, None, None]


def score_block(queries, key_heads, segments):
    scores = jnp.einsum(
        "sqgrd,skgd->sgrqk", queries, key_heads, preferred_element_type=jnp.float32
    ) * HEAD_SIZE ** (-0.5)
    return jnp.where(allowed_pairs(segments), scores, NEG_FILL)


def rms_scale(features):
    return lax.rsqrt(jnp.mean(features * features, axis=-1, keepdims=True) + EPS)


def norm_back(features, inverse, gain_vector, upstream):
    scaled = gain_vector * upstream
    return inverse * scaled - features * (inverse * inverse * inverse) * jnp.mean(
        scaled * features, axis=-1, keepdims=True
    )


def widen(shard_rows):
    return lax.all_gather(shard_rows, "tensor", axis=0, tiled=True)


def narrow(partial_value):
    return lax.psum_scatter(
        partial_value.astype(jnp.bfloat16), "tensor", scatter_dimension=0, tiled=True
    ).astype(jnp.float32)


def local(
    block_in,
    cotangent,
    segment_ids,
    attn_gain,
    qkv_weight,
    out_weight,
    mlp_gain,
    gate_weight,
    up_weight,
    down_weight,
):
    qkv_full, gate_full, up_full, gain_attn_raw, gain_mlp_raw = (
        lax.all_gather(qkv_weight, "dp", axis=0, tiled=True),
        lax.all_gather(gate_weight, "dp", axis=0, tiled=True),
        lax.all_gather(up_weight, "dp", axis=0, tiled=True),
        lax.all_gather(attn_gain, "dp", axis=0, tiled=True),
        lax.all_gather(mlp_gain, "dp", axis=0, tiled=True),
    )
    out_cols, down_cols = (
        lax.all_gather(out_weight, "dp", axis=1, tiled=True),
        lax.all_gather(down_weight, "dp", axis=1, tiled=True),
    )
    seq_count, length = segment_ids.shape
    repeat_factor = QUERY_HEADS // KEY_VALUE_HEADS
    groups = qkv_full.shape[1] // ((repeat_factor + 2) * HEAD_SIZE)
    gain_attn = gain_attn_raw.astype(jnp.float32)
    gain_mlp = gain_mlp_raw.astype(jnp.float32)
    residual = block_in.astype(jnp.float32)
    scale_attn = rms_scale(residual)
    normed1 = widen((residual * scale_attn * gain_attn).astype(jnp.bfloat16))
    projected = jnp.dot(normed1, qkv_full, preferred_element_type=jnp.float32).reshape(
        seq_count, length, groups, repeat_factor + 2, HEAD_SIZE
    )
    cosine_table, sine_table = rotary_tables(segment_ids)
    cos_query = cosine_table[:, :, None, None, :]
    sin_query = sine_table[:, :, None, None, :]
    cos_key = cosine_table[:, :, None, :]
    sin_key = sine_table[:, :, None, :]
    queries = rotate(projected[:, :, :, :repeat_factor], cos_query, sin_query).astype(jnp.bfloat16)
    key_heads = rotate(projected[:, :, :, repeat_factor], cos_key, sin_key).astype(jnp.bfloat16)
    values = projected[:, :, :, repeat_factor + 1].astype(jnp.bfloat16)
    scores = score_block(queries, key_heads, segment_ids)
    highest = jnp.max(scores, axis=-1, keepdims=True)
    log_total = highest + jnp.log(jnp.sum(jnp.exp(scores - highest), axis=-1, keepdims=True))
    probability = jnp.exp(scores - log_total).astype(jnp.bfloat16)
    attended = jnp.einsum(
        "sgrqk,skgd->sqgrd", probability, values, preferred_element_type=jnp.float32
    ).astype(jnp.bfloat16)
    attn_flat = attended.reshape(seq_count * length, groups * repeat_factor * HEAD_SIZE)
    attn_delta = lax.psum_scatter(
        jnp.dot(attn_flat, out_cols, preferred_element_type=jnp.float32).astype(jnp.bfloat16),
        "tensor",
        scatter_dimension=0,
        tiled=True,
    ).astype(jnp.float32)
    hidden1 = residual + attn_delta
    scale_mlp = rms_scale(hidden1)
    normed2 = widen((hidden1 * scale_mlp * gain_mlp).astype(jnp.bfloat16))
    gate = jnp.dot(normed2, gate_full, preferred_element_type=jnp.float32)
    up_value = jnp.dot(normed2, up_full, preferred_element_type=jnp.float32)
    sigmoid_gate = jax.nn.sigmoid(gate)
    activated = (gate * sigmoid_gate * up_value).astype(jnp.bfloat16)
    mlp_delta = narrow(jnp.dot(activated, down_cols, preferred_element_type=jnp.float32))
    block_out = (hidden1 + mlp_delta).astype(jnp.bfloat16)
    grad_rows = widen(cotangent)
    down_part = jnp.einsum("tf,td->fd", activated, grad_rows, preferred_element_type=jnp.float32)
    act_grad = jnp.einsum("td,fd->tf", grad_rows, down_cols, preferred_element_type=jnp.float32)
    gate_delta = (act_grad * up_value * sigmoid_gate * (1.0 + gate * (1.0 - sigmoid_gate))).astype(
        jnp.bfloat16
    )
    up_delta = (act_grad * gate * sigmoid_gate).astype(jnp.bfloat16)
    gate_part = jnp.einsum("td,tf->df", normed2, gate_delta, preferred_element_type=jnp.float32)
    up_part = jnp.einsum("td,tf->df", normed2, up_delta, preferred_element_type=jnp.float32)
    normed2_term = jnp.einsum(
        "tf,df->td", gate_delta, gate_full, preferred_element_type=jnp.float32
    ) + jnp.einsum("tf,df->td", up_delta, up_full, preferred_element_type=jnp.float32)
    normed2_grad = narrow(normed2_term)
    mlp_gain_part = jnp.sum(normed2_grad * hidden1 * scale_mlp, axis=0)
    hidden1_grad = cotangent.astype(jnp.float32) + norm_back(
        hidden1, scale_mlp, gain_mlp, normed2_grad
    )
    hidden1_rounded = hidden1_grad.astype(jnp.bfloat16)
    grad_full = lax.all_gather(hidden1_rounded, "tensor", axis=0, tiled=True)
    attended_grad = jnp.einsum(
        "td,hd->th", grad_full, out_cols, preferred_element_type=jnp.float32
    ).astype(jnp.bfloat16)
    out_part = jnp.einsum("th,td->hd", attn_flat, grad_full, preferred_element_type=jnp.float32)
    attended_grad = attended_grad.reshape(seq_count, length, groups, repeat_factor, HEAD_SIZE)
    prob_full = jnp.exp(score_block(queries, key_heads, segment_ids) - log_total)
    prob_grad = jnp.einsum(
        "sqgrd,skgd->sgrqk", attended_grad, values, preferred_element_type=jnp.float32
    )
    inner_sum = jnp.sum(prob_full * prob_grad, axis=-1, keepdims=True)
    score_grad = (prob_full * (prob_grad - inner_sum) * HEAD_SIZE ** (-0.5)).astype(jnp.bfloat16)
    query_grad = jnp.einsum(
        "sgrqk,skgd->sqgrd", score_grad, key_heads, preferred_element_type=jnp.float32
    )
    key_grad = jnp.einsum(
        "sgrqk,sqgrd->skgd", score_grad, queries, preferred_element_type=jnp.float32
    )
    value_grad = jnp.einsum(
        "sgrqk,sqgrd->skgd",
        prob_full.astype(jnp.bfloat16),
        attended_grad,
        preferred_element_type=jnp.float32,
    )
    projected_grad = jnp.concatenate(
        [
            unrotate(query_grad, cos_query, sin_query),
            unrotate(key_grad, cos_key, sin_key)[:, :, :, None],
            value_grad[:, :, :, None],
        ],
        axis=3,
    )
    projected_grad = projected_grad.astype(jnp.bfloat16).reshape(
        seq_count * length, groups * (repeat_factor + 2) * HEAD_SIZE
    )
    qkv_part = jnp.einsum("td,tc->dc", normed1, projected_grad, preferred_element_type=jnp.float32)
    normed1_grad = narrow(
        jnp.einsum("tc,dc->td", projected_grad, qkv_full, preferred_element_type=jnp.float32)
    )
    attn_gain_part = jnp.sum(normed1_grad * residual * scale_attn, axis=0)
    input_grad = (hidden1_grad + norm_back(residual, scale_attn, gain_attn, normed1_grad)).astype(
        jnp.bfloat16
    )
    attn_gain_total, mlp_gain_total = lax.psum((attn_gain_part, mlp_gain_part), "tensor")
    attn_gain_grad, qkv_grad, gate_grad, up_grad, mlp_gain_grad = (
        lax.psum_scatter(
            attn_gain_total.astype(jnp.bfloat16), "dp", scatter_dimension=0, tiled=True
        ).astype(jnp.float32),
        lax.psum_scatter(
            qkv_part.astype(jnp.bfloat16), "dp", scatter_dimension=0, tiled=True
        ).astype(jnp.float32),
        lax.psum_scatter(
            gate_part.astype(jnp.bfloat16), "dp", scatter_dimension=0, tiled=True
        ).astype(jnp.float32),
        lax.psum_scatter(
            up_part.astype(jnp.bfloat16), "dp", scatter_dimension=0, tiled=True
        ).astype(jnp.float32),
        lax.psum_scatter(
            mlp_gain_total.astype(jnp.bfloat16), "dp", scatter_dimension=0, tiled=True
        ).astype(jnp.float32),
    )
    out_grad, down_grad = (
        lax.psum_scatter(
            out_part.astype(jnp.bfloat16), "dp", scatter_dimension=1, tiled=True
        ).astype(jnp.float32),
        lax.psum_scatter(
            down_part.astype(jnp.bfloat16), "dp", scatter_dimension=1, tiled=True
        ).astype(jnp.float32),
    )
    return (
        block_out,
        input_grad,
        attn_gain_grad,
        qkv_grad,
        out_grad,
        mlp_gain_grad,
        gate_grad,
        up_grad,
        down_grad,
    )


GROUP = 4
WINDOW = 256
LANES = 384
TILE = 128


MESH = pl.DeviceIdType.MESH


class Transfer:
    def __init__(self, copy, sends=None, receives=None):
        self.copy, self.sends, self.receives = copy, sends, receives

    def _when(self, condition, action):
        if condition is None:
            action()
        else:
            pl.when(condition)(action)

    def start(self):
        self._when(self.sends, self.copy.start)
        return self

    def wait_recv(self):
        self._when(self.receives, self.copy.wait_recv)

    def wait_send(self):
        self._when(self.sends, self.copy.wait_send)


class Links:
    def __init__(self, n_dp, n_tensor, out_sems, in_sems, local_sems):
        self.n_dp, self.n_tensor = n_dp, n_tensor
        self.out_sems, self.in_sems, self.local_sems = out_sems, in_sems, local_sems
        self.d_at, self.z_at = lax.axis_index("dp"), lax.axis_index("tensor")
        self.used, self.used_local = 0, 0
        self.sent, self.saved = [], []

    def barrier(self):
        barrier = pltpu.get_barrier_semaphore()
        for k in range(1, self.n_dp):
            pl.semaphore_signal(
                barrier,
                inc=1,
                device_id={"dp": self.d_at ^ k, "tensor": self.z_at},
                device_id_type=MESH,
            )
        for s in range(1, self.n_tensor):
            pl.semaphore_signal(
                barrier,
                inc=1,
                device_id={"dp": self.d_at, "tensor": lax.rem(self.z_at + s, self.n_tensor)},
                device_id_type=MESH,
            )
        pl.semaphore_wait(barrier, self.n_dp - 1 + self.n_tensor - 1)

    def plan(self, source, target, bit=0, shift=0, sends=None, receives=None):
        slot = self.used
        self.used += 1
        copy = pltpu.make_async_remote_copy(
            src_ref=source,
            dst_ref=target,
            send_sem=self.out_sems.at[slot],
            recv_sem=self.in_sems.at[slot],
            device_id={
                "dp": self.d_at ^ bit,
                "tensor": lax.rem(self.z_at + self.n_tensor + shift, self.n_tensor),
            },
            device_id_type=MESH,
        )
        transfer = Transfer(copy, sends, receives)
        self.sent.append(transfer)
        return transfer

    def send(self, source, target, bit=0, shift=0):
        return self.plan(source, target, bit, shift).start()

    def move(self, source, target):
        copy = pltpu.make_async_copy(source, target, self.local_sems.at[self.used_local])
        self.used_local += 1
        copy.start()
        return copy

    def save(self, source, target):
        self.saved.append(self.move(source, target))

    def finish(self):
        for transfer in self.sent:
            transfer.wait_send()
        for copy in self.saved:
            copy.wait()


class Spread:
    def __init__(self, links, own_piece, target, columns):
        self.links, self.own_piece, self.target, self.columns = links, own_piece, target, columns
        self.ahead, self.back, self.swaps = [], [], []

    def _slot(self, index):
        n = self.links.n_tensor
        return self.target.at[lax.rem(index + n, n), :, self.columns]

    def issue(self):
        links, n, z = self.links, self.links.n_tensor, self.links.z_at
        own = self._slot(z)
        for s in range(1, n):
            up_from, down_from = z - (s - 1), z + (s - 1)
            up_source = self.own_piece if s == 1 else self._slot(up_from)
            down_source = self.own_piece if s == 1 else self._slot(down_from)
            self.ahead.append(
                links.plan(
                    up_source, self._slot(up_from), shift=1,
                    sends=(z < n - 1) & (up_from >= 0), receives=z >= s,
                )
            )
            self.back.append(
                links.plan(
                    down_source, self._slot(down_from), shift=-1,
                    sends=(z > 0) & (down_from < n), receives=z + s < n,
                )
            )
        self.ahead[0].start()
        self.back[0].start()
        self.swaps.append(links.plan(self.own_piece, own, bit=GROUP).start())

    def step(self, s):
        links, n, z = self.links, self.links.n_tensor, self.links.z_at
        for arrivals, piece, here in (
            (self.ahead, z - s, z >= s),
            (self.back, z + s, z + s < n),
        ):
            arrivals[s - 1].wait_recv()
            if s < n - 1:
                arrivals[s].start()
            slot = self._slot(piece)
            self.swaps.append(
                links.plan(slot, slot, bit=GROUP, sends=here, receives=here).start()
            )

    def wait(self):
        for swap in self.swaps:
            swap.wait_recv()


def kernel_forward(
    n_dp, n_tensor,
    tokens, cot, out_w, gate_w, up_w, down_w, qkv_w, segments, gain_rows, fixed,
    normed1_out, normed2_out, hidden_out, query_out, keyval_out, log_out, att_out,
    cos_out, sin_out, qkv_out, out_out, small_out, cot_out, gate_out, up_out, down_out,
    x_all, n1_all, first, dealt, first_piece, qkv, obuf, gbuf, ubuf, dbuf, piece, outw,
    small, small_all, stream, parts, recv, queries, keyvals,
    att, by_repeat, logs, cosine, sine, low_col, to_core, from_core, to_across, from_across,
    hidden, n2_all, stage, out_sems, in_sems, local_sems,
):
    f32, bf16 = jnp.float32, jnp.bfloat16
    links = Links(n_dp, n_tensor, out_sems, in_sems, local_sems)
    send, move, save = links.send, links.move, links.save
    d_at, z_at = links.d_at, links.z_at
    member = d_at % GROUP
    core = d_at % 2
    upper = d_at // GROUP
    rows, width = tokens.shape
    half = width // 2
    chunk = qkv_w.shape[0]
    contract = (((1,), (1,)), ((), ()))
    columns = pl.ds(pl.multiple_of(upper * half, half), half)

    turned = qkv_w[...].T
    quarter = turned.shape[0] // GROUP
    for i in range(GROUP):
        first[i] = turned[i * quarter : (i + 1) * quarter]
    ids = segments[...]
    seqs, length = ids.shape
    begin = jnp.zeros_like(ids)
    for value in range(3):
        count = jnp.sum((ids == value).astype(jnp.int32), axis=1, keepdims=True)
        begin = begin + jnp.where(ids > value, count, 0)
    begin = begin.astype(f32)
    for i in range(seqs):
        stream[:, i * length : (i + 1) * length] = jnp.broadcast_to(
            begin[i : i + 1] + float(i * length), (stream.shape[0], length)
        )
    window = stream[:, pl.ds(pl.multiple_of(z_at * rows, TILE), rows)]
    here = lax.broadcasted_iota(jnp.int32, window.shape, 1) + z_at * rows
    small[...] = window
    small[0:1] = here.astype(f32)[0:1] - window[0:1]
    small[2:4, :chunk] = gain_rows[...].astype(f32)

    @pl.when(z_at == 0)
    def _():
        keyvals[:, :WINDOW, :] = jnp.zeros_like(keyvals[:, :WINDOW, :])

    links.barrier()

    deals = [send(first.at[member ^ k], dealt.at[member], bit=k) for k in range(1, GROUP)]
    beside = send(tokens, x_all.at[2], bit=1)
    smalls = [send(small, small_all.at[d_at], bit=k) for k in range(1, n_dp)]
    rests = []

    def rows_of(ref, at):
        size = ref.shape[0] // GROUP
        return ref.at[pl.ds(pl.multiple_of(at * size, 16), size), :]

    def columns_of(ref, at):
        size = ref.shape[1] // GROUP
        return ref.at[:, pl.ds(pl.multiple_of(at * size, TILE), size)]

    pairs = [(out_w, obuf, rows_of), (gate_w, gbuf, columns_of), (up_w, ubuf, columns_of)]
    pairs.append((down_w, dbuf, rows_of))
    for ref, buffer, take in pairs:
        for k in range(1, GROUP):
            rests.append(send(take(ref, member ^ k), buffer.at[member], bit=k))
    own = [move(tokens, x_all.at[0])]
    for ref, buffer, take in pairs:
        own.append(move(take(ref, member), buffer.at[member]))
    cot_stage = move(cot, stage)
    small_all[d_at] = small[...]
    dealt[member] = first[member]

    entries = lax.broadcasted_iota(jnp.int32, (WINDOW, LANES), 0).astype(f32)
    angles = entries * fixed[0:1]

    def split(table):
        pieces = []
        for _ in range(3):
            pieces.append(table.astype(bf16))
            table = table - pieces[-1].astype(f32)
        return pieces

    cos_parts, sin_parts = split(jnp.cos(angles)), split(jnp.sin(angles))
    second = fixed[1:2]
    own_turns = jnp.where(core == 0, jnp.ones_like(second), fixed[2:3])

    for copy in deals:
        copy.wait_recv()
    for i in range(GROUP):
        first_piece[:, i * chunk : (i + 1) * chunk] = dealt[i]
    spread_first = Spread(links, first_piece, qkv, columns)
    spread_first.issue()
    save(first_piece, qkv.at[z_at, :, columns])
    own_qkv = links.saved.pop()
    for copy in own:
        copy.wait()
    cot_stage.wait()
    save(stage, cot_out.at[0])
    spread_first.step(1)
    for copy in smalls:
        copy.wait_recv()
    spread_first.step(2)
    gains = []
    for row in (2, 3):
        gains.append(
            jnp.concatenate([small_all[i, row : row + 1, :chunk] for i in range(n_dp)], axis=1)
        )
    for copy in rests:
        copy.wait_recv()
    across = send(tokens, x_all.at[1], bit=2)
    sizes = [obuf.shape[1], gbuf.shape[2], ubuf.shape[2], dbuf.shape[1]]
    starts = [sum(sizes[:i]) for i in range(len(sizes))]
    spreads = []
    for index, (target, buffer) in enumerate(
        ((outw, obuf), (gate_out, gbuf), (up_out, ubuf), (down_out, dbuf))
    ):
        at = slice(starts[index], starts[index] + sizes[index])
        for i in range(GROUP):
            value = buffer[i]
            piece[at, i * chunk : (i + 1) * chunk] = (
                value.T if value.shape[0] == chunk and sizes[index] != chunk else value
            )
        own_piece = piece.at[pl.ds(starts[index], sizes[index])]
        spreads.append(Spread(links, own_piece, target, columns))
    out_spread, gate_spread, up_spread, down_spread = spreads
    saves = [move(s.own_piece, s.target.at[z_at, :, columns]) for s in spreads]
    out_spread.issue()
    spread_first.step(3)
    gate_spread.issue()
    beside.wait_recv()
    own_qkv.wait()
    spread_first.wait()

    def project_block(m, k):
        features = x_all[m].astype(f32)
        scale = lax.rsqrt(jnp.mean(features * features, axis=1, keepdims=True) + EPS)
        normal = (features * scale * gains[0]).astype(bf16)
        n1_all[m] = normal
        units = qkv.shape[0] * qkv.shape[1]
        product = lax.dot_general(
            normal, qkv[...].reshape(units, width), contract, preferred_element_type=f32
        )
        info = small_all[d_at ^ k].T
        key = lax.broadcasted_iota(jnp.int32, (rows, WINDOW), 1)
        chosen = (info[:, 0:1].astype(jnp.int32) == key).astype(bf16)

        def pick(table):
            total = jnp.dot(chosen, table[0], preferred_element_type=f32)
            for part in table[1:]:
                total += jnp.dot(chosen, part, preferred_element_type=f32)
            return total

        cos_here, sin_here = pick(cos_parts), pick(sin_parts)
        parts[m] = turn(product, cos_here, sin_here, second, own_turns, 1.0).astype(bf16)
        if m < 2:
            cosine[m] = cos_here
            sine[m] = sin_here
            low_col[m] = info[:, 1:2].astype(jnp.int32) - z_at * rows + WINDOW

    is_first = core == 0
    halos = [
        links.plan(
            keyvals.at[m, pl.ds(rows, WINDOW)], keyvals.at[m, pl.ds(0, WINDOW)], shift=1,
            sends=z_at < n_tensor - 1, receives=z_at > 0,
        )
        for m in range(2)
    ]

    def take_block(m, swap):
        swap.wait_recv()
        mine, other = parts[m], recv[m]
        queries[m] = jnp.where(is_first, mine, other)
        keyvals[m, WINDOW:, :] = jnp.where(is_first, other, mine)
        halos[m].start()

    project_block(2, 1)
    part_swap = send(parts.at[2], recv.at[0], bit=1)
    project_block(0, 0)
    take_block(0, part_swap)
    out_spread.step(1)
    across.wait_recv()
    both = send(x_all.at[1], x_all.at[3], bit=1)
    cot_across = send(cot, cot_out.at[1], bit=2)
    cot_beside = send(cot, cot_out.at[2], bit=1)
    out_spread.step(2)
    project_block(1, 2)
    both.wait_recv()
    project_block(3, 3)
    part_swap = send(parts.at[3], recv.at[1], bit=1)
    out_spread.step(3)
    save(n1_all, normed1_out)
    save(cosine, cos_out)
    save(sine, sin_out)
    take_block(1, part_swap)
    gate_spread.step(1)
    save(queries, query_out)
    heads = queries.shape[2] // HEAD_SIZE
    repeat = QUERY_HEADS // KEY_VALUE_HEADS
    span = TILE + WINDOW

    def attend_tile(m, start):
        key = lax.broadcasted_iota(jnp.int32, (TILE, span), 1)
        query = lax.broadcasted_iota(jnp.int32, (TILE, span), 0)
        lowest = low_col[m, pl.ds(start, TILE), :] - start
        allowed = (key >= lowest) & (key <= query + WINDOW)
        for head in range(heads):
            group, r = head // repeat, head % repeat
            base = group * 2 * HEAD_SIZE
            q = queries[m, pl.ds(start, TILE), head * HEAD_SIZE : (head + 1) * HEAD_SIZE]
            k = keyvals[m, pl.ds(start, span), base : base + HEAD_SIZE]
            v = keyvals[m, pl.ds(start, span), base + HEAD_SIZE : base + 2 * HEAD_SIZE]
            s = lax.dot_general(q, k, contract, preferred_element_type=f32) * HEAD_SIZE ** (-0.5)
            s = jnp.where(allowed, s, NEG_FILL)
            highest = jnp.max(s, axis=1, keepdims=True)
            e = jnp.exp(s - highest)
            whole = jnp.sum(e, axis=1, keepdims=True)
            p = (e * (1.0 / whole)).astype(bf16)
            o = jnp.dot(p, v, preferred_element_type=f32).astype(bf16)
            logs[m, pl.ds(start, TILE), head : head + 1] = highest + jnp.log(whole)
            by_repeat[r, m, pl.ds(start, TILE), group * HEAD_SIZE : (group + 1) * HEAD_SIZE] = o

    tiles = rows // TILE
    free = -(-WINDOW // TILE)
    for tile in range(free, tiles):
        attend_tile(1, tile * TILE)
        attend_tile(0, tile * TILE)
    gate_spread.step(2)
    halos[0].wait_recv()
    halos[1].wait_recv()
    up_spread.issue()
    for tile in range(free):
        attend_tile(1, tile * TILE)
    att_swap1 = send(by_repeat.at[1 - core, 1], att.at[3], bit=1)
    gate_spread.step(3)
    attend_tile(0, 0)
    up_spread.step(1)
    for tile in range(1, free):
        attend_tile(0, tile * TILE)
    att_swap0 = send(by_repeat.at[1 - core, 0], att.at[2], bit=1)
    save(keyvals, keyval_out)
    save(logs, log_out)
    att[0] = by_repeat[core, 0]
    att[1] = by_repeat[core, 1]
    down_spread.issue()
    cot_across.wait_recv()
    cot_both = send(cot_out.at[1], cot_out.at[3], bit=1)

    saves[0].wait()
    out_spread.wait()

    def project_out(b):
        units = outw.shape[0] * outw.shape[1]
        return jnp.dot(att[b], outw[...].reshape(units, width), preferred_element_type=f32)

    att_swap1.wait_recv()
    to_core[1] = project_out(3).astype(bf16)
    core_send1 = send(to_core.at[1], from_core.at[1], bit=1)
    hidden[...] = project_out(1)
    att_swap0.wait_recv()
    to_core[0] = project_out(2).astype(bf16)
    core_send0 = send(to_core.at[0], from_core.at[0], bit=1)
    core_send1.wait_recv()
    across_sends = []
    for i in range(tiles):
        at = pl.ds(i * TILE, TILE)
        to_across[at] = (hidden[at, :] + from_core[1, at, :].astype(f32)).astype(bf16)
        across_sends.append(send(to_across.at[at], from_across.at[at], bit=2))
    hidden[...] = project_out(0) + x_all[0].astype(f32)
    core_send0.wait_recv()
    hidden[...] += from_core[0].astype(f32)
    save(att, att_out)
    up_spread.step(2)
    steps = [(up_spread, 3), (down_spread, 1), (down_spread, 2), (down_spread, 3)]
    last = []
    for i in range(tiles):
        at = pl.ds(i * TILE, TILE)
        across_sends[i].wait_recv()
        value = hidden[at, :] + from_across[at, :].astype(f32)
        hidden[at, :] = value
        scale = lax.rsqrt(jnp.mean(value * value, axis=1, keepdims=True) + EPS)
        n2_all[0, at, :] = (value * scale * gains[1]).astype(bf16)
        last.append(send(n2_all.at[0, at], n2_all.at[1, at], bit=2))
        last.append(send(n2_all.at[0, at], n2_all.at[2, at], bit=1))
        if i in (1, 2):
            spread, s = steps.pop(0)
            spread.step(s)
    save(hidden, hidden_out)
    save(qkv, qkv_out)
    save(outw, out_out)
    save(small_all, small_out)
    ends = []
    for i in range(tiles):
        at = pl.ds(i * TILE, TILE)
        last[2 * i].wait_recv()
        ends.append(send(n2_all.at[1, at], n2_all.at[3, at], bit=1))
        if i < 2:
            spread, s = steps.pop(0)
            spread.step(s)
    for copy in ends + last[1::2]:
        copy.wait_recv()
    save(n2_all, normed2_out)
    for copy in saves[1:]:
        copy.wait()
    for spread in (gate_spread, up_spread, down_spread):
        spread.wait()
    for copy in (cot_beside, cot_both):
        copy.wait_recv()
    links.finish()


def forward(
    n_dp, n_tensor, tokens, cot, segments, gain_rows, qkv_w, out_w, gate_w, up_w, down_w
):
    rows, width = tokens.shape
    f32, bf16 = jnp.float32, jnp.bfloat16
    vmem = pl.BlockSpec(memory_space=pltpu.VMEM)
    hbm = pl.BlockSpec(memory_space=pl.ANY)
    chunk = qkv_w.shape[0]
    quarter = qkv_w.shape[1] // GROUP
    sizes = [
        out_w.shape[0] // GROUP, gate_w.shape[1] // GROUP, up_w.shape[1] // GROUP,
        down_w.shape[0] // GROUP,
    ]
    units = quarter * n_tensor
    heads = units // HEAD_SIZE
    lane = np.arange(LANES)
    within = lane % HEAD_SIZE
    fixed = np.zeros((8, LANES), np.float32)
    fixed[0] = np.power(ROPE_BASE, -(2.0 * (within % (HEAD_SIZE // 2))) / HEAD_SIZE)
    fixed[1] = within >= HEAD_SIZE // 2
    fixed[2] = lane % (2 * HEAD_SIZE) < HEAD_SIZE
    fixed[3] = 1.0

    def shape(dims, dtype=bf16):
        return jax.ShapeDtypeStruct(tuple(dims), dtype)

    full = (GROUP, rows, width)
    qkv_shape = (n_tensor, quarter, width)
    out_shape = (n_tensor, sizes[0], width)
    att_shape = (GROUP, rows, units // 2)
    small_shape = (n_dp, 8, rows)
    table = (2, rows, LANES)
    outs = [
        shape(full),
        shape(full),
        shape((rows, width), f32),
        shape((2, rows, units)),
        shape((2, rows + WINDOW, units)),
        shape((2, rows, heads), f32),
        shape(att_shape),
        shape(table, f32),
        shape(table, f32),
        shape(qkv_shape),
        shape(out_shape),
        shape(small_shape, f32),
        shape(full),
    ] + [shape((n_tensor, size, width)) for size in sizes[1:]]
    scratch = [
        pltpu.VMEM(full, bf16),
        pltpu.VMEM(full, bf16),
        pltpu.VMEM((GROUP, quarter, chunk), bf16),
        pltpu.VMEM((GROUP, quarter, chunk), bf16),
        pltpu.VMEM((quarter, width // 2), bf16),
        pltpu.VMEM(qkv_shape, bf16),
        pltpu.VMEM((GROUP, sizes[0], chunk), bf16),
        pltpu.VMEM((GROUP, chunk, sizes[1]), bf16),
        pltpu.VMEM((GROUP, chunk, sizes[2]), bf16),
        pltpu.VMEM((GROUP, sizes[3], chunk), bf16),
        pltpu.VMEM((sum(sizes), width // 2), bf16),
        pltpu.VMEM(out_shape, bf16),
        pltpu.VMEM((8, rows), f32),
        pltpu.VMEM(small_shape, f32),
        pltpu.VMEM((8, n_tensor * rows), f32),
        pltpu.VMEM((GROUP, rows, units), bf16),
        pltpu.VMEM((2, rows, units), bf16),
        pltpu.VMEM((2, rows, units), bf16),
        pltpu.VMEM((2, rows + WINDOW, units), bf16),
        pltpu.VMEM(att_shape, bf16),
        pltpu.VMEM((2, 2, rows, units // 2), bf16),
        pltpu.VMEM((2, rows, heads), f32),
        pltpu.VMEM(table, f32),
        pltpu.VMEM(table, f32),
        pltpu.VMEM((2, rows, 1), jnp.int32),
        pltpu.VMEM((2, rows, width), bf16),
        pltpu.VMEM((2, rows, width), bf16),
        pltpu.VMEM((rows, width), bf16),
        pltpu.VMEM((rows, width), bf16),
        pltpu.VMEM((rows, width), f32),
        pltpu.VMEM(full, bf16),
        pltpu.VMEM((rows, width), bf16),
        pltpu.SemaphoreType.DMA((128,)),
        pltpu.SemaphoreType.DMA((128,)),
        pltpu.SemaphoreType.DMA((40,)),
    ]
    results = pl.pallas_call(
        functools.partial(kernel_forward, n_dp, n_tensor),
        in_specs=[hbm] * 6 + [vmem] * 4,
        out_specs=[hbm] * len(outs),
        out_shape=outs,
        scratch_shapes=scratch,
        compiler_params=pltpu.CompilerParams(
            collective_id=0, has_side_effects=True, vmem_limit_bytes=60 * 1024 * 1024
        ),
        name="forward",
    )(
        tokens, cot, out_w, gate_w, up_w, down_w, qkv_w, segments, gain_rows, jnp.asarray(fixed)
    )
    return results, jnp.asarray(fixed)


def turn(value, cosine, sine, second, turns, sign):
    width = value.shape[1]
    half = HEAD_SIZE // 2
    c = turns * cosine + (1.0 - turns)
    u = (sign * turns * second) * sine
    d = (sign * turns * (second - 1.0)) * sine
    pieces = []
    up = pltpu.roll(value, half, 1)
    down = pltpu.roll(value, width - half, 1)
    for i in range(width // LANES):
        at = slice(i * LANES, (i + 1) * LANES)
        pieces.append(value[:, at] * c + up[:, at] * u + down[:, at] * d)
    return jnp.concatenate(pieces, axis=1)


def allowed_tile(lowest, start):
    low = lowest[0, pl.ds(start, TILE), :]
    key = lax.broadcasted_iota(jnp.int32, (TILE, TILE + WINDOW), 1)
    query = lax.broadcasted_iota(jnp.int32, (TILE, TILE + WINDOW), 0)
    return (key >= low) & (key <= query + WINDOW)


def kernel_attend_back(
    core_ref, queries_ref, keyvals_ref, lowest, log_total, grads, grads_other, cosine, sine, lanes,
    query_out, key_out, halo_out, totals, query_total,
):
    core = core_ref[0]
    queries, keyvals = queries_ref.at[0], keyvals_ref.at[0]
    totals[...] = jnp.zeros_like(totals)
    heads = queries.shape[1] // HEAD_SIZE
    repeat = QUERY_HEADS // KEY_VALUE_HEADS
    scale = HEAD_SIZE ** (-0.5)

    def body(tile, carry):
        start = pl.multiple_of(tile * TILE, TILE)
        allowed = allowed_tile(lowest, start)
        mine = grads[0, pl.ds(start, TILE), :]
        other = grads_other[0, pl.ds(start, TILE), :]
        first = core == 0
        by_repeat = (jnp.where(first, mine, other), jnp.where(first, other, mine))
        for group in range(heads // repeat):
            base = group * 2 * HEAD_SIZE
            k = keyvals[pl.ds(start, TILE + WINDOW), base : base + HEAD_SIZE]
            v = keyvals[pl.ds(start, TILE + WINDOW), base + HEAD_SIZE : base + 2 * HEAD_SIZE]
            key_sum = None
            for r in range(repeat):
                head = group * repeat + r
                q = queries[pl.ds(start, TILE), head * HEAD_SIZE : (head + 1) * HEAD_SIZE]
                g = by_repeat[r][:, group * HEAD_SIZE : (group + 1) * HEAD_SIZE]
                s = lax.dot_general(
                    q, k, (((1,), (1,)), ((), ())), preferred_element_type=jnp.float32
                ) * scale
                total = log_total[0, pl.ds(start, TILE), head : head + 1]
                p = jnp.exp(jnp.where(allowed, s, NEG_FILL) - total)
                pg = lax.dot_general(
                    g, v, (((1,), (1,)), ((), ())), preferred_element_type=jnp.float32
                )
                inner = jnp.sum(p * pg, axis=1, keepdims=True)
                sg = (p * (pg - inner) * scale).astype(jnp.bfloat16)
                query_total[:, head * HEAD_SIZE : (head + 1) * HEAD_SIZE] = jnp.dot(
                    sg, k, preferred_element_type=jnp.float32
                )
                dk = lax.dot_general(
                    sg, q, (((0,), (0,)), ((), ())), preferred_element_type=jnp.float32
                )
                dv = lax.dot_general(
                    p.astype(jnp.bfloat16), g, (((0,), (0,)), ((), ())),
                    preferred_element_type=jnp.float32,
                )
                both = jnp.concatenate([dk, dv], axis=1)
                key_sum = both if key_sum is None else key_sum + both
            totals[pl.ds(start, TILE + WINDOW), base : base + 2 * HEAD_SIZE] += key_sum
        rows = pl.ds(start, TILE)
        query_out[0, rows, :] = turn(
            query_total[...], cosine[0, rows, :], sine[0, rows, :], lanes[0:1], lanes[2:3], -1.0
        ).astype(jnp.bfloat16)
        return carry

    lax.fori_loop(0, queries.shape[0] // TILE, body, 0)
    key_out[0] = totals[WINDOW:]
    halo_out[0] = totals[:WINDOW].astype(jnp.bfloat16)


def attend_back(
    core, queries, keyvals, lowest, log_total, grads, grads_other, cosine, sine, lanes
):
    pairs, rows, units = queries.shape
    heads = units // HEAD_SIZE
    spec = pl.BlockSpec((1, rows, units), lambda i: (i, 0, 0))
    half_spec = pl.BlockSpec((1, rows, units // 2), lambda i: (i, 0, 0))
    halo_spec = pl.BlockSpec((1, WINDOW, units), lambda i: (i, 0, 0))
    table_spec = pl.BlockSpec((1, rows, LANES), lambda i: (i, 0, 0))
    return pl.pallas_call(
        kernel_attend_back,
        grid=(pairs,),
        in_specs=[
            pl.BlockSpec(memory_space=pltpu.SMEM),
            spec,
            pl.BlockSpec((1, rows + WINDOW, units), lambda i: (i, 0, 0)),
            pl.BlockSpec((1, rows, 1), lambda i: (i, 0, 0)),
            pl.BlockSpec((1, rows, heads), lambda i: (i, 0, 0)),
            half_spec,
            half_spec,
            table_spec,
            table_spec,
            pl.BlockSpec(lanes.shape, lambda i: (0, 0)),
        ],
        out_specs=[spec, spec, halo_spec],
        out_shape=[
            jax.ShapeDtypeStruct((pairs, rows, units), jnp.bfloat16),
            jax.ShapeDtypeStruct((pairs, rows, units), jnp.float32),
            jax.ShapeDtypeStruct((pairs, WINDOW, units), jnp.bfloat16),
        ],
        scratch_shapes=[
            pltpu.VMEM((rows + WINDOW, units), jnp.float32),
            pltpu.VMEM((TILE, units), jnp.float32),
        ],
        name="attend_back",
    )(core, queries, keyvals, lowest, log_total, grads, grads_other, cosine, sine, lanes)


def kernel_finish_keys(key_sum, halo, cosine, sine, lanes, out):
    rows = key_sum.shape[1]
    full = key_sum[0]
    tail = full[rows - WINDOW :] + halo[0].astype(jnp.float32)
    full = jnp.concatenate([full[: rows - WINDOW], tail], axis=0)
    out[0] = turn(full, cosine[0], sine[0], lanes[0:1], lanes[1:2], -1.0).astype(jnp.bfloat16)


def finish_keys(key_sum, halo, cosine, sine, lanes):
    pairs, rows, units = key_sum.shape
    spec = pl.BlockSpec((1, rows, units), lambda i: (i, 0, 0))
    table_spec = pl.BlockSpec((1, rows, LANES), lambda i: (i, 0, 0))
    return pl.pallas_call(
        kernel_finish_keys,
        grid=(pairs,),
        in_specs=[
            spec,
            pl.BlockSpec((1, WINDOW, units), lambda i: (i, 0, 0)),
            table_spec,
            table_spec,
            pl.BlockSpec(lanes.shape, lambda i: (0, 0)),
        ],
        out_specs=spec,
        out_shape=jax.ShapeDtypeStruct((pairs, rows, units), jnp.bfloat16),
        name="finish_keys",
    )(key_sum, halo, cosine, sine, lanes)


def fast_local(
    n_dp,
    n_tensor,
    block_in,
    cotangent,
    segment_ids,
    attn_gain,
    qkv_weight,
    out_weight,
    mlp_gain,
    gate_weight,
    up_weight,
    down_weight,
):
    bf16, f32 = jnp.bfloat16, jnp.float32
    d_at = lax.axis_index("dp")
    z_at = lax.axis_index("tensor")
    core = d_at % 2
    member = d_at % GROUP
    upper = d_at // GROUP
    rows, width = block_in.shape
    seqs, length = segment_ids.shape
    half = width // 2

    def swap(value, bit):
        return lax.ppermute(value, "dp", [(i, i ^ bit) for i in range(n_dp)])

    def gather_pair(value):
        return jnp.stack([value, swap(value, 2)])

    def gather(value):
        pair = gather_pair(value)
        return jnp.concatenate([pair, swap(pair, 1)], axis=0)

    def scatter(partial_value):
        blocks = partial_value.reshape(GROUP, rows, partial_value.shape[-1])
        got = swap(blocks[2:].astype(bf16), 1)
        pair = blocks[:2].astype(f32) + got.astype(f32)
        return pair[0] + swap(pair[1].astype(bf16), 2).astype(f32)

    part = attn_gain.shape[0]
    (
        normed1, normed2, hidden1, queries, keyvals, log_total, attended, cosine, sine, qkv_full,
        out_full, smalls, grad_rows, gate_full, up_full, down_full,
    ), fixed = forward(
        n_dp, n_tensor, block_in, cotangent, segment_ids, jnp.stack([attn_gain, mlp_gain]),
        qkv_weight, out_weight, gate_weight, up_weight, down_weight,
    )
    lanes = fixed[1:]
    residual = block_in
    qkv_full, out_full, gate_full, up_full, down_full = [
        w.reshape(-1, width) for w in (qkv_full, out_full, gate_full, up_full, down_full)
    ]
    gain_attn = smalls[:, 2, :part].reshape(width)
    gain_mlp = smalls[:, 3, :part].reshape(width)
    lowest = jnp.stack(
        [lax.dynamic_index_in_dim(smalls, i, 0, keepdims=False)[1] for i in (d_at, d_at ^ 2)]
    ).astype(jnp.int32)
    tile_at = jnp.arange(rows, dtype=jnp.int32) // TILE * TILE
    lowest = (lowest - z_at * rows + WINDOW - tile_at[None, :])[:, :, None]
    core_arg = core.astype(jnp.int32).reshape(1)
    residual = residual.astype(f32)
    scale_attn = rms_scale(residual)
    scale_mlp = rms_scale(hidden1)
    attn_flat = attended.reshape(GROUP * rows, attended.shape[-1])
    normed2 = normed2.reshape(GROUP * rows, width)
    grad_rows = grad_rows.reshape(GROUP * rows, width)

    def to_units(tokens, weight):
        return jnp.einsum("td,ud->tu", tokens, weight, preferred_element_type=f32)

    def grad_of(left, right):
        return jnp.einsum("tu,td->ud", left, right, preferred_element_type=f32).astype(bf16)

    gate = to_units(normed2, gate_full)
    up_value = to_units(normed2, up_full)
    sigmoid_gate = jax.nn.sigmoid(gate)
    activated = (gate * sigmoid_gate * up_value).astype(bf16)
    act_grad = to_units(grad_rows, down_full)
    gate_delta = (act_grad * up_value * sigmoid_gate * (1.0 + gate * (1.0 - sigmoid_gate))).astype(
        bf16
    )
    up_delta = (act_grad * gate * sigmoid_gate).astype(bf16)
    normed2_term = jnp.dot(gate_delta, gate_full, preferred_element_type=f32) + jnp.dot(
        up_delta, up_full, preferred_element_type=f32
    )
    normed2_grad = scatter(normed2_term.astype(bf16))
    mlp_delta = scatter(jnp.dot(activated, down_full, preferred_element_type=f32).astype(bf16))
    block_out = (hidden1 + mlp_delta).astype(bf16)
    down_part = grad_of(activated, grad_rows)
    gate_part = grad_of(gate_delta, normed2)
    up_part = grad_of(up_delta, normed2)
    hidden1_grad = cotangent.astype(f32) + norm_back(hidden1, scale_mlp, gain_mlp, normed2_grad)
    grad_full = gather(hidden1_grad.astype(bf16)).reshape(GROUP * rows, width)
    attended_grad = to_units(grad_full, out_full).astype(bf16)
    out_part = grad_of(attn_flat, grad_full)
    attended_grad = attended_grad.reshape(GROUP, rows, attended_grad.shape[-1])
    grads_other = swap(attended_grad[2:], 1)
    query_grad, key_sum, halo_grad = attend_back(
        core_arg, queries, keyvals, lowest, log_total, attended_grad[:2], grads_other, cosine, sine, lanes
    )
    halo_back = lax.ppermute(halo_grad, "tensor", [(i + 1, i) for i in range(n_tensor - 1)])
    key_grad = finish_keys(key_sum, halo_back, cosine, sine, lanes)
    kept = jnp.where(core == 0, query_grad, key_grad)
    passed = jnp.where(core == 0, key_grad, query_grad)
    projected_grad = jnp.concatenate([kept, swap(passed, 1)], axis=0)
    projected_grad = projected_grad.reshape(GROUP * rows, projected_grad.shape[-1])
    normed1_flat = normed1.reshape(GROUP * rows, width)
    normed1_grad = scatter(
        jnp.dot(projected_grad, qkv_full, preferred_element_type=f32).astype(bf16)
    )
    qkv_part = grad_of(projected_grad, normed1_flat)
    input_grad = (
        hidden1_grad + norm_back(residual, scale_attn, gain_attn, normed1_grad)
    ).astype(bf16)

    def overlap(weight, grad):
        return jnp.sum(weight.astype(f32) * grad.astype(f32), axis=0)

    def with_row(part_grad, row):
        blocks = part_grad.reshape(n_tensor, -1, width)
        extra = jnp.zeros((n_tensor, 16, width), bf16).at[:, 0].set(row.astype(bf16))
        return jnp.concatenate([blocks, extra], axis=1).reshape(-1, width)

    def collect(part_grad):
        other = lax.dynamic_slice_in_dim(part_grad, (1 - upper) * half, half, axis=1)
        mine = lax.dynamic_slice_in_dim(part_grad, upper * half, half, axis=1)
        summed = mine.astype(f32) + swap(other, GROUP).astype(f32)
        piece = lax.psum_scatter(
            summed.astype(bf16), "tensor", scatter_dimension=0, tiled=True
        )
        units = piece.shape[0]
        columns = piece.reshape(units, GROUP, half // GROUP).transpose(1, 0, 2)
        pieces = [lax.dynamic_index_in_dim(columns, member, 0, keepdims=False)]
        for k in range(1, GROUP):
            sent = lax.dynamic_index_in_dim(columns, member ^ k, 0, keepdims=False)
            pieces.append(swap(sent, k))
        stacked = jnp.stack(pieces)
        return jnp.stack(
            [lax.dynamic_index_in_dim(stacked, member ^ i, 0, keepdims=False) for i in range(GROUP)]
        )

    def flat(blocks):
        return blocks.reshape(-1, blocks.shape[2])

    def row_of(blocks, gain):
        return jnp.sum(blocks[:, -16].astype(f32), axis=0) / gain.astype(f32)

    mlp_row = overlap(gate_full, gate_part) + overlap(up_full, up_part)
    down_grad = flat(collect(down_part)).astype(f32)
    gate_grad = flat(collect(gate_part)).T.astype(f32)
    up_blocks = collect(with_row(up_part, mlp_row))
    up_grad = flat(up_blocks[:, :-16]).T.astype(f32)
    out_grad = flat(collect(out_part)).astype(f32)
    qkv_blocks = collect(with_row(qkv_part, overlap(qkv_full, qkv_part)))
    qkv_grad = flat(qkv_blocks[:, :-16]).T.astype(f32)
    gains = [row_of(qkv_blocks, attn_gain), row_of(up_blocks, mlp_gain)]
    return (
        block_out,
        input_grad,
        gains[0],
        qkv_grad,
        out_grad,
        gains[1],
        gate_grad,
        up_grad,
        down_grad,
    )


def solution(mesh):
    in_specs = (
        P(("dp", "tensor"), None),
        P(("dp", "tensor"), None),
        P("dp", None),
        P("dp"),
        P("dp", "tensor"),
        P("tensor", "dp"),
        P("dp"),
        P("dp", "tensor"),
        P("dp", "tensor"),
        P("tensor", "dp"),
    )
    out_specs = (
        P(("dp", "tensor"), None),
        P(("dp", "tensor"), None),
        P("dp"),
        P("dp", "tensor"),
        P("tensor", "dp"),
        P("dp"),
        P("dp", "tensor"),
        P("dp", "tensor"),
        P("tensor", "dp"),
    )
    n_dp, n_tensor = mesh.shape["dp"], mesh.shape["tensor"]

    def body(*arrays):
        rows = arrays[0].shape[0]
        groups = arrays[4].shape[1] // (4 * HEAD_SIZE)
        if n_dp == 2 * GROUP and groups == 2 and rows >= WINDOW and rows % TILE == 0:
            return fast_local(n_dp, n_tensor, *arrays)
        return local(*arrays)

    return jax.shard_map(body, mesh=mesh, in_specs=in_specs, out_specs=out_specs, check_vma=False)
```

```python
import functools

import jax
import jax.numpy as jnp
import numpy as np
from jax import lax
from jax.experimental import pallas as pl
from jax.experimental.pallas import tpu as pltpu
from jax.sharding import PartitionSpec as P

QUERY_HEADS = 16
KEY_VALUE_HEADS = 8
HEAD_SIZE = 96


EPS = 1e-05
ROPE_BASE = 100000.0
NEG_FILL = -1e30


def doc_positions(segments):
    length = segments.shape[1]
    position_index = jnp.broadcast_to(jnp.arange(length, dtype=jnp.int32)[None, :], segments.shape)
    change = jnp.concatenate(
        [jnp.ones((segments.shape[0], 1), dtype=bool), segments[:, 1:] != segments[:, :-1]], axis=1
    )
    starts = lax.cummax(jnp.where(change, position_index, jnp.zeros_like(position_index)), axis=1)
    return position_index - starts


def rotary_tables(segments):
    half_dim = HEAD_SIZE // 2
    frequency = jnp.power(ROPE_BASE, -(2.0 * jnp.arange(half_dim, dtype=jnp.float32)) / HEAD_SIZE)
    angles = doc_positions(segments).astype(jnp.float32)[..., None] * frequency
    cosine_table = jnp.concatenate([jnp.cos(angles), jnp.cos(angles)], axis=-1)
    sine_table = jnp.concatenate([jnp.sin(angles), jnp.sin(angles)], axis=-1)
    return (cosine_table, sine_table)


def rotate(vector, cosine_table, sine_table):
    half_dim = vector.shape[-1] // 2
    turned = jnp.concatenate([-vector[..., half_dim:], vector[..., :half_dim]], axis=-1)
    return vector * cosine_table + turned * sine_table


def unrotate(vector, cosine_table, sine_table):
    half_dim = vector.shape[-1] // 2
    shifted = vector * sine_table
    returned = jnp.concatenate([shifted[..., half_dim:], -shifted[..., :half_dim]], axis=-1)
    return vector * cosine_table + returned


def allowed_pairs(segments):
    length = segments.shape[1]
    offsets = jnp.arange(length)
    causal = offsets[None, :] <= offsets[:, None]
    same_doc = segments[:, :, None] == segments[:, None, :]
    return (causal[None] & same_doc)[:, None, None]


def score_block(queries, key_heads, segments):
    scores = jnp.einsum(
        "sqgrd,skgd->sgrqk", queries, key_heads, preferred_element_type=jnp.float32
    ) * HEAD_SIZE ** (-0.5)
    return jnp.where(allowed_pairs(segments), scores, NEG_FILL)


def rms_scale(features):
    return lax.rsqrt(jnp.mean(features * features, axis=-1, keepdims=True) + EPS)


def norm_back(features, inverse, gain_vector, upstream):
    scaled = gain_vector * upstream
    return inverse * scaled - features * (inverse * inverse * inverse) * jnp.mean(
        scaled * features, axis=-1, keepdims=True
    )


def widen(shard_rows):
    return lax.all_gather(shard_rows, "tensor", axis=0, tiled=True)


def narrow(partial_value):
    return lax.psum_scatter(
        partial_value.astype(jnp.bfloat16), "tensor", scatter_dimension=0, tiled=True
    ).astype(jnp.float32)


def local(
    block_in,
    cotangent,
    segment_ids,
    attn_gain,
    qkv_weight,
    out_weight,
    mlp_gain,
    gate_weight,
    up_weight,
    down_weight,
):
    qkv_full, gate_full, up_full, gain_attn_raw, gain_mlp_raw = (
        lax.all_gather(qkv_weight, "dp", axis=0, tiled=True),
        lax.all_gather(gate_weight, "dp", axis=0, tiled=True),
        lax.all_gather(up_weight, "dp", axis=0, tiled=True),
        lax.all_gather(attn_gain, "dp", axis=0, tiled=True),
        lax.all_gather(mlp_gain, "dp", axis=0, tiled=True),
    )
    out_cols, down_cols = (
        lax.all_gather(out_weight, "dp", axis=1, tiled=True),
        lax.all_gather(down_weight, "dp", axis=1, tiled=True),
    )
    seq_count, length = segment_ids.shape
    repeat_factor = QUERY_HEADS // KEY_VALUE_HEADS
    groups = qkv_full.shape[1] // ((repeat_factor + 2) * HEAD_SIZE)
    gain_attn = gain_attn_raw.astype(jnp.float32)
    gain_mlp = gain_mlp_raw.astype(jnp.float32)
    residual = block_in.astype(jnp.float32)
    scale_attn = rms_scale(residual)
    normed1 = widen((residual * scale_attn * gain_attn).astype(jnp.bfloat16))
    projected = jnp.dot(normed1, qkv_full, preferred_element_type=jnp.float32).reshape(
        seq_count, length, groups, repeat_factor + 2, HEAD_SIZE
    )
    cosine_table, sine_table = rotary_tables(segment_ids)
    cos_query = cosine_table[:, :, None, None, :]
    sin_query = sine_table[:, :, None, None, :]
    cos_key = cosine_table[:, :, None, :]
    sin_key = sine_table[:, :, None, :]
    queries = rotate(projected[:, :, :, :repeat_factor], cos_query, sin_query).astype(jnp.bfloat16)
    key_heads = rotate(projected[:, :, :, repeat_factor], cos_key, sin_key).astype(jnp.bfloat16)
    values = projected[:, :, :, repeat_factor + 1].astype(jnp.bfloat16)
    scores = score_block(queries, key_heads, segment_ids)
    highest = jnp.max(scores, axis=-1, keepdims=True)
    log_total = highest + jnp.log(jnp.sum(jnp.exp(scores - highest), axis=-1, keepdims=True))
    probability = jnp.exp(scores - log_total).astype(jnp.bfloat16)
    attended = jnp.einsum(
        "sgrqk,skgd->sqgrd", probability, values, preferred_element_type=jnp.float32
    ).astype(jnp.bfloat16)
    attn_flat = attended.reshape(seq_count * length, groups * repeat_factor * HEAD_SIZE)
    attn_delta = lax.psum_scatter(
        jnp.dot(attn_flat, out_cols, preferred_element_type=jnp.float32).astype(jnp.bfloat16),
        "tensor",
        scatter_dimension=0,
        tiled=True,
    ).astype(jnp.float32)
    hidden1 = residual + attn_delta
    scale_mlp = rms_scale(hidden1)
    normed2 = widen((hidden1 * scale_mlp * gain_mlp).astype(jnp.bfloat16))
    gate = jnp.dot(normed2, gate_full, preferred_element_type=jnp.float32)
    up_value = jnp.dot(normed2, up_full, preferred_element_type=jnp.float32)
    sigmoid_gate = jax.nn.sigmoid(gate)
    activated = (gate * sigmoid_gate * up_value).astype(jnp.bfloat16)
    mlp_delta = narrow(jnp.dot(activated, down_cols, preferred_element_type=jnp.float32))
    block_out = (hidden1 + mlp_delta).astype(jnp.bfloat16)
    grad_rows = widen(cotangent)
    down_part = jnp.einsum("tf,td->fd", activated, grad_rows, preferred_element_type=jnp.float32)
    act_grad = jnp.einsum("td,fd->tf", grad_rows, down_cols, preferred_element_type=jnp.float32)
    gate_delta = (act_grad * up_value * sigmoid_gate * (1.0 + gate * (1.0 - sigmoid_gate))).astype(
        jnp.bfloat16
    )
    up_delta = (act_grad * gate * sigmoid_gate).astype(jnp.bfloat16)
    gate_part = jnp.einsum("td,tf->df", normed2, gate_delta, preferred_element_type=jnp.float32)
    up_part = jnp.einsum("td,tf->df", normed2, up_delta, preferred_element_type=jnp.float32)
    normed2_term = jnp.einsum(
        "tf,df->td", gate_delta, gate_full, preferred_element_type=jnp.float32
    ) + jnp.einsum("tf,df->td", up_delta, up_full, preferred_element_type=jnp.float32)
    normed2_grad = narrow(normed2_term)
    mlp_gain_part = jnp.sum(normed2_grad * hidden1 * scale_mlp, axis=0)
    hidden1_grad = cotangent.astype(jnp.float32) + norm_back(
        hidden1, scale_mlp, gain_mlp, normed2_grad
    )
    hidden1_rounded = hidden1_grad.astype(jnp.bfloat16)
    grad_full = lax.all_gather(hidden1_rounded, "tensor", axis=0, tiled=True)
    attended_grad = jnp.einsum(
        "td,hd->th", grad_full, out_cols, preferred_element_type=jnp.float32
    ).astype(jnp.bfloat16)
    out_part = jnp.einsum("th,td->hd", attn_flat, grad_full, preferred_element_type=jnp.float32)
    attended_grad = attended_grad.reshape(seq_count, length, groups, repeat_factor, HEAD_SIZE)
    prob_full = jnp.exp(score_block(queries, key_heads, segment_ids) - log_total)
    prob_grad = jnp.einsum(
        "sqgrd,skgd->sgrqk", attended_grad, values, preferred_element_type=jnp.float32
    )
    inner_sum = jnp.sum(prob_full * prob_grad, axis=-1, keepdims=True)
    score_grad = (prob_full * (prob_grad - inner_sum) * HEAD_SIZE ** (-0.5)).astype(jnp.bfloat16)
    query_grad = jnp.einsum(
        "sgrqk,skgd->sqgrd", score_grad, key_heads, preferred_element_type=jnp.float32
    )
    key_grad = jnp.einsum(
        "sgrqk,sqgrd->skgd", score_grad, queries, preferred_element_type=jnp.float32
    )
    value_grad = jnp.einsum(
        "sgrqk,sqgrd->skgd",
        prob_full.astype(jnp.bfloat16),
        attended_grad,
        preferred_element_type=jnp.float32,
    )
    projected_grad = jnp.concatenate(
        [
            unrotate(query_grad, cos_query, sin_query),
            unrotate(key_grad, cos_key, sin_key)[:, :, :, None],
            value_grad[:, :, :, None],
        ],
        axis=3,
    )
    projected_grad = projected_grad.astype(jnp.bfloat16).reshape(
        seq_count * length, groups * (repeat_factor + 2) * HEAD_SIZE
    )
    qkv_part = jnp.einsum("td,tc->dc", normed1, projected_grad, preferred_element_type=jnp.float32)
    normed1_grad = narrow(
        jnp.einsum("tc,dc->td", projected_grad, qkv_full, preferred_element_type=jnp.float32)
    )
    attn_gain_part = jnp.sum(normed1_grad * residual * scale_attn, axis=0)
    input_grad = (hidden1_grad + norm_back(residual, scale_attn, gain_attn, normed1_grad)).astype(
        jnp.bfloat16
    )
    attn_gain_total, mlp_gain_total = lax.psum((attn_gain_part, mlp_gain_part), "tensor")
    attn_gain_grad, qkv_grad, gate_grad, up_grad, mlp_gain_grad = (
        lax.psum_scatter(
            attn_gain_total.astype(jnp.bfloat16), "dp", scatter_dimension=0, tiled=True
        ).astype(jnp.float32),
        lax.psum_scatter(
            qkv_part.astype(jnp.bfloat16), "dp", scatter_dimension=0, tiled=True
        ).astype(jnp.float32),
        lax.psum_scatter(
            gate_part.astype(jnp.bfloat16), "dp", scatter_dimension=0, tiled=True
        ).astype(jnp.float32),
        lax.psum_scatter(
            up_part.astype(jnp.bfloat16), "dp", scatter_dimension=0, tiled=True
        ).astype(jnp.float32),
        lax.psum_scatter(
            mlp_gain_total.astype(jnp.bfloat16), "dp", scatter_dimension=0, tiled=True
        ).astype(jnp.float32),
    )
    out_grad, down_grad = (
        lax.psum_scatter(
            out_part.astype(jnp.bfloat16), "dp", scatter_dimension=1, tiled=True
        ).astype(jnp.float32),
        lax.psum_scatter(
            down_part.astype(jnp.bfloat16), "dp", scatter_dimension=1, tiled=True
        ).astype(jnp.float32),
    )
    return (
        block_out,
        input_grad,
        attn_gain_grad,
        qkv_grad,
        out_grad,
        mlp_gain_grad,
        gate_grad,
        up_grad,
        down_grad,
    )


GROUP = 4
WINDOW = 256
LANES = 384
TILE = 128


MESH = pl.DeviceIdType.MESH


class Transfer:
    def __init__(self, copy, sends=None, receives=None):
        self.copy, self.sends, self.receives = copy, sends, receives

    def _when(self, condition, action):
        if condition is None:
            action()
        else:
            pl.when(condition)(action)

    def start(self):
        self._when(self.sends, self.copy.start)
        return self

    def wait_recv(self):
        self._when(self.receives, self.copy.wait_recv)

    def wait_send(self):
        self._when(self.sends, self.copy.wait_send)


class Links:
    def __init__(self, n_dp, n_tensor, out_sems, in_sems, local_sems):
        self.n_dp, self.n_tensor = n_dp, n_tensor
        self.out_sems, self.in_sems, self.local_sems = out_sems, in_sems, local_sems
        self.d_at, self.z_at = lax.axis_index("dp"), lax.axis_index("tensor")
        self.used, self.used_local = 0, 0
        self.sent, self.saved = [], []

    def barrier(self):
        barrier = pltpu.get_barrier_semaphore()
        for k in range(1, self.n_dp):
            pl.semaphore_signal(
                barrier,
                inc=1,
                device_id={"dp": self.d_at ^ k, "tensor": self.z_at},
                device_id_type=MESH,
            )
        for s in range(1, self.n_tensor):
            pl.semaphore_signal(
                barrier,
                inc=1,
                device_id={"dp": self.d_at, "tensor": lax.rem(self.z_at + s, self.n_tensor)},
                device_id_type=MESH,
            )
        pl.semaphore_wait(barrier, self.n_dp - 1 + self.n_tensor - 1)

    def plan(self, source, target, bit=0, shift=0, sends=None, receives=None):
        slot = self.used
        self.used += 1
        copy = pltpu.make_async_remote_copy(
            src_ref=source,
            dst_ref=target,
            send_sem=self.out_sems.at[slot],
            recv_sem=self.in_sems.at[slot],
            device_id={
                "dp": self.d_at ^ bit,
                "tensor": lax.rem(self.z_at + self.n_tensor + shift, self.n_tensor),
            },
            device_id_type=MESH,
        )
        transfer = Transfer(copy, sends, receives)
        self.sent.append(transfer)
        return transfer

    def send(self, source, target, bit=0, shift=0):
        return self.plan(source, target, bit, shift).start()

    def move(self, source, target):
        copy = pltpu.make_async_copy(source, target, self.local_sems.at[self.used_local])
        self.used_local += 1
        copy.start()
        return copy

    def save(self, source, target):
        self.saved.append(self.move(source, target))

    def finish(self):
        for transfer in self.sent:
            transfer.wait_send()
        for copy in self.saved:
            copy.wait()


class Spread:
    def __init__(self, links, own_piece, target, columns):
        self.links, self.own_piece, self.target, self.columns = links, own_piece, target, columns
        self.ahead, self.back, self.swaps = [], [], []

    def _slot(self, index):
        n = self.links.n_tensor
        return self.target.at[lax.rem(index + n, n), :, self.columns]

    def issue(self):
        links, n, z = self.links, self.links.n_tensor, self.links.z_at
        own = self._slot(z)
        for s in range(1, n):
            up_from, down_from = z - (s - 1), z + (s - 1)
            up_source = self.own_piece if s == 1 else self._slot(up_from)
            down_source = self.own_piece if s == 1 else self._slot(down_from)
            self.ahead.append(
                links.plan(
                    up_source, self._slot(up_from), shift=1,
                    sends=(z < n - 1) & (up_from >= 0), receives=z >= s,
                )
            )
            self.back.append(
                links.plan(
                    down_source, self._slot(down_from), shift=-1,
                    sends=(z > 0) & (down_from < n), receives=z + s < n,
                )
            )
        self.ahead[0].start()
        self.back[0].start()
        self.swaps.append(links.plan(self.own_piece, own, bit=GROUP).start())

    def step(self, s):
        links, n, z = self.links, self.links.n_tensor, self.links.z_at
        for arrivals, piece, here in (
            (self.ahead, z - s, z >= s),
            (self.back, z + s, z + s < n),
        ):
            arrivals[s - 1].wait_recv()
            if s < n - 1:
                arrivals[s].start()
            slot = self._slot(piece)
            self.swaps.append(
                links.plan(slot, slot, bit=GROUP, sends=here, receives=here).start()
            )

    def wait(self):
        for swap in self.swaps:
            swap.wait_recv()


def kernel_forward(
    n_dp, n_tensor,
    tokens, cot, out_w, gate_w, up_w, down_w, qkv_w, segments, gain_rows, fixed,
    normed1_out, normed2_out, hidden_out, query_out, keyval_out, log_out, att_out,
    cos_out, sin_out, qkv_out, out_out, small_out, cot_out, gate_out, up_out, down_out,
    x_all, n1_all, first, dealt, first_piece, qkv, obuf, gbuf, ubuf, dbuf, piece, outw,
    small, small_all, stream, parts, recv, queries, keyvals,
    att, by_repeat, logs, cosine, sine, low_col, to_core, from_core, to_across, from_across,
    hidden, n2_all, stage, out_sems, in_sems, local_sems,
):
    f32, bf16 = jnp.float32, jnp.bfloat16
    links = Links(n_dp, n_tensor, out_sems, in_sems, local_sems)
    send, move, save = links.send, links.move, links.save
    d_at, z_at = links.d_at, links.z_at
    member = d_at % GROUP
    core = d_at % 2
    upper = d_at // GROUP
    rows, width = tokens.shape
    half = width // 2
    chunk = qkv_w.shape[0]
    contract = (((1,), (1,)), ((), ()))
    columns = pl.ds(pl.multiple_of(upper * half, half), half)

    turned = qkv_w[...].T
    quarter = turned.shape[0] // GROUP
    for i in range(GROUP):
        first[i] = turned[i * quarter : (i + 1) * quarter]
    ids = segments[...]
    seqs, length = ids.shape
    begin = jnp.zeros_like(ids)
    for value in range(3):
        count = jnp.sum((ids == value).astype(jnp.int32), axis=1, keepdims=True)
        begin = begin + jnp.where(ids > value, count, 0)
    begin = begin.astype(f32)
    for i in range(seqs):
        stream[:, i * length : (i + 1) * length] = jnp.broadcast_to(
            begin[i : i + 1] + float(i * length), (stream.shape[0], length)
        )
    window = stream[:, pl.ds(pl.multiple_of(z_at * rows, TILE), rows)]
    here = lax.broadcasted_iota(jnp.int32, window.shape, 1) + z_at * rows
    small[...] = window
    small[0:1] = here.astype(f32)[0:1] - window[0:1]
    small[2:4, :chunk] = gain_rows[...].astype(f32)

    @pl.when(z_at == 0)
    def _():
        keyvals[:, :WINDOW, :] = jnp.zeros_like(keyvals[:, :WINDOW, :])

    links.barrier()

    deals = [send(first.at[member ^ k], dealt.at[member], bit=k) for k in range(1, GROUP)]
    beside = send(tokens, x_all.at[2], bit=1)
    smalls = [send(small, small_all.at[d_at], bit=k) for k in range(1, n_dp)]
    rests = []

    def rows_of(ref, at):
        size = ref.shape[0] // GROUP
        return ref.at[pl.ds(pl.multiple_of(at * size, 16), size), :]

    def columns_of(ref, at):
        size = ref.shape[1] // GROUP
        return ref.at[:, pl.ds(pl.multiple_of(at * size, TILE), size)]

    pairs = [(out_w, obuf, rows_of), (gate_w, gbuf, columns_of), (up_w, ubuf, columns_of)]
    pairs.append((down_w, dbuf, rows_of))
    for ref, buffer, take in pairs:
        for k in range(1, GROUP):
            rests.append(send(take(ref, member ^ k), buffer.at[member], bit=k))
    own = [move(tokens, x_all.at[0])]
    for ref, buffer, take in pairs:
        own.append(move(take(ref, member), buffer.at[member]))
    cot_stage = move(cot, stage)
    small_all[d_at] = small[...]
    dealt[member] = first[member]

    entries = lax.broadcasted_iota(jnp.int32, (WINDOW, LANES), 0).astype(f32)
    angles = entries * fixed[0:1]

    def split(table):
        pieces = []
        for _ in range(3):
            pieces.append(table.astype(bf16))
            table = table - pieces[-1].astype(f32)
        return pieces

    cos_parts, sin_parts = split(jnp.cos(angles)), split(jnp.sin(angles))
    second = fixed[1:2]
    own_turns = jnp.where(core == 0, jnp.ones_like(second), fixed[2:3])

    for copy in deals:
        copy.wait_recv()
    for i in range(GROUP):
        first_piece[:, i * chunk : (i + 1) * chunk] = dealt[i]
    spread_first = Spread(links, first_piece, qkv, columns)
    spread_first.issue()
    save(first_piece, qkv.at[z_at, :, columns])
    own_qkv = links.saved.pop()
    for copy in own:
        copy.wait()
    cot_stage.wait()
    save(stage, cot_out.at[0])
    spread_first.step(1)
    for copy in smalls:
        copy.wait_recv()
    spread_first.step(2)
    gains = []
    for row in (2, 3):
        gains.append(
            jnp.concatenate([small_all[i, row : row + 1, :chunk] for i in range(n_dp)], axis=1)
        )
    for copy in rests:
        copy.wait_recv()
    across = send(tokens, x_all.at[1], bit=2)
    sizes = [obuf.shape[1], gbuf.shape[2], ubuf.shape[2], dbuf.shape[1]]
    starts = [sum(sizes[:i]) for i in range(len(sizes))]
    spreads = []
    for index, (target, buffer) in enumerate(
        ((outw, obuf), (gate_out, gbuf), (up_out, ubuf), (down_out, dbuf))
    ):
        at = slice(starts[index], starts[index] + sizes[index])
        for i in range(GROUP):
            value = buffer[i]
            piece[at, i * chunk : (i + 1) * chunk] = (
                value.T if value.shape[0] == chunk and sizes[index] != chunk else value
            )
        own_piece = piece.at[pl.ds(starts[index], sizes[index])]
        spreads.append(Spread(links, own_piece, target, columns))
    out_spread, gate_spread, up_spread, down_spread = spreads
    saves = [move(s.own_piece, s.target.at[z_at, :, columns]) for s in spreads]
    out_spread.issue()
    spread_first.step(3)
    gate_spread.issue()
    beside.wait_recv()
    own_qkv.wait()
    spread_first.wait()

    def project_block(m, k):
        features = x_all[m].astype(f32)
        scale = lax.rsqrt(jnp.mean(features * features, axis=1, keepdims=True) + EPS)
        normal = (features * scale * gains[0]).astype(bf16)
        n1_all[m] = normal
        units = qkv.shape[0] * qkv.shape[1]
        product = lax.dot_general(
            normal, qkv[...].reshape(units, width), contract, preferred_element_type=f32
        )
        info = small_all[d_at ^ k].T
        key = lax.broadcasted_iota(jnp.int32, (rows, WINDOW), 1)
        chosen = (info[:, 0:1].astype(jnp.int32) == key).astype(bf16)

        def pick(table):
            total = jnp.dot(chosen, table[0], preferred_element_type=f32)
            for part in table[1:]:
                total += jnp.dot(chosen, part, preferred_element_type=f32)
            return total

        cos_here, sin_here = pick(cos_parts), pick(sin_parts)
        parts[m] = turn(product, cos_here, sin_here, second, own_turns, 1.0).astype(bf16)
        if m < 2:
            cosine[m] = cos_here
            sine[m] = sin_here
            low_col[m] = info[:, 1:2].astype(jnp.int32) - z_at * rows + WINDOW

    is_first = core == 0
    halos = [
        links.plan(
            keyvals.at[m, pl.ds(rows, WINDOW)], keyvals.at[m, pl.ds(0, WINDOW)], shift=1,
            sends=z_at < n_tensor - 1, receives=z_at > 0,
        )
        for m in range(2)
    ]

    def take_block(m, swap):
        swap.wait_recv()
        mine, other = parts[m], recv[m]
        queries[m] = jnp.where(is_first, mine, other)
        keyvals[m, WINDOW:, :] = jnp.where(is_first, other, mine)
        halos[m].start()

    project_block(2, 1)
    part_swap = send(parts.at[2], recv.at[0], bit=1)
    project_block(0, 0)
    take_block(0, part_swap)
    out_spread.step(1)
    across.wait_recv()
    both = send(x_all.at[1], x_all.at[3], bit=1)
    cot_across = send(cot, cot_out.at[1], bit=2)
    cot_beside = send(cot, cot_out.at[2], bit=1)
    out_spread.step(2)
    project_block(1, 2)
    both.wait_recv()
    project_block(3, 3)
    part_swap = send(parts.at[3], recv.at[1], bit=1)
    out_spread.step(3)
    save(n1_all, normed1_out)
    save(cosine, cos_out)
    save(sine, sin_out)
    take_block(1, part_swap)
    gate_spread.step(1)
    save(queries, query_out)
    heads = queries.shape[2] // HEAD_SIZE
    repeat = QUERY_HEADS // KEY_VALUE_HEADS
    span = TILE + WINDOW

    def attend_tile(m, start):
        key = lax.broadcasted_iota(jnp.int32, (TILE, span), 1)
        query = lax.broadcasted_iota(jnp.int32, (TILE, span), 0)
        lowest = low_col[m, pl.ds(start, TILE), :] - start
        allowed = (key >= lowest) & (key <= query + WINDOW)
        for head in range(heads):
            group, r = head // repeat, head % repeat
            base = group * 2 * HEAD_SIZE
            q = queries[m, pl.ds(start, TILE), head * HEAD_SIZE : (head + 1) * HEAD_SIZE]
            k = keyvals[m, pl.ds(start, span), base : base + HEAD_SIZE]
            v = keyvals[m, pl.ds(start, span), base + HEAD_SIZE : base + 2 * HEAD_SIZE]
            s = lax.dot_general(q, k, contract, preferred_element_type=f32) * HEAD_SIZE ** (-0.5)
            s = jnp.where(allowed, s, NEG_FILL)
            highest = jnp.max(s, axis=1, keepdims=True)
            e = jnp.exp(s - highest)
            whole = jnp.sum(e, axis=1, keepdims=True)
            p = (e * (1.0 / whole)).astype(bf16)
            o = jnp.dot(p, v, preferred_element_type=f32).astype(bf16)
            logs[m, pl.ds(start, TILE), head : head + 1] = highest + jnp.log(whole)
            by_repeat[r, m, pl.ds(start, TILE), group * HEAD_SIZE : (group + 1) * HEAD_SIZE] = o

    tiles = rows // TILE
    free = -(-WINDOW // TILE)
    for tile in range(free, tiles):
        attend_tile(1, tile * TILE)
        attend_tile(0, tile * TILE)
    gate_spread.step(2)
    halos[0].wait_recv()
    halos[1].wait_recv()
    up_spread.issue()
    for tile in range(free):
        attend_tile(1, tile * TILE)
    att_swap1 = send(by_repeat.at[1 - core, 1], att.at[3], bit=1)
    gate_spread.step(3)
    attend_tile(0, 0)
    up_spread.step(1)
    for tile in range(1, free):
        attend_tile(0, tile * TILE)
    att_swap0 = send(by_repeat.at[1 - core, 0], att.at[2], bit=1)
    save(keyvals, keyval_out)
    save(logs, log_out)
    att[0] = by_repeat[core, 0]
    att[1] = by_repeat[core, 1]
    down_spread.issue()
    cot_across.wait_recv()
    cot_both = send(cot_out.at[1], cot_out.at[3], bit=1)

    saves[0].wait()
    out_spread.wait()

    def project_out(b):
        units = outw.shape[0] * outw.shape[1]
        return jnp.dot(att[b], outw[...].reshape(units, width), preferred_element_type=f32)

    att_swap1.wait_recv()
    to_core[1] = project_out(3).astype(bf16)
    core_send1 = send(to_core.at[1], from_core.at[1], bit=1)
    hidden[...] = project_out(1)
    att_swap0.wait_recv()
    to_core[0] = project_out(2).astype(bf16)
    core_send0 = send(to_core.at[0], from_core.at[0], bit=1)
    core_send1.wait_recv()
    across_sends = []
    for i in range(tiles):
        at = pl.ds(i * TILE, TILE)
        to_across[at] = (hidden[at, :] + from_core[1, at, :].astype(f32)).astype(bf16)
        across_sends.append(send(to_across.at[at], from_across.at[at], bit=2))
    hidden[...] = project_out(0) + x_all[0].astype(f32)
    core_send0.wait_recv()
    hidden[...] += from_core[0].astype(f32)
    save(att, att_out)
    up_spread.step(2)
    steps = [(up_spread, 3), (down_spread, 1), (down_spread, 2), (down_spread, 3)]
    last = []
    for i in range(tiles):
        at = pl.ds(i * TILE, TILE)
        across_sends[i].wait_recv()
        value = hidden[at, :] + from_across[at, :].astype(f32)
        hidden[at, :] = value
        scale = lax.rsqrt(jnp.mean(value * value, axis=1, keepdims=True) + EPS)
        n2_all[0, at, :] = (value * scale * gains[1]).astype(bf16)
        last.append(send(n2_all.at[0, at], n2_all.at[1, at], bit=2))
        last.append(send(n2_all.at[0, at], n2_all.at[2, at], bit=1))
        if i in (1, 2):
            spread, s = steps.pop(0)
            spread.step(s)
    save(hidden, hidden_out)
    save(qkv, qkv_out)
    save(outw, out_out)
    save(small_all, small_out)
    ends = []
    for i in range(tiles):
        at = pl.ds(i * TILE, TILE)
        last[2 * i].wait_recv()
        ends.append(send(n2_all.at[1, at], n2_all.at[3, at], bit=1))
        if i < 2:
            spread, s = steps.pop(0)
            spread.step(s)
    for copy in ends + last[1::2]:
        copy.wait_recv()
    save(n2_all, normed2_out)
    for copy in saves[1:]:
        copy.wait()
    for spread in (gate_spread, up_spread, down_spread):
        spread.wait()
    for copy in (cot_beside, cot_both):
        copy.wait_recv()
    links.finish()


def forward(
    n_dp, n_tensor, tokens, cot, segments, gain_rows, qkv_w, out_w, gate_w, up_w, down_w
):
    rows, width = tokens.shape
    f32, bf16 = jnp.float32, jnp.bfloat16
    vmem = pl.BlockSpec(memory_space=pltpu.VMEM)
    hbm = pl.BlockSpec(memory_space=pl.ANY)
    chunk = qkv_w.shape[0]
    quarter = qkv_w.shape[1] // GROUP
    sizes = [
        out_w.shape[0] // GROUP, gate_w.shape[1] // GROUP, up_w.shape[1] // GROUP,
        down_w.shape[0] // GROUP,
    ]
    units = quarter * n_tensor
    heads = units // HEAD_SIZE
    lane = np.arange(LANES)
    within = lane % HEAD_SIZE
    fixed = np.zeros((8, LANES), np.float32)
    fixed[0] = np.power(ROPE_BASE, -(2.0 * (within % (HEAD_SIZE // 2))) / HEAD_SIZE)
    fixed[1] = within >= HEAD_SIZE // 2
    fixed[2] = lane % (2 * HEAD_SIZE) < HEAD_SIZE
    fixed[3] = 1.0

    def shape(dims, dtype=bf16):
        return jax.ShapeDtypeStruct(tuple(dims), dtype)

    full = (GROUP, rows, width)
    qkv_shape = (n_tensor, quarter, width)
    out_shape = (n_tensor, sizes[0], width)
    att_shape = (GROUP, rows, units // 2)
    small_shape = (n_dp, 8, rows)
    table = (2, rows, LANES)
    outs = [
        shape(full),
        shape(full),
        shape((rows, width), f32),
        shape((2, rows, units)),
        shape((2, rows + WINDOW, units)),
        shape((2, rows, heads), f32),
        shape(att_shape),
        shape(table, f32),
        shape(table, f32),
        shape(qkv_shape),
        shape(out_shape),
        shape(small_shape, f32),
        shape(full),
    ] + [shape((n_tensor, size, width)) for size in sizes[1:]]
    scratch = [
        pltpu.VMEM(full, bf16),
        pltpu.VMEM(full, bf16),
        pltpu.VMEM((GROUP, quarter, chunk), bf16),
        pltpu.VMEM((GROUP, quarter, chunk), bf16),
        pltpu.VMEM((quarter, width // 2), bf16),
        pltpu.VMEM(qkv_shape, bf16),
        pltpu.VMEM((GROUP, sizes[0], chunk), bf16),
        pltpu.VMEM((GROUP, chunk, sizes[1]), bf16),
        pltpu.VMEM((GROUP, chunk, sizes[2]), bf16),
        pltpu.VMEM((GROUP, sizes[3], chunk), bf16),
        pltpu.VMEM((sum(sizes), width // 2), bf16),
        pltpu.VMEM(out_shape, bf16),
        pltpu.VMEM((8, rows), f32),
        pltpu.VMEM(small_shape, f32),
        pltpu.VMEM((8, n_tensor * rows), f32),
        pltpu.VMEM((GROUP, rows, units), bf16),
        pltpu.VMEM((2, rows, units), bf16),
        pltpu.VMEM((2, rows, units), bf16),
        pltpu.VMEM((2, rows + WINDOW, units), bf16),
        pltpu.VMEM(att_shape, bf16),
        pltpu.VMEM((2, 2, rows, units // 2), bf16),
        pltpu.VMEM((2, rows, heads), f32),
        pltpu.VMEM(table, f32),
        pltpu.VMEM(table, f32),
        pltpu.VMEM((2, rows, 1), jnp.int32),
        pltpu.VMEM((2, rows, width), bf16),
        pltpu.VMEM((2, rows, width), bf16),
        pltpu.VMEM((rows, width), bf16),
        pltpu.VMEM((rows, width), bf16),
        pltpu.VMEM((rows, width), f32),
        pltpu.VMEM(full, bf16),
        pltpu.VMEM((rows, width), bf16),
        pltpu.SemaphoreType.DMA((128,)),
        pltpu.SemaphoreType.DMA((128,)),
        pltpu.SemaphoreType.DMA((40,)),
    ]
    results = pl.pallas_call(
        functools.partial(kernel_forward, n_dp, n_tensor),
        in_specs=[hbm] * 6 + [vmem] * 4,
        out_specs=[hbm] * len(outs),
        out_shape=outs,
        scratch_shapes=scratch,
        compiler_params=pltpu.CompilerParams(
            collective_id=0, has_side_effects=True, vmem_limit_bytes=60 * 1024 * 1024
        ),
        name="forward",
    )(
        tokens, cot, out_w, gate_w, up_w, down_w, qkv_w, segments, gain_rows, jnp.asarray(fixed)
    )
    return results, jnp.asarray(fixed)


def turn(value, cosine, sine, second, turns, sign):
    width = value.shape[1]
    half = HEAD_SIZE // 2
    c = turns * cosine + (1.0 - turns)
    u = (sign * turns * second) * sine
    d = (sign * turns * (second - 1.0)) * sine
    pieces = []
    up = pltpu.roll(value, half, 1)
    down = pltpu.roll(value, width - half, 1)
    for i in range(width // LANES):
        at = slice(i * LANES, (i + 1) * LANES)
        pieces.append(value[:, at] * c + up[:, at] * u + down[:, at] * d)
    return jnp.concatenate(pieces, axis=1)


class Collect:
    def __init__(self, links, part, swapped, stage, arrived, late, blocks, target, mine, other):
        self.links, self.part, self.swapped, self.stage = links, part, swapped, stage
        self.arrived, self.late, self.blocks, self.target = arrived, late, blocks, target
        self.mine, self.other = mine, other
        self.swaps, self.loads, self.deals = {}, [], []

    def issue(self, order):
        links = self.links
        for p in order:
            self.swaps[p] = links.send(
                self.part.at[p, :, self.other], self.swapped.at[p], bit=GROUP
            )
        if self.stage is not None:
            self.loads = [links.move(self.part.at[:, :, self.mine], self.stage)]

    def load(self, received):
        links = self.links
        self.loads = [
            links.move(self.part.at[:, :, self.mine], self.stage),
            links.move(received, self.swapped),
        ]

    def step(self, p):
        links, n, z = self.links, self.links.n_tensor, self.links.z_at
        f32, bf16 = jnp.float32, jnp.bfloat16
        while self.loads:
            self.loads.pop().wait()
        if p in self.swaps:
            self.swaps[p].wait_recv()
        own = self.stage[p] if self.stage is not None else self.part[p, :, self.mine]
        self.swapped[p] = (own.astype(f32) + self.swapped[p].astype(f32)).astype(bf16)
        if not hasattr(self, "ahead"):
            self.ahead, self.back, self.back_last = [None] * n, [None] * n, [None] * n
        source = self.swapped.at[p]
        self.ahead[p] = links.plan(
            source, self.arrived.at[p], shift=1, sends=z < p, receives=(z > 0) & (z <= p)
        )
        self.back[p] = links.plan(
            source, self.arrived.at[p], shift=-1, sends=z > p + 1,
            receives=(z > p) & (z < n - 1),
        )
        self.back_last[p] = links.plan(
            source, self.late, shift=-1, sends=z == p + 1, receives=(z == p) & (z < n - 1)
        )

        @pl.when((z == 0) & (z < p))
        def _():
            self.ahead[p].copy.start()

        @pl.when((z == n - 1) & (z > p + 1))
        def _():
            self.back[p].copy.start()

        @pl.when((z == n - 1) & (z == p + 1))
        def _():
            self.back_last[p].copy.start()

    def relay(self, p):
        links, n, z = self.links, self.links.n_tensor, self.links.z_at
        f32, bf16 = jnp.float32, jnp.bfloat16
        inner = (z > 0) & (z < n - 1)

        def add():
            self.swapped[p] = (
                self.swapped[p].astype(f32) + self.arrived[p].astype(f32)
            ).astype(bf16)

        @pl.when(inner & (z < p))
        def _():
            self.ahead[p].copy.wait_recv()
            add()
            self.ahead[p].copy.start()

        @pl.when(inner & (z > p))
        def _():
            self.back[p].copy.wait_recv()
            add()

        @pl.when(inner & (z > p + 1))
        def _():
            self.back[p].copy.start()

        @pl.when(inner & (z == p + 1))
        def _():
            self.back_last[p].copy.start()

    def finish(self):
        links, n, z = self.links, self.links.n_tensor, self.links.z_at
        f32, bf16 = jnp.float32, jnp.bfloat16
        member = links.d_at % GROUP
        for p in range(n):

            @pl.when((z == p) & (z > 0))
            def _(p=p):
                self.ahead[p].copy.wait_recv()

            @pl.when((z == p) & (z < n - 1))
            def _(p=p):
                self.back_last[p].copy.wait_recv()

        below = jnp.where(z > 0, self.arrived[z].astype(f32), 0.0)
        above = jnp.where(z < n - 1, self.late[...].astype(f32), 0.0)
        total = (self.swapped[z].astype(f32) + below + above).astype(bf16)
        chunk = self.blocks.shape[2]
        for i in range(GROUP):
            self.blocks[i] = total[:, i * chunk : (i + 1) * chunk]
        for k in range(1, GROUP):
            self.deals.append(
                links.send(self.blocks.at[member ^ k], self.target.at[member], bit=k)
            )
        links.save(self.blocks.at[member], self.target.at[member])

    def wait(self):
        for deal in self.deals:
            deal.wait_recv()


def kernel_backward(
    n_dp, n_tensor,
    grad_own, hidden1, mlp_part, n1_in, query_in, keyval_in, log_in, att_in,
    cos_in, sin_in, qkv_in, out_in, small_in, down_in, gate_in, up_in, down_got, gate_got,
    mlp_row, fixed,
    normed_out, block_out, qkv_out, out_out, gate_out, up_out, down_out,
    g_all, n1_all, qkv, outw, queries, keyvals, logs, att, cosine, sine, gains, low_col,
    att_grad, other_grad, totals, query_total, pass_on, delta, halo_send, halo_recv,
    to_core, from_core, to_across, from_across, mlp_across, hidden, stage, gate_stage,
    down_swap, gate_swap, up_swap, out_swap, qkv_swap,
    down_come, gate_come, up_come, out_come, qkv_come,
    down_late, gate_late, up_late, out_late, qkv_late,
    down_block, gate_block, up_block, out_block, qkv_block,
    out_sems, in_sems, local_sems,
):
    f32, bf16 = jnp.float32, jnp.bfloat16
    links = Links(n_dp, n_tensor, out_sems, in_sems, local_sems)
    send, move, save = links.send, links.move, links.save
    d_at, z_at = links.d_at, links.z_at
    core = d_at % 2
    upper = d_at // GROUP
    rows, width = grad_own.shape
    half = width // 2
    contract = (((1,), (1,)), ((), ()))
    over_rows = (((0,), (0,)), ((), ()))
    mine = pl.ds(pl.multiple_of(upper * half, half), half)
    other = pl.ds(pl.multiple_of((1 - upper) * half, half), half)
    tiles = rows // TILE
    span = TILE + WINDOW
    quarter = qkv.shape[1]
    out_quarter = outw.shape[1]
    extra = qkv_swap.shape[1] - quarter

    loads = [
        move(grad_own, g_all.at[0]), move(out_in, outw), move(query_in, queries),
        move(keyval_in, keyvals), move(log_in, logs), move(cos_in, cosine), move(sin_in, sine),
        move(mlp_part.at[pl.ds(0, 2)], to_core), move(hidden1, hidden), move(att_in, att),
        move(qkv_in, qkv), move(n1_in, n1_all),
    ]
    small = pltpu.make_async_copy(small_in, gains, local_sems.at[links.used_local])
    links.used_local += 1
    small.start()
    links.barrier()
    across = send(grad_own, g_all.at[1], bit=2)
    beside = send(grad_own, g_all.at[2], bit=1)
    mlp_core = send(mlp_part.at[pl.ds(2, 2)], from_core, bit=1)
    order = []
    for i in range((n_tensor + 1) // 2):
        order.extend(dict.fromkeys((n_tensor - 1 - i, i)))

    down = Collect(
        links, down_in, down_swap, stage, down_come, down_late, down_block, down_out, mine, other
    )
    gate = Collect(
        links, gate_in, gate_swap, gate_stage, gate_come, gate_late, gate_block, gate_out, mine, other
    )
    up = Collect(links, up_in, up_swap, stage, up_come, up_late, up_block, up_out, mine, other)
    out_part = g_all.at[:, pl.ds(quarter + extra, out_quarter), :]
    qkv_part = g_all.at[:, pl.ds(0, quarter + extra), :]
    out_collect = Collect(
        links, out_part, out_swap, None, out_come, out_late, out_block, out_out, mine, other
    )
    qkv_collect = Collect(
        links, qkv_part, qkv_swap, None, qkv_come, qkv_late, qkv_block, qkv_out, mine, other
    )
    down.load(down_got)
    gate.load(gate_got)
    small.wait()
    for m, k in ((0, 0), (1, 2)):
        info = gains[d_at ^ k].T
        low_col[m] = info[:, 1:2].astype(jnp.int32) - z_at * rows + WINDOW
    loads[0].wait()
    loads[1].wait()

    def attended_back(b):
        units = outw.shape[0] * outw.shape[1]
        att_grad[b] = lax.dot_general(
            g_all[b], outw[...].reshape(units, width), contract, preferred_element_type=f32
        ).astype(bf16)

    attended_back(0)
    beside.wait_recv()
    attended_back(2)
    grad_swap = send(att_grad.at[2], other_grad.at[0], bit=1)
    for p in order:
        down.step(p)
    up.issue(order)
    for copy in loads[2:]:
        copy.wait()
    mlp_core.wait_recv()
    heads = queries.shape[2] // HEAD_SIZE
    repeat = QUERY_HEADS // KEY_VALUE_HEADS
    scale = HEAD_SIZE ** (-0.5)
    is_first = core == 0
    second, keys_turn, all_turn = fixed[1:2], fixed[2:3], fixed[3:4]

    def back_tile(m, tile):
        start = tile * TILE
        at = slice(start, start + TILE)
        reach = slice(start, start + span)
        key = lax.broadcasted_iota(jnp.int32, (TILE, span), 1)
        query = lax.broadcasted_iota(jnp.int32, (TILE, span), 0)
        allowed = (key >= low_col[m, at, :] - start) & (key <= query + WINDOW)
        own, others = att_grad[m, at, :], other_grad[m, at, :]
        by_repeat = (jnp.where(is_first, own, others), jnp.where(is_first, others, own))
        for group in range(heads // repeat):
            base = group * 2 * HEAD_SIZE
            k = keyvals[m, reach, base : base + HEAD_SIZE]
            v = keyvals[m, reach, base + HEAD_SIZE : base + 2 * HEAD_SIZE]
            key_sum = None
            for r in range(repeat):
                head = group * repeat + r
                q = queries[m, at, head * HEAD_SIZE : (head + 1) * HEAD_SIZE]
                g = by_repeat[r][:, group * HEAD_SIZE : (group + 1) * HEAD_SIZE]
                s = lax.dot_general(q, k, contract, preferred_element_type=f32) * scale
                total = logs[m, at, head : head + 1]
                p = jnp.exp(jnp.where(allowed, s, NEG_FILL) - total)
                pg = lax.dot_general(g, v, contract, preferred_element_type=f32)
                inner = jnp.sum(p * pg, axis=1, keepdims=True)
                sg = (p * (pg - inner) * scale).astype(bf16)
                query_total[:, head * HEAD_SIZE : (head + 1) * HEAD_SIZE] = jnp.dot(
                    sg, k, preferred_element_type=f32
                )
                dk = lax.dot_general(sg, q, over_rows, preferred_element_type=f32)
                dv = lax.dot_general(p.astype(bf16), g, over_rows, preferred_element_type=f32)
                both = jnp.concatenate([dk, dv], axis=1)
                key_sum = both if key_sum is None else key_sum + both
            totals[reach, base : base + 2 * HEAD_SIZE] += key_sum
        turned = turn(
            query_total[...], cosine[m, at, :], sine[m, at, :], second, all_turn, -1.0
        ).astype(bf16)

        @pl.when(is_first)
        def _():
            delta[m, at, :] = turned

        @pl.when(core != 0)
        def _():
            pass_on[m, at, :] = turned

    halos = [
        links.plan(
            halo_send.at[m], halo_recv.at[m], shift=-1, sends=z_at > 0,
            receives=z_at < n_tensor - 1,
        )
        for m in range(2)
    ]

    def send_halo(m):
        halo_send[m] = totals[:WINDOW].astype(bf16)
        halos[m].start()

    def finish_block(m, full):
        halos[m].wait_recv()
        tail = full[rows - WINDOW :] + jnp.where(
            z_at < n_tensor - 1, halo_recv[m].astype(f32), 0.0
        )
        full = jnp.concatenate([full[: rows - WINDOW], tail], axis=0)
        turned = turn(full, cosine[m], sine[m], second, keys_turn, -1.0).astype(bf16)

        @pl.when(is_first)
        def _():
            pass_on[m] = turned

        @pl.when(core != 0)
        def _():
            delta[m] = turned

        return send(pass_on.at[m], delta.at[2 + m], bit=1)

    free = -(-WINDOW // TILE)
    totals[...] = jnp.zeros_like(totals)
    grad_swap.wait_recv()
    back_tile(0, 0)
    down.relay(order[0])
    for tile in range(1, free):
        back_tile(0, tile)
    send_halo(0)
    for tile in range(free, tiles):
        back_tile(0, tile)
    down.relay(order[1])
    across.wait_recv()
    both = send(g_all.at[1], g_all.at[3], bit=1)
    to_across[...] = (to_core[1].astype(f32) + from_core[1].astype(f32)).astype(bf16)
    mlp_send = send(to_across, mlp_across, bit=2)
    hidden[...] += to_core[0].astype(f32) + from_core[0].astype(f32)
    attended_back(1)
    both.wait_recv()
    attended_back(3)
    grad_swap = send(att_grad.at[3], other_grad.at[1], bit=1)
    for p in order[2:]:
        down.relay(p)
    for p in order[:2]:
        gate.step(p)

    def weight_grad(left, right, at):
        total = None
        for b in range(GROUP):
            term = lax.dot_general(
                left[b, :, at], right[b], over_rows, preferred_element_type=f32
            )
            total = term if total is None else total + term
        return total

    out_grad = weight_grad(att, g_all, slice(0, n_tensor * out_quarter)).astype(bf16)
    both.wait_send()
    links.sent.remove(both)
    out_part[...] = out_grad.reshape(n_tensor, out_quarter, width)
    swap0 = finish_block(0, totals[WINDOW:])
    totals[...] = jnp.zeros_like(totals)
    grad_swap.wait_recv()
    for tile in range(free):
        back_tile(1, tile)
    send_halo(1)
    out_collect.issue(order)
    for p in order[2:]:
        gate.step(p)
    for tile in range(free, tiles):
        back_tile(1, tile)
    gate.relay(order[0])
    swap1 = finish_block(1, totals[WINDOW:])

    def project_back(b):
        units = qkv.shape[0] * quarter
        return jnp.dot(delta[b], qkv[...].reshape(units, width), preferred_element_type=f32)

    mlp_send.wait_recv()
    mlp_across[...] = (hidden[...] + mlp_across[...].astype(f32)).astype(bf16)
    save(mlp_across, block_out)
    mlp_send.wait_send()
    links.sent.remove(mlp_send)
    swap1.wait_recv()
    to_core[1] = project_back(3).astype(bf16)
    core_send1 = send(to_core.at[1], from_core.at[1], bit=1)
    hidden[...] = project_back(1)
    swap0.wait_recv()
    to_core[0] = project_back(2).astype(bf16)
    core_send0 = send(to_core.at[0], from_core.at[0], bit=1)
    core_send1.wait_recv()
    across_sends = []
    for i in range(tiles):
        at = pl.ds(i * TILE, TILE)
        to_across[at] = (hidden[at, :] + from_core[1, at, :].astype(f32)).astype(bf16)
        across_sends.append(send(to_across.at[at], from_across.at[at], bit=2))
    hidden[...] = project_back(0)
    core_send0.wait_recv()
    hidden[...] += from_core[0].astype(f32)
    attn_row = None
    for p in range(n_tensor):
        at = slice(p * quarter, (p + 1) * quarter)
        grad = weight_grad(delta, n1_all, at)
        row = jnp.sum(grad * qkv[p].astype(f32), axis=0, keepdims=True)
        attn_row = row if attn_row is None else attn_row + row
        qkv_part[p, :quarter, :] = grad.astype(bf16)
    ending = jnp.concatenate(
        [attn_row, mlp_row[...], jnp.zeros((extra - 2, width), f32)], axis=0
    ).astype(bf16)
    for p in range(n_tensor):
        qkv_part[p, quarter:, :] = ending
    qkv_collect.issue(order)
    for p in order[1:]:
        gate.relay(p)
    for p in order:
        up.step(p)
    down.finish()
    for p in order:
        out_collect.step(p)
    for i in range(tiles):
        at = pl.ds(i * TILE, TILE)
        across_sends[i].wait_recv()
        hidden[at, :] += from_across[at, :].astype(f32)
    save(hidden, normed_out)
    for p in order:
        up.relay(p)
        qkv_collect.step(p)
    gate.finish()
    for p in order:
        out_collect.relay(p)
    up.finish()
    for p in order:
        qkv_collect.relay(p)
    out_collect.finish()
    qkv_collect.finish()
    for collect in (down, gate, up, out_collect, qkv_collect):
        collect.wait()
    links.finish()


def backward(
    n_dp, n_tensor, grad_own, hidden1, mlp_part, normed1, queries, keyvals, logs, attended,
    cosine, sine, qkv_full, out_full, smalls, down_part, gate_part, up_part, down_got, gate_got,
    mlp_row, fixed,
):
    f32, bf16 = jnp.float32, jnp.bfloat16
    rows, width = grad_own.shape
    half = width // 2
    chunk = width // n_dp
    units = queries.shape[2]
    vmem = pl.BlockSpec(memory_space=pltpu.VMEM)
    hbm = pl.BlockSpec(memory_space=pl.ANY)
    extra = 16
    quarters = [
        down_part.shape[1], gate_part.shape[1], up_part.shape[1], out_full.shape[1],
        qkv_full.shape[1] + extra,
    ]

    def shape(dims, dtype=bf16):
        return jax.ShapeDtypeStruct(tuple(dims), dtype)

    def finals(index):
        return shape((GROUP, quarters[index], chunk))

    outs = [shape((rows, width), f32), shape((rows, width))]
    outs += [finals(4), finals(3), finals(1), finals(2), finals(0)]
    full = (GROUP, rows, width)
    scratch = [
        pltpu.VMEM(full, bf16),
        pltpu.VMEM(full, bf16),
        pltpu.VMEM(qkv_full.shape, bf16),
        pltpu.VMEM(out_full.shape, bf16),
        pltpu.VMEM(queries.shape, bf16),
        pltpu.VMEM(keyvals.shape, bf16),
        pltpu.VMEM(logs.shape, f32),
        pltpu.VMEM(attended.shape, bf16),
        pltpu.VMEM(cosine.shape, f32),
        pltpu.VMEM(sine.shape, f32),
        pltpu.VMEM(smalls.shape, f32),
        pltpu.VMEM((2, rows, 1), jnp.int32),
        pltpu.VMEM(attended.shape, bf16),
        pltpu.VMEM((2,) + attended.shape[1:], bf16),
        pltpu.VMEM((rows + WINDOW, units), f32),
        pltpu.VMEM((TILE, units), f32),
        pltpu.VMEM((2, rows, units), bf16),
        pltpu.VMEM((GROUP, rows, units), bf16),
        pltpu.VMEM((2, WINDOW, units), bf16),
        pltpu.VMEM((2, WINDOW, units), bf16),
        pltpu.VMEM((2, rows, width), bf16),
        pltpu.VMEM((2, rows, width), bf16),
        pltpu.VMEM((rows, width), bf16),
        pltpu.VMEM((rows, width), bf16),
        pltpu.VMEM((rows, width), bf16),
        pltpu.VMEM((rows, width), f32),
        pltpu.VMEM((n_tensor, quarters[0], half), bf16),
        pltpu.VMEM((n_tensor, quarters[1], half), bf16),
    ]
    scratch += [pltpu.VMEM((n_tensor, q, half), bf16) for q in quarters]
    scratch += [pltpu.VMEM((n_tensor, q, half), bf16) for q in quarters]
    scratch += [pltpu.VMEM((q, half), bf16) for q in quarters]
    scratch += [pltpu.VMEM((GROUP, q, chunk), bf16) for q in quarters]
    scratch += [
        pltpu.SemaphoreType.DMA((160,)),
        pltpu.SemaphoreType.DMA((160,)),
        pltpu.SemaphoreType.DMA((40,)),
    ]
    return pl.pallas_call(
        functools.partial(kernel_backward, n_dp, n_tensor),
        in_specs=[hbm] * 18 + [vmem] * 2,
        out_specs=[hbm] * len(outs),
        out_shape=outs,
        scratch_shapes=scratch,
        compiler_params=pltpu.CompilerParams(
            collective_id=1, has_side_effects=True, vmem_limit_bytes=67043328
        ),
        name="backward",
    )(
        grad_own, hidden1, mlp_part, normed1, queries, keyvals, logs, attended, cosine, sine,
        qkv_full, out_full, smalls, down_part, gate_part, up_part, down_got, gate_got, mlp_row, fixed,
    )


def fast_local(
    n_dp,
    n_tensor,
    block_in,
    cotangent,
    segment_ids,
    attn_gain,
    qkv_weight,
    out_weight,
    mlp_gain,
    gate_weight,
    up_weight,
    down_weight,
):
    bf16, f32 = jnp.bfloat16, jnp.float32
    d_at = lax.axis_index("dp")
    z_at = lax.axis_index("tensor")
    core = d_at % 2
    member = d_at % GROUP
    upper = d_at // GROUP
    rows, width = block_in.shape
    seqs, length = segment_ids.shape
    half = width // 2

    def swap(value, bit):
        return lax.ppermute(value, "dp", [(i, i ^ bit) for i in range(n_dp)])

    def gather_pair(value):
        return jnp.stack([value, swap(value, 2)])

    def gather(value):
        pair = gather_pair(value)
        return jnp.concatenate([pair, swap(pair, 1)], axis=0)

    def scatter(partial_value):
        blocks = partial_value.reshape(GROUP, rows, partial_value.shape[-1])
        got = swap(blocks[2:].astype(bf16), 1)
        pair = blocks[:2].astype(f32) + got.astype(f32)
        return pair[0] + swap(pair[1].astype(bf16), 2).astype(f32)

    part = attn_gain.shape[0]
    (
        normed1, normed2, hidden1, queries, keyvals, log_total, attended, cosine, sine, qkv_full,
        out_full, smalls, grad_rows, gate_full, up_full, down_full,
    ), fixed = forward(
        n_dp, n_tensor, block_in, cotangent, segment_ids, jnp.stack([attn_gain, mlp_gain]),
        qkv_weight, out_weight, gate_weight, up_weight, down_weight,
    )
    gate_flat, up_flat, down_flat = [
        w.reshape(-1, width) for w in (gate_full, up_full, down_full)
    ]
    gain_attn = smalls[:, 2, :part].reshape(width)
    gain_mlp = smalls[:, 3, :part].reshape(width)
    residual = block_in.astype(f32)
    scale_attn = rms_scale(residual)
    scale_mlp = rms_scale(hidden1)
    normed2 = normed2.reshape(GROUP * rows, width)
    grad_rows = grad_rows.reshape(GROUP * rows, width)

    def to_units(tokens, weight):
        return jnp.einsum("td,ud->tu", tokens, weight, preferred_element_type=f32)

    def grad_of(left, right):
        return jnp.einsum("tu,td->ud", left, right, preferred_element_type=f32).astype(bf16)

    gate = to_units(normed2, gate_flat)
    up_value = to_units(normed2, up_flat)
    sigmoid_gate = jax.nn.sigmoid(gate)
    activated = (gate * sigmoid_gate * up_value).astype(bf16)
    act_grad = to_units(grad_rows, down_flat)
    gate_delta = (act_grad * up_value * sigmoid_gate * (1.0 + gate * (1.0 - sigmoid_gate))).astype(
        bf16
    )
    up_delta = (act_grad * gate * sigmoid_gate).astype(bf16)
    normed2_term = jnp.dot(gate_delta, gate_flat, preferred_element_type=f32) + jnp.dot(
        up_delta, up_flat, preferred_element_type=f32
    )
    normed2_grad = scatter(normed2_term.astype(bf16))
    mlp_part = jnp.dot(activated, down_flat, preferred_element_type=f32).astype(bf16)
    down_part = grad_of(activated, grad_rows)
    gate_part = grad_of(gate_delta, normed2)
    up_part = grad_of(up_delta, normed2)
    hidden1_grad = cotangent.astype(f32) + norm_back(hidden1, scale_mlp, gain_mlp, normed2_grad)

    def overlap(weight, grad):
        return jnp.sum(weight.astype(f32) * grad.astype(f32), axis=0, keepdims=True)

    def by_tensor(grad):
        return grad.reshape(n_tensor, -1, width)

    def crossed(grad):
        other = lax.dynamic_slice_in_dim(grad, (1 - upper) * half, half, axis=1)
        return by_tensor_half(swap(other, GROUP))

    def by_tensor_half(grad):
        return grad.reshape(n_tensor, -1, half)

    mlp_row = overlap(gate_flat, gate_part) + overlap(up_flat, up_part)
    normed1_grad, block_out, qkv_blocks, out_blocks, gate_blocks, up_blocks, down_blocks = backward(
        n_dp, n_tensor, hidden1_grad.astype(bf16), hidden1, mlp_part.reshape(GROUP, rows, width),
        normed1, queries, keyvals, log_total, attended, cosine, sine, qkv_full, out_full, smalls,
        by_tensor(down_part), by_tensor(gate_part), by_tensor(up_part), crossed(down_part),
        crossed(gate_part), mlp_row, fixed,
    )
    input_grad = (
        hidden1_grad + norm_back(residual, scale_attn, gain_attn, normed1_grad)
    ).astype(bf16)

    def flat(blocks):
        return blocks.reshape(-1, blocks.shape[2])

    quarter = qkv_full.shape[1]

    def row_of(index, gain):
        return jnp.sum(qkv_blocks[:, quarter + index].astype(f32), axis=0) / gain.astype(f32)

    down_grad = flat(down_blocks).astype(f32)
    gate_grad = flat(gate_blocks).T.astype(f32)
    up_grad = flat(up_blocks).T.astype(f32)
    out_grad = flat(out_blocks).astype(f32)
    qkv_grad = flat(qkv_blocks[:, :quarter]).T.astype(f32)
    gains = [row_of(0, attn_gain), row_of(1, mlp_gain)]
    return (
        block_out,
        input_grad,
        gains[0],
        qkv_grad,
        out_grad,
        gains[1],
        gate_grad,
        up_grad,
        down_grad,
    )


def solution(mesh):
    in_specs = (
        P(("dp", "tensor"), None),
        P(("dp", "tensor"), None),
        P("dp", None),
        P("dp"),
        P("dp", "tensor"),
        P("tensor", "dp"),
        P("dp"),
        P("dp", "tensor"),
        P("dp", "tensor"),
        P("tensor", "dp"),
    )
    out_specs = (
        P(("dp", "tensor"), None),
        P(("dp", "tensor"), None),
        P("dp"),
        P("dp", "tensor"),
        P("tensor", "dp"),
        P("dp"),
        P("dp", "tensor"),
        P("dp", "tensor"),
        P("tensor", "dp"),
    )
    n_dp, n_tensor = mesh.shape["dp"], mesh.shape["tensor"]

    def body(*arrays):
        rows = arrays[0].shape[0]
        groups = arrays[4].shape[1] // (4 * HEAD_SIZE)
        if n_dp == 2 * GROUP and groups == 2 and rows >= WINDOW and rows % TILE == 0:
            return fast_local(n_dp, n_tensor, *arrays)
        return local(*arrays)

    return jax.shard_map(body, mesh=mesh, in_specs=in_specs, out_specs=out_specs, check_vma=False)
```

```python
import functools

import jax
import jax.numpy as jnp
import numpy as np
from jax import lax
from jax.experimental import pallas as pl
from jax.experimental.pallas import tpu as pltpu
from jax.sharding import PartitionSpec as P

QUERY_HEADS = 16
KEY_VALUE_HEADS = 8
HEAD_SIZE = 96


EPS = 1e-05
ROPE_BASE = 100000.0
NEG_FILL = -1e30


def doc_positions(segments):
    length = segments.shape[1]
    position_index = jnp.broadcast_to(jnp.arange(length, dtype=jnp.int32)[None, :], segments.shape)
    change = jnp.concatenate(
        [jnp.ones((segments.shape[0], 1), dtype=bool), segments[:, 1:] != segments[:, :-1]], axis=1
    )
    starts = lax.cummax(jnp.where(change, position_index, jnp.zeros_like(position_index)), axis=1)
    return position_index - starts


def rotary_tables(segments):
    half_dim = HEAD_SIZE // 2
    frequency = jnp.power(ROPE_BASE, -(2.0 * jnp.arange(half_dim, dtype=jnp.float32)) / HEAD_SIZE)
    angles = doc_positions(segments).astype(jnp.float32)[..., None] * frequency
    cosine_table = jnp.concatenate([jnp.cos(angles), jnp.cos(angles)], axis=-1)
    sine_table = jnp.concatenate([jnp.sin(angles), jnp.sin(angles)], axis=-1)
    return (cosine_table, sine_table)


def rotate(vector, cosine_table, sine_table):
    half_dim = vector.shape[-1] // 2
    turned = jnp.concatenate([-vector[..., half_dim:], vector[..., :half_dim]], axis=-1)
    return vector * cosine_table + turned * sine_table


def unrotate(vector, cosine_table, sine_table):
    half_dim = vector.shape[-1] // 2
    shifted = vector * sine_table
    returned = jnp.concatenate([shifted[..., half_dim:], -shifted[..., :half_dim]], axis=-1)
    return vector * cosine_table + returned


def allowed_pairs(segments):
    length = segments.shape[1]
    offsets = jnp.arange(length)
    causal = offsets[None, :] <= offsets[:, None]
    same_doc = segments[:, :, None] == segments[:, None, :]
    return (causal[None] & same_doc)[:, None, None]


def score_block(queries, key_heads, segments):
    scores = jnp.einsum(
        "sqgrd,skgd->sgrqk", queries, key_heads, preferred_element_type=jnp.float32
    ) * HEAD_SIZE ** (-0.5)
    return jnp.where(allowed_pairs(segments), scores, NEG_FILL)


def rms_scale(features):
    return lax.rsqrt(jnp.mean(features * features, axis=-1, keepdims=True) + EPS)


def norm_back(features, inverse, gain_vector, upstream):
    scaled = gain_vector * upstream
    return inverse * scaled - features * (inverse * inverse * inverse) * jnp.mean(
        scaled * features, axis=-1, keepdims=True
    )


def widen(shard_rows):
    return lax.all_gather(shard_rows, "tensor", axis=0, tiled=True)


def narrow(partial_value):
    return lax.psum_scatter(
        partial_value.astype(jnp.bfloat16), "tensor", scatter_dimension=0, tiled=True
    ).astype(jnp.float32)


def local(
    block_in,
    cotangent,
    segment_ids,
    attn_gain,
    qkv_weight,
    out_weight,
    mlp_gain,
    gate_weight,
    up_weight,
    down_weight,
):
    qkv_full, gate_full, up_full, gain_attn_raw, gain_mlp_raw = (
        lax.all_gather(qkv_weight, "dp", axis=0, tiled=True),
        lax.all_gather(gate_weight, "dp", axis=0, tiled=True),
        lax.all_gather(up_weight, "dp", axis=0, tiled=True),
        lax.all_gather(attn_gain, "dp", axis=0, tiled=True),
        lax.all_gather(mlp_gain, "dp", axis=0, tiled=True),
    )
    out_cols, down_cols = (
        lax.all_gather(out_weight, "dp", axis=1, tiled=True),
        lax.all_gather(down_weight, "dp", axis=1, tiled=True),
    )
    seq_count, length = segment_ids.shape
    repeat_factor = QUERY_HEADS // KEY_VALUE_HEADS
    groups = qkv_full.shape[1] // ((repeat_factor + 2) * HEAD_SIZE)
    gain_attn = gain_attn_raw.astype(jnp.float32)
    gain_mlp = gain_mlp_raw.astype(jnp.float32)
    residual = block_in.astype(jnp.float32)
    scale_attn = rms_scale(residual)
    normed1 = widen((residual * scale_attn * gain_attn).astype(jnp.bfloat16))
    projected = jnp.dot(normed1, qkv_full, preferred_element_type=jnp.float32).reshape(
        seq_count, length, groups, repeat_factor + 2, HEAD_SIZE
    )
    cosine_table, sine_table = rotary_tables(segment_ids)
    cos_query = cosine_table[:, :, None, None, :]
    sin_query = sine_table[:, :, None, None, :]
    cos_key = cosine_table[:, :, None, :]
    sin_key = sine_table[:, :, None, :]
    queries = rotate(projected[:, :, :, :repeat_factor], cos_query, sin_query).astype(jnp.bfloat16)
    key_heads = rotate(projected[:, :, :, repeat_factor], cos_key, sin_key).astype(jnp.bfloat16)
    values = projected[:, :, :, repeat_factor + 1].astype(jnp.bfloat16)
    scores = score_block(queries, key_heads, segment_ids)
    highest = jnp.max(scores, axis=-1, keepdims=True)
    log_total = highest + jnp.log(jnp.sum(jnp.exp(scores - highest), axis=-1, keepdims=True))
    probability = jnp.exp(scores - log_total).astype(jnp.bfloat16)
    attended = jnp.einsum(
        "sgrqk,skgd->sqgrd", probability, values, preferred_element_type=jnp.float32
    ).astype(jnp.bfloat16)
    attn_flat = attended.reshape(seq_count * length, groups * repeat_factor * HEAD_SIZE)
    attn_delta = lax.psum_scatter(
        jnp.dot(attn_flat, out_cols, preferred_element_type=jnp.float32).astype(jnp.bfloat16),
        "tensor",
        scatter_dimension=0,
        tiled=True,
    ).astype(jnp.float32)
    hidden1 = residual + attn_delta
    scale_mlp = rms_scale(hidden1)
    normed2 = widen((hidden1 * scale_mlp * gain_mlp).astype(jnp.bfloat16))
    gate = jnp.dot(normed2, gate_full, preferred_element_type=jnp.float32)
    up_value = jnp.dot(normed2, up_full, preferred_element_type=jnp.float32)
    sigmoid_gate = jax.nn.sigmoid(gate)
    activated = (gate * sigmoid_gate * up_value).astype(jnp.bfloat16)
    mlp_delta = narrow(jnp.dot(activated, down_cols, preferred_element_type=jnp.float32))
    block_out = (hidden1 + mlp_delta).astype(jnp.bfloat16)
    grad_rows = widen(cotangent)
    down_part = jnp.einsum("tf,td->fd", activated, grad_rows, preferred_element_type=jnp.float32)
    act_grad = jnp.einsum("td,fd->tf", grad_rows, down_cols, preferred_element_type=jnp.float32)
    gate_delta = (act_grad * up_value * sigmoid_gate * (1.0 + gate * (1.0 - sigmoid_gate))).astype(
        jnp.bfloat16
    )
    up_delta = (act_grad * gate * sigmoid_gate).astype(jnp.bfloat16)
    gate_part = jnp.einsum("td,tf->df", normed2, gate_delta, preferred_element_type=jnp.float32)
    up_part = jnp.einsum("td,tf->df", normed2, up_delta, preferred_element_type=jnp.float32)
    normed2_term = jnp.einsum(
        "tf,df->td", gate_delta, gate_full, preferred_element_type=jnp.float32
    ) + jnp.einsum("tf,df->td", up_delta, up_full, preferred_element_type=jnp.float32)
    normed2_grad = narrow(normed2_term)
    mlp_gain_part = jnp.sum(normed2_grad * hidden1 * scale_mlp, axis=0)
    hidden1_grad = cotangent.astype(jnp.float32) + norm_back(
        hidden1, scale_mlp, gain_mlp, normed2_grad
    )
    hidden1_rounded = hidden1_grad.astype(jnp.bfloat16)
    grad_full = lax.all_gather(hidden1_rounded, "tensor", axis=0, tiled=True)
    attended_grad = jnp.einsum(
        "td,hd->th", grad_full, out_cols, preferred_element_type=jnp.float32
    ).astype(jnp.bfloat16)
    out_part = jnp.einsum("th,td->hd", attn_flat, grad_full, preferred_element_type=jnp.float32)
    attended_grad = attended_grad.reshape(seq_count, length, groups, repeat_factor, HEAD_SIZE)
    prob_full = jnp.exp(score_block(queries, key_heads, segment_ids) - log_total)
    prob_grad = jnp.einsum(
        "sqgrd,skgd->sgrqk", attended_grad, values, preferred_element_type=jnp.float32
    )
    inner_sum = jnp.sum(prob_full * prob_grad, axis=-1, keepdims=True)
    score_grad = (prob_full * (prob_grad - inner_sum) * HEAD_SIZE ** (-0.5)).astype(jnp.bfloat16)
    query_grad = jnp.einsum(
        "sgrqk,skgd->sqgrd", score_grad, key_heads, preferred_element_type=jnp.float32
    )
    key_grad = jnp.einsum(
        "sgrqk,sqgrd->skgd", score_grad, queries, preferred_element_type=jnp.float32
    )
    value_grad = jnp.einsum(
        "sgrqk,sqgrd->skgd",
        prob_full.astype(jnp.bfloat16),
        attended_grad,
        preferred_element_type=jnp.float32,
    )
    projected_grad = jnp.concatenate(
        [
            unrotate(query_grad, cos_query, sin_query),
            unrotate(key_grad, cos_key, sin_key)[:, :, :, None],
            value_grad[:, :, :, None],
        ],
        axis=3,
    )
    projected_grad = projected_grad.astype(jnp.bfloat16).reshape(
        seq_count * length, groups * (repeat_factor + 2) * HEAD_SIZE
    )
    qkv_part = jnp.einsum("td,tc->dc", normed1, projected_grad, preferred_element_type=jnp.float32)
    normed1_grad = narrow(
        jnp.einsum("tc,dc->td", projected_grad, qkv_full, preferred_element_type=jnp.float32)
    )
    attn_gain_part = jnp.sum(normed1_grad * residual * scale_attn, axis=0)
    input_grad = (hidden1_grad + norm_back(residual, scale_attn, gain_attn, normed1_grad)).astype(
        jnp.bfloat16
    )
    attn_gain_total, mlp_gain_total = lax.psum((attn_gain_part, mlp_gain_part), "tensor")
    attn_gain_grad, qkv_grad, gate_grad, up_grad, mlp_gain_grad = (
        lax.psum_scatter(
            attn_gain_total.astype(jnp.bfloat16), "dp", scatter_dimension=0, tiled=True
        ).astype(jnp.float32),
        lax.psum_scatter(
            qkv_part.astype(jnp.bfloat16), "dp", scatter_dimension=0, tiled=True
        ).astype(jnp.float32),
        lax.psum_scatter(
            gate_part.astype(jnp.bfloat16), "dp", scatter_dimension=0, tiled=True
        ).astype(jnp.float32),
        lax.psum_scatter(
            up_part.astype(jnp.bfloat16), "dp", scatter_dimension=0, tiled=True
        ).astype(jnp.float32),
        lax.psum_scatter(
            mlp_gain_total.astype(jnp.bfloat16), "dp", scatter_dimension=0, tiled=True
        ).astype(jnp.float32),
    )
    out_grad, down_grad = (
        lax.psum_scatter(
            out_part.astype(jnp.bfloat16), "dp", scatter_dimension=1, tiled=True
        ).astype(jnp.float32),
        lax.psum_scatter(
            down_part.astype(jnp.bfloat16), "dp", scatter_dimension=1, tiled=True
        ).astype(jnp.float32),
    )
    return (
        block_out,
        input_grad,
        attn_gain_grad,
        qkv_grad,
        out_grad,
        mlp_gain_grad,
        gate_grad,
        up_grad,
        down_grad,
    )


GROUP = 4
WINDOW = 256
LANES = 384
TILE = 128


MESH = pl.DeviceIdType.MESH


class Transfer:
    def __init__(self, copy, sends=None, receives=None):
        self.copy, self.sends, self.receives = copy, sends, receives

    def _when(self, condition, action):
        if condition is None:
            action()
        else:
            pl.when(condition)(action)

    def start(self):
        self._when(self.sends, self.copy.start)
        return self

    def wait_recv(self):
        self._when(self.receives, self.copy.wait_recv)

    def wait_send(self):
        self._when(self.sends, self.copy.wait_send)


class Links:
    def __init__(self, n_dp, n_tensor, out_sems, in_sems, local_sems):
        self.n_dp, self.n_tensor = n_dp, n_tensor
        self.out_sems, self.in_sems, self.local_sems = out_sems, in_sems, local_sems
        self.d_at, self.z_at = lax.axis_index("dp"), lax.axis_index("tensor")
        self.used, self.used_local = 0, 0
        self.sent, self.saved = [], []

    def barrier(self):
        barrier = pltpu.get_barrier_semaphore()
        for k in range(1, self.n_dp):
            pl.semaphore_signal(
                barrier,
                inc=1,
                device_id={"dp": self.d_at ^ k, "tensor": self.z_at},
                device_id_type=MESH,
            )
        for s in range(1, self.n_tensor):
            pl.semaphore_signal(
                barrier,
                inc=1,
                device_id={"dp": self.d_at, "tensor": lax.rem(self.z_at + s, self.n_tensor)},
                device_id_type=MESH,
            )
        pl.semaphore_wait(barrier, self.n_dp - 1 + self.n_tensor - 1)

    def plan(self, source, target, bit=0, shift=0, sends=None, receives=None):
        slot = self.used
        self.used += 1
        copy = pltpu.make_async_remote_copy(
            src_ref=source,
            dst_ref=target,
            send_sem=self.out_sems.at[slot],
            recv_sem=self.in_sems.at[slot],
            device_id={
                "dp": self.d_at ^ bit,
                "tensor": lax.rem(self.z_at + self.n_tensor + shift, self.n_tensor),
            },
            device_id_type=MESH,
        )
        transfer = Transfer(copy, sends, receives)
        self.sent.append(transfer)
        return transfer

    def send(self, source, target, bit=0, shift=0):
        return self.plan(source, target, bit, shift).start()

    def move(self, source, target):
        copy = pltpu.make_async_copy(source, target, self.local_sems.at[self.used_local])
        self.used_local += 1
        copy.start()
        return copy

    def save(self, source, target):
        self.saved.append(self.move(source, target))

    def finish(self):
        for transfer in self.sent:
            transfer.wait_send()
        for copy in self.saved:
            copy.wait()


class Spread:
    def __init__(self, links, own_piece, target, columns):
        self.links, self.own_piece, self.target, self.columns = links, own_piece, target, columns
        self.ahead, self.back, self.swaps = [], [], []

    def _slot(self, index):
        n = self.links.n_tensor
        return self.target.at[lax.rem(index + n, n), :, self.columns]

    def issue(self):
        links, n, z = self.links, self.links.n_tensor, self.links.z_at
        own = self._slot(z)
        for s in range(1, n):
            up_from, down_from = z - (s - 1), z + (s - 1)
            up_source = self.own_piece if s == 1 else self._slot(up_from)
            down_source = self.own_piece if s == 1 else self._slot(down_from)
            self.ahead.append(
                links.plan(
                    up_source, self._slot(up_from), shift=1,
                    sends=(z < n - 1) & (up_from >= 0), receives=z >= s,
                )
            )
            self.back.append(
                links.plan(
                    down_source, self._slot(down_from), shift=-1,
                    sends=(z > 0) & (down_from < n), receives=z + s < n,
                )
            )
        self.ahead[0].start()
        self.back[0].start()
        self.swaps.append(links.plan(self.own_piece, own, bit=GROUP).start())

    def step(self, s):
        links, n, z = self.links, self.links.n_tensor, self.links.z_at
        for arrivals, piece, here in (
            (self.ahead, z - s, z >= s),
            (self.back, z + s, z + s < n),
        ):
            arrivals[s - 1].wait_recv()
            if s < n - 1:
                arrivals[s].start()
            slot = self._slot(piece)
            self.swaps.append(
                links.plan(slot, slot, bit=GROUP, sends=here, receives=here).start()
            )

    def wait(self):
        for swap in self.swaps:
            swap.wait_recv()


def kernel_forward(
    n_dp, n_tensor,
    tokens, cot, out_w, gate_w, up_w, down_w, qkv_w, segments, gain_rows, fixed,
    normed1_out, normed2_out, hidden_out, query_out, keyval_out, log_out, att_out,
    cos_out, sin_out, qkv_out, out_out, small_out, cot_out, gate_out, up_out, down_out,
    x_all, n1_all, first, dealt, first_piece, qkv, obuf, gbuf, ubuf, dbuf, piece, outw,
    small, small_all, stream, parts, recv, queries, keyvals,
    att, by_repeat, logs, cosine, sine, low_col, to_core, from_core, to_across, from_across,
    hidden, n2_all, stage, out_sems, in_sems, local_sems,
):
    f32, bf16 = jnp.float32, jnp.bfloat16
    links = Links(n_dp, n_tensor, out_sems, in_sems, local_sems)
    send, move, save = links.send, links.move, links.save
    d_at, z_at = links.d_at, links.z_at
    member = d_at % GROUP
    core = d_at % 2
    upper = d_at // GROUP
    rows, width = tokens.shape
    half = width // 2
    chunk = qkv_w.shape[0]
    contract = (((1,), (1,)), ((), ()))
    columns = pl.ds(pl.multiple_of(upper * half, half), half)

    turned = qkv_w[...].T
    quarter = turned.shape[0] // GROUP
    for i in range(GROUP):
        first[i] = turned[i * quarter : (i + 1) * quarter]
    ids = segments[...]
    seqs, length = ids.shape
    begin = jnp.zeros_like(ids)
    for value in range(3):
        count = jnp.sum((ids == value).astype(jnp.int32), axis=1, keepdims=True)
        begin = begin + jnp.where(ids > value, count, 0)
    begin = begin.astype(f32)
    for i in range(seqs):
        stream[:, i * length : (i + 1) * length] = jnp.broadcast_to(
            begin[i : i + 1] + float(i * length), (stream.shape[0], length)
        )
    window = stream[:, pl.ds(pl.multiple_of(z_at * rows, TILE), rows)]
    here = lax.broadcasted_iota(jnp.int32, window.shape, 1) + z_at * rows
    small[...] = window
    small[0:1] = here.astype(f32)[0:1] - window[0:1]
    small[2:4, :chunk] = gain_rows[...].astype(f32)

    @pl.when(z_at == 0)
    def _():
        keyvals[:, :WINDOW, :] = jnp.zeros_like(keyvals[:, :WINDOW, :])

    links.barrier()

    deals = [send(first.at[member ^ k], dealt.at[member], bit=k) for k in range(1, GROUP)]
    beside = send(tokens, x_all.at[2], bit=1)
    smalls = [send(small, small_all.at[d_at], bit=k) for k in range(1, n_dp)]
    rests = []

    def rows_of(ref, at):
        size = ref.shape[0] // GROUP
        return ref.at[pl.ds(pl.multiple_of(at * size, 16), size), :]

    def columns_of(ref, at):
        size = ref.shape[1] // GROUP
        return ref.at[:, pl.ds(pl.multiple_of(at * size, TILE), size)]

    pairs = [(out_w, obuf, rows_of), (gate_w, gbuf, columns_of), (up_w, ubuf, columns_of)]
    pairs.append((down_w, dbuf, rows_of))
    for ref, buffer, take in pairs:
        for k in range(1, GROUP):
            rests.append(send(take(ref, member ^ k), buffer.at[member], bit=k))
    own = [move(tokens, x_all.at[0])]
    for ref, buffer, take in pairs:
        own.append(move(take(ref, member), buffer.at[member]))
    cot_stage = move(cot, stage)
    small_all[d_at] = small[...]
    dealt[member] = first[member]

    entries = lax.broadcasted_iota(jnp.int32, (WINDOW, LANES), 0).astype(f32)
    angles = entries * fixed[0:1]

    def split(table):
        pieces = []
        for _ in range(3):
            pieces.append(table.astype(bf16))
            table = table - pieces[-1].astype(f32)
        return pieces

    cos_parts, sin_parts = split(jnp.cos(angles)), split(jnp.sin(angles))
    second = fixed[1:2]
    own_turns = jnp.where(core == 0, jnp.ones_like(second), fixed[2:3])

    for copy in deals:
        copy.wait_recv()
    for i in range(GROUP):
        first_piece[:, i * chunk : (i + 1) * chunk] = dealt[i]
    spread_first = Spread(links, first_piece, qkv, columns)
    spread_first.issue()
    save(first_piece, qkv.at[z_at, :, columns])
    own_qkv = links.saved.pop()
    for copy in own:
        copy.wait()
    cot_stage.wait()
    save(stage, cot_out.at[0])
    spread_first.step(1)
    for copy in smalls:
        copy.wait_recv()
    spread_first.step(2)
    gains = []
    for row in (2, 3):
        gains.append(
            jnp.concatenate([small_all[i, row : row + 1, :chunk] for i in range(n_dp)], axis=1)
        )
    for copy in rests:
        copy.wait_recv()
    across = send(tokens, x_all.at[1], bit=2)
    sizes = [obuf.shape[1], gbuf.shape[2], ubuf.shape[2], dbuf.shape[1]]
    starts = [sum(sizes[:i]) for i in range(len(sizes))]
    spreads = []
    for index, (target, buffer) in enumerate(
        ((outw, obuf), (gate_out, gbuf), (up_out, ubuf), (down_out, dbuf))
    ):
        at = slice(starts[index], starts[index] + sizes[index])
        for i in range(GROUP):
            value = buffer[i]
            piece[at, i * chunk : (i + 1) * chunk] = (
                value.T if value.shape[0] == chunk and sizes[index] != chunk else value
            )
        own_piece = piece.at[pl.ds(starts[index], sizes[index])]
        spreads.append(Spread(links, own_piece, target, columns))
    out_spread, gate_spread, up_spread, down_spread = spreads
    saves = [move(s.own_piece, s.target.at[z_at, :, columns]) for s in spreads]
    out_spread.issue()
    spread_first.step(3)
    gate_spread.issue()
    beside.wait_recv()
    own_qkv.wait()
    spread_first.wait()

    def project_block(m, k):
        features = x_all[m].astype(f32)
        scale = lax.rsqrt(jnp.mean(features * features, axis=1, keepdims=True) + EPS)
        normal = (features * scale * gains[0]).astype(bf16)
        n1_all[m] = normal
        units = qkv.shape[0] * qkv.shape[1]
        product = lax.dot_general(
            normal, qkv[...].reshape(units, width), contract, preferred_element_type=f32
        )
        info = small_all[d_at ^ k].T
        key = lax.broadcasted_iota(jnp.int32, (rows, WINDOW), 1)
        chosen = (info[:, 0:1].astype(jnp.int32) == key).astype(bf16)

        def pick(table):
            total = jnp.dot(chosen, table[0], preferred_element_type=f32)
            for part in table[1:]:
                total += jnp.dot(chosen, part, preferred_element_type=f32)
            return total

        cos_here, sin_here = pick(cos_parts), pick(sin_parts)
        parts[m] = turn(product, cos_here, sin_here, second, own_turns, 1.0).astype(bf16)
        if m < 2:
            cosine[m] = cos_here
            sine[m] = sin_here
            low_col[m] = info[:, 1:2].astype(jnp.int32) - z_at * rows + WINDOW

    is_first = core == 0
    halos = [
        links.plan(
            keyvals.at[m, pl.ds(rows, WINDOW)], keyvals.at[m, pl.ds(0, WINDOW)], shift=1,
            sends=z_at < n_tensor - 1, receives=z_at > 0,
        )
        for m in range(2)
    ]

    def take_block(m, swap):
        swap.wait_recv()
        mine, other = parts[m], recv[m]
        queries[m] = jnp.where(is_first, mine, other)
        keyvals[m, WINDOW:, :] = jnp.where(is_first, other, mine)
        halos[m].start()

    project_block(2, 1)
    part_swap = send(parts.at[2], recv.at[0], bit=1)
    project_block(0, 0)
    take_block(0, part_swap)
    out_spread.step(1)
    across.wait_recv()
    both = send(x_all.at[1], x_all.at[3], bit=1)
    cot_across = send(cot, cot_out.at[1], bit=2)
    cot_beside = send(cot, cot_out.at[2], bit=1)
    out_spread.step(2)
    project_block(1, 2)
    both.wait_recv()
    project_block(3, 3)
    part_swap = send(parts.at[3], recv.at[1], bit=1)
    out_spread.step(3)
    save(n1_all, normed1_out)
    save(cosine, cos_out)
    save(sine, sin_out)
    take_block(1, part_swap)
    gate_spread.step(1)
    save(queries, query_out)
    heads = queries.shape[2] // HEAD_SIZE
    repeat = QUERY_HEADS // KEY_VALUE_HEADS
    span = TILE + WINDOW

    def attend_tile(m, start):
        key = lax.broadcasted_iota(jnp.int32, (TILE, span), 1)
        query = lax.broadcasted_iota(jnp.int32, (TILE, span), 0)
        lowest = low_col[m, pl.ds(start, TILE), :] - start
        allowed = (key >= lowest) & (key <= query + WINDOW)
        for head in range(heads):
            group, r = head // repeat, head % repeat
            base = group * 2 * HEAD_SIZE
            q = queries[m, pl.ds(start, TILE), head * HEAD_SIZE : (head + 1) * HEAD_SIZE]
            k = keyvals[m, pl.ds(start, span), base : base + HEAD_SIZE]
            v = keyvals[m, pl.ds(start, span), base + HEAD_SIZE : base + 2 * HEAD_SIZE]
            s = lax.dot_general(q, k, contract, preferred_element_type=f32) * HEAD_SIZE ** (-0.5)
            s = jnp.where(allowed, s, NEG_FILL)
            highest = jnp.max(s, axis=1, keepdims=True)
            e = jnp.exp(s - highest)
            whole = jnp.sum(e, axis=1, keepdims=True)
            p = (e * (1.0 / whole)).astype(bf16)
            o = jnp.dot(p, v, preferred_element_type=f32).astype(bf16)
            logs[m, pl.ds(start, TILE), head : head + 1] = highest + jnp.log(whole)
            by_repeat[r, m, pl.ds(start, TILE), group * HEAD_SIZE : (group + 1) * HEAD_SIZE] = o

    tiles = rows // TILE
    free = -(-WINDOW // TILE)
    for tile in range(free, tiles):
        attend_tile(1, tile * TILE)
        attend_tile(0, tile * TILE)
    gate_spread.step(2)
    halos[0].wait_recv()
    halos[1].wait_recv()
    up_spread.issue()
    for tile in range(free):
        attend_tile(1, tile * TILE)
    att_swap1 = send(by_repeat.at[1 - core, 1], att.at[3], bit=1)
    gate_spread.step(3)
    attend_tile(0, 0)
    up_spread.step(1)
    for tile in range(1, free):
        attend_tile(0, tile * TILE)
    att_swap0 = send(by_repeat.at[1 - core, 0], att.at[2], bit=1)
    save(keyvals, keyval_out)
    save(logs, log_out)
    att[0] = by_repeat[core, 0]
    att[1] = by_repeat[core, 1]
    down_spread.issue()
    cot_across.wait_recv()
    cot_both = send(cot_out.at[1], cot_out.at[3], bit=1)

    saves[0].wait()
    out_spread.wait()

    def project_out(b):
        units = outw.shape[0] * outw.shape[1]
        return jnp.dot(att[b], outw[...].reshape(units, width), preferred_element_type=f32)

    att_swap1.wait_recv()
    to_core[1] = project_out(3).astype(bf16)
    core_send1 = send(to_core.at[1], from_core.at[1], bit=1)
    hidden[...] = project_out(1)
    att_swap0.wait_recv()
    to_core[0] = project_out(2).astype(bf16)
    core_send0 = send(to_core.at[0], from_core.at[0], bit=1)
    core_send1.wait_recv()
    across_sends = []
    for i in range(tiles):
        at = pl.ds(i * TILE, TILE)
        to_across[at] = (hidden[at, :] + from_core[1, at, :].astype(f32)).astype(bf16)
        across_sends.append(send(to_across.at[at], from_across.at[at], bit=2))
    hidden[...] = project_out(0) + x_all[0].astype(f32)
    core_send0.wait_recv()
    hidden[...] += from_core[0].astype(f32)
    save(att, att_out)
    up_spread.step(2)
    steps = [(up_spread, 3), (down_spread, 1), (down_spread, 2), (down_spread, 3)]
    last = []
    for i in range(tiles):
        at = pl.ds(i * TILE, TILE)
        across_sends[i].wait_recv()
        value = hidden[at, :] + from_across[at, :].astype(f32)
        hidden[at, :] = value
        scale = lax.rsqrt(jnp.mean(value * value, axis=1, keepdims=True) + EPS)
        n2_all[0, at, :] = (value * scale * gains[1]).astype(bf16)
        last.append(send(n2_all.at[0, at], n2_all.at[1, at], bit=2))
        last.append(send(n2_all.at[0, at], n2_all.at[2, at], bit=1))
        if i in (1, 2):
            spread, s = steps.pop(0)
            spread.step(s)
    save(hidden, hidden_out)
    save(qkv, qkv_out)
    save(outw, out_out)
    save(small_all, small_out)
    ends = []
    for i in range(tiles):
        at = pl.ds(i * TILE, TILE)
        last[2 * i].wait_recv()
        ends.append(send(n2_all.at[1, at], n2_all.at[3, at], bit=1))
        if i < 2:
            spread, s = steps.pop(0)
            spread.step(s)
    for copy in ends + last[1::2]:
        copy.wait_recv()
    save(n2_all, normed2_out)
    for copy in saves[1:]:
        copy.wait()
    for spread in (gate_spread, up_spread, down_spread):
        spread.wait()
    for copy in (cot_beside, cot_both):
        copy.wait_recv()
    links.finish()


def forward(
    n_dp, n_tensor, tokens, cot, segments, gain_rows, qkv_w, out_w, gate_w, up_w, down_w
):
    rows, width = tokens.shape
    f32, bf16 = jnp.float32, jnp.bfloat16
    vmem = pl.BlockSpec(memory_space=pltpu.VMEM)
    hbm = pl.BlockSpec(memory_space=pl.ANY)
    chunk = qkv_w.shape[0]
    quarter = qkv_w.shape[1] // GROUP
    sizes = [
        out_w.shape[0] // GROUP, gate_w.shape[1] // GROUP, up_w.shape[1] // GROUP,
        down_w.shape[0] // GROUP,
    ]
    units = quarter * n_tensor
    heads = units // HEAD_SIZE
    lane = np.arange(LANES)
    within = lane % HEAD_SIZE
    fixed = np.zeros((8, LANES), np.float32)
    fixed[0] = np.power(ROPE_BASE, -(2.0 * (within % (HEAD_SIZE // 2))) / HEAD_SIZE)
    fixed[1] = within >= HEAD_SIZE // 2
    fixed[2] = lane % (2 * HEAD_SIZE) < HEAD_SIZE
    fixed[3] = 1.0

    def shape(dims, dtype=bf16):
        return jax.ShapeDtypeStruct(tuple(dims), dtype)

    full = (GROUP, rows, width)
    qkv_shape = (n_tensor, quarter, width)
    out_shape = (n_tensor, sizes[0], width)
    att_shape = (GROUP, rows, units // 2)
    small_shape = (n_dp, 8, rows)
    table = (2, rows, LANES)
    outs = [
        shape(full),
        shape(full),
        shape((rows, width), f32),
        shape((2, rows, units)),
        shape((2, rows + WINDOW, units)),
        shape((2, rows, heads), f32),
        shape(att_shape),
        shape(table, f32),
        shape(table, f32),
        shape(qkv_shape),
        shape(out_shape),
        shape(small_shape, f32),
        shape(full),
    ] + [shape((n_tensor, size, width)) for size in sizes[1:]]
    scratch = [
        pltpu.VMEM(full, bf16),
        pltpu.VMEM(full, bf16),
        pltpu.VMEM((GROUP, quarter, chunk), bf16),
        pltpu.VMEM((GROUP, quarter, chunk), bf16),
        pltpu.VMEM((quarter, width // 2), bf16),
        pltpu.VMEM(qkv_shape, bf16),
        pltpu.VMEM((GROUP, sizes[0], chunk), bf16),
        pltpu.VMEM((GROUP, chunk, sizes[1]), bf16),
        pltpu.VMEM((GROUP, chunk, sizes[2]), bf16),
        pltpu.VMEM((GROUP, sizes[3], chunk), bf16),
        pltpu.VMEM((sum(sizes), width // 2), bf16),
        pltpu.VMEM(out_shape, bf16),
        pltpu.VMEM((8, rows), f32),
        pltpu.VMEM(small_shape, f32),
        pltpu.VMEM((8, n_tensor * rows), f32),
        pltpu.VMEM((GROUP, rows, units), bf16),
        pltpu.VMEM((2, rows, units), bf16),
        pltpu.VMEM((2, rows, units), bf16),
        pltpu.VMEM((2, rows + WINDOW, units), bf16),
        pltpu.VMEM(att_shape, bf16),
        pltpu.VMEM((2, 2, rows, units // 2), bf16),
        pltpu.VMEM((2, rows, heads), f32),
        pltpu.VMEM(table, f32),
        pltpu.VMEM(table, f32),
        pltpu.VMEM((2, rows, 1), jnp.int32),
        pltpu.VMEM((2, rows, width), bf16),
        pltpu.VMEM((2, rows, width), bf16),
        pltpu.VMEM((rows, width), bf16),
        pltpu.VMEM((rows, width), bf16),
        pltpu.VMEM((rows, width), f32),
        pltpu.VMEM(full, bf16),
        pltpu.VMEM((rows, width), bf16),
        pltpu.SemaphoreType.DMA((128,)),
        pltpu.SemaphoreType.DMA((128,)),
        pltpu.SemaphoreType.DMA((40,)),
    ]
    results = pl.pallas_call(
        functools.partial(kernel_forward, n_dp, n_tensor),
        in_specs=[hbm] * 6 + [vmem] * 4,
        out_specs=[hbm] * len(outs),
        out_shape=outs,
        scratch_shapes=scratch,
        compiler_params=pltpu.CompilerParams(
            collective_id=0, has_side_effects=True, vmem_limit_bytes=60 * 1024 * 1024
        ),
        name="forward",
    )(
        tokens, cot, out_w, gate_w, up_w, down_w, qkv_w, segments, gain_rows, jnp.asarray(fixed)
    )
    return results, jnp.asarray(fixed)


def turn(value, cosine, sine, second, turns, sign):
    width = value.shape[1]
    half = HEAD_SIZE // 2
    c = turns * cosine + (1.0 - turns)
    u = (sign * turns * second) * sine
    d = (sign * turns * (second - 1.0)) * sine
    pieces = []
    up = pltpu.roll(value, half, 1)
    down = pltpu.roll(value, width - half, 1)
    for i in range(width // LANES):
        at = slice(i * LANES, (i + 1) * LANES)
        pieces.append(value[:, at] * c + up[:, at] * u + down[:, at] * d)
    return jnp.concatenate(pieces, axis=1)


def kernel_feed(
    n_dp, n_tensor,
    n2_in, cot_in, hidden_in, gate_in, up_in, down_in, smalls,
    grad_out, grad_own_out, mlp_out, down_out, gate_out, up_out, down_got, row_out,
    n2_all, cot_all, gate_w, up_w, down_w, active, gate_delta, up_delta,
    down_part, gate_part, up_part, to_core, from_core, to_across, from_across, hidden, total,
    rounded, row, out_sems, in_sems, local_sems,
):
    f32, bf16 = jnp.float32, jnp.bfloat16
    links = Links(n_dp, n_tensor, out_sems, in_sems, local_sems)
    send, move, save = links.send, links.move, links.save
    upper = links.d_at // GROUP
    rows, width = hidden.shape
    half = width // 2
    chunk = width // n_dp
    size = gate_w.shape[1]
    units = n_tensor * size
    contract = (((1,), (1,)), ((), ()))
    over_rows = (((0,), (0,)), ((), ()))
    other = pl.ds(pl.multiple_of((1 - upper) * half, half), half)
    tiles = rows // TILE

    loads = [
        move(gate_in, gate_w), move(n2_in, n2_all), move(up_in, up_w), move(down_in, down_w),
        move(cot_in, cot_all), move(hidden_in, hidden),
    ]
    links.barrier()
    for copy in loads[:-1]:
        copy.wait()

    def inner(i, carry):
        m, p = i // n_tensor, i % n_tensor
        at = pl.ds(pl.multiple_of(p * size, TILE), size)
        gate = lax.dot_general(n2_all[m], gate_w[p], contract, preferred_element_type=f32)
        up_value = lax.dot_general(n2_all[m], up_w[p], contract, preferred_element_type=f32)
        act_grad = lax.dot_general(cot_all[m], down_w[p], contract, preferred_element_type=f32)
        sigmoid = jax.nn.sigmoid(gate)
        silu = gate * sigmoid
        active[m, :, at] = (silu * up_value).astype(bf16)
        gate_delta[m, :, at] = (
            act_grad * up_value * sigmoid * (1.0 + gate * (1.0 - sigmoid))
        ).astype(bf16)
        up_delta[m, :, at] = (act_grad * silu).astype(bf16)
        return carry

    lax.fori_loop(0, GROUP * n_tensor, inner, 0)

    def back(m):
        return jnp.dot(
            gate_delta[m], gate_w[...].reshape(units, width), preferred_element_type=f32
        ) + jnp.dot(up_delta[m], up_w[...].reshape(units, width), preferred_element_type=f32)

    to_core[1] = back(3).astype(bf16)
    core_send1 = send(to_core.at[1], from_core.at[1], bit=1)
    total[...] = back(1)
    core_send1.wait_recv()
    across = []
    for i in range(tiles):
        at = pl.ds(i * TILE, TILE)
        to_across[at] = (total[at, :] + from_core[1, at, :].astype(f32)).astype(bf16)
        across.append(send(to_across.at[at], from_across.at[at], bit=2))
    to_core[0] = back(2).astype(bf16)
    core_send0 = send(to_core.at[0], from_core.at[0], bit=1)
    total[...] = back(0)

    order = []
    for i in range((n_tensor + 1) // 2):
        order.extend(dict.fromkeys((n_tensor - 1 - i, i)))

    def grads(left, right, part, target, weight=None):
        for p in order:
            at = slice(p * size, (p + 1) * size)
            grad = lax.dot_general(
                left[...].reshape(GROUP * rows, units)[:, at],
                right[...].reshape(GROUP * rows, width),
                over_rows,
                preferred_element_type=f32,
            )
            part[p] = grad.astype(bf16)
            if weight is not None:
                row[...] += jnp.sum(grad * weight[p].astype(f32), axis=0, keepdims=True)
            else:
                swaps.append(send(part.at[p, :, other], down_got.at[p], bit=GROUP))
            save(part.at[p], target.at[p])

    swaps = []
    row[...] = jnp.zeros_like(row)
    grads(active, cot_all, down_part, down_out)
    core_send0.wait_recv()
    total[...] += from_core[0].astype(f32)
    grads(gate_delta, n2_all, gate_part, gate_out, gate_w)
    grads(up_delta, n2_all, up_part, up_out, up_w)
    save(row, row_out)
    for m in range(GROUP):
        n2_all[m] = jnp.dot(
            active[m], down_w[...].reshape(units, width), preferred_element_type=f32
        ).astype(bf16)
        save(n2_all.at[m], mlp_out.at[m])
    gain = jnp.concatenate([smalls[i, 3:4, :chunk] for i in range(n_dp)], axis=1)
    loads[-1].wait()
    for i in range(tiles):
        at = pl.ds(i * TILE, TILE)
        across[i].wait_recv()
        upstream = total[at, :] + from_across[at, :].astype(f32)
        features = hidden[at, :]
        inverse = lax.rsqrt(jnp.mean(features * features, axis=1, keepdims=True) + EPS)
        scaled = gain * upstream
        mean = jnp.mean(scaled * features, axis=1, keepdims=True)
        result = cot_all[0, at, :].astype(f32) + (
            inverse * scaled - features * (inverse * inverse * inverse) * mean
        )
        total[at, :] = result
        rounded[at, :] = result.astype(bf16)
    save(total, grad_out)
    save(rounded, grad_own_out)
    for copy in swaps:
        copy.wait_recv()
    links.finish()


def feed(n_dp, n_tensor, normed2, grad_rows, hidden1, gate_w, up_w, down_w, smalls):
    f32, bf16 = jnp.float32, jnp.bfloat16
    rows, width = hidden1.shape
    half = width // 2
    vmem = pl.BlockSpec(memory_space=pltpu.VMEM)
    hbm = pl.BlockSpec(memory_space=pl.ANY)
    weight = gate_w.shape
    inner = (GROUP, rows, n_tensor * weight[1])

    def shape(dims, dtype=bf16):
        return jax.ShapeDtypeStruct(tuple(dims), dtype)

    outs = [
        shape((rows, width), f32), shape((rows, width)), shape(normed2.shape),
        shape(weight), shape(weight), shape(weight), shape((n_tensor, weight[1], half)),
        shape((1, width), f32),
    ]
    scratch = [
        pltpu.VMEM(normed2.shape, bf16),
        pltpu.VMEM(normed2.shape, bf16),
        pltpu.VMEM(weight, bf16),
        pltpu.VMEM(weight, bf16),
        pltpu.VMEM(weight, bf16),
        pltpu.VMEM(inner, bf16),
        pltpu.VMEM(inner, bf16),
        pltpu.VMEM(inner, bf16),
        pltpu.VMEM(weight, bf16),
        pltpu.VMEM(weight, bf16),
        pltpu.VMEM(weight, bf16),
        pltpu.VMEM((2, rows, width), bf16),
        pltpu.VMEM((2, rows, width), bf16),
        pltpu.VMEM((rows, width), bf16),
        pltpu.VMEM((rows, width), bf16),
        pltpu.VMEM((rows, width), f32),
        pltpu.VMEM((rows, width), f32),
        pltpu.VMEM((rows, width), bf16),
        pltpu.VMEM((1, width), f32),
        pltpu.SemaphoreType.DMA((16,)),
        pltpu.SemaphoreType.DMA((16,)),
        pltpu.SemaphoreType.DMA((40,)),
    ]
    return pl.pallas_call(
        functools.partial(kernel_feed, n_dp, n_tensor),
        in_specs=[hbm] * 6 + [vmem],
        out_specs=[hbm] * len(outs),
        out_shape=outs,
        scratch_shapes=scratch,
        compiler_params=pltpu.CompilerParams(
            collective_id=2, has_side_effects=True, vmem_limit_bytes=67043328
        ),
        name="feed",
    )(normed2, grad_rows, hidden1, gate_w, up_w, down_w, smalls)


class Collect:
    def __init__(
        self, links, part, swapped, stage, arrived, late, blocks, target, mine, other, turned=False
    ):
        self.turned = turned
        self.links, self.part, self.swapped, self.stage = links, part, swapped, stage
        self.arrived, self.late, self.blocks, self.target = arrived, late, blocks, target
        self.mine, self.other = mine, other
        self.swaps, self.loads, self.deals = {}, [], []

    def issue(self, order):
        links = self.links
        for p in order:
            self.swaps[p] = links.send(
                self.part.at[p, :, self.other], self.swapped.at[p], bit=GROUP
            )
        if self.stage is not None:
            self.loads = [links.move(self.part.at[:, :, self.mine], self.stage)]

    def load(self, received):
        links = self.links
        self.loads = [
            links.move(self.part.at[:, :, self.mine], self.stage),
            links.move(received, self.swapped),
        ]

    def step(self, p):
        links, n, z = self.links, self.links.n_tensor, self.links.z_at
        f32, bf16 = jnp.float32, jnp.bfloat16
        while self.loads:
            self.loads.pop().wait()
        if p in self.swaps:
            self.swaps[p].wait_recv()
        own = self.stage[p] if self.stage is not None else self.part[p, :, self.mine]
        self.swapped[p] = (own.astype(f32) + self.swapped[p].astype(f32)).astype(bf16)
        if not hasattr(self, "ahead"):
            self.ahead, self.back, self.back_last = [None] * n, [None] * n, [None] * n
        source = self.swapped.at[p]
        self.ahead[p] = links.plan(
            source, self.arrived.at[p], shift=1, sends=z < p, receives=(z > 0) & (z <= p)
        )
        self.back[p] = links.plan(
            source, self.arrived.at[p], shift=-1, sends=z > p + 1,
            receives=(z > p) & (z < n - 1),
        )
        self.back_last[p] = links.plan(
            source, self.late, shift=-1, sends=z == p + 1, receives=(z == p) & (z < n - 1)
        )

        @pl.when((z == 0) & (z < p))
        def _():
            self.ahead[p].copy.start()

        @pl.when((z == n - 1) & (z > p + 1))
        def _():
            self.back[p].copy.start()

        @pl.when((z == n - 1) & (z == p + 1))
        def _():
            self.back_last[p].copy.start()

    def relay(self, i):
        links, n, z = self.links, self.links.n_tensor, self.links.z_at
        f32, bf16 = jnp.float32, jnp.bfloat16

        def add(p):
            self.swapped[p] = (
                self.swapped[p].astype(f32) + self.arrived[p].astype(f32)
            ).astype(bf16)

        for p in range(n):
            at = i - (n - 1) + p
            if 0 < at < n - 1 and at < p:

                @pl.when(z == at)
                def _(p=p):
                    self.ahead[p].copy.wait_recv()
                    add(p)
                    self.ahead[p].copy.start()

            at = n - 1 - i + p
            if 0 < at < n - 1 and at > p:

                @pl.when(z == at)
                def _(p=p, at=at):
                    self.back[p].copy.wait_recv()
                    add(p)
                    (self.back_last if at == p + 1 else self.back)[p].copy.start()

    def finish(self):
        links, n, z = self.links, self.links.n_tensor, self.links.z_at
        f32, bf16 = jnp.float32, jnp.bfloat16
        member = links.d_at % GROUP
        for p in range(n):

            @pl.when((z == p) & (z > 0))
            def _(p=p):
                self.ahead[p].copy.wait_recv()

            @pl.when((z == p) & (z < n - 1))
            def _(p=p):
                self.back_last[p].copy.wait_recv()

        below = jnp.where(z > 0, self.arrived[z].astype(f32), 0.0)
        above = jnp.where(z < n - 1, self.late[...].astype(f32), 0.0)
        total = (self.swapped[z].astype(f32) + below + above).astype(bf16)
        chunk = total.shape[1] // GROUP
        size = self.blocks.shape[2 if self.turned else 1]
        place = pl.ds(pl.multiple_of(member * size, 16), size)
        if self.turned:
            place = pl.ds(pl.multiple_of(member * size, TILE), size)
        for i in range(GROUP):
            block = total[:, i * chunk : (i + 1) * chunk]
            self.blocks[i] = block.T if self.turned else block
        if self.turned:
            target = self.target.at[:, place]
        elif len(self.target.shape) == 2:
            target = self.target.at[place, :]
        else:
            target = self.target.at[member]
        for k in range(1, GROUP):
            self.deals.append(links.send(self.blocks.at[member ^ k], target, bit=k))
        links.save(self.blocks.at[member], target)

    def wait(self):
        for deal in self.deals:
            deal.wait_recv()


def kernel_backward(
    n_dp, n_tensor,
    grad_own, hidden_grad, tokens, hidden1, mlp_part, n1_in, query_in, keyval_in, log_in, att_in,
    cos_in, sin_in, qkv_in, out_in, small_in, down_in, gate_in, up_in, down_got,
    mlp_row, fixed,
    input_out, block_out, qkv_out, out_out, gate_out, up_out, down_out,
    g_all, n1_all, qkv, outw, queries, keyvals, logs, att, cosine, sine, gains, low_col,
    att_grad, other_grad, totals, query_total, pass_on, delta, halo_send, halo_recv,
    to_core, from_core, to_across, from_across, mlp_across, hidden, stage, gate_stage,
    down_swap, gate_swap, up_swap, out_swap, qkv_swap,
    down_come, gate_come, up_come, out_come, qkv_come,
    down_late, gate_late, up_late, out_late, qkv_late,
    down_block, gate_block, up_block, out_block, qkv_block,
    out_sems, in_sems, local_sems,
):
    f32, bf16 = jnp.float32, jnp.bfloat16
    links = Links(n_dp, n_tensor, out_sems, in_sems, local_sems)
    send, move, save = links.send, links.move, links.save
    d_at, z_at = links.d_at, links.z_at
    core = d_at % 2
    upper = d_at // GROUP
    rows, width = grad_own.shape
    half = width // 2
    contract = (((1,), (1,)), ((), ()))
    over_rows = (((0,), (0,)), ((), ()))
    mine = pl.ds(pl.multiple_of(upper * half, half), half)
    other = pl.ds(pl.multiple_of((1 - upper) * half, half), half)
    tiles = rows // TILE
    span = TILE + WINDOW
    quarter = qkv.shape[1]
    out_quarter = outw.shape[1]
    extra = qkv_swap.shape[1] - quarter

    loads = [
        move(grad_own, g_all.at[0]), move(out_in, outw), move(query_in, queries),
        move(keyval_in, keyvals), move(log_in, logs), move(cos_in, cosine), move(sin_in, sine),
        move(mlp_part.at[pl.ds(0, 2)], to_core), move(hidden1, hidden), move(att_in, att),
        move(qkv_in, qkv), move(n1_in, n1_all),
    ]
    small = pltpu.make_async_copy(small_in, gains, local_sems.at[links.used_local])
    links.used_local += 1
    small.start()
    links.barrier()
    across = send(grad_own, g_all.at[1], bit=2)
    beside = send(grad_own, g_all.at[2], bit=1)
    mlp_core = send(mlp_part.at[pl.ds(2, 2)], from_core, bit=1)
    order = []
    for i in range((n_tensor + 1) // 2):
        order.extend(dict.fromkeys((n_tensor - 1 - i, i)))

    down = Collect(
        links, down_in, down_swap, stage, down_come, down_late, down_block, down_out, mine, other
    )
    gate = Collect(
        links, gate_in, gate_swap, gate_stage, gate_come, gate_late, gate_block, gate_out, mine, other,
        turned=True,
    )
    up = Collect(
        links, up_in, up_swap, stage, up_come, up_late, up_block, up_out, mine, other, turned=True
    )
    out_part = g_all.at[:, pl.ds(quarter + extra, out_quarter), :]
    qkv_part = g_all.at[:, pl.ds(0, quarter + extra), :]
    out_collect = Collect(
        links, out_part, out_swap, None, out_come, out_late, out_block, out_out, mine, other
    )
    qkv_collect = Collect(
        links, qkv_part, qkv_swap, None, qkv_come, qkv_late, qkv_block, qkv_out, mine, other
    )
    down.load(down_got)
    gate.issue(order)
    small.wait()
    for m, k in ((0, 0), (1, 2)):
        info = gains[d_at ^ k].T
        low_col[m] = info[:, 1:2].astype(jnp.int32) - z_at * rows + WINDOW
    loads[0].wait()
    loads[1].wait()

    def attended_back(b):
        units = outw.shape[0] * outw.shape[1]
        att_grad[b] = lax.dot_general(
            g_all[b], outw[...].reshape(units, width), contract, preferred_element_type=f32
        ).astype(bf16)

    attended_back(0)
    beside.wait_recv()
    attended_back(2)
    grad_swap = send(att_grad.at[2], other_grad.at[0], bit=1)
    for p in order:
        down.step(p)
    up.issue(order)
    for copy in loads[2:]:
        copy.wait()
    mlp_core.wait_recv()
    heads = queries.shape[2] // HEAD_SIZE
    repeat = QUERY_HEADS // KEY_VALUE_HEADS
    scale = HEAD_SIZE ** (-0.5)
    is_first = core == 0
    second, keys_turn, all_turn = fixed[1:2], fixed[2:3], fixed[3:4]

    def back_tile(m, tile):
        start = tile * TILE
        at = slice(start, start + TILE)
        reach = slice(start, start + span)
        key = lax.broadcasted_iota(jnp.int32, (TILE, span), 1)
        query = lax.broadcasted_iota(jnp.int32, (TILE, span), 0)
        allowed = (key >= low_col[m, at, :] - start) & (key <= query + WINDOW)
        own, others = att_grad[m, at, :], other_grad[m, at, :]
        by_repeat = (jnp.where(is_first, own, others), jnp.where(is_first, others, own))
        for group in range(heads // repeat):
            base = group * 2 * HEAD_SIZE
            k = keyvals[m, reach, base : base + HEAD_SIZE]
            v = keyvals[m, reach, base + HEAD_SIZE : base + 2 * HEAD_SIZE]
            key_sum = None
            for r in range(repeat):
                head = group * repeat + r
                q = queries[m, at, head * HEAD_SIZE : (head + 1) * HEAD_SIZE]
                g = by_repeat[r][:, group * HEAD_SIZE : (group + 1) * HEAD_SIZE]
                s = lax.dot_general(q, k, contract, preferred_element_type=f32) * scale
                total = logs[m, at, head : head + 1]
                p = jnp.exp(jnp.where(allowed, s, NEG_FILL) - total)
                pg = lax.dot_general(g, v, contract, preferred_element_type=f32)
                inner = jnp.sum(p * pg, axis=1, keepdims=True)
                sg = (p * (pg - inner) * scale).astype(bf16)
                query_total[:, head * HEAD_SIZE : (head + 1) * HEAD_SIZE] = jnp.dot(
                    sg, k, preferred_element_type=f32
                )
                dk = lax.dot_general(sg, q, over_rows, preferred_element_type=f32)
                dv = lax.dot_general(p.astype(bf16), g, over_rows, preferred_element_type=f32)
                both = jnp.concatenate([dk, dv], axis=1)
                key_sum = both if key_sum is None else key_sum + both
            totals[m, reach, base : base + 2 * HEAD_SIZE] += key_sum
        turned = turn(
            query_total[...], cosine[m, at, :], sine[m, at, :], second, all_turn, -1.0
        ).astype(bf16)

        @pl.when(is_first)
        def _():
            delta[m, at, :] = turned

        @pl.when(core != 0)
        def _():
            pass_on[m, at, :] = turned

    halos = [
        links.plan(
            halo_send.at[m], halo_recv.at[m], shift=-1, sends=z_at > 0,
            receives=z_at < n_tensor - 1,
        )
        for m in range(2)
    ]

    def send_halo(m):
        halo_send[m] = totals[m, :WINDOW].astype(bf16)
        halos[m].start()

    def finish_block(m):
        halos[m].wait_recv()
        full = totals[m, WINDOW:]
        tail = full[rows - WINDOW :] + jnp.where(
            z_at < n_tensor - 1, halo_recv[m].astype(f32), 0.0
        )
        full = jnp.concatenate([full[: rows - WINDOW], tail], axis=0)
        turned = turn(full, cosine[m], sine[m], second, keys_turn, -1.0).astype(bf16)

        @pl.when(is_first)
        def _():
            pass_on[m] = turned

        @pl.when(core != 0)
        def _():
            delta[m] = turned

        return send(pass_on.at[m], delta.at[2 + m], bit=1)

    first_steps = n_tensor // 2
    free = -(-WINDOW // TILE)
    totals[...] = jnp.zeros_like(totals)
    grad_swap.wait_recv()
    for tile in range(free):
        back_tile(0, tile)
    send_halo(0)
    down.relay(1)
    gate.step(order[0])
    for tile in range(free, tiles):
        back_tile(0, tile)
    for p in order[1:first_steps]:
        gate.step(p)
    for i in range(2, n_tensor - 1):
        down.relay(i)
    across.wait_recv()
    both = send(g_all.at[1], g_all.at[3], bit=1)
    to_across[...] = (to_core[1].astype(f32) + from_core[1].astype(f32)).astype(bf16)
    mlp_send = send(to_across, mlp_across, bit=2)
    hidden[...] += to_core[0].astype(f32) + from_core[0].astype(f32)
    attended_back(1)
    both.wait_recv()
    attended_back(3)
    grad_swap = send(att_grad.at[3], other_grad.at[1], bit=1)

    def weight_grad(left, right, at):
        total = None
        for b in range(GROUP):
            term = lax.dot_general(
                left[b, :, at], right[b], over_rows, preferred_element_type=f32
            )
            total = term if total is None else total + term
        return total

    out_grad = weight_grad(att, g_all, slice(0, n_tensor * out_quarter)).astype(bf16)
    both.wait_send()
    links.sent.remove(both)
    out_part[...] = out_grad.reshape(n_tensor, out_quarter, width)
    grad_swap.wait_recv()
    back_tile(1, 0)
    down.finish()
    for tile in range(1, free):
        back_tile(1, tile)
    send_halo(1)
    for p in order[first_steps:]:
        gate.step(p)
    for tile in range(free, tiles):
        back_tile(1, tile)
    swap0 = finish_block(0)
    gate.relay(1)
    up.step(order[0])
    swap1 = finish_block(1)

    def project_back(b):
        units = qkv.shape[0] * quarter
        return jnp.dot(delta[b], qkv[...].reshape(units, width), preferred_element_type=f32)

    mlp_send.wait_recv()
    mlp_across[...] = (hidden[...] + mlp_across[...].astype(f32)).astype(bf16)
    save(mlp_across, block_out)
    mlp_send.wait_send()
    links.sent.remove(mlp_send)
    swap1.wait_recv()
    to_core[1] = project_back(3).astype(bf16)
    core_send1 = send(to_core.at[1], from_core.at[1], bit=1)
    hidden[...] = project_back(1)
    swap0.wait_recv()
    to_core[0] = project_back(2).astype(bf16)
    core_send0 = send(to_core.at[0], from_core.at[0], bit=1)
    core_send1.wait_recv()
    across_sends = []
    for i in range(tiles):
        at = pl.ds(i * TILE, TILE)
        to_across[at] = (hidden[at, :] + from_core[1, at, :].astype(f32)).astype(bf16)
        across_sends.append(send(to_across.at[at], from_across.at[at], bit=2))
    hidden[...] = project_back(0)
    core_send0.wait_recv()
    hidden[...] += from_core[0].astype(f32)
    for p in order[1 : n_tensor - 1]:
        up.step(p)
    attn_row = None
    for p in range(n_tensor):
        at = slice(p * quarter, (p + 1) * quarter)
        grad = weight_grad(delta, n1_all, at)
        row = jnp.sum(grad * qkv[p].astype(f32), axis=0, keepdims=True)
        attn_row = row if attn_row is None else attn_row + row
        qkv_part[p, :quarter, :] = grad.astype(bf16)
    ending = jnp.concatenate(
        [attn_row, mlp_row[...], jnp.zeros((extra - 2, width), f32)], axis=0
    ).astype(bf16)
    for p in range(n_tensor):
        qkv_part[p, quarter:, :] = ending
    qkv_collect.issue(order)
    out_collect.issue(order)
    finals = [
        move(tokens, n1_all.at[0]),
        move(hidden_grad.at[:, pl.ds(0, half)], totals.at[0, pl.ds(0, rows)]),
        move(hidden_grad.at[:, pl.ds(half, half)], totals.at[1, pl.ds(0, rows)]),
    ]
    for p in order[n_tensor - 1 :]:
        up.step(p)
    for i in range(2, n_tensor - 1):
        gate.relay(i)
    gain = jnp.concatenate([gains[i, 2:3, : width // n_dp] for i in range(n_dp)], axis=1)
    for copy in finals:
        copy.wait()
    for i in range(tiles):
        at = pl.ds(i * TILE, TILE)
        across_sends[i].wait_recv()
        upstream = hidden[at, :] + from_across[at, :].astype(f32)
        features = n1_all[0, at, :].astype(f32)
        inverse = lax.rsqrt(jnp.mean(features * features, axis=1, keepdims=True) + EPS)
        scaled = gain * upstream
        mean = jnp.mean(scaled * features, axis=1, keepdims=True)
        change = inverse * scaled - features * (inverse * inverse * inverse) * mean
        n1_all[1, at, :half] = (totals[0, at, :] + change[:, :half]).astype(bf16)
        n1_all[1, at, half:] = (totals[1, at, :] + change[:, half:]).astype(bf16)
        if i == 1:
            up.relay(1)
    save(n1_all.at[1], input_out)
    gate.finish()
    for p in order[: n_tensor - 1]:
        qkv_collect.step(p)
    for i in range(2, n_tensor - 1):
        up.relay(i)
    for p in order[n_tensor - 1 :]:
        qkv_collect.step(p)
    qkv_collect.relay(1)
    up.finish()
    for p in order:
        out_collect.step(p)
    for i in range(2, n_tensor - 1):
        qkv_collect.relay(i)
    out_collect.relay(1)
    qkv_collect.finish()
    for i in range(2, n_tensor - 1):
        out_collect.relay(i)
    out_collect.finish()
    for collect in (down, gate, up, out_collect, qkv_collect):
        collect.wait()
    links.finish()


def backward(
    n_dp, n_tensor, grad_own, hidden_grad, tokens, hidden1, mlp_part, normed1, queries, keyvals, logs, attended,
    cosine, sine, qkv_full, out_full, smalls, down_part, gate_part, up_part, down_got,
    mlp_row, fixed,
):
    f32, bf16 = jnp.float32, jnp.bfloat16
    rows, width = grad_own.shape
    half = width // 2
    chunk = width // n_dp
    units = queries.shape[2]
    vmem = pl.BlockSpec(memory_space=pltpu.VMEM)
    hbm = pl.BlockSpec(memory_space=pl.ANY)
    extra = 16
    quarters = [
        down_part.shape[1], gate_part.shape[1], up_part.shape[1], out_full.shape[1],
        qkv_full.shape[1] + extra,
    ]

    def shape(dims, dtype=bf16):
        return jax.ShapeDtypeStruct(tuple(dims), dtype)

    def finals(index):
        return shape((GROUP, quarters[index], chunk))

    outs = [
        shape((rows, width)), shape((rows, width)), finals(4), shape((GROUP * quarters[3], chunk)),
        shape((chunk, GROUP * quarters[1])), shape((chunk, GROUP * quarters[2])),
        shape((GROUP * quarters[0], chunk)),
    ]
    full = (GROUP, rows, width)
    scratch = [
        pltpu.VMEM(full, bf16),
        pltpu.VMEM(full, bf16),
        pltpu.VMEM(qkv_full.shape, bf16),
        pltpu.VMEM(out_full.shape, bf16),
        pltpu.VMEM(queries.shape, bf16),
        pltpu.VMEM(keyvals.shape, bf16),
        pltpu.VMEM(logs.shape, f32),
        pltpu.VMEM(attended.shape, bf16),
        pltpu.VMEM(cosine.shape, f32),
        pltpu.VMEM(sine.shape, f32),
        pltpu.VMEM(smalls.shape, f32),
        pltpu.VMEM((2, rows, 1), jnp.int32),
        pltpu.VMEM(attended.shape, bf16),
        pltpu.VMEM((2,) + attended.shape[1:], bf16),
        pltpu.VMEM((2, rows + WINDOW, units), f32),
        pltpu.VMEM((TILE, units), f32),
        pltpu.VMEM((2, rows, units), bf16),
        pltpu.VMEM((GROUP, rows, units), bf16),
        pltpu.VMEM((2, WINDOW, units), bf16),
        pltpu.VMEM((2, WINDOW, units), bf16),
        pltpu.VMEM((2, rows, width), bf16),
        pltpu.VMEM((2, rows, width), bf16),
        pltpu.VMEM((rows, width), bf16),
        pltpu.VMEM((rows, width), bf16),
        pltpu.VMEM((rows, width), bf16),
        pltpu.VMEM((rows, width), f32),
        pltpu.VMEM((n_tensor, quarters[0], half), bf16),
        pltpu.VMEM((n_tensor, quarters[1], half), bf16),
    ]
    scratch += [pltpu.VMEM((n_tensor, q, half), bf16) for q in quarters]
    scratch += [pltpu.VMEM((n_tensor, q, half), bf16) for q in quarters]
    scratch += [pltpu.VMEM((q, half), bf16) for q in quarters]
    scratch += [
        pltpu.VMEM((GROUP, chunk, q) if turned else (GROUP, q, chunk), bf16)
        for q, turned in zip(quarters, (False, True, True, False, False))
    ]
    scratch += [
        pltpu.SemaphoreType.DMA((160,)),
        pltpu.SemaphoreType.DMA((160,)),
        pltpu.SemaphoreType.DMA((40,)),
    ]
    return pl.pallas_call(
        functools.partial(kernel_backward, n_dp, n_tensor),
        in_specs=[hbm] * 19 + [vmem] * 2,
        out_specs=[hbm] * len(outs),
        out_shape=outs,
        scratch_shapes=scratch,
        compiler_params=pltpu.CompilerParams(
            collective_id=1, has_side_effects=True, vmem_limit_bytes=67043328
        ),
        name="backward",
    )(
        grad_own, hidden_grad, tokens, hidden1, mlp_part, normed1, queries, keyvals, logs, attended, cosine, sine,
        qkv_full, out_full, smalls, down_part, gate_part, up_part, down_got, mlp_row, fixed,
    )


def fast_local(
    n_dp,
    n_tensor,
    block_in,
    cotangent,
    segment_ids,
    attn_gain,
    qkv_weight,
    out_weight,
    mlp_gain,
    gate_weight,
    up_weight,
    down_weight,
):
    bf16, f32 = jnp.bfloat16, jnp.float32
    rows, width = block_in.shape
    part = attn_gain.shape[0]
    (
        normed1, normed2, hidden1, queries, keyvals, log_total, attended, cosine, sine, qkv_full,
        out_full, smalls, grad_rows, gate_full, up_full, down_full,
    ), fixed = forward(
        n_dp, n_tensor, block_in, cotangent, segment_ids, jnp.stack([attn_gain, mlp_gain]),
        qkv_weight, out_weight, gate_weight, up_weight, down_weight,
    )
    (
        hidden1_grad, grad_own, mlp_part, down_part, gate_part, up_part, down_got, mlp_row,
    ) = feed(n_dp, n_tensor, normed2, grad_rows, hidden1, gate_full, up_full, down_full, smalls)
    input_grad, block_out, qkv_blocks, out_grad, gate_grad, up_grad, down_grad = backward(
        n_dp, n_tensor, grad_own, hidden1_grad, block_in, hidden1, mlp_part, normed1, queries,
        keyvals, log_total, attended, cosine, sine, qkv_full, out_full, smalls, down_part, gate_part, up_part, down_got, mlp_row,
        fixed,
    )
    quarter = qkv_full.shape[1]

    def row_of(index, gain):
        return jnp.sum(qkv_blocks[:, quarter + index].astype(f32), axis=0) / gain.astype(f32)

    blocks = qkv_blocks[:, :quarter]
    qkv_grad = blocks.reshape(-1, blocks.shape[2]).T.astype(f32)
    gains = [row_of(0, attn_gain), row_of(1, mlp_gain)]
    return (
        block_out,
        input_grad,
        gains[0],
        qkv_grad,
        out_grad.astype(f32),
        gains[1],
        gate_grad.astype(f32),
        up_grad.astype(f32),
        down_grad.astype(f32),
    )


def solution(mesh):
    in_specs = (
        P(("dp", "tensor"), None),
        P(("dp", "tensor"), None),
        P("dp", None),
        P("dp"),
        P("dp", "tensor"),
        P("tensor", "dp"),
        P("dp"),
        P("dp", "tensor"),
        P("dp", "tensor"),
        P("tensor", "dp"),
    )
    out_specs = (
        P(("dp", "tensor"), None),
        P(("dp", "tensor"), None),
        P("dp"),
        P("dp", "tensor"),
        P("tensor", "dp"),
        P("dp"),
        P("dp", "tensor"),
        P("dp", "tensor"),
        P("tensor", "dp"),
    )
    n_dp, n_tensor = mesh.shape["dp"], mesh.shape["tensor"]

    def body(*arrays):
        rows = arrays[0].shape[0]
        groups = arrays[4].shape[1] // (4 * HEAD_SIZE)
        if n_dp == 2 * GROUP and groups == 2 and rows >= WINDOW and rows % TILE == 0:
            return fast_local(n_dp, n_tensor, *arrays)
        return local(*arrays)

    return jax.shard_map(body, mesh=mesh, in_specs=in_specs, out_specs=out_specs, check_vma=False)
```

```python
import functools

import jax
import jax.numpy as jnp
import numpy as np
from jax import lax
from jax.experimental import pallas as pl
from jax.experimental.pallas import tpu as pltpu
from jax.sharding import PartitionSpec as P

QUERY_HEADS = 16
KEY_VALUE_HEADS = 8
HEAD_SIZE = 96


EPS = 1e-05
ROPE_BASE = 100000.0
NEG_FILL = -1e30


def doc_positions(segments):
    length = segments.shape[1]
    position_index = jnp.broadcast_to(jnp.arange(length, dtype=jnp.int32)[None, :], segments.shape)
    change = jnp.concatenate(
        [jnp.ones((segments.shape[0], 1), dtype=bool), segments[:, 1:] != segments[:, :-1]], axis=1
    )
    starts = lax.cummax(jnp.where(change, position_index, jnp.zeros_like(position_index)), axis=1)
    return position_index - starts


def rotary_tables(segments):
    half_dim = HEAD_SIZE // 2
    frequency = jnp.power(ROPE_BASE, -(2.0 * jnp.arange(half_dim, dtype=jnp.float32)) / HEAD_SIZE)
    angles = doc_positions(segments).astype(jnp.float32)[..., None] * frequency
    cosine_table = jnp.concatenate([jnp.cos(angles), jnp.cos(angles)], axis=-1)
    sine_table = jnp.concatenate([jnp.sin(angles), jnp.sin(angles)], axis=-1)
    return (cosine_table, sine_table)


def rotate(vector, cosine_table, sine_table):
    half_dim = vector.shape[-1] // 2
    turned = jnp.concatenate([-vector[..., half_dim:], vector[..., :half_dim]], axis=-1)
    return vector * cosine_table + turned * sine_table


def unrotate(vector, cosine_table, sine_table):
    half_dim = vector.shape[-1] // 2
    shifted = vector * sine_table
    returned = jnp.concatenate([shifted[..., half_dim:], -shifted[..., :half_dim]], axis=-1)
    return vector * cosine_table + returned


def allowed_pairs(segments):
    length = segments.shape[1]
    offsets = jnp.arange(length)
    causal = offsets[None, :] <= offsets[:, None]
    same_doc = segments[:, :, None] == segments[:, None, :]
    return (causal[None] & same_doc)[:, None, None]


def score_block(queries, key_heads, segments):
    scores = jnp.einsum(
        "sqgrd,skgd->sgrqk", queries, key_heads, preferred_element_type=jnp.float32
    ) * HEAD_SIZE ** (-0.5)
    return jnp.where(allowed_pairs(segments), scores, NEG_FILL)


def rms_scale(features):
    return lax.rsqrt(jnp.mean(features * features, axis=-1, keepdims=True) + EPS)


def norm_back(features, inverse, gain_vector, upstream):
    scaled = gain_vector * upstream
    return inverse * scaled - features * (inverse * inverse * inverse) * jnp.mean(
        scaled * features, axis=-1, keepdims=True
    )


def widen(shard_rows):
    return lax.all_gather(shard_rows, "tensor", axis=0, tiled=True)


def narrow(partial_value):
    return lax.psum_scatter(
        partial_value.astype(jnp.bfloat16), "tensor", scatter_dimension=0, tiled=True
    ).astype(jnp.float32)


def local(
    block_in,
    cotangent,
    segment_ids,
    attn_gain,
    qkv_weight,
    out_weight,
    mlp_gain,
    gate_weight,
    up_weight,
    down_weight,
):
    qkv_full, gate_full, up_full, gain_attn_raw, gain_mlp_raw = (
        lax.all_gather(qkv_weight, "dp", axis=0, tiled=True),
        lax.all_gather(gate_weight, "dp", axis=0, tiled=True),
        lax.all_gather(up_weight, "dp", axis=0, tiled=True),
        lax.all_gather(attn_gain, "dp", axis=0, tiled=True),
        lax.all_gather(mlp_gain, "dp", axis=0, tiled=True),
    )
    out_cols, down_cols = (
        lax.all_gather(out_weight, "dp", axis=1, tiled=True),
        lax.all_gather(down_weight, "dp", axis=1, tiled=True),
    )
    seq_count, length = segment_ids.shape
    repeat_factor = QUERY_HEADS // KEY_VALUE_HEADS
    groups = qkv_full.shape[1] // ((repeat_factor + 2) * HEAD_SIZE)
    gain_attn = gain_attn_raw.astype(jnp.float32)
    gain_mlp = gain_mlp_raw.astype(jnp.float32)
    residual = block_in.astype(jnp.float32)
    scale_attn = rms_scale(residual)
    normed1 = widen((residual * scale_attn * gain_attn).astype(jnp.bfloat16))
    projected = jnp.dot(normed1, qkv_full, preferred_element_type=jnp.float32).reshape(
        seq_count, length, groups, repeat_factor + 2, HEAD_SIZE
    )
    cosine_table, sine_table = rotary_tables(segment_ids)
    cos_query = cosine_table[:, :, None, None, :]
    sin_query = sine_table[:, :, None, None, :]
    cos_key = cosine_table[:, :, None, :]
    sin_key = sine_table[:, :, None, :]
    queries = rotate(projected[:, :, :, :repeat_factor], cos_query, sin_query).astype(jnp.bfloat16)
    key_heads = rotate(projected[:, :, :, repeat_factor], cos_key, sin_key).astype(jnp.bfloat16)
    values = projected[:, :, :, repeat_factor + 1].astype(jnp.bfloat16)
    scores = score_block(queries, key_heads, segment_ids)
    highest = jnp.max(scores, axis=-1, keepdims=True)
    log_total = highest + jnp.log(jnp.sum(jnp.exp(scores - highest), axis=-1, keepdims=True))
    probability = jnp.exp(scores - log_total).astype(jnp.bfloat16)
    attended = jnp.einsum(
        "sgrqk,skgd->sqgrd", probability, values, preferred_element_type=jnp.float32
    ).astype(jnp.bfloat16)
    attn_flat = attended.reshape(seq_count * length, groups * repeat_factor * HEAD_SIZE)
    attn_delta = lax.psum_scatter(
        jnp.dot(attn_flat, out_cols, preferred_element_type=jnp.float32).astype(jnp.bfloat16),
        "tensor",
        scatter_dimension=0,
        tiled=True,
    ).astype(jnp.float32)
    hidden1 = residual + attn_delta
    scale_mlp = rms_scale(hidden1)
    normed2 = widen((hidden1 * scale_mlp * gain_mlp).astype(jnp.bfloat16))
    gate = jnp.dot(normed2, gate_full, preferred_element_type=jnp.float32)
    up_value = jnp.dot(normed2, up_full, preferred_element_type=jnp.float32)
    sigmoid_gate = jax.nn.sigmoid(gate)
    activated = (gate * sigmoid_gate * up_value).astype(jnp.bfloat16)
    mlp_delta = narrow(jnp.dot(activated, down_cols, preferred_element_type=jnp.float32))
    block_out = (hidden1 + mlp_delta).astype(jnp.bfloat16)
    grad_rows = widen(cotangent)
    down_part = jnp.einsum("tf,td->fd", activated, grad_rows, preferred_element_type=jnp.float32)
    act_grad = jnp.einsum("td,fd->tf", grad_rows, down_cols, preferred_element_type=jnp.float32)
    gate_delta = (act_grad * up_value * sigmoid_gate * (1.0 + gate * (1.0 - sigmoid_gate))).astype(
        jnp.bfloat16
    )
    up_delta = (act_grad * gate * sigmoid_gate).astype(jnp.bfloat16)
    gate_part = jnp.einsum("td,tf->df", normed2, gate_delta, preferred_element_type=jnp.float32)
    up_part = jnp.einsum("td,tf->df", normed2, up_delta, preferred_element_type=jnp.float32)
    normed2_term = jnp.einsum(
        "tf,df->td", gate_delta, gate_full, preferred_element_type=jnp.float32
    ) + jnp.einsum("tf,df->td", up_delta, up_full, preferred_element_type=jnp.float32)
    normed2_grad = narrow(normed2_term)
    mlp_gain_part = jnp.sum(normed2_grad * hidden1 * scale_mlp, axis=0)
    hidden1_grad = cotangent.astype(jnp.float32) + norm_back(
        hidden1, scale_mlp, gain_mlp, normed2_grad
    )
    hidden1_rounded = hidden1_grad.astype(jnp.bfloat16)
    grad_full = lax.all_gather(hidden1_rounded, "tensor", axis=0, tiled=True)
    attended_grad = jnp.einsum(
        "td,hd->th", grad_full, out_cols, preferred_element_type=jnp.float32
    ).astype(jnp.bfloat16)
    out_part = jnp.einsum("th,td->hd", attn_flat, grad_full, preferred_element_type=jnp.float32)
    attended_grad = attended_grad.reshape(seq_count, length, groups, repeat_factor, HEAD_SIZE)
    prob_full = jnp.exp(score_block(queries, key_heads, segment_ids) - log_total)
    prob_grad = jnp.einsum(
        "sqgrd,skgd->sgrqk", attended_grad, values, preferred_element_type=jnp.float32
    )
    inner_sum = jnp.sum(prob_full * prob_grad, axis=-1, keepdims=True)
    score_grad = (prob_full * (prob_grad - inner_sum) * HEAD_SIZE ** (-0.5)).astype(jnp.bfloat16)
    query_grad = jnp.einsum(
        "sgrqk,skgd->sqgrd", score_grad, key_heads, preferred_element_type=jnp.float32
    )
    key_grad = jnp.einsum(
        "sgrqk,sqgrd->skgd", score_grad, queries, preferred_element_type=jnp.float32
    )
    value_grad = jnp.einsum(
        "sgrqk,sqgrd->skgd",
        prob_full.astype(jnp.bfloat16),
        attended_grad,
        preferred_element_type=jnp.float32,
    )
    projected_grad = jnp.concatenate(
        [
            unrotate(query_grad, cos_query, sin_query),
            unrotate(key_grad, cos_key, sin_key)[:, :, :, None],
            value_grad[:, :, :, None],
        ],
        axis=3,
    )
    projected_grad = projected_grad.astype(jnp.bfloat16).reshape(
        seq_count * length, groups * (repeat_factor + 2) * HEAD_SIZE
    )
    qkv_part = jnp.einsum("td,tc->dc", normed1, projected_grad, preferred_element_type=jnp.float32)
    normed1_grad = narrow(
        jnp.einsum("tc,dc->td", projected_grad, qkv_full, preferred_element_type=jnp.float32)
    )
    attn_gain_part = jnp.sum(normed1_grad * residual * scale_attn, axis=0)
    input_grad = (hidden1_grad + norm_back(residual, scale_attn, gain_attn, normed1_grad)).astype(
        jnp.bfloat16
    )
    attn_gain_total, mlp_gain_total = lax.psum((attn_gain_part, mlp_gain_part), "tensor")
    attn_gain_grad, qkv_grad, gate_grad, up_grad, mlp_gain_grad = (
        lax.psum_scatter(
            attn_gain_total.astype(jnp.bfloat16), "dp", scatter_dimension=0, tiled=True
        ).astype(jnp.float32),
        lax.psum_scatter(
            qkv_part.astype(jnp.bfloat16), "dp", scatter_dimension=0, tiled=True
        ).astype(jnp.float32),
        lax.psum_scatter(
            gate_part.astype(jnp.bfloat16), "dp", scatter_dimension=0, tiled=True
        ).astype(jnp.float32),
        lax.psum_scatter(
            up_part.astype(jnp.bfloat16), "dp", scatter_dimension=0, tiled=True
        ).astype(jnp.float32),
        lax.psum_scatter(
            mlp_gain_total.astype(jnp.bfloat16), "dp", scatter_dimension=0, tiled=True
        ).astype(jnp.float32),
    )
    out_grad, down_grad = (
        lax.psum_scatter(
            out_part.astype(jnp.bfloat16), "dp", scatter_dimension=1, tiled=True
        ).astype(jnp.float32),
        lax.psum_scatter(
            down_part.astype(jnp.bfloat16), "dp", scatter_dimension=1, tiled=True
        ).astype(jnp.float32),
    )
    return (
        block_out,
        input_grad,
        attn_gain_grad,
        qkv_grad,
        out_grad,
        mlp_gain_grad,
        gate_grad,
        up_grad,
        down_grad,
    )


GROUP = 4
WINDOW = 256
LANES = 384
TILE = 128


MESH = pl.DeviceIdType.MESH


class Transfer:
    def __init__(self, copy, sends=None, receives=None):
        self.copy, self.sends, self.receives = copy, sends, receives

    def _when(self, condition, action):
        if condition is None:
            action()
        else:
            pl.when(condition)(action)

    def start(self):
        self._when(self.sends, self.copy.start)
        return self

    def wait_recv(self):
        self._when(self.receives, self.copy.wait_recv)

    def wait_send(self):
        self._when(self.sends, self.copy.wait_send)


class Links:
    def __init__(self, n_dp, n_tensor, out_sems, in_sems, local_sems):
        self.n_dp, self.n_tensor = n_dp, n_tensor
        self.out_sems, self.in_sems, self.local_sems = out_sems, in_sems, local_sems
        self.d_at, self.z_at = lax.axis_index("dp"), lax.axis_index("tensor")
        self.used, self.used_local = 0, 0
        self.sent, self.saved = [], []

    def barrier(self):
        barrier = pltpu.get_barrier_semaphore()
        for k in range(1, self.n_dp):
            pl.semaphore_signal(
                barrier,
                inc=1,
                device_id={"dp": self.d_at ^ k, "tensor": self.z_at},
                device_id_type=MESH,
            )
        for s in range(1, self.n_tensor):
            pl.semaphore_signal(
                barrier,
                inc=1,
                device_id={"dp": self.d_at, "tensor": lax.rem(self.z_at + s, self.n_tensor)},
                device_id_type=MESH,
            )
        pl.semaphore_wait(barrier, self.n_dp - 1 + self.n_tensor - 1)

    def plan(self, source, target, bit=0, shift=0, sends=None, receives=None):
        slot = self.used
        self.used += 1
        copy = pltpu.make_async_remote_copy(
            src_ref=source,
            dst_ref=target,
            send_sem=self.out_sems.at[slot],
            recv_sem=self.in_sems.at[slot],
            device_id={
                "dp": self.d_at ^ bit,
                "tensor": lax.rem(self.z_at + self.n_tensor + shift, self.n_tensor),
            },
            device_id_type=MESH,
        )
        transfer = Transfer(copy, sends, receives)
        self.sent.append(transfer)
        return transfer

    def send(self, source, target, bit=0, shift=0):
        return self.plan(source, target, bit, shift).start()

    def move(self, source, target):
        copy = pltpu.make_async_copy(source, target, self.local_sems.at[self.used_local])
        self.used_local += 1
        copy.start()
        return copy

    def save(self, source, target):
        self.saved.append(self.move(source, target))

    def finish(self):
        for transfer in self.sent:
            transfer.wait_send()
        for copy in self.saved:
            copy.wait()


class Spread:
    def __init__(self, links, own_piece, target, columns):
        self.links, self.own_piece, self.target, self.columns = links, own_piece, target, columns
        self.ahead, self.back, self.swaps = [], [], []

    def _slot(self, index):
        n = self.links.n_tensor
        return self.target.at[lax.rem(index + n, n), :, self.columns]

    def issue(self):
        links, n, z = self.links, self.links.n_tensor, self.links.z_at
        own = self._slot(z)
        for s in range(1, n):
            up_from, down_from = z - (s - 1), z + (s - 1)
            up_source = self.own_piece if s == 1 else self._slot(up_from)
            down_source = self.own_piece if s == 1 else self._slot(down_from)
            self.ahead.append(
                links.plan(
                    up_source, self._slot(up_from), shift=1,
                    sends=(z < n - 1) & (up_from >= 0), receives=z >= s,
                )
            )
            self.back.append(
                links.plan(
                    down_source, self._slot(down_from), shift=-1,
                    sends=(z > 0) & (down_from < n), receives=z + s < n,
                )
            )
        self.ahead[0].start()
        self.back[0].start()
        self.swaps.append(links.plan(self.own_piece, own, bit=GROUP).start())

    def step(self, s):
        links, n, z = self.links, self.links.n_tensor, self.links.z_at
        for arrivals, piece, here in (
            (self.ahead, z - s, z >= s),
            (self.back, z + s, z + s < n),
        ):
            arrivals[s - 1].wait_recv()
            if s < n - 1:
                arrivals[s].start()
            slot = self._slot(piece)
            self.swaps.append(
                links.plan(slot, slot, bit=GROUP, sends=here, receives=here).start()
            )

    def wait(self):
        for swap in self.swaps:
            swap.wait_recv()


def kernel_forward(
    n_dp, n_tensor,
    tokens, cot, gate_w, up_w, down_w, out_w, qkv_w, segments, gain_rows, fixed,
    normed1_out, normed2_out, hidden_out, query_out, keyval_out, log_out, att_out,
    cos_out, sin_out, qkv_out, out_out, small_out, cot_out, gate_out, up_out, down_out,
    x_all, n1_all, first, dealt, first_piece, qkv, out_parcel, obuf, gbuf, ubuf, dbuf, piece, outw,
    small, small_all, stream, parts, recv, queries, keyvals,
    att, by_repeat, logs, cosine, sine, low_col, to_core, from_core, to_across, from_across,
    hidden, n2_all, stage, out_sems, in_sems, local_sems,
):
    f32, bf16 = jnp.float32, jnp.bfloat16
    links = Links(n_dp, n_tensor, out_sems, in_sems, local_sems)
    send, move, save = links.send, links.move, links.save
    d_at, z_at = links.d_at, links.z_at
    member = d_at % GROUP
    core = d_at % 2
    upper = d_at // GROUP
    rows, width = tokens.shape
    half = width // 2
    chunk = qkv_w.shape[0]
    contract = (((1,), (1,)), ((), ()))
    columns = pl.ds(pl.multiple_of(upper * half, half), half)

    turned = qkv_w[...].T
    quarter = turned.shape[0] // GROUP
    for i in range(GROUP):
        first[i] = turned[i * quarter : (i + 1) * quarter]
    turned = out_w[...].T
    out_quarter = turned.shape[0] // GROUP
    for i in range(GROUP):
        out_parcel[i] = turned[i * out_quarter : (i + 1) * out_quarter]
    ids = segments[...]
    seqs, length = ids.shape
    begin = jnp.zeros_like(ids)
    for value in range(3):
        count = jnp.sum((ids == value).astype(jnp.int32), axis=1, keepdims=True)
        begin = begin + jnp.where(ids > value, count, 0)
    begin = begin.astype(f32)
    for i in range(seqs):
        stream[:, i * length : (i + 1) * length] = jnp.broadcast_to(
            begin[i : i + 1] + float(i * length), (stream.shape[0], length)
        )
    window = stream[:, pl.ds(pl.multiple_of(z_at * rows, TILE), rows)]
    here = lax.broadcasted_iota(jnp.int32, window.shape, 1) + z_at * rows
    small[...] = window
    small[0:1] = here.astype(f32)[0:1] - window[0:1]
    small[2:4, :chunk] = gain_rows[...].astype(f32)

    @pl.when(z_at == 0)
    def _():
        keyvals[:, :WINDOW, :] = jnp.zeros_like(keyvals[:, :WINDOW, :])

    links.barrier()

    deals = [send(first.at[member ^ k], dealt.at[member], bit=k) for k in range(1, GROUP)]
    beside = send(tokens, x_all.at[2], bit=1)
    smalls = [send(small, small_all.at[d_at], bit=k) for k in range(1, n_dp)]
    def columns_of(ref, at):
        size = ref.shape[1] // GROUP
        return ref.at[:, pl.ds(pl.multiple_of(at * size, TILE), size)]

    def parcel_of(ref, at):
        return ref.at[at]

    pairs = [
        (out_parcel, obuf, parcel_of), (gate_w, gbuf, columns_of), (up_w, ubuf, columns_of),
        (down_w, dbuf, columns_of),
    ]

    def deal(group):
        return [
            send(take(ref, member ^ k), buffer.at[member], bit=k)
            for ref, buffer, take in group
            for k in range(1, GROUP)
        ]

    rests = deal(pairs[:2])
    across = send(tokens, x_all.at[1], bit=2)
    late_rests = deal(pairs[2:])
    own = [move(tokens, x_all.at[0])]
    for ref, buffer, take in pairs:
        own.append(move(take(ref, member), buffer.at[member]))
    cot_stage = move(cot, stage)
    small_all[d_at] = small[...]
    dealt[member] = first[member]

    entries = lax.broadcasted_iota(jnp.int32, (WINDOW, LANES), 0).astype(f32)
    angles = entries * fixed[0:1]

    def split(table):
        pieces = []
        for _ in range(3):
            pieces.append(table.astype(bf16))
            table = table - pieces[-1].astype(f32)
        return pieces

    cos_parts, sin_parts = split(jnp.cos(angles)), split(jnp.sin(angles))
    second = fixed[1:2]
    own_turns = jnp.where(core == 0, jnp.ones_like(second), fixed[2:3])

    for copy in deals:
        copy.wait_recv()
    for i in range(GROUP):
        first_piece[:, i * chunk : (i + 1) * chunk] = dealt[i]
    spread_first = Spread(links, first_piece, qkv, columns)
    spread_first.issue()
    save(first_piece, qkv.at[z_at, :, columns])
    own_qkv = links.saved.pop()
    for copy in own:
        copy.wait()
    cot_stage.wait()
    save(stage, cot_out.at[0])
    spread_first.step(1)
    for copy in smalls:
        copy.wait_recv()
    spread_first.step(2)
    gains = []
    for row in (2, 3):
        gains.append(
            jnp.concatenate([small_all[i, row : row + 1, :chunk] for i in range(n_dp)], axis=1)
        )
    for copy in rests:
        copy.wait_recv()
    sizes = [obuf.shape[1], gbuf.shape[2], ubuf.shape[2], dbuf.shape[2]]
    starts = [sum(sizes[:i]) for i in range(len(sizes))]
    saves = []

    def prepare(index, target, buffer):
        at = slice(starts[index], starts[index] + sizes[index])
        for i in range(GROUP):
            piece[at, i * chunk : (i + 1) * chunk] = buffer[i] if index == 0 else buffer[i].T
        own_piece = piece.at[pl.ds(starts[index], sizes[index])]
        saves.append(move(own_piece, target.at[z_at, :, columns]))
        return Spread(links, own_piece, target, columns)

    out_spread = prepare(0, outw, obuf)
    gate_spread = prepare(1, gate_out, gbuf)
    out_spread.issue()
    spread_first.step(3)
    gate_spread.issue()
    beside.wait_recv()
    own_qkv.wait()
    spread_first.wait()

    def project_block(m, k):
        features = x_all[m].astype(f32)
        scale = lax.rsqrt(jnp.mean(features * features, axis=1, keepdims=True) + EPS)
        normal = (features * scale * gains[0]).astype(bf16)
        n1_all[m] = normal
        units = qkv.shape[0] * qkv.shape[1]
        product = lax.dot_general(
            normal, qkv[...].reshape(units, width), contract, preferred_element_type=f32
        )
        info = small_all[d_at ^ k].T
        key = lax.broadcasted_iota(jnp.int32, (rows, WINDOW), 1)
        chosen = (info[:, 0:1].astype(jnp.int32) == key).astype(bf16)

        def pick(table):
            total = jnp.dot(chosen, table[0], preferred_element_type=f32)
            for part in table[1:]:
                total += jnp.dot(chosen, part, preferred_element_type=f32)
            return total

        cos_here, sin_here = pick(cos_parts), pick(sin_parts)
        parts[m] = turn(product, cos_here, sin_here, second, own_turns, 1.0).astype(bf16)
        if m < 2:
            cosine[m] = cos_here
            sine[m] = sin_here
            low_col[m] = info[:, 1:2].astype(jnp.int32) - z_at * rows + WINDOW

    is_first = core == 0
    halos = [
        links.plan(
            keyvals.at[m, pl.ds(rows, WINDOW)], keyvals.at[m, pl.ds(0, WINDOW)], shift=1,
            sends=z_at < n_tensor - 1, receives=z_at > 0,
        )
        for m in range(2)
    ]

    def take_block(m, swap):
        swap.wait_recv()
        mine, other = parts[m], recv[m]
        queries[m] = jnp.where(is_first, mine, other)
        keyvals[m, WINDOW:, :] = jnp.where(is_first, other, mine)
        halos[m].start()

    project_block(2, 1)
    part_swap = send(parts.at[2], recv.at[0], bit=1)
    project_block(0, 0)
    take_block(0, part_swap)
    out_spread.step(1)
    across.wait_recv()
    both = send(x_all.at[1], x_all.at[3], bit=1)
    cot_across = send(cot, cot_out.at[1], bit=2)
    cot_beside = send(cot, cot_out.at[2], bit=1)
    out_spread.step(2)
    project_block(1, 2)
    both.wait_recv()
    project_block(3, 3)
    part_swap = send(parts.at[3], recv.at[1], bit=1)
    out_spread.step(3)
    save(n1_all, normed1_out)
    save(cosine, cos_out)
    save(sine, sin_out)
    take_block(1, part_swap)
    gate_spread.step(1)
    for copy in late_rests:
        copy.wait_recv()
    up_spread = prepare(2, up_out, ubuf)
    down_spread = prepare(3, down_out, dbuf)
    up_spread.issue()
    save(queries, query_out)
    heads = queries.shape[2] // HEAD_SIZE
    repeat = QUERY_HEADS // KEY_VALUE_HEADS
    span = TILE + WINDOW

    def attend_tile(m, start):
        key = lax.broadcasted_iota(jnp.int32, (TILE, span), 1)
        query = lax.broadcasted_iota(jnp.int32, (TILE, span), 0)
        lowest = low_col[m, pl.ds(start, TILE), :] - start
        allowed = (key >= lowest) & (key <= query + WINDOW)
        for head in range(heads):
            group, r = head // repeat, head % repeat
            base = group * 2 * HEAD_SIZE
            q = queries[m, pl.ds(start, TILE), head * HEAD_SIZE : (head + 1) * HEAD_SIZE]
            k = keyvals[m, pl.ds(start, span), base : base + HEAD_SIZE]
            v = keyvals[m, pl.ds(start, span), base + HEAD_SIZE : base + 2 * HEAD_SIZE]
            s = lax.dot_general(q, k, contract, preferred_element_type=f32) * HEAD_SIZE ** (-0.5)
            s = jnp.where(allowed, s, NEG_FILL)
            highest = jnp.max(s, axis=1, keepdims=True)
            e = jnp.exp(s - highest)
            whole = jnp.sum(e, axis=1, keepdims=True)
            p = (e * (1.0 / whole)).astype(bf16)
            o = jnp.dot(p, v, preferred_element_type=f32).astype(bf16)
            logs[m, pl.ds(start, TILE), head : head + 1] = highest + jnp.log(whole)
            by_repeat[r, m, pl.ds(start, TILE), group * HEAD_SIZE : (group + 1) * HEAD_SIZE] = o

    tiles = rows // TILE
    free = -(-WINDOW // TILE)
    for tile in range(free, tiles):
        attend_tile(1, tile * TILE)
        attend_tile(0, tile * TILE)
    halos[0].wait_recv()
    halos[1].wait_recv()
    for tile in range(free):
        attend_tile(1, tile * TILE)
    att_swap1 = send(by_repeat.at[1 - core, 1], att.at[3], bit=1)
    gate_spread.step(2)
    for tile in range(free):
        attend_tile(0, tile * TILE)
    att_swap0 = send(by_repeat.at[1 - core, 0], att.at[2], bit=1)
    gate_spread.step(3)
    save(keyvals, keyval_out)
    save(logs, log_out)
    att[0] = by_repeat[core, 0]
    att[1] = by_repeat[core, 1]
    down_spread.issue()
    cot_across.wait_recv()
    cot_both = send(cot_out.at[1], cot_out.at[3], bit=1)

    saves[0].wait()
    out_spread.wait()

    def project_out(b):
        units = outw.shape[0] * outw.shape[1]
        return jnp.dot(att[b], outw[...].reshape(units, width), preferred_element_type=f32)

    att_swap1.wait_recv()
    to_core[1] = project_out(3).astype(bf16)
    core_send1 = send(to_core.at[1], from_core.at[1], bit=1)
    hidden[...] = project_out(1)
    att_swap0.wait_recv()
    to_core[0] = project_out(2).astype(bf16)
    core_send0 = send(to_core.at[0], from_core.at[0], bit=1)
    core_send1.wait_recv()
    across_sends = []
    for i in range(tiles):
        at = pl.ds(i * TILE, TILE)
        to_across[at] = (hidden[at, :] + from_core[1, at, :].astype(f32)).astype(bf16)
        across_sends.append(send(to_across.at[at], from_across.at[at], bit=2))
    hidden[...] = project_out(0) + x_all[0].astype(f32)
    core_send0.wait_recv()
    hidden[...] += from_core[0].astype(f32)
    save(att, att_out)
    up_spread.step(1)
    steps = [
        (up_spread, 2), (up_spread, 3), (down_spread, 1), (down_spread, 2), (down_spread, 3),
    ]
    last = []
    for i in range(tiles):
        at = pl.ds(i * TILE, TILE)
        across_sends[i].wait_recv()
        value = hidden[at, :] + from_across[at, :].astype(f32)
        hidden[at, :] = value
        scale = lax.rsqrt(jnp.mean(value * value, axis=1, keepdims=True) + EPS)
        n2_all[0, at, :] = (value * scale * gains[1]).astype(bf16)
        last.append(send(n2_all.at[0, at], n2_all.at[1, at], bit=2))
        last.append(send(n2_all.at[0, at], n2_all.at[2, at], bit=1))
        if i < 3:
            spread, s = steps.pop(0)
            spread.step(s)
    save(hidden, hidden_out)
    save(qkv, qkv_out)
    save(outw, out_out)
    save(small_all, small_out)
    ends = []
    for i in range(tiles):
        at = pl.ds(i * TILE, TILE)
        last[2 * i].wait_recv()
        ends.append(send(n2_all.at[1, at], n2_all.at[3, at], bit=1))
        if i < 2:
            spread, s = steps.pop(0)
            spread.step(s)
    for copy in ends + last[1::2]:
        copy.wait_recv()
    save(n2_all, normed2_out)
    for copy in saves[1:]:
        copy.wait()
    for spread in (gate_spread, up_spread, down_spread):
        spread.wait()
    for copy in (cot_beside, cot_both):
        copy.wait_recv()
    links.finish()


def forward(
    n_dp, n_tensor, tokens, cot, segments, gain_rows, qkv_w, out_w, gate_w, up_w, down_w
):
    out_w, down_w = out_w.T, down_w.T
    rows, width = tokens.shape
    f32, bf16 = jnp.float32, jnp.bfloat16
    vmem = pl.BlockSpec(memory_space=pltpu.VMEM)
    hbm = pl.BlockSpec(memory_space=pl.ANY)
    chunk = qkv_w.shape[0]
    quarter = qkv_w.shape[1] // GROUP
    sizes = [
        out_w.shape[1] // GROUP, gate_w.shape[1] // GROUP, up_w.shape[1] // GROUP,
        down_w.shape[1] // GROUP,
    ]
    units = quarter * n_tensor
    heads = units // HEAD_SIZE
    lane = np.arange(LANES)
    within = lane % HEAD_SIZE
    fixed = np.zeros((8, LANES), np.float32)
    fixed[0] = np.power(ROPE_BASE, -(2.0 * (within % (HEAD_SIZE // 2))) / HEAD_SIZE)
    fixed[1] = within >= HEAD_SIZE // 2
    fixed[2] = lane % (2 * HEAD_SIZE) < HEAD_SIZE
    fixed[3] = 1.0

    def shape(dims, dtype=bf16):
        return jax.ShapeDtypeStruct(tuple(dims), dtype)

    full = (GROUP, rows, width)
    qkv_shape = (n_tensor, quarter, width)
    out_shape = (n_tensor, sizes[0], width)
    att_shape = (GROUP, rows, units // 2)
    small_shape = (n_dp, 8, rows)
    table = (2, rows, LANES)
    outs = [
        shape(full),
        shape(full),
        shape((rows, width), f32),
        shape((2, rows, units)),
        shape((2, rows + WINDOW, units)),
        shape((2, rows, heads), f32),
        shape(att_shape),
        shape(table, f32),
        shape(table, f32),
        shape(qkv_shape),
        shape(out_shape),
        shape(small_shape, f32),
        shape(full),
    ] + [shape((n_tensor, size, width)) for size in sizes[1:]]
    scratch = [
        pltpu.VMEM(full, bf16),
        pltpu.VMEM(full, bf16),
        pltpu.VMEM((GROUP, quarter, chunk), bf16),
        pltpu.VMEM((GROUP, quarter, chunk), bf16),
        pltpu.VMEM((quarter, width // 2), bf16),
        pltpu.VMEM(qkv_shape, bf16),
        pltpu.VMEM((GROUP, sizes[0], chunk), bf16),
        pltpu.VMEM((GROUP, sizes[0], chunk), bf16),
        pltpu.VMEM((GROUP, chunk, sizes[1]), bf16),
        pltpu.VMEM((GROUP, chunk, sizes[2]), bf16),
        pltpu.VMEM((GROUP, chunk, sizes[3]), bf16),
        pltpu.VMEM((sum(sizes), width // 2), bf16),
        pltpu.VMEM(out_shape, bf16),
        pltpu.VMEM((8, rows), f32),
        pltpu.VMEM(small_shape, f32),
        pltpu.VMEM((8, n_tensor * rows), f32),
        pltpu.VMEM((GROUP, rows, units), bf16),
        pltpu.VMEM((2, rows, units), bf16),
        pltpu.VMEM((2, rows, units), bf16),
        pltpu.VMEM((2, rows + WINDOW, units), bf16),
        pltpu.VMEM(att_shape, bf16),
        pltpu.VMEM((2, 2, rows, units // 2), bf16),
        pltpu.VMEM((2, rows, heads), f32),
        pltpu.VMEM(table, f32),
        pltpu.VMEM(table, f32),
        pltpu.VMEM((2, rows, 1), jnp.int32),
        pltpu.VMEM((2, rows, width), bf16),
        pltpu.VMEM((2, rows, width), bf16),
        pltpu.VMEM((rows, width), bf16),
        pltpu.VMEM((rows, width), bf16),
        pltpu.VMEM((rows, width), f32),
        pltpu.VMEM(full, bf16),
        pltpu.VMEM((rows, width), bf16),
        pltpu.SemaphoreType.DMA((128,)),
        pltpu.SemaphoreType.DMA((128,)),
        pltpu.SemaphoreType.DMA((40,)),
    ]
    results = pl.pallas_call(
        functools.partial(kernel_forward, n_dp, n_tensor),
        in_specs=[hbm] * 5 + [vmem] * 5,
        out_specs=[hbm] * len(outs),
        out_shape=outs,
        scratch_shapes=scratch,
        compiler_params=pltpu.CompilerParams(
            collective_id=0, has_side_effects=True, vmem_limit_bytes=60 * 1024 * 1024
        ),
        name="forward",
    )(
        tokens, cot, gate_w, up_w, down_w, out_w, qkv_w, segments, gain_rows, jnp.asarray(fixed)
    )
    return results, jnp.asarray(fixed)


def turn(value, cosine, sine, second, turns, sign):
    width = value.shape[1]
    half = HEAD_SIZE // 2
    c = turns * cosine + (1.0 - turns)
    u = (sign * turns * second) * sine
    d = (sign * turns * (second - 1.0)) * sine
    pieces = []
    up = pltpu.roll(value, half, 1)
    down = pltpu.roll(value, width - half, 1)
    for i in range(width // LANES):
        at = slice(i * LANES, (i + 1) * LANES)
        pieces.append(value[:, at] * c + up[:, at] * u + down[:, at] * d)
    return jnp.concatenate(pieces, axis=1)


def kernel_feed(
    n_dp, n_tensor,
    n2_in, cot_in, hidden_in, gate_in, up_in, down_in, smalls,
    grad_out, grad_own_out, mlp_out, down_out, gate_out, up_out, down_got, row_out,
    n2_all, cot_all, gate_w, up_w, down_w, active, gate_delta, up_delta,
    down_part, gate_part, up_part, to_core, from_core, to_across, from_across, hidden, total,
    rounded, row, out_sems, in_sems, local_sems,
):
    f32, bf16 = jnp.float32, jnp.bfloat16
    links = Links(n_dp, n_tensor, out_sems, in_sems, local_sems)
    send, move, save = links.send, links.move, links.save
    upper = links.d_at // GROUP
    rows, width = hidden.shape
    half = width // 2
    chunk = width // n_dp
    size = gate_w.shape[1]
    units = n_tensor * size
    contract = (((1,), (1,)), ((), ()))
    over_rows = (((0,), (0,)), ((), ()))
    other = pl.ds(pl.multiple_of((1 - upper) * half, half), half)
    tiles = rows // TILE

    loads = [
        move(gate_in, gate_w), move(n2_in, n2_all), move(up_in, up_w), move(down_in, down_w),
        move(cot_in, cot_all), move(hidden_in, hidden),
    ]
    links.barrier()
    for copy in loads[:-1]:
        copy.wait()

    def inner(i, carry):
        m, p = i // n_tensor, i % n_tensor
        at = pl.ds(pl.multiple_of(p * size, TILE), size)
        gate = lax.dot_general(n2_all[m], gate_w[p], contract, preferred_element_type=f32)
        up_value = lax.dot_general(n2_all[m], up_w[p], contract, preferred_element_type=f32)
        act_grad = lax.dot_general(cot_all[m], down_w[p], contract, preferred_element_type=f32)
        sigmoid = jax.nn.sigmoid(gate)
        silu = gate * sigmoid
        active[m, :, at] = (silu * up_value).astype(bf16)
        gate_delta[m, :, at] = (
            act_grad * up_value * sigmoid * (1.0 + gate * (1.0 - sigmoid))
        ).astype(bf16)
        up_delta[m, :, at] = (act_grad * silu).astype(bf16)
        return carry

    lax.fori_loop(0, GROUP * n_tensor, inner, 0)

    def back(m):
        return jnp.dot(
            gate_delta[m], gate_w[...].reshape(units, width), preferred_element_type=f32
        ) + jnp.dot(up_delta[m], up_w[...].reshape(units, width), preferred_element_type=f32)

    to_core[1] = back(3).astype(bf16)
    core_send1 = send(to_core.at[1], from_core.at[1], bit=1)
    total[...] = back(1)
    core_send1.wait_recv()
    across = []
    for i in range(tiles):
        at = pl.ds(i * TILE, TILE)
        to_across[at] = (total[at, :] + from_core[1, at, :].astype(f32)).astype(bf16)
        across.append(send(to_across.at[at], from_across.at[at], bit=2))
    to_core[0] = back(2).astype(bf16)
    core_send0 = send(to_core.at[0], from_core.at[0], bit=1)
    total[...] = back(0)

    order = []
    for i in range((n_tensor + 1) // 2):
        order.extend(dict.fromkeys((n_tensor - 1 - i, i)))

    def grads(left, right, part, target, weight=None):
        for p in order:
            at = slice(p * size, (p + 1) * size)
            grad = lax.dot_general(
                left[...].reshape(GROUP * rows, units)[:, at],
                right[...].reshape(GROUP * rows, width),
                over_rows,
                preferred_element_type=f32,
            )
            part[p] = grad.astype(bf16)
            if weight is not None:
                row[...] += jnp.sum(grad * weight[p].astype(f32), axis=0, keepdims=True)
            elif p in order[: n_tensor // 2]:
                swaps.append(send(part.at[p, :, other], down_got.at[p], bit=GROUP))
            save(part.at[p], target.at[p])

    swaps = []
    row[...] = jnp.zeros_like(row)
    grads(active, cot_all, down_part, down_out)
    core_send0.wait_recv()
    total[...] += from_core[0].astype(f32)
    grads(gate_delta, n2_all, gate_part, gate_out, gate_w)
    grads(up_delta, n2_all, up_part, up_out, up_w)
    save(row, row_out)
    for m in range(GROUP):
        n2_all[m] = jnp.dot(
            active[m], down_w[...].reshape(units, width), preferred_element_type=f32
        ).astype(bf16)
        save(n2_all.at[m], mlp_out.at[m])
    gain = jnp.concatenate([smalls[i, 3:4, :chunk] for i in range(n_dp)], axis=1)
    loads[-1].wait()
    for i in range(tiles):
        at = pl.ds(i * TILE, TILE)
        across[i].wait_recv()
        upstream = total[at, :] + from_across[at, :].astype(f32)
        features = hidden[at, :]
        inverse = lax.rsqrt(jnp.mean(features * features, axis=1, keepdims=True) + EPS)
        scaled = gain * upstream
        mean = jnp.mean(scaled * features, axis=1, keepdims=True)
        result = cot_all[0, at, :].astype(f32) + (
            inverse * scaled - features * (inverse * inverse * inverse) * mean
        )
        total[at, :] = result
        rounded[at, :] = result.astype(bf16)
    save(total, grad_out)
    save(rounded, grad_own_out)
    for copy in swaps:
        copy.wait_recv()
    links.finish()


def feed(n_dp, n_tensor, normed2, grad_rows, hidden1, gate_w, up_w, down_w, smalls):
    f32, bf16 = jnp.float32, jnp.bfloat16
    rows, width = hidden1.shape
    half = width // 2
    vmem = pl.BlockSpec(memory_space=pltpu.VMEM)
    hbm = pl.BlockSpec(memory_space=pl.ANY)
    weight = gate_w.shape
    inner = (GROUP, rows, n_tensor * weight[1])

    def shape(dims, dtype=bf16):
        return jax.ShapeDtypeStruct(tuple(dims), dtype)

    outs = [
        shape((rows, width), f32), shape((rows, width)), shape(normed2.shape),
        shape(weight), shape(weight), shape(weight), shape((n_tensor, weight[1], half)),
        shape((1, width), f32),
    ]
    scratch = [
        pltpu.VMEM(normed2.shape, bf16),
        pltpu.VMEM(normed2.shape, bf16),
        pltpu.VMEM(weight, bf16),
        pltpu.VMEM(weight, bf16),
        pltpu.VMEM(weight, bf16),
        pltpu.VMEM(inner, bf16),
        pltpu.VMEM(inner, bf16),
        pltpu.VMEM(inner, bf16),
        pltpu.VMEM(weight, bf16),
        pltpu.VMEM(weight, bf16),
        pltpu.VMEM(weight, bf16),
        pltpu.VMEM((2, rows, width), bf16),
        pltpu.VMEM((2, rows, width), bf16),
        pltpu.VMEM((rows, width), bf16),
        pltpu.VMEM((rows, width), bf16),
        pltpu.VMEM((rows, width), f32),
        pltpu.VMEM((rows, width), f32),
        pltpu.VMEM((rows, width), bf16),
        pltpu.VMEM((1, width), f32),
        pltpu.SemaphoreType.DMA((16,)),
        pltpu.SemaphoreType.DMA((16,)),
        pltpu.SemaphoreType.DMA((40,)),
    ]
    return pl.pallas_call(
        functools.partial(kernel_feed, n_dp, n_tensor),
        in_specs=[hbm] * 6 + [vmem],
        out_specs=[hbm] * len(outs),
        out_shape=outs,
        scratch_shapes=scratch,
        compiler_params=pltpu.CompilerParams(
            collective_id=2, has_side_effects=True, vmem_limit_bytes=67043328
        ),
        name="feed",
    )(normed2, grad_rows, hidden1, gate_w, up_w, down_w, smalls)


class Collect:
    def __init__(
        self, links, part, swapped, stage, arrived, late, blocks, target, mine, other, turned=False
    ):
        self.turned = turned
        self.links, self.part, self.swapped, self.stage = links, part, swapped, stage
        self.arrived, self.late, self.blocks, self.target = arrived, late, blocks, target
        self.mine, self.other = mine, other
        self.swaps, self.loads, self.deals = {}, [], []

    def issue(self, order):
        links = self.links
        for p in order:
            self.swaps[p] = links.send(
                self.part.at[p, :, self.other], self.swapped.at[p], bit=GROUP
            )
        if self.stage is not None:
            self.loads = [links.move(self.part.at[:, :, self.mine], self.stage)]

    def load(self, received, order):
        links = self.links
        count = links.n_tensor // 2
        self.issue(order[count:])
        self.loads += [links.move(received.at[p], self.swapped.at[p]) for p in order[:count]]

    def step(self, p):
        links, n, z = self.links, self.links.n_tensor, self.links.z_at
        f32, bf16 = jnp.float32, jnp.bfloat16
        while self.loads:
            self.loads.pop().wait()
        if p in self.swaps:
            self.swaps[p].wait_recv()
        own = self.stage[p] if self.stage is not None else self.part[p, :, self.mine]
        self.swapped[p] = (own.astype(f32) + self.swapped[p].astype(f32)).astype(bf16)
        if not hasattr(self, "ahead"):
            self.ahead, self.back, self.back_last = [None] * n, [None] * n, [None] * n
        source = self.swapped.at[p]
        self.ahead[p] = links.plan(
            source, self.arrived.at[p], shift=1, sends=z < p, receives=(z > 0) & (z <= p)
        )
        self.back[p] = links.plan(
            source, self.arrived.at[p], shift=-1, sends=z > p + 1,
            receives=(z > p) & (z < n - 1),
        )
        self.back_last[p] = links.plan(
            source, self.late, shift=-1, sends=z == p + 1, receives=(z == p) & (z < n - 1)
        )

        @pl.when((z == 0) & (z < p))
        def _():
            self.ahead[p].copy.start()

        @pl.when((z == n - 1) & (z > p + 1))
        def _():
            self.back[p].copy.start()

        @pl.when((z == n - 1) & (z == p + 1))
        def _():
            self.back_last[p].copy.start()

    def relay(self, i):
        links, n, z = self.links, self.links.n_tensor, self.links.z_at
        f32, bf16 = jnp.float32, jnp.bfloat16

        def add(p):
            self.swapped[p] = (
                self.swapped[p].astype(f32) + self.arrived[p].astype(f32)
            ).astype(bf16)

        for p in range(n):
            at = i - (n - 1) + p
            if 0 < at < n - 1 and at < p:

                @pl.when(z == at)
                def _(p=p):
                    self.ahead[p].copy.wait_recv()
                    add(p)
                    self.ahead[p].copy.start()

            at = n - 1 - i + p
            if 0 < at < n - 1 and at > p:

                @pl.when(z == at)
                def _(p=p, at=at):
                    self.back[p].copy.wait_recv()
                    add(p)
                    (self.back_last if at == p + 1 else self.back)[p].copy.start()

    def finish(self):
        links, n, z = self.links, self.links.n_tensor, self.links.z_at
        f32, bf16 = jnp.float32, jnp.bfloat16
        member = links.d_at % GROUP
        for p in range(n):

            @pl.when((z == p) & (z > 0))
            def _(p=p):
                self.ahead[p].copy.wait_recv()

            @pl.when((z == p) & (z < n - 1))
            def _(p=p):
                self.back_last[p].copy.wait_recv()

        below = jnp.where(z > 0, self.arrived[z].astype(f32), 0.0)
        above = jnp.where(z < n - 1, self.late[...].astype(f32), 0.0)
        total = (self.swapped[z].astype(f32) + below + above).astype(bf16)
        chunk = total.shape[1] // GROUP
        size = self.blocks.shape[2 if self.turned else 1]
        place = pl.ds(pl.multiple_of(member * size, 16), size)
        if self.turned:
            place = pl.ds(pl.multiple_of(member * size, TILE), size)
        for i in range(GROUP):
            block = total[:, i * chunk : (i + 1) * chunk]
            self.blocks[i] = block.T if self.turned else block
        if self.turned:
            target = self.target.at[:, place]
        elif len(self.target.shape) == 2:
            target = self.target.at[place, :]
        else:
            target = self.target.at[member]
        for k in range(1, GROUP):
            self.deals.append(links.send(self.blocks.at[member ^ k], target, bit=k))
        links.save(self.blocks.at[member], target)

    def wait(self):
        for deal in self.deals:
            deal.wait_recv()


def kernel_backward(
    n_dp, n_tensor,
    grad_own, hidden_grad, tokens, hidden1, mlp_part, n1_in, query_in, keyval_in, log_in, att_in,
    cos_in, sin_in, qkv_in, out_in, small_in, down_in, gate_in, up_in, down_got,
    mlp_row, fixed,
    input_out, block_out, qkv_out, out_out, gate_out, up_out, down_out,
    g_all, n1_all, qkv, outw, queries, keyvals, logs, att, cosine, sine, gains, low_col,
    att_grad, other_grad, totals, query_total, pass_on, delta, halo_send, halo_recv,
    to_core, from_core, to_across, from_across, mlp_across, hidden, stage, gate_stage,
    down_swap, gate_swap, up_swap, out_swap, qkv_swap,
    down_come, gate_come, up_come, out_come, qkv_come,
    down_late, gate_late, up_late, out_late, qkv_late,
    down_block, gate_block, up_block, out_block, qkv_block,
    out_sems, in_sems, local_sems,
):
    f32, bf16 = jnp.float32, jnp.bfloat16
    links = Links(n_dp, n_tensor, out_sems, in_sems, local_sems)
    send, move, save = links.send, links.move, links.save
    d_at, z_at = links.d_at, links.z_at
    core = d_at % 2
    upper = d_at // GROUP
    rows, width = grad_own.shape
    half = width // 2
    contract = (((1,), (1,)), ((), ()))
    over_rows = (((0,), (0,)), ((), ()))
    mine = pl.ds(pl.multiple_of(upper * half, half), half)
    other = pl.ds(pl.multiple_of((1 - upper) * half, half), half)
    tiles = rows // TILE
    span = TILE + WINDOW
    quarter = qkv.shape[1]
    out_quarter = outw.shape[1]
    extra = qkv_swap.shape[1] - quarter

    loads = [
        move(grad_own, g_all.at[0]), move(out_in, outw), move(query_in, queries),
        move(keyval_in, keyvals), move(log_in, logs), move(cos_in, cosine), move(sin_in, sine),
        move(mlp_part.at[pl.ds(0, 2)], to_core), move(hidden1, hidden), move(att_in, att),
        move(qkv_in, qkv), move(n1_in, n1_all),
    ]
    small = pltpu.make_async_copy(small_in, gains, local_sems.at[links.used_local])
    links.used_local += 1
    small.start()
    links.barrier()
    across = send(grad_own, g_all.at[1], bit=2)
    beside = send(grad_own, g_all.at[2], bit=1)
    mlp_core = send(mlp_part.at[pl.ds(2, 2)], from_core, bit=1)
    order = []
    for i in range((n_tensor + 1) // 2):
        order.extend(dict.fromkeys((n_tensor - 1 - i, i)))

    down = Collect(
        links, down_in, down_swap, stage, down_come, down_late, down_block, down_out, mine, other,
        turned=True,
    )
    gate = Collect(
        links, gate_in, gate_swap, gate_stage, gate_come, gate_late, gate_block, gate_out, mine, other,
        turned=True,
    )
    up = Collect(
        links, up_in, up_swap, stage, up_come, up_late, up_block, up_out, mine, other, turned=True
    )
    out_part = g_all.at[:, pl.ds(quarter + extra, out_quarter), :]
    qkv_part = g_all.at[:, pl.ds(0, quarter + extra), :]
    out_collect = Collect(
        links, out_part, out_swap, None, out_come, out_late, out_block, out_out, mine, other
    )
    qkv_collect = Collect(
        links, qkv_part, qkv_swap, None, qkv_come, qkv_late, qkv_block, qkv_out, mine, other
    )
    down.load(down_got, order)
    gate.issue(order)
    small.wait()
    for m, k in ((0, 0), (1, 2)):
        info = gains[d_at ^ k].T
        low_col[m] = info[:, 1:2].astype(jnp.int32) - z_at * rows + WINDOW
    loads[0].wait()
    loads[1].wait()

    def attended_back(b):
        units = outw.shape[0] * outw.shape[1]
        att_grad[b] = lax.dot_general(
            g_all[b], outw[...].reshape(units, width), contract, preferred_element_type=f32
        ).astype(bf16)

    attended_back(0)
    beside.wait_recv()
    attended_back(2)
    grad_swap = send(att_grad.at[2], other_grad.at[0], bit=1)
    first_steps = n_tensor // 2
    for p in order[:first_steps]:
        down.step(p)
    for copy in loads[2:]:
        copy.wait()
    mlp_core.wait_recv()
    heads = queries.shape[2] // HEAD_SIZE
    repeat = QUERY_HEADS // KEY_VALUE_HEADS
    scale = HEAD_SIZE ** (-0.5)
    is_first = core == 0
    second, keys_turn, all_turn = fixed[1:2], fixed[2:3], fixed[3:4]

    def back_tile(m, tile):
        start = tile * TILE
        at = slice(start, start + TILE)
        reach = slice(start, start + span)
        key = lax.broadcasted_iota(jnp.int32, (TILE, span), 1)
        query = lax.broadcasted_iota(jnp.int32, (TILE, span), 0)
        allowed = (key >= low_col[m, at, :] - start) & (key <= query + WINDOW)
        own, others = att_grad[m, at, :], other_grad[m, at, :]
        by_repeat = (jnp.where(is_first, own, others), jnp.where(is_first, others, own))
        for group in range(heads // repeat):
            base = group * 2 * HEAD_SIZE
            k = keyvals[m, reach, base : base + HEAD_SIZE]
            v = keyvals[m, reach, base + HEAD_SIZE : base + 2 * HEAD_SIZE]
            key_sum = None
            for r in range(repeat):
                head = group * repeat + r
                q = queries[m, at, head * HEAD_SIZE : (head + 1) * HEAD_SIZE]
                g = by_repeat[r][:, group * HEAD_SIZE : (group + 1) * HEAD_SIZE]
                s = lax.dot_general(q, k, contract, preferred_element_type=f32) * scale
                total = logs[m, at, head : head + 1]
                p = jnp.exp(jnp.where(allowed, s, NEG_FILL) - total)
                pg = lax.dot_general(g, v, contract, preferred_element_type=f32)
                inner = jnp.sum(p * pg, axis=1, keepdims=True)
                sg = (p * (pg - inner) * scale).astype(bf16)
                query_total[:, head * HEAD_SIZE : (head + 1) * HEAD_SIZE] = jnp.dot(
                    sg, k, preferred_element_type=f32
                )
                dk = lax.dot_general(sg, q, over_rows, preferred_element_type=f32)
                dv = lax.dot_general(p.astype(bf16), g, over_rows, preferred_element_type=f32)
                both = jnp.concatenate([dk, dv], axis=1)
                key_sum = both if key_sum is None else key_sum + both
            totals[m, reach, base : base + 2 * HEAD_SIZE] += key_sum
        turned = turn(
            query_total[...], cosine[m, at, :], sine[m, at, :], second, all_turn, -1.0
        ).astype(bf16)

        @pl.when(is_first)
        def _():
            delta[m, at, :] = turned

        @pl.when(core != 0)
        def _():
            pass_on[m, at, :] = turned

    halos = [
        links.plan(
            halo_send.at[m], halo_recv.at[m], shift=-1, sends=z_at > 0,
            receives=z_at < n_tensor - 1,
        )
        for m in range(2)
    ]

    def send_halo(m):
        halo_send[m] = totals[m, :WINDOW].astype(bf16)
        halos[m].start()

    def finish_block(m):
        halos[m].wait_recv()
        full = totals[m, WINDOW:]
        tail = full[rows - WINDOW :] + jnp.where(
            z_at < n_tensor - 1, halo_recv[m].astype(f32), 0.0
        )
        full = jnp.concatenate([full[: rows - WINDOW], tail], axis=0)
        turned = turn(full, cosine[m], sine[m], second, keys_turn, -1.0).astype(bf16)

        @pl.when(is_first)
        def _():
            pass_on[m] = turned

        @pl.when(core != 0)
        def _():
            delta[m] = turned

        return send(pass_on.at[m], delta.at[2 + m], bit=1)

    free = -(-WINDOW // TILE)
    totals[...] = jnp.zeros_like(totals)
    grad_swap.wait_recv()
    for tile in range(free):
        back_tile(0, tile)
    down.relay(1)
    send_halo(0)
    down.step(order[first_steps])
    for tile in range(free, tiles):
        back_tile(0, tile)
    for p in order[first_steps + 1 :]:
        down.step(p)
    up.issue(order)
    across.wait_recv()
    both = send(g_all.at[1], g_all.at[3], bit=1)
    to_across[...] = (to_core[1].astype(f32) + from_core[1].astype(f32)).astype(bf16)
    mlp_send = send(to_across, mlp_across, bit=2)
    hidden[...] += to_core[0].astype(f32) + from_core[0].astype(f32)
    attended_back(1)
    both.wait_recv()
    attended_back(3)
    grad_swap = send(att_grad.at[3], other_grad.at[1], bit=1)
    gate.step(order[0])

    def weight_grad(left, right, at):
        total = None
        for b in range(GROUP):
            term = lax.dot_general(
                left[b, :, at], right[b], over_rows, preferred_element_type=f32
            )
            total = term if total is None else total + term
        return total

    out_grad = weight_grad(att, g_all, slice(0, n_tensor * out_quarter)).astype(bf16)
    both.wait_send()
    links.sent.remove(both)
    out_part[...] = out_grad.reshape(n_tensor, out_quarter, width)
    grad_swap.wait_recv()
    gate.step(order[1])
    back_tile(1, 0)
    for i in range(2, n_tensor - 1):
        down.relay(i)
    for tile in range(1, free):
        back_tile(1, tile)
    send_halo(1)
    for tile in range(free, tiles):
        back_tile(1, tile)
    for p in order[2 : n_tensor - 1]:
        gate.step(p)
    swap0 = finish_block(0)
    gate.relay(1)
    swap1 = finish_block(1)
    down.finish()
    for p in order[n_tensor - 1 :]:
        gate.step(p)

    def project_back(b):
        units = qkv.shape[0] * quarter
        return jnp.dot(delta[b], qkv[...].reshape(units, width), preferred_element_type=f32)

    mlp_send.wait_recv()
    mlp_across[...] = (hidden[...] + mlp_across[...].astype(f32)).astype(bf16)
    save(mlp_across, block_out)
    mlp_send.wait_send()
    links.sent.remove(mlp_send)
    swap1.wait_recv()
    to_core[1] = project_back(3).astype(bf16)
    core_send1 = send(to_core.at[1], from_core.at[1], bit=1)
    hidden[...] = project_back(1)
    swap0.wait_recv()
    to_core[0] = project_back(2).astype(bf16)
    core_send0 = send(to_core.at[0], from_core.at[0], bit=1)
    core_send1.wait_recv()
    across_sends = []
    for i in range(tiles):
        at = pl.ds(i * TILE, TILE)
        to_across[at] = (hidden[at, :] + from_core[1, at, :].astype(f32)).astype(bf16)
        across_sends.append(send(to_across.at[at], from_across.at[at], bit=2))
    hidden[...] = project_back(0)
    core_send0.wait_recv()
    hidden[...] += from_core[0].astype(f32)
    up.step(order[0])
    attn_row = None
    for p in range(n_tensor):
        at = slice(p * quarter, (p + 1) * quarter)
        grad = weight_grad(delta, n1_all, at)
        row = jnp.sum(grad * qkv[p].astype(f32), axis=0, keepdims=True)
        attn_row = row if attn_row is None else attn_row + row
        qkv_part[p, :quarter, :] = grad.astype(bf16)
    ending = jnp.concatenate(
        [attn_row, mlp_row[...], jnp.zeros((extra - 2, width), f32)], axis=0
    ).astype(bf16)
    for p in range(n_tensor):
        qkv_part[p, quarter:, :] = ending
    qkv_collect.issue(order)
    out_collect.issue(order)
    finals = [
        move(tokens, n1_all.at[0]),
        move(hidden_grad.at[:, pl.ds(0, half)], totals.at[0, pl.ds(0, rows)]),
        move(hidden_grad.at[:, pl.ds(half, half)], totals.at[1, pl.ds(0, rows)]),
    ]
    up.step(order[1])
    gain = jnp.concatenate([gains[i, 2:3, : width // n_dp] for i in range(n_dp)], axis=1)
    for copy in finals:
        copy.wait()
    for i in range(tiles):
        at = pl.ds(i * TILE, TILE)
        across_sends[i].wait_recv()
        upstream = hidden[at, :] + from_across[at, :].astype(f32)
        features = n1_all[0, at, :].astype(f32)
        inverse = lax.rsqrt(jnp.mean(features * features, axis=1, keepdims=True) + EPS)
        scaled = gain * upstream
        mean = jnp.mean(scaled * features, axis=1, keepdims=True)
        change = inverse * scaled - features * (inverse * inverse * inverse) * mean
        n1_all[1, at, :half] = (totals[0, at, :] + change[:, :half]).astype(bf16)
        n1_all[1, at, half:] = (totals[1, at, :] + change[:, half:]).astype(bf16)
        if i == 0:
            for j in range(2, n_tensor - 1):
                gate.relay(j)
        if i == 1:
            for p in order[2 : n_tensor - 1]:
                up.step(p)
    save(n1_all.at[1], input_out)
    gate.finish()
    for p in order[n_tensor - 1 :]:
        up.step(p)
    up.relay(1)
    for p in order[:2]:
        qkv_collect.step(p)
    for i in range(2, n_tensor - 1):
        up.relay(i)
    for p in order[2 : n_tensor - 1]:
        qkv_collect.step(p)
    up.finish()
    for p in order[n_tensor - 1 :]:
        qkv_collect.step(p)
    qkv_collect.relay(1)
    for p in order[:2]:
        out_collect.step(p)
    for i in range(2, n_tensor - 1):
        qkv_collect.relay(i)
    for p in order[2:]:
        out_collect.step(p)
    out_collect.relay(1)
    qkv_collect.finish()
    for i in range(2, n_tensor - 1):
        out_collect.relay(i)
    out_collect.finish()
    for collect in (down, gate, up, out_collect, qkv_collect):
        collect.wait()
    links.finish()


def backward(
    n_dp, n_tensor, grad_own, hidden_grad, tokens, hidden1, mlp_part, normed1, queries, keyvals, logs, attended,
    cosine, sine, qkv_full, out_full, smalls, down_part, gate_part, up_part, down_got,
    mlp_row, fixed,
):
    f32, bf16 = jnp.float32, jnp.bfloat16
    rows, width = grad_own.shape
    half = width // 2
    chunk = width // n_dp
    units = queries.shape[2]
    vmem = pl.BlockSpec(memory_space=pltpu.VMEM)
    hbm = pl.BlockSpec(memory_space=pl.ANY)
    extra = 16
    quarters = [
        down_part.shape[1], gate_part.shape[1], up_part.shape[1], out_full.shape[1],
        qkv_full.shape[1] + extra,
    ]

    def shape(dims, dtype=bf16):
        return jax.ShapeDtypeStruct(tuple(dims), dtype)

    def finals(index):
        return shape((GROUP, quarters[index], chunk))

    outs = [
        shape((rows, width)), shape((rows, width)), finals(4), shape((GROUP * quarters[3], chunk)),
        shape((chunk, GROUP * quarters[1])), shape((chunk, GROUP * quarters[2])),
        shape((chunk, GROUP * quarters[0])),
    ]
    full = (GROUP, rows, width)
    scratch = [
        pltpu.VMEM(full, bf16),
        pltpu.VMEM(full, bf16),
        pltpu.VMEM(qkv_full.shape, bf16),
        pltpu.VMEM(out_full.shape, bf16),
        pltpu.VMEM(queries.shape, bf16),
        pltpu.VMEM(keyvals.shape, bf16),
        pltpu.VMEM(logs.shape, f32),
        pltpu.VMEM(attended.shape, bf16),
        pltpu.VMEM(cosine.shape, f32),
        pltpu.VMEM(sine.shape, f32),
        pltpu.VMEM(smalls.shape, f32),
        pltpu.VMEM((2, rows, 1), jnp.int32),
        pltpu.VMEM(attended.shape, bf16),
        pltpu.VMEM((2,) + attended.shape[1:], bf16),
        pltpu.VMEM((2, rows + WINDOW, units), f32),
        pltpu.VMEM((TILE, units), f32),
        pltpu.VMEM((2, rows, units), bf16),
        pltpu.VMEM((GROUP, rows, units), bf16),
        pltpu.VMEM((2, WINDOW, units), bf16),
        pltpu.VMEM((2, WINDOW, units), bf16),
        pltpu.VMEM((2, rows, width), bf16),
        pltpu.VMEM((2, rows, width), bf16),
        pltpu.VMEM((rows, width), bf16),
        pltpu.VMEM((rows, width), bf16),
        pltpu.VMEM((rows, width), bf16),
        pltpu.VMEM((rows, width), f32),
        pltpu.VMEM((n_tensor, quarters[0], half), bf16),
        pltpu.VMEM((n_tensor, quarters[1], half), bf16),
    ]
    scratch += [pltpu.VMEM((n_tensor, q, half), bf16) for q in quarters]
    scratch += [pltpu.VMEM((n_tensor, q, half), bf16) for q in quarters]
    scratch += [pltpu.VMEM((q, half), bf16) for q in quarters]
    scratch += [
        pltpu.VMEM((GROUP, chunk, q) if turned else (GROUP, q, chunk), bf16)
        for q, turned in zip(quarters, (True, True, True, False, False))
    ]
    scratch += [
        pltpu.SemaphoreType.DMA((160,)),
        pltpu.SemaphoreType.DMA((160,)),
        pltpu.SemaphoreType.DMA((40,)),
    ]
    return pl.pallas_call(
        functools.partial(kernel_backward, n_dp, n_tensor),
        in_specs=[hbm] * 19 + [vmem] * 2,
        out_specs=[hbm] * len(outs),
        out_shape=outs,
        scratch_shapes=scratch,
        compiler_params=pltpu.CompilerParams(
            collective_id=1, has_side_effects=True, vmem_limit_bytes=67043328
        ),
        name="backward",
    )(
        grad_own, hidden_grad, tokens, hidden1, mlp_part, normed1, queries, keyvals, logs, attended, cosine, sine,
        qkv_full, out_full, smalls, down_part, gate_part, up_part, down_got, mlp_row, fixed,
    )


def fast_local(
    n_dp,
    n_tensor,
    block_in,
    cotangent,
    segment_ids,
    attn_gain,
    qkv_weight,
    out_weight,
    mlp_gain,
    gate_weight,
    up_weight,
    down_weight,
):
    bf16, f32 = jnp.bfloat16, jnp.float32
    rows, width = block_in.shape
    part = attn_gain.shape[0]
    (
        normed1, normed2, hidden1, queries, keyvals, log_total, attended, cosine, sine, qkv_full,
        out_full, smalls, grad_rows, gate_full, up_full, down_full,
    ), fixed = forward(
        n_dp, n_tensor, block_in, cotangent, segment_ids, jnp.stack([attn_gain, mlp_gain]),
        qkv_weight, out_weight, gate_weight, up_weight, down_weight,
    )
    (
        hidden1_grad, grad_own, mlp_part, down_part, gate_part, up_part, down_got, mlp_row,
    ) = feed(n_dp, n_tensor, normed2, grad_rows, hidden1, gate_full, up_full, down_full, smalls)
    input_grad, block_out, qkv_blocks, out_grad, gate_grad, up_grad, down_grad = backward(
        n_dp, n_tensor, grad_own, hidden1_grad, block_in, hidden1, mlp_part, normed1, queries,
        keyvals, log_total, attended, cosine, sine, qkv_full, out_full, smalls, down_part, gate_part, up_part, down_got, mlp_row,
        fixed,
    )
    quarter = qkv_full.shape[1]

    def row_of(index, gain):
        return jnp.sum(qkv_blocks[:, quarter + index].astype(f32), axis=0) / gain.astype(f32)

    blocks = qkv_blocks[:, :quarter]
    qkv_grad = blocks.reshape(-1, blocks.shape[2]).T.astype(f32)
    gains = [row_of(0, attn_gain), row_of(1, mlp_gain)]
    return (
        block_out,
        input_grad,
        gains[0],
        qkv_grad,
        out_grad.astype(f32),
        gains[1],
        gate_grad.astype(f32),
        up_grad.astype(f32),
        down_grad.T.astype(f32),
    )


def solution(mesh):
    in_specs = (
        P(("dp", "tensor"), None),
        P(("dp", "tensor"), None),
        P("dp", None),
        P("dp"),
        P("dp", "tensor"),
        P("tensor", "dp"),
        P("dp"),
        P("dp", "tensor"),
        P("dp", "tensor"),
        P("tensor", "dp"),
    )
    out_specs = (
        P(("dp", "tensor"), None),
        P(("dp", "tensor"), None),
        P("dp"),
        P("dp", "tensor"),
        P("tensor", "dp"),
        P("dp"),
        P("dp", "tensor"),
        P("dp", "tensor"),
        P("tensor", "dp"),
    )
    n_dp, n_tensor = mesh.shape["dp"], mesh.shape["tensor"]

    def body(*arrays):
        rows = arrays[0].shape[0]
        groups = arrays[4].shape[1] // (4 * HEAD_SIZE)
        if n_dp == 2 * GROUP and groups == 2 and rows >= WINDOW and rows % TILE == 0:
            return fast_local(n_dp, n_tensor, *arrays)
        return local(*arrays)

    return jax.shard_map(body, mesh=mesh, in_specs=in_specs, out_specs=out_specs, check_vma=False)
```

```python
import functools

import jax
import jax.numpy as jnp
import numpy as np
from jax import lax
from jax.experimental import pallas as pl
from jax.experimental.pallas import tpu as pltpu
from jax.sharding import PartitionSpec as P

QUERY_HEADS = 16
KEY_VALUE_HEADS = 8
HEAD_SIZE = 96


EPS = 1e-05
ROPE_BASE = 100000.0
NEG_FILL = -1e30


def doc_positions(segments):
    length = segments.shape[1]
    position_index = jnp.broadcast_to(jnp.arange(length, dtype=jnp.int32)[None, :], segments.shape)
    change = jnp.concatenate(
        [jnp.ones((segments.shape[0], 1), dtype=bool), segments[:, 1:] != segments[:, :-1]], axis=1
    )
    starts = lax.cummax(jnp.where(change, position_index, jnp.zeros_like(position_index)), axis=1)
    return position_index - starts


def rotary_tables(segments):
    half_dim = HEAD_SIZE // 2
    frequency = jnp.power(ROPE_BASE, -(2.0 * jnp.arange(half_dim, dtype=jnp.float32)) / HEAD_SIZE)
    angles = doc_positions(segments).astype(jnp.float32)[..., None] * frequency
    cosine_table = jnp.concatenate([jnp.cos(angles), jnp.cos(angles)], axis=-1)
    sine_table = jnp.concatenate([jnp.sin(angles), jnp.sin(angles)], axis=-1)
    return (cosine_table, sine_table)


def rotate(vector, cosine_table, sine_table):
    half_dim = vector.shape[-1] // 2
    turned = jnp.concatenate([-vector[..., half_dim:], vector[..., :half_dim]], axis=-1)
    return vector * cosine_table + turned * sine_table


def unrotate(vector, cosine_table, sine_table):
    half_dim = vector.shape[-1] // 2
    shifted = vector * sine_table
    returned = jnp.concatenate([shifted[..., half_dim:], -shifted[..., :half_dim]], axis=-1)
    return vector * cosine_table + returned


def allowed_pairs(segments):
    length = segments.shape[1]
    offsets = jnp.arange(length)
    causal = offsets[None, :] <= offsets[:, None]
    same_doc = segments[:, :, None] == segments[:, None, :]
    return (causal[None] & same_doc)[:, None, None]


def score_block(queries, key_heads, segments):
    scores = jnp.einsum(
        "sqgrd,skgd->sgrqk", queries, key_heads, preferred_element_type=jnp.float32
    ) * HEAD_SIZE ** (-0.5)
    return jnp.where(allowed_pairs(segments), scores, NEG_FILL)


def rms_scale(features):
    return lax.rsqrt(jnp.mean(features * features, axis=-1, keepdims=True) + EPS)


def norm_back(features, inverse, gain_vector, upstream):
    scaled = gain_vector * upstream
    return inverse * scaled - features * (inverse * inverse * inverse) * jnp.mean(
        scaled * features, axis=-1, keepdims=True
    )


def widen(shard_rows):
    return lax.all_gather(shard_rows, "tensor", axis=0, tiled=True)


def narrow(partial_value):
    return lax.psum_scatter(
        partial_value.astype(jnp.bfloat16), "tensor", scatter_dimension=0, tiled=True
    ).astype(jnp.float32)


def local(
    block_in,
    cotangent,
    segment_ids,
    attn_gain,
    qkv_weight,
    out_weight,
    mlp_gain,
    gate_weight,
    up_weight,
    down_weight,
):
    qkv_full, gate_full, up_full, gain_attn_raw, gain_mlp_raw = (
        lax.all_gather(qkv_weight, "dp", axis=0, tiled=True),
        lax.all_gather(gate_weight, "dp", axis=0, tiled=True),
        lax.all_gather(up_weight, "dp", axis=0, tiled=True),
        lax.all_gather(attn_gain, "dp", axis=0, tiled=True),
        lax.all_gather(mlp_gain, "dp", axis=0, tiled=True),
    )
    out_cols, down_cols = (
        lax.all_gather(out_weight, "dp", axis=1, tiled=True),
        lax.all_gather(down_weight, "dp", axis=1, tiled=True),
    )
    seq_count, length = segment_ids.shape
    repeat_factor = QUERY_HEADS // KEY_VALUE_HEADS
    groups = qkv_full.shape[1] // ((repeat_factor + 2) * HEAD_SIZE)
    gain_attn = gain_attn_raw.astype(jnp.float32)
    gain_mlp = gain_mlp_raw.astype(jnp.float32)
    residual = block_in.astype(jnp.float32)
    scale_attn = rms_scale(residual)
    normed1 = widen((residual * scale_attn * gain_attn).astype(jnp.bfloat16))
    projected = jnp.dot(normed1, qkv_full, preferred_element_type=jnp.float32).reshape(
        seq_count, length, groups, repeat_factor + 2, HEAD_SIZE
    )
    cosine_table, sine_table = rotary_tables(segment_ids)
    cos_query = cosine_table[:, :, None, None, :]
    sin_query = sine_table[:, :, None, None, :]
    cos_key = cosine_table[:, :, None, :]
    sin_key = sine_table[:, :, None, :]
    queries = rotate(projected[:, :, :, :repeat_factor], cos_query, sin_query).astype(jnp.bfloat16)
    key_heads = rotate(projected[:, :, :, repeat_factor], cos_key, sin_key).astype(jnp.bfloat16)
    values = projected[:, :, :, repeat_factor + 1].astype(jnp.bfloat16)
    scores = score_block(queries, key_heads, segment_ids)
    highest = jnp.max(scores, axis=-1, keepdims=True)
    log_total = highest + jnp.log(jnp.sum(jnp.exp(scores - highest), axis=-1, keepdims=True))
    probability = jnp.exp(scores - log_total).astype(jnp.bfloat16)
    attended = jnp.einsum(
        "sgrqk,skgd->sqgrd", probability, values, preferred_element_type=jnp.float32
    ).astype(jnp.bfloat16)
    attn_flat = attended.reshape(seq_count * length, groups * repeat_factor * HEAD_SIZE)
    attn_delta = lax.psum_scatter(
        jnp.dot(attn_flat, out_cols, preferred_element_type=jnp.float32).astype(jnp.bfloat16),
        "tensor",
        scatter_dimension=0,
        tiled=True,
    ).astype(jnp.float32)
    hidden1 = residual + attn_delta
    scale_mlp = rms_scale(hidden1)
    normed2 = widen((hidden1 * scale_mlp * gain_mlp).astype(jnp.bfloat16))
    gate = jnp.dot(normed2, gate_full, preferred_element_type=jnp.float32)
    up_value = jnp.dot(normed2, up_full, preferred_element_type=jnp.float32)
    sigmoid_gate = jax.nn.sigmoid(gate)
    activated = (gate * sigmoid_gate * up_value).astype(jnp.bfloat16)
    mlp_delta = narrow(jnp.dot(activated, down_cols, preferred_element_type=jnp.float32))
    block_out = (hidden1 + mlp_delta).astype(jnp.bfloat16)
    grad_rows = widen(cotangent)
    down_part = jnp.einsum("tf,td->fd", activated, grad_rows, preferred_element_type=jnp.float32)
    act_grad = jnp.einsum("td,fd->tf", grad_rows, down_cols, preferred_element_type=jnp.float32)
    gate_delta = (act_grad * up_value * sigmoid_gate * (1.0 + gate * (1.0 - sigmoid_gate))).astype(
        jnp.bfloat16
    )
    up_delta = (act_grad * gate * sigmoid_gate).astype(jnp.bfloat16)
    gate_part = jnp.einsum("td,tf->df", normed2, gate_delta, preferred_element_type=jnp.float32)
    up_part = jnp.einsum("td,tf->df", normed2, up_delta, preferred_element_type=jnp.float32)
    normed2_term = jnp.einsum(
        "tf,df->td", gate_delta, gate_full, preferred_element_type=jnp.float32
    ) + jnp.einsum("tf,df->td", up_delta, up_full, preferred_element_type=jnp.float32)
    normed2_grad = narrow(normed2_term)
    mlp_gain_part = jnp.sum(normed2_grad * hidden1 * scale_mlp, axis=0)
    hidden1_grad = cotangent.astype(jnp.float32) + norm_back(
        hidden1, scale_mlp, gain_mlp, normed2_grad
    )
    hidden1_rounded = hidden1_grad.astype(jnp.bfloat16)
    grad_full = lax.all_gather(hidden1_rounded, "tensor", axis=0, tiled=True)
    attended_grad = jnp.einsum(
        "td,hd->th", grad_full, out_cols, preferred_element_type=jnp.float32
    ).astype(jnp.bfloat16)
    out_part = jnp.einsum("th,td->hd", attn_flat, grad_full, preferred_element_type=jnp.float32)
    attended_grad = attended_grad.reshape(seq_count, length, groups, repeat_factor, HEAD_SIZE)
    prob_full = jnp.exp(score_block(queries, key_heads, segment_ids) - log_total)
    prob_grad = jnp.einsum(
        "sqgrd,skgd->sgrqk", attended_grad, values, preferred_element_type=jnp.float32
    )
    inner_sum = jnp.sum(prob_full * prob_grad, axis=-1, keepdims=True)
    score_grad = (prob_full * (prob_grad - inner_sum) * HEAD_SIZE ** (-0.5)).astype(jnp.bfloat16)
    query_grad = jnp.einsum(
        "sgrqk,skgd->sqgrd", score_grad, key_heads, preferred_element_type=jnp.float32
    )
    key_grad = jnp.einsum(
        "sgrqk,sqgrd->skgd", score_grad, queries, preferred_element_type=jnp.float32
    )
    value_grad = jnp.einsum(
        "sgrqk,sqgrd->skgd",
        prob_full.astype(jnp.bfloat16),
        attended_grad,
        preferred_element_type=jnp.float32,
    )
    projected_grad = jnp.concatenate(
        [
            unrotate(query_grad, cos_query, sin_query),
            unrotate(key_grad, cos_key, sin_key)[:, :, :, None],
            value_grad[:, :, :, None],
        ],
        axis=3,
    )
    projected_grad = projected_grad.astype(jnp.bfloat16).reshape(
        seq_count * length, groups * (repeat_factor + 2) * HEAD_SIZE
    )
    qkv_part = jnp.einsum("td,tc->dc", normed1, projected_grad, preferred_element_type=jnp.float32)
    normed1_grad = narrow(
        jnp.einsum("tc,dc->td", projected_grad, qkv_full, preferred_element_type=jnp.float32)
    )
    attn_gain_part = jnp.sum(normed1_grad * residual * scale_attn, axis=0)
    input_grad = (hidden1_grad + norm_back(residual, scale_attn, gain_attn, normed1_grad)).astype(
        jnp.bfloat16
    )
    attn_gain_total, mlp_gain_total = lax.psum((attn_gain_part, mlp_gain_part), "tensor")
    attn_gain_grad, qkv_grad, gate_grad, up_grad, mlp_gain_grad = (
        lax.psum_scatter(
            attn_gain_total.astype(jnp.bfloat16), "dp", scatter_dimension=0, tiled=True
        ).astype(jnp.float32),
        lax.psum_scatter(
            qkv_part.astype(jnp.bfloat16), "dp", scatter_dimension=0, tiled=True
        ).astype(jnp.float32),
        lax.psum_scatter(
            gate_part.astype(jnp.bfloat16), "dp", scatter_dimension=0, tiled=True
        ).astype(jnp.float32),
        lax.psum_scatter(
            up_part.astype(jnp.bfloat16), "dp", scatter_dimension=0, tiled=True
        ).astype(jnp.float32),
        lax.psum_scatter(
            mlp_gain_total.astype(jnp.bfloat16), "dp", scatter_dimension=0, tiled=True
        ).astype(jnp.float32),
    )
    out_grad, down_grad = (
        lax.psum_scatter(
            out_part.astype(jnp.bfloat16), "dp", scatter_dimension=1, tiled=True
        ).astype(jnp.float32),
        lax.psum_scatter(
            down_part.astype(jnp.bfloat16), "dp", scatter_dimension=1, tiled=True
        ).astype(jnp.float32),
    )
    return (
        block_out,
        input_grad,
        attn_gain_grad,
        qkv_grad,
        out_grad,
        mlp_gain_grad,
        gate_grad,
        up_grad,
        down_grad,
    )


GROUP = 4
WINDOW = 256
LANES = 384
TILE = 128


MESH = pl.DeviceIdType.MESH


class Transfer:
    def __init__(self, copy, sends=None, receives=None):
        self.copy, self.sends, self.receives = copy, sends, receives

    def _when(self, condition, action):
        if condition is None:
            action()
        else:
            pl.when(condition)(action)

    def start(self):
        self._when(self.sends, self.copy.start)
        return self

    def wait_recv(self):
        self._when(self.receives, self.copy.wait_recv)

    def wait_send(self):
        self._when(self.sends, self.copy.wait_send)


class Links:
    def __init__(self, n_dp, n_tensor, out_sems, in_sems, local_sems):
        self.n_dp, self.n_tensor = n_dp, n_tensor
        self.out_sems, self.in_sems, self.local_sems = out_sems, in_sems, local_sems
        self.d_at, self.z_at = lax.axis_index("dp"), lax.axis_index("tensor")
        self.used, self.used_local = 0, 0
        self.sent, self.saved = [], []

    def barrier(self):
        barrier = pltpu.get_barrier_semaphore()
        for k in range(1, self.n_dp):
            pl.semaphore_signal(
                barrier,
                inc=1,
                device_id={"dp": self.d_at ^ k, "tensor": self.z_at},
                device_id_type=MESH,
            )
        for s in range(1, self.n_tensor):
            pl.semaphore_signal(
                barrier,
                inc=1,
                device_id={"dp": self.d_at, "tensor": lax.rem(self.z_at + s, self.n_tensor)},
                device_id_type=MESH,
            )
        pl.semaphore_wait(barrier, self.n_dp - 1 + self.n_tensor - 1)

    def plan(self, source, target, bit=0, shift=0, sends=None, receives=None):
        slot = self.used
        self.used += 1
        copy = pltpu.make_async_remote_copy(
            src_ref=source,
            dst_ref=target,
            send_sem=self.out_sems.at[slot],
            recv_sem=self.in_sems.at[slot],
            device_id={
                "dp": self.d_at ^ bit,
                "tensor": lax.rem(self.z_at + self.n_tensor + shift, self.n_tensor),
            },
            device_id_type=MESH,
        )
        transfer = Transfer(copy, sends, receives)
        self.sent.append(transfer)
        return transfer

    def send(self, source, target, bit=0, shift=0):
        return self.plan(source, target, bit, shift).start()

    def move(self, source, target):
        copy = pltpu.make_async_copy(source, target, self.local_sems.at[self.used_local])
        self.used_local += 1
        copy.start()
        return copy

    def save(self, source, target):
        self.saved.append(self.move(source, target))

    def finish(self):
        for transfer in self.sent:
            transfer.wait_send()
        for copy in self.saved:
            copy.wait()


class Spread:
    def __init__(self, links, own_piece, target, columns):
        self.links, self.own_piece, self.target, self.columns = links, own_piece, target, columns
        self.ahead, self.back, self.swaps = [], [], []

    def _slot(self, index):
        n = self.links.n_tensor
        return self.target.at[lax.rem(index + n, n), :, self.columns]

    def issue(self):
        links, n, z = self.links, self.links.n_tensor, self.links.z_at
        own = self._slot(z)
        for s in range(1, n):
            up_from, down_from = z - (s - 1), z + (s - 1)
            up_source = self.own_piece if s == 1 else self._slot(up_from)
            down_source = self.own_piece if s == 1 else self._slot(down_from)
            self.ahead.append(
                links.plan(
                    up_source, self._slot(up_from), shift=1,
                    sends=(z < n - 1) & (up_from >= 0), receives=z >= s,
                )
            )
            self.back.append(
                links.plan(
                    down_source, self._slot(down_from), shift=-1,
                    sends=(z > 0) & (down_from < n), receives=z + s < n,
                )
            )
        self.ahead[0].start()
        self.back[0].start()
        self.swaps.append(links.plan(self.own_piece, own, bit=GROUP).start())

    def step(self, s):
        links, n, z = self.links, self.links.n_tensor, self.links.z_at
        for arrivals, piece, here in (
            (self.ahead, z - s, z >= s),
            (self.back, z + s, z + s < n),
        ):
            arrivals[s - 1].wait_recv()
            if s < n - 1:
                arrivals[s].start()
            slot = self._slot(piece)
            self.swaps.append(
                links.plan(slot, slot, bit=GROUP, sends=here, receives=here).start()
            )

    def wait(self):
        for swap in self.swaps:
            swap.wait_recv()


def kernel_forward(
    n_dp, n_tensor,
    tokens, cot, gate_w, up_w, down_w, out_w, qkv_w, segments, gain_rows, fixed,
    normed1_out, normed2_out, hidden_out, query_out, keyval_out, log_out, att_out,
    cos_out, sin_out, qkv_out, out_out, small_out, cot_out, gate_out, up_out, down_out,
    x_all, n1_all, first, dealt, first_piece, qkv, out_parcel, obuf, gbuf, ubuf, dbuf, piece, outw,
    small, small_all, stream, parts, recv, queries, keyvals,
    att, by_repeat, logs, cosine, sine, low_col, to_core, from_core, to_across, from_across,
    hidden, n2_all, stage, out_sems, in_sems, local_sems,
):
    f32, bf16 = jnp.float32, jnp.bfloat16
    links = Links(n_dp, n_tensor, out_sems, in_sems, local_sems)
    send, move, save = links.send, links.move, links.save
    d_at, z_at = links.d_at, links.z_at
    member = d_at % GROUP
    core = d_at % 2
    upper = d_at // GROUP
    rows, width = tokens.shape
    half = width // 2
    chunk = qkv_w.shape[0]
    contract = (((1,), (1,)), ((), ()))
    columns = pl.ds(pl.multiple_of(upper * half, half), half)

    turned = qkv_w[...].T
    quarter = turned.shape[0] // GROUP
    for i in range(GROUP):
        first[i] = turned[i * quarter : (i + 1) * quarter]
    turned = out_w[...].T
    out_quarter = turned.shape[0] // GROUP
    for i in range(GROUP):
        out_parcel[i] = turned[i * out_quarter : (i + 1) * out_quarter]
    ids = segments[...]
    seqs, length = ids.shape
    begin = jnp.zeros_like(ids)
    for value in range(3):
        count = jnp.sum((ids == value).astype(jnp.int32), axis=1, keepdims=True)
        begin = begin + jnp.where(ids > value, count, 0)
    begin = begin.astype(f32)
    for i in range(seqs):
        stream[:, i * length : (i + 1) * length] = jnp.broadcast_to(
            begin[i : i + 1] + float(i * length), (stream.shape[0], length)
        )
    window = stream[:, pl.ds(pl.multiple_of(z_at * rows, TILE), rows)]
    here = lax.broadcasted_iota(jnp.int32, window.shape, 1) + z_at * rows
    small[...] = window
    small[0:1] = here.astype(f32)[0:1] - window[0:1]
    small[2:4, :chunk] = gain_rows[...].astype(f32)

    @pl.when(z_at == 0)
    def _():
        keyvals[:, :WINDOW, :] = jnp.zeros_like(keyvals[:, :WINDOW, :])

    links.barrier()

    deals = [send(first.at[member ^ k], dealt.at[member], bit=k) for k in range(1, GROUP)]
    beside = send(tokens, x_all.at[2], bit=1)
    smalls = [send(small, small_all.at[d_at], bit=k) for k in range(1, n_dp)]
    def columns_of(ref, at):
        size = ref.shape[1] // GROUP
        return ref.at[:, pl.ds(pl.multiple_of(at * size, TILE), size)]

    def parcel_of(ref, at):
        return ref.at[at]

    pairs = [
        (out_parcel, obuf, parcel_of), (gate_w, gbuf, columns_of), (up_w, ubuf, columns_of),
        (down_w, dbuf, columns_of),
    ]

    def deal(group):
        return [
            send(take(ref, member ^ k), buffer.at[member], bit=k)
            for ref, buffer, take in group
            for k in range(1, GROUP)
        ]

    rests = deal(pairs[:2])
    across = send(tokens, x_all.at[1], bit=2)
    late_rests = deal(pairs[2:])
    own = [move(tokens, x_all.at[0])]
    for ref, buffer, take in pairs:
        own.append(move(take(ref, member), buffer.at[member]))
    cot_stage = move(cot, stage)
    small_all[d_at] = small[...]
    dealt[member] = first[member]

    entries = lax.broadcasted_iota(jnp.int32, (WINDOW, LANES), 0).astype(f32)
    angles = entries * fixed[0:1]

    def split(table):
        pieces = []
        for _ in range(3):
            pieces.append(table.astype(bf16))
            table = table - pieces[-1].astype(f32)
        return pieces

    cos_parts, sin_parts = split(jnp.cos(angles)), split(jnp.sin(angles))
    second = fixed[1:2]
    own_turns = jnp.where(core == 0, jnp.ones_like(second), fixed[2:3])

    for copy in deals:
        copy.wait_recv()
    for i in range(GROUP):
        first_piece[:, i * chunk : (i + 1) * chunk] = dealt[i]
    spread_first = Spread(links, first_piece, qkv, columns)
    spread_first.issue()
    save(first_piece, qkv.at[z_at, :, columns])
    own_qkv = links.saved.pop()
    for copy in own:
        copy.wait()
    cot_stage.wait()
    save(stage, cot_out.at[0])
    spread_first.step(1)
    for copy in smalls:
        copy.wait_recv()
    spread_first.step(2)
    gains = []
    for row in (2, 3):
        gains.append(
            jnp.concatenate([small_all[i, row : row + 1, :chunk] for i in range(n_dp)], axis=1)
        )
    for copy in rests:
        copy.wait_recv()
    sizes = [obuf.shape[1], gbuf.shape[2], ubuf.shape[2], dbuf.shape[2]]
    starts = [sum(sizes[:i]) for i in range(len(sizes))]
    saves = []

    def prepare(index, target, buffer):
        at = slice(starts[index], starts[index] + sizes[index])
        for i in range(GROUP):
            piece[at, i * chunk : (i + 1) * chunk] = buffer[i] if index == 0 else buffer[i].T
        own_piece = piece.at[pl.ds(starts[index], sizes[index])]
        saves.append(move(own_piece, target.at[z_at, :, columns]))
        return Spread(links, own_piece, target, columns)

    out_spread = prepare(0, outw, obuf)
    gate_spread = prepare(1, gate_out, gbuf)
    out_spread.issue()
    spread_first.step(3)
    gate_spread.issue()
    beside.wait_recv()
    own_qkv.wait()
    spread_first.wait()

    def project_block(m, k):
        features = x_all[m].astype(f32)
        scale = lax.rsqrt(jnp.mean(features * features, axis=1, keepdims=True) + EPS)
        normal = (features * scale * gains[0]).astype(bf16)
        n1_all[m] = normal
        units = qkv.shape[0] * qkv.shape[1]
        product = lax.dot_general(
            normal, qkv[...].reshape(units, width), contract, preferred_element_type=f32
        )
        info = small_all[d_at ^ k].T
        key = lax.broadcasted_iota(jnp.int32, (rows, WINDOW), 1)
        chosen = (info[:, 0:1].astype(jnp.int32) == key).astype(bf16)

        def pick(table):
            total = jnp.dot(chosen, table[0], preferred_element_type=f32)
            for part in table[1:]:
                total += jnp.dot(chosen, part, preferred_element_type=f32)
            return total

        cos_here, sin_here = pick(cos_parts), pick(sin_parts)
        parts[m] = turn(product, cos_here, sin_here, second, own_turns, 1.0).astype(bf16)
        if m < 2:
            cosine[m] = cos_here
            sine[m] = sin_here
            low_col[m] = info[:, 1:2].astype(jnp.int32) - z_at * rows + WINDOW

    is_first = core == 0
    halos = [
        links.plan(
            keyvals.at[m, pl.ds(rows, WINDOW)], keyvals.at[m, pl.ds(0, WINDOW)], shift=1,
            sends=z_at < n_tensor - 1, receives=z_at > 0,
        )
        for m in range(2)
    ]

    def take_block(m, swap):
        swap.wait_recv()
        mine, other = parts[m], recv[m]
        queries[m] = jnp.where(is_first, mine, other)
        keyvals[m, WINDOW:, :] = jnp.where(is_first, other, mine)
        halos[m].start()

    project_block(2, 1)
    part_swap = send(parts.at[2], recv.at[0], bit=1)
    project_block(0, 0)
    take_block(0, part_swap)
    out_spread.step(1)
    across.wait_recv()
    both = send(x_all.at[1], x_all.at[3], bit=1)
    cot_across = send(cot, cot_out.at[1], bit=2)
    cot_beside = send(cot, cot_out.at[2], bit=1)
    project_block(1, 2)
    both.wait_recv()
    project_block(3, 3)
    part_swap = send(parts.at[3], recv.at[1], bit=1)
    save(n1_all, normed1_out)
    save(cosine, cos_out)
    save(sine, sin_out)
    take_block(1, part_swap)
    out_spread.step(2)
    gate_spread.step(1)
    for copy in late_rests:
        copy.wait_recv()
    up_spread = prepare(2, up_out, ubuf)
    down_spread = prepare(3, down_out, dbuf)
    save(queries, query_out)
    heads = queries.shape[2] // HEAD_SIZE
    repeat = QUERY_HEADS // KEY_VALUE_HEADS
    span = TILE + WINDOW

    def attend_tile(m, start):
        key = lax.broadcasted_iota(jnp.int32, (TILE, span), 1)
        query = lax.broadcasted_iota(jnp.int32, (TILE, span), 0)
        lowest = low_col[m, pl.ds(start, TILE), :] - start
        allowed = (key >= lowest) & (key <= query + WINDOW)
        for head in range(heads):
            group, r = head // repeat, head % repeat
            base = group * 2 * HEAD_SIZE
            q = queries[m, pl.ds(start, TILE), head * HEAD_SIZE : (head + 1) * HEAD_SIZE]
            k = keyvals[m, pl.ds(start, span), base : base + HEAD_SIZE]
            v = keyvals[m, pl.ds(start, span), base + HEAD_SIZE : base + 2 * HEAD_SIZE]
            s = lax.dot_general(q, k, contract, preferred_element_type=f32) * HEAD_SIZE ** (-0.5)
            s = jnp.where(allowed, s, NEG_FILL)
            highest = jnp.max(s, axis=1, keepdims=True)
            e = jnp.exp(s - highest)
            whole = jnp.sum(e, axis=1, keepdims=True)
            p = (e * (1.0 / whole)).astype(bf16)
            o = jnp.dot(p, v, preferred_element_type=f32).astype(bf16)
            logs[m, pl.ds(start, TILE), head : head + 1] = highest + jnp.log(whole)
            by_repeat[r, m, pl.ds(start, TILE), group * HEAD_SIZE : (group + 1) * HEAD_SIZE] = o

    tiles = rows // TILE
    free = -(-WINDOW // TILE)

    def attend_tiles(blocks, first_tile, last_tile):
        count = last_tile - first_tile

        def body(i, carry):
            m = blocks[0] + (i // count) * (blocks[-1] - blocks[0])
            attend_tile(m, pl.multiple_of((first_tile + i % count) * TILE, TILE))
            return carry

        lax.fori_loop(0, count * len(blocks), body, 0)

    attend_tiles((1, 0), free, tiles)
    out_spread.step(3)
    up_spread.issue()
    halos[0].wait_recv()
    halos[1].wait_recv()
    attend_tiles((1,), 0, free)
    att_swap1 = send(by_repeat.at[1 - core, 1], att.at[3], bit=1)
    gate_spread.step(2)
    attend_tiles((0,), 0, free)
    att_swap0 = send(by_repeat.at[1 - core, 0], att.at[2], bit=1)
    save(keyvals, keyval_out)
    save(logs, log_out)
    att[0] = by_repeat[core, 0]
    att[1] = by_repeat[core, 1]
    down_spread.issue()
    cot_across.wait_recv()
    cot_both = send(cot_out.at[1], cot_out.at[3], bit=1)

    saves[0].wait()
    out_spread.wait()

    def project_out(b):
        units = outw.shape[0] * outw.shape[1]
        return jnp.dot(att[b], outw[...].reshape(units, width), preferred_element_type=f32)

    att_swap1.wait_recv()
    to_core[1] = project_out(3).astype(bf16)
    core_send1 = send(to_core.at[1], from_core.at[1], bit=1)
    hidden[...] = project_out(1)
    att_swap0.wait_recv()
    to_core[0] = project_out(2).astype(bf16)
    core_send0 = send(to_core.at[0], from_core.at[0], bit=1)
    core_send1.wait_recv()
    across_sends = []
    for i in range(tiles):
        at = pl.ds(i * TILE, TILE)
        to_across[at] = (hidden[at, :] + from_core[1, at, :].astype(f32)).astype(bf16)
        across_sends.append(send(to_across.at[at], from_across.at[at], bit=2))
    hidden[...] = project_out(0) + x_all[0].astype(f32)
    core_send0.wait_recv()
    hidden[...] += from_core[0].astype(f32)
    save(att, att_out)
    gate_spread.step(3)
    up_spread.step(1)
    steps = [
        (up_spread, 2), (up_spread, 3), (down_spread, 1), (down_spread, 2), (down_spread, 3),
    ]
    last = []
    for i in range(tiles):
        at = pl.ds(i * TILE, TILE)
        across_sends[i].wait_recv()
        value = hidden[at, :] + from_across[at, :].astype(f32)
        hidden[at, :] = value
        scale = lax.rsqrt(jnp.mean(value * value, axis=1, keepdims=True) + EPS)
        n2_all[0, at, :] = (value * scale * gains[1]).astype(bf16)
        last.append(send(n2_all.at[0, at], n2_all.at[1, at], bit=2))
        last.append(send(n2_all.at[0, at], n2_all.at[2, at], bit=1))
        if i < 3:
            spread, s = steps.pop(0)
            spread.step(s)
    save(hidden, hidden_out)
    save(qkv, qkv_out)
    save(outw, out_out)
    save(small_all, small_out)
    ends = []
    for i in range(tiles):
        at = pl.ds(i * TILE, TILE)
        last[2 * i].wait_recv()
        ends.append(send(n2_all.at[1, at], n2_all.at[3, at], bit=1))
        if i < 2:
            spread, s = steps.pop(0)
            spread.step(s)
    for copy in ends + last[1::2]:
        copy.wait_recv()
    save(n2_all, normed2_out)
    for copy in saves[1:]:
        copy.wait()
    for spread in (gate_spread, up_spread, down_spread):
        spread.wait()
    for copy in (cot_beside, cot_both):
        copy.wait_recv()
    links.finish()


def forward(
    n_dp, n_tensor, tokens, cot, segments, gain_rows, qkv_w, out_w, gate_w, up_w, down_w
):
    out_w, down_w = out_w.T, down_w.T
    rows, width = tokens.shape
    f32, bf16 = jnp.float32, jnp.bfloat16
    vmem = pl.BlockSpec(memory_space=pltpu.VMEM)
    hbm = pl.BlockSpec(memory_space=pl.ANY)
    chunk = qkv_w.shape[0]
    quarter = qkv_w.shape[1] // GROUP
    sizes = [
        out_w.shape[1] // GROUP, gate_w.shape[1] // GROUP, up_w.shape[1] // GROUP,
        down_w.shape[1] // GROUP,
    ]
    units = quarter * n_tensor
    heads = units // HEAD_SIZE
    lane = np.arange(LANES)
    within = lane % HEAD_SIZE
    fixed = np.zeros((8, LANES), np.float32)
    fixed[0] = np.power(ROPE_BASE, -(2.0 * (within % (HEAD_SIZE // 2))) / HEAD_SIZE)
    fixed[1] = within >= HEAD_SIZE // 2
    fixed[2] = lane % (2 * HEAD_SIZE) < HEAD_SIZE
    fixed[3] = 1.0

    def shape(dims, dtype=bf16):
        return jax.ShapeDtypeStruct(tuple(dims), dtype)

    full = (GROUP, rows, width)
    qkv_shape = (n_tensor, quarter, width)
    out_shape = (n_tensor, sizes[0], width)
    att_shape = (GROUP, rows, units // 2)
    small_shape = (n_dp, 8, rows)
    table = (2, rows, LANES)
    outs = [
        shape(full),
        shape(full),
        shape((rows, width), f32),
        shape((2, rows, units)),
        shape((2, rows + WINDOW, units)),
        shape((2, rows, heads), f32),
        shape(att_shape),
        shape(table, f32),
        shape(table, f32),
        shape(qkv_shape),
        shape(out_shape),
        shape(small_shape, f32),
        shape(full),
    ] + [shape((n_tensor, size, width)) for size in sizes[1:]]
    scratch = [
        pltpu.VMEM(full, bf16),
        pltpu.VMEM(full, bf16),
        pltpu.VMEM((GROUP, quarter, chunk), bf16),
        pltpu.VMEM((GROUP, quarter, chunk), bf16),
        pltpu.VMEM((quarter, width // 2), bf16),
        pltpu.VMEM(qkv_shape, bf16),
        pltpu.VMEM((GROUP, sizes[0], chunk), bf16),
        pltpu.VMEM((GROUP, sizes[0], chunk), bf16),
        pltpu.VMEM((GROUP, chunk, sizes[1]), bf16),
        pltpu.VMEM((GROUP, chunk, sizes[2]), bf16),
        pltpu.VMEM((GROUP, chunk, sizes[3]), bf16),
        pltpu.VMEM((sum(sizes), width // 2), bf16),
        pltpu.VMEM(out_shape, bf16),
        pltpu.VMEM((8, rows), f32),
        pltpu.VMEM(small_shape, f32),
        pltpu.VMEM((8, n_tensor * rows), f32),
        pltpu.VMEM((GROUP, rows, units), bf16),
        pltpu.VMEM((2, rows, units), bf16),
        pltpu.VMEM((2, rows, units), bf16),
        pltpu.VMEM((2, rows + WINDOW, units), bf16),
        pltpu.VMEM(att_shape, bf16),
        pltpu.VMEM((2, 2, rows, units // 2), bf16),
        pltpu.VMEM((2, rows, heads), f32),
        pltpu.VMEM(table, f32),
        pltpu.VMEM(table, f32),
        pltpu.VMEM((2, rows, 1), jnp.int32),
        pltpu.VMEM((2, rows, width), bf16),
        pltpu.VMEM((2, rows, width), bf16),
        pltpu.VMEM((rows, width), bf16),
        pltpu.VMEM((rows, width), bf16),
        pltpu.VMEM((rows, width), f32),
        pltpu.VMEM(full, bf16),
        pltpu.VMEM((rows, width), bf16),
        pltpu.SemaphoreType.DMA((128,)),
        pltpu.SemaphoreType.DMA((128,)),
        pltpu.SemaphoreType.DMA((40,)),
    ]
    results = pl.pallas_call(
        functools.partial(kernel_forward, n_dp, n_tensor),
        in_specs=[hbm] * 5 + [vmem] * 5,
        out_specs=[hbm] * len(outs),
        out_shape=outs,
        scratch_shapes=scratch,
        compiler_params=pltpu.CompilerParams(
            collective_id=0, has_side_effects=True, vmem_limit_bytes=60 * 1024 * 1024
        ),
        name="forward",
    )(
        tokens, cot, gate_w, up_w, down_w, out_w, qkv_w, segments, gain_rows, jnp.asarray(fixed)
    )
    return results, jnp.asarray(fixed)


def turn(value, cosine, sine, second, turns, sign):
    width = value.shape[1]
    half = HEAD_SIZE // 2
    c = turns * cosine + (1.0 - turns)
    u = (sign * turns * second) * sine
    d = (sign * turns * (second - 1.0)) * sine
    pieces = []
    up = pltpu.roll(value, half, 1)
    down = pltpu.roll(value, width - half, 1)
    for i in range(width // LANES):
        at = slice(i * LANES, (i + 1) * LANES)
        pieces.append(value[:, at] * c + up[:, at] * u + down[:, at] * d)
    return jnp.concatenate(pieces, axis=1)


def kernel_feed(
    n_dp, n_tensor,
    n2_in, cot_in, hidden_in, gate_in, up_in, down_in, smalls,
    grad_out, grad_own_out, mlp_out, down_out, gate_out, up_out, down_got, row_out,
    n2_all, cot_all, gate_w, up_w, down_w, active, gate_delta, up_delta,
    down_part, gate_part, up_part, to_core, from_core, to_across, from_across, hidden, total,
    rounded, row, out_sems, in_sems, local_sems,
):
    f32, bf16 = jnp.float32, jnp.bfloat16
    links = Links(n_dp, n_tensor, out_sems, in_sems, local_sems)
    send, move, save = links.send, links.move, links.save
    upper = links.d_at // GROUP
    rows, width = hidden.shape
    half = width // 2
    chunk = width // n_dp
    size = gate_w.shape[1]
    units = n_tensor * size
    contract = (((1,), (1,)), ((), ()))
    over_rows = (((0,), (0,)), ((), ()))
    other = pl.ds(pl.multiple_of((1 - upper) * half, half), half)
    tiles = rows // TILE

    loads = [
        move(gate_in, gate_w), move(n2_in, n2_all), move(up_in, up_w), move(down_in, down_w),
        move(cot_in, cot_all), move(hidden_in, hidden),
    ]
    links.barrier()
    for copy in loads[:-1]:
        copy.wait()

    def inner(i, carry):
        turn_at, p = i // n_tensor, i % n_tensor
        m = 3 - 2 * (turn_at % 2) - turn_at // 2
        at = pl.ds(pl.multiple_of(p * size, TILE), size)
        gate = lax.dot_general(n2_all[m], gate_w[p], contract, preferred_element_type=f32)
        up_value = lax.dot_general(n2_all[m], up_w[p], contract, preferred_element_type=f32)
        act_grad = lax.dot_general(cot_all[m], down_w[p], contract, preferred_element_type=f32)
        sigmoid = jax.nn.sigmoid(gate)
        silu = gate * sigmoid
        active[m, :, at] = (silu * up_value).astype(bf16)
        gate_delta[m, :, at] = (
            act_grad * up_value * sigmoid * (1.0 + gate * (1.0 - sigmoid))
        ).astype(bf16)
        up_delta[m, :, at] = (act_grad * silu).astype(bf16)
        return carry

    lax.fori_loop(0, 2 * n_tensor, inner, 0)

    def back(m):
        return jnp.dot(
            gate_delta[m], gate_w[...].reshape(units, width), preferred_element_type=f32
        ) + jnp.dot(up_delta[m], up_w[...].reshape(units, width), preferred_element_type=f32)

    to_core[1] = back(3).astype(bf16)
    core_send1 = send(to_core.at[1], from_core.at[1], bit=1)
    total[...] = back(1)
    core_send1.wait_recv()
    across = []
    for i in range(tiles):
        at = pl.ds(i * TILE, TILE)
        to_across[at] = (total[at, :] + from_core[1, at, :].astype(f32)).astype(bf16)
        across.append(send(to_across.at[at], from_across.at[at], bit=2))
    lax.fori_loop(2 * n_tensor, GROUP * n_tensor, inner, 0)

    order = []
    for i in range((n_tensor + 1) // 2):
        order.extend(dict.fromkeys((n_tensor - 1 - i, i)))

    def grads(left, right, part, target, weight=None):
        def one(p, carry):
            at = pl.ds(pl.multiple_of(p * size, TILE), size)
            grad = lax.dot_general(
                left[:, :, at].reshape(GROUP * rows, size),
                right[...].reshape(GROUP * rows, width),
                over_rows,
                preferred_element_type=f32,
            )
            part[p] = grad.astype(bf16)
            if weight is not None:
                row[...] += jnp.sum(grad * weight[p].astype(f32), axis=0, keepdims=True)
            return carry

        lax.fori_loop(0, n_tensor, one, 0)
        save(part, target)

    row[...] = jnp.zeros_like(row)
    grads(active, cot_all, down_part, down_out)
    swaps = [
        send(down_part.at[p, :, other], down_got.at[p], bit=GROUP) for p in order[: n_tensor - 1]
    ]
    to_core[0] = back(2).astype(bf16)
    core_send0 = send(to_core.at[0], from_core.at[0], bit=1)
    total[...] = back(0)
    core_send0.wait_recv()
    total[...] += from_core[0].astype(f32)
    grads(gate_delta, n2_all, gate_part, gate_out, gate_w)
    grads(up_delta, n2_all, up_part, up_out, up_w)
    save(row, row_out)

    def feed_out(m, carry):
        n2_all[m] = jnp.dot(
            active[m], down_w[...].reshape(units, width), preferred_element_type=f32
        ).astype(bf16)
        return carry

    lax.fori_loop(0, GROUP, feed_out, 0)
    save(n2_all, mlp_out)
    gain = jnp.concatenate([smalls[i, 3:4, :chunk] for i in range(n_dp)], axis=1)
    loads[-1].wait()
    for i in range(tiles):
        at = pl.ds(i * TILE, TILE)
        across[i].wait_recv()
        upstream = total[at, :] + from_across[at, :].astype(f32)
        features = hidden[at, :]
        inverse = lax.rsqrt(jnp.mean(features * features, axis=1, keepdims=True) + EPS)
        scaled = gain * upstream
        mean = jnp.mean(scaled * features, axis=1, keepdims=True)
        result = cot_all[0, at, :].astype(f32) + (
            inverse * scaled - features * (inverse * inverse * inverse) * mean
        )
        total[at, :] = result
        rounded[at, :] = result.astype(bf16)
    save(total, grad_out)
    save(rounded, grad_own_out)
    for copy in swaps:
        copy.wait_recv()
    links.finish()


def feed(n_dp, n_tensor, normed2, grad_rows, hidden1, gate_w, up_w, down_w, smalls):
    f32, bf16 = jnp.float32, jnp.bfloat16
    rows, width = hidden1.shape
    half = width // 2
    vmem = pl.BlockSpec(memory_space=pltpu.VMEM)
    hbm = pl.BlockSpec(memory_space=pl.ANY)
    weight = gate_w.shape
    inner = (GROUP, rows, n_tensor * weight[1])

    def shape(dims, dtype=bf16):
        return jax.ShapeDtypeStruct(tuple(dims), dtype)

    outs = [
        shape((rows, width), f32), shape((rows, width)), shape(normed2.shape),
        shape(weight), shape(weight), shape(weight), shape((n_tensor, weight[1], half)),
        shape((1, width), f32),
    ]
    scratch = [
        pltpu.VMEM(normed2.shape, bf16),
        pltpu.VMEM(normed2.shape, bf16),
        pltpu.VMEM(weight, bf16),
        pltpu.VMEM(weight, bf16),
        pltpu.VMEM(weight, bf16),
        pltpu.VMEM(inner, bf16),
        pltpu.VMEM(inner, bf16),
        pltpu.VMEM(inner, bf16),
        pltpu.VMEM(weight, bf16),
        pltpu.VMEM(weight, bf16),
        pltpu.VMEM(weight, bf16),
        pltpu.VMEM((2, rows, width), bf16),
        pltpu.VMEM((2, rows, width), bf16),
        pltpu.VMEM((rows, width), bf16),
        pltpu.VMEM((rows, width), bf16),
        pltpu.VMEM((rows, width), f32),
        pltpu.VMEM((rows, width), f32),
        pltpu.VMEM((rows, width), bf16),
        pltpu.VMEM((1, width), f32),
        pltpu.SemaphoreType.DMA((16,)),
        pltpu.SemaphoreType.DMA((16,)),
        pltpu.SemaphoreType.DMA((40,)),
    ]
    return pl.pallas_call(
        functools.partial(kernel_feed, n_dp, n_tensor),
        in_specs=[hbm] * 6 + [vmem],
        out_specs=[hbm] * len(outs),
        out_shape=outs,
        scratch_shapes=scratch,
        compiler_params=pltpu.CompilerParams(
            collective_id=2, has_side_effects=True, vmem_limit_bytes=67043328
        ),
        name="feed",
    )(normed2, grad_rows, hidden1, gate_w, up_w, down_w, smalls)


class Collect:
    def __init__(
        self, links, part, swapped, stage, arrived, late, blocks, target, mine, other, turned=False
    ):
        self.turned = turned
        self.links, self.part, self.swapped, self.stage = links, part, swapped, stage
        self.arrived, self.late, self.blocks, self.target = arrived, late, blocks, target
        self.mine, self.other = mine, other
        self.swaps, self.loads, self.deals = {}, [], []

    def issue(self, order):
        links = self.links
        for p in order:
            self.swaps[p] = links.send(
                self.part.at[p, :, self.other], self.swapped.at[p], bit=GROUP
            )
        if self.stage is not None:
            self.loads = [links.move(self.part.at[:, :, self.mine], self.stage)]

    def load(self, received, order):
        links = self.links
        count = links.n_tensor - 1
        self.issue(order[count:])
        self.loads += [links.move(received.at[p], self.swapped.at[p]) for p in order[:count]]

    def step(self, p):
        links, n, z = self.links, self.links.n_tensor, self.links.z_at
        f32, bf16 = jnp.float32, jnp.bfloat16
        while self.loads:
            self.loads.pop().wait()
        if p in self.swaps:
            self.swaps[p].wait_recv()
        own = self.stage[p] if self.stage is not None else self.part[p, :, self.mine]
        self.swapped[p] = (own.astype(f32) + self.swapped[p].astype(f32)).astype(bf16)
        if not hasattr(self, "ahead"):
            self.ahead, self.back, self.back_last = [None] * n, [None] * n, [None] * n
        source = self.swapped.at[p]
        self.ahead[p] = links.plan(
            source, self.arrived.at[p], shift=1, sends=z < p, receives=(z > 0) & (z <= p)
        )
        self.back[p] = links.plan(
            source, self.arrived.at[p], shift=-1, sends=z > p + 1,
            receives=(z > p) & (z < n - 1),
        )
        self.back_last[p] = links.plan(
            source, self.late, shift=-1, sends=z == p + 1, receives=(z == p) & (z < n - 1)
        )

        @pl.when((z == 0) & (z < p))
        def _():
            self.ahead[p].copy.start()

        @pl.when((z == n - 1) & (z > p + 1))
        def _():
            self.back[p].copy.start()

        @pl.when((z == n - 1) & (z == p + 1))
        def _():
            self.back_last[p].copy.start()

    def relay(self, i):
        links, n, z = self.links, self.links.n_tensor, self.links.z_at
        f32, bf16 = jnp.float32, jnp.bfloat16

        def add(p):
            self.swapped[p] = (
                self.swapped[p].astype(f32) + self.arrived[p].astype(f32)
            ).astype(bf16)

        for p in range(n):
            at = i - (n - 1) + p
            if 0 < at < n - 1 and at < p:

                @pl.when(z == at)
                def _(p=p):
                    self.ahead[p].copy.wait_recv()
                    add(p)
                    self.ahead[p].copy.start()

            at = n - 1 - i + p
            if 0 < at < n - 1 and at > p:

                @pl.when(z == at)
                def _(p=p, at=at):
                    self.back[p].copy.wait_recv()
                    add(p)
                    (self.back_last if at == p + 1 else self.back)[p].copy.start()

    def finish(self):
        links, n, z = self.links, self.links.n_tensor, self.links.z_at
        f32, bf16 = jnp.float32, jnp.bfloat16
        member = links.d_at % GROUP
        for p in range(n):

            @pl.when((z == p) & (z > 0))
            def _(p=p):
                self.ahead[p].copy.wait_recv()

            @pl.when((z == p) & (z < n - 1))
            def _(p=p):
                self.back_last[p].copy.wait_recv()

        below = jnp.where(z > 0, self.arrived[z].astype(f32), 0.0)
        above = jnp.where(z < n - 1, self.late[...].astype(f32), 0.0)
        total = (self.swapped[z].astype(f32) + below + above).astype(bf16)
        chunk = total.shape[1] // GROUP
        size = self.blocks.shape[2 if self.turned else 1]
        place = pl.ds(pl.multiple_of(member * size, 16), size)
        if self.turned:
            place = pl.ds(pl.multiple_of(member * size, TILE), size)
        for i in range(GROUP):
            block = total[:, i * chunk : (i + 1) * chunk]
            self.blocks[i] = block.T if self.turned else block
        if self.turned:
            target = self.target.at[:, place]
        elif len(self.target.shape) == 2:
            target = self.target.at[place, :]
        else:
            target = self.target.at[member]
        for k in range(1, GROUP):
            self.deals.append(links.send(self.blocks.at[member ^ k], target, bit=k))
        links.save(self.blocks.at[member], target)

    def wait(self):
        for deal in self.deals:
            deal.wait_recv()


def kernel_backward(
    n_dp, n_tensor,
    grad_own, hidden_grad, tokens, hidden1, mlp_part, n1_in, query_in, keyval_in, log_in, att_in,
    cos_in, sin_in, qkv_in, out_in, small_in, down_in, gate_in, up_in, down_got,
    mlp_row, fixed,
    input_out, block_out, qkv_out, out_out, gate_out, up_out, down_out,
    g_all, n1_all, qkv, outw, queries, keyvals, logs, att, cosine, sine, gains, low_col,
    att_grad, other_grad, totals, query_total, pass_on, delta, halo_send, halo_recv,
    to_core, from_core, to_across, from_across, mlp_across, hidden, stage, gate_stage,
    down_swap, gate_swap, up_swap, out_swap, qkv_swap,
    down_come, gate_come, up_come, out_come, qkv_come,
    down_late, gate_late, up_late, out_late, qkv_late,
    down_block, gate_block, up_block, out_block, qkv_block,
    out_sems, in_sems, local_sems,
):
    f32, bf16 = jnp.float32, jnp.bfloat16
    links = Links(n_dp, n_tensor, out_sems, in_sems, local_sems)
    send, move, save = links.send, links.move, links.save
    d_at, z_at = links.d_at, links.z_at
    core = d_at % 2
    upper = d_at // GROUP
    rows, width = grad_own.shape
    half = width // 2
    contract = (((1,), (1,)), ((), ()))
    over_rows = (((0,), (0,)), ((), ()))
    mine = pl.ds(pl.multiple_of(upper * half, half), half)
    other = pl.ds(pl.multiple_of((1 - upper) * half, half), half)
    tiles = rows // TILE
    span = TILE + WINDOW
    quarter = qkv.shape[1]
    out_quarter = outw.shape[1]
    extra = qkv_swap.shape[1] - quarter

    loads = [
        move(grad_own, g_all.at[0]), move(out_in, outw), move(query_in, queries),
        move(keyval_in, keyvals), move(log_in, logs), move(cos_in, cosine), move(sin_in, sine),
        move(mlp_part.at[pl.ds(0, 2)], to_core), move(hidden1, hidden), move(att_in, att),
        move(qkv_in, qkv), move(n1_in, n1_all),
    ]
    small = pltpu.make_async_copy(small_in, gains, local_sems.at[links.used_local])
    links.used_local += 1
    small.start()
    links.barrier()
    across = send(grad_own, g_all.at[1], bit=2)
    beside = send(grad_own, g_all.at[2], bit=1)
    mlp_core = send(mlp_part.at[pl.ds(2, 2)], from_core, bit=1)
    order = []
    for i in range((n_tensor + 1) // 2):
        order.extend(dict.fromkeys((n_tensor - 1 - i, i)))

    down = Collect(
        links, down_in, down_swap, stage, down_come, down_late, down_block, down_out, mine, other,
        turned=True,
    )
    gate = Collect(
        links, gate_in, gate_swap, gate_stage, gate_come, gate_late, gate_block, gate_out, mine, other,
        turned=True,
    )
    up = Collect(
        links, up_in, up_swap, stage, up_come, up_late, up_block, up_out, mine, other, turned=True
    )
    out_part = g_all.at[:, pl.ds(quarter + extra, out_quarter), :]
    qkv_part = g_all.at[:, pl.ds(0, quarter + extra), :]
    out_collect = Collect(
        links, out_part, out_swap, None, out_come, out_late, out_block, out_out, mine, other
    )
    qkv_collect = Collect(
        links, qkv_part, qkv_swap, None, qkv_come, qkv_late, qkv_block, qkv_out, mine, other
    )
    down.load(down_got, order)
    gate.issue(order)
    small.wait()
    for m, k in ((0, 0), (1, 2)):
        info = gains[d_at ^ k].T
        low_col[m] = info[:, 1:2].astype(jnp.int32) - z_at * rows + WINDOW
    loads[0].wait()
    loads[1].wait()

    def attended_back(b):
        units = outw.shape[0] * outw.shape[1]
        att_grad[b] = lax.dot_general(
            g_all[b], outw[...].reshape(units, width), contract, preferred_element_type=f32
        ).astype(bf16)

    attended_back(0)
    beside.wait_recv()
    attended_back(2)
    grad_swap = send(att_grad.at[2], other_grad.at[0], bit=1)
    for p in order[: n_tensor - 1]:
        down.step(p)
    for copy in loads[2:]:
        copy.wait()
    mlp_core.wait_recv()
    heads = queries.shape[2] // HEAD_SIZE
    repeat = QUERY_HEADS // KEY_VALUE_HEADS
    scale = HEAD_SIZE ** (-0.5)
    is_first = core == 0
    second, keys_turn, all_turn = fixed[1:2], fixed[2:3], fixed[3:4]

    def back_tile(m, tile):
        start = tile * TILE
        at = slice(start, start + TILE)
        reach = slice(start, start + span)
        key = lax.broadcasted_iota(jnp.int32, (TILE, span), 1)
        query = lax.broadcasted_iota(jnp.int32, (TILE, span), 0)
        allowed = (key >= low_col[m, at, :] - start) & (key <= query + WINDOW)
        own, others = att_grad[m, at, :], other_grad[m, at, :]
        by_repeat = (jnp.where(is_first, own, others), jnp.where(is_first, others, own))
        for group in range(heads // repeat):
            base = group * 2 * HEAD_SIZE
            k = keyvals[m, reach, base : base + HEAD_SIZE]
            v = keyvals[m, reach, base + HEAD_SIZE : base + 2 * HEAD_SIZE]
            key_sum = None
            for r in range(repeat):
                head = group * repeat + r
                q = queries[m, at, head * HEAD_SIZE : (head + 1) * HEAD_SIZE]
                g = by_repeat[r][:, group * HEAD_SIZE : (group + 1) * HEAD_SIZE]
                s = lax.dot_general(q, k, contract, preferred_element_type=f32) * scale
                total = logs[m, at, head : head + 1]
                p = jnp.exp(jnp.where(allowed, s, NEG_FILL) - total)
                pg = lax.dot_general(g, v, contract, preferred_element_type=f32)
                inner = jnp.sum(p * pg, axis=1, keepdims=True)
                sg = (p * (pg - inner) * scale).astype(bf16)
                query_total[:, head * HEAD_SIZE : (head + 1) * HEAD_SIZE] = jnp.dot(
                    sg, k, preferred_element_type=f32
                )
                dk = lax.dot_general(sg, q, over_rows, preferred_element_type=f32)
                dv = lax.dot_general(p.astype(bf16), g, over_rows, preferred_element_type=f32)
                both = jnp.concatenate([dk, dv], axis=1)
                key_sum = both if key_sum is None else key_sum + both
            totals[m, reach, base : base + 2 * HEAD_SIZE] += key_sum
        turned = turn(
            query_total[...], cosine[m, at, :], sine[m, at, :], second, all_turn, -1.0
        ).astype(bf16)

        @pl.when(is_first)
        def _():
            delta[m, at, :] = turned

        @pl.when(core != 0)
        def _():
            pass_on[m, at, :] = turned

    halos = [
        links.plan(
            halo_send.at[m], halo_recv.at[m], shift=-1, sends=z_at > 0,
            receives=z_at < n_tensor - 1,
        )
        for m in range(2)
    ]

    def back_tiles(m, first_tile, last_tile):
        for tile in range(first_tile, last_tile):
            back_tile(m, tile)

    def send_halo(m):
        halo_send[m] = totals[m, :WINDOW].astype(bf16)
        halos[m].start()

    def finish_block(m):
        halos[m].wait_recv()
        full = totals[m, WINDOW:]
        tail = full[rows - WINDOW :] + jnp.where(
            z_at < n_tensor - 1, halo_recv[m].astype(f32), 0.0
        )
        full = jnp.concatenate([full[: rows - WINDOW], tail], axis=0)
        turned = turn(full, cosine[m], sine[m], second, keys_turn, -1.0).astype(bf16)

        @pl.when(is_first)
        def _():
            pass_on[m] = turned

        @pl.when(core != 0)
        def _():
            delta[m] = turned

        return send(pass_on.at[m], delta.at[2 + m], bit=1)

    free = -(-WINDOW // TILE)
    totals[...] = jnp.zeros_like(totals)
    grad_swap.wait_recv()
    back_tiles(0, 0, free)
    down.relay(1)
    send_halo(0)
    for p in order[n_tensor - 1 :]:
        down.step(p)
    up.issue(order)
    back_tiles(0, free, tiles)
    across.wait_recv()
    both = send(g_all.at[1], g_all.at[3], bit=1)
    to_across[...] = (to_core[1].astype(f32) + from_core[1].astype(f32)).astype(bf16)
    mlp_send = send(to_across, mlp_across, bit=2)
    hidden[...] += to_core[0].astype(f32) + from_core[0].astype(f32)
    attended_back(1)
    both.wait_recv()
    attended_back(3)
    grad_swap = send(att_grad.at[3], other_grad.at[1], bit=1)
    gate.step(order[0])

    def weight_grad(left, right, at):
        total = None
        for b in range(GROUP):
            term = lax.dot_general(
                left[b, :, at], right[b], over_rows, preferred_element_type=f32
            )
            total = term if total is None else total + term
        return total

    out_grad = weight_grad(att, g_all, slice(0, n_tensor * out_quarter)).astype(bf16)
    both.wait_send()
    links.sent.remove(both)
    out_part[...] = out_grad.reshape(n_tensor, out_quarter, width)
    grad_swap.wait_recv()
    back_tiles(1, 0, free)
    for i in range(2, n_tensor - 1):
        down.relay(i)
    send_halo(1)
    gate.step(order[1])
    back_tiles(1, free, tiles)
    for p in order[2 : n_tensor - 1]:
        gate.step(p)
    swap0 = finish_block(0)
    gate.relay(1)
    swap1 = finish_block(1)
    down.finish()
    for p in order[n_tensor - 1 :]:
        gate.step(p)

    def project_back(b):
        units = qkv.shape[0] * quarter
        return jnp.dot(delta[b], qkv[...].reshape(units, width), preferred_element_type=f32)

    mlp_send.wait_recv()
    mlp_across[...] = (hidden[...] + mlp_across[...].astype(f32)).astype(bf16)
    save(mlp_across, block_out)
    mlp_send.wait_send()
    links.sent.remove(mlp_send)
    swap1.wait_recv()
    to_core[1] = project_back(3).astype(bf16)
    core_send1 = send(to_core.at[1], from_core.at[1], bit=1)
    hidden[...] = project_back(1)
    swap0.wait_recv()
    to_core[0] = project_back(2).astype(bf16)
    core_send0 = send(to_core.at[0], from_core.at[0], bit=1)
    core_send1.wait_recv()
    across_sends = []
    for i in range(tiles):
        at = pl.ds(i * TILE, TILE)
        to_across[at] = (hidden[at, :] + from_core[1, at, :].astype(f32)).astype(bf16)
        across_sends.append(send(to_across.at[at], from_across.at[at], bit=2))
    hidden[...] = project_back(0)
    core_send0.wait_recv()
    hidden[...] += from_core[0].astype(f32)
    up.step(order[0])
    attn_row = None
    for p in range(n_tensor):
        at = slice(p * quarter, (p + 1) * quarter)
        grad = weight_grad(delta, n1_all, at)
        row = jnp.sum(grad * qkv[p].astype(f32), axis=0, keepdims=True)
        attn_row = row if attn_row is None else attn_row + row
        qkv_part[p, :quarter, :] = grad.astype(bf16)
    ending = jnp.concatenate(
        [attn_row, mlp_row[...], jnp.zeros((extra - 2, width), f32)], axis=0
    ).astype(bf16)
    for p in range(n_tensor):
        qkv_part[p, quarter:, :] = ending
    qkv_collect.issue(order)
    out_collect.issue(order)
    finals = [
        move(tokens, n1_all.at[0]),
        move(hidden_grad.at[:, pl.ds(0, half)], totals.at[0, pl.ds(0, rows)]),
        move(hidden_grad.at[:, pl.ds(half, half)], totals.at[1, pl.ds(0, rows)]),
    ]
    up.step(order[1])
    gain = jnp.concatenate([gains[i, 2:3, : width // n_dp] for i in range(n_dp)], axis=1)
    for copy in finals:
        copy.wait()
    for i in range(tiles):
        at = pl.ds(i * TILE, TILE)
        across_sends[i].wait_recv()
        upstream = hidden[at, :] + from_across[at, :].astype(f32)
        features = n1_all[0, at, :].astype(f32)
        inverse = lax.rsqrt(jnp.mean(features * features, axis=1, keepdims=True) + EPS)
        scaled = gain * upstream
        mean = jnp.mean(scaled * features, axis=1, keepdims=True)
        change = inverse * scaled - features * (inverse * inverse * inverse) * mean
        n1_all[1, at, :half] = (totals[0, at, :] + change[:, :half]).astype(bf16)
        n1_all[1, at, half:] = (totals[1, at, :] + change[:, half:]).astype(bf16)
        if i == 0:
            for j in range(2, n_tensor - 1):
                gate.relay(j)
        if i == 1:
            for p in order[2 : n_tensor - 1]:
                up.step(p)
    save(n1_all.at[1], input_out)
    gate.finish()
    for p in order[n_tensor - 1 :]:
        up.step(p)
    up.relay(1)
    for p in order[:2]:
        qkv_collect.step(p)
    for i in range(2, n_tensor - 1):
        up.relay(i)
    for p in order[2 : n_tensor - 1]:
        qkv_collect.step(p)
    up.finish()
    for p in order[n_tensor - 1 :]:
        qkv_collect.step(p)
    qkv_collect.relay(1)
    for p in order[:2]:
        out_collect.step(p)
    for i in range(2, n_tensor - 1):
        qkv_collect.relay(i)
    for p in order[2:]:
        out_collect.step(p)
    out_collect.relay(1)
    qkv_collect.finish()
    for i in range(2, n_tensor - 1):
        out_collect.relay(i)
    out_collect.finish()
    for collect in (down, gate, up, out_collect, qkv_collect):
        collect.wait()
    links.finish()


def backward(
    n_dp, n_tensor, grad_own, hidden_grad, tokens, hidden1, mlp_part, normed1, queries, keyvals, logs, attended,
    cosine, sine, qkv_full, out_full, smalls, down_part, gate_part, up_part, down_got,
    mlp_row, fixed,
):
    f32, bf16 = jnp.float32, jnp.bfloat16
    rows, width = grad_own.shape
    half = width // 2
    chunk = width // n_dp
    units = queries.shape[2]
    vmem = pl.BlockSpec(memory_space=pltpu.VMEM)
    hbm = pl.BlockSpec(memory_space=pl.ANY)
    extra = 16
    quarters = [
        down_part.shape[1], gate_part.shape[1], up_part.shape[1], out_full.shape[1],
        qkv_full.shape[1] + extra,
    ]

    def shape(dims, dtype=bf16):
        return jax.ShapeDtypeStruct(tuple(dims), dtype)

    def finals(index):
        return shape((GROUP, quarters[index], chunk))

    outs = [
        shape((rows, width)), shape((rows, width)), finals(4), shape((GROUP * quarters[3], chunk)),
        shape((chunk, GROUP * quarters[1])), shape((chunk, GROUP * quarters[2])),
        shape((chunk, GROUP * quarters[0])),
    ]
    full = (GROUP, rows, width)
    scratch = [
        pltpu.VMEM(full, bf16),
        pltpu.VMEM(full, bf16),
        pltpu.VMEM(qkv_full.shape, bf16),
        pltpu.VMEM(out_full.shape, bf16),
        pltpu.VMEM(queries.shape, bf16),
        pltpu.VMEM(keyvals.shape, bf16),
        pltpu.VMEM(logs.shape, f32),
        pltpu.VMEM(attended.shape, bf16),
        pltpu.VMEM(cosine.shape, f32),
        pltpu.VMEM(sine.shape, f32),
        pltpu.VMEM(smalls.shape, f32),
        pltpu.VMEM((2, rows, 1), jnp.int32),
        pltpu.VMEM(attended.shape, bf16),
        pltpu.VMEM((2,) + attended.shape[1:], bf16),
        pltpu.VMEM((2, rows + WINDOW, units), f32),
        pltpu.VMEM((TILE, units), f32),
        pltpu.VMEM((2, rows, units), bf16),
        pltpu.VMEM((GROUP, rows, units), bf16),
        pltpu.VMEM((2, WINDOW, units), bf16),
        pltpu.VMEM((2, WINDOW, units), bf16),
        pltpu.VMEM((2, rows, width), bf16),
        pltpu.VMEM((2, rows, width), bf16),
        pltpu.VMEM((rows, width), bf16),
        pltpu.VMEM((rows, width), bf16),
        pltpu.VMEM((rows, width), bf16),
        pltpu.VMEM((rows, width), f32),
        pltpu.VMEM((n_tensor, quarters[0], half), bf16),
        pltpu.VMEM((n_tensor, quarters[1], half), bf16),
    ]
    scratch += [pltpu.VMEM((n_tensor, q, half), bf16) for q in quarters]
    scratch += [pltpu.VMEM((n_tensor, q, half), bf16) for q in quarters]
    scratch += [pltpu.VMEM((q, half), bf16) for q in quarters]
    scratch += [
        pltpu.VMEM((GROUP, chunk, q) if turned else (GROUP, q, chunk), bf16)
        for q, turned in zip(quarters, (True, True, True, False, False))
    ]
    scratch += [
        pltpu.SemaphoreType.DMA((160,)),
        pltpu.SemaphoreType.DMA((160,)),
        pltpu.SemaphoreType.DMA((40,)),
    ]
    return pl.pallas_call(
        functools.partial(kernel_backward, n_dp, n_tensor),
        in_specs=[hbm] * 19 + [vmem] * 2,
        out_specs=[hbm] * len(outs),
        out_shape=outs,
        scratch_shapes=scratch,
        compiler_params=pltpu.CompilerParams(
            collective_id=1, has_side_effects=True, vmem_limit_bytes=67043328
        ),
        name="backward",
    )(
        grad_own, hidden_grad, tokens, hidden1, mlp_part, normed1, queries, keyvals, logs, attended, cosine, sine,
        qkv_full, out_full, smalls, down_part, gate_part, up_part, down_got, mlp_row, fixed,
    )


def fast_local(
    n_dp,
    n_tensor,
    block_in,
    cotangent,
    segment_ids,
    attn_gain,
    qkv_weight,
    out_weight,
    mlp_gain,
    gate_weight,
    up_weight,
    down_weight,
):
    bf16, f32 = jnp.bfloat16, jnp.float32
    rows, width = block_in.shape
    part = attn_gain.shape[0]
    (
        normed1, normed2, hidden1, queries, keyvals, log_total, attended, cosine, sine, qkv_full,
        out_full, smalls, grad_rows, gate_full, up_full, down_full,
    ), fixed = forward(
        n_dp, n_tensor, block_in, cotangent, segment_ids, jnp.stack([attn_gain, mlp_gain]),
        qkv_weight, out_weight, gate_weight, up_weight, down_weight,
    )
    (
        hidden1_grad, grad_own, mlp_part, down_part, gate_part, up_part, down_got, mlp_row,
    ) = feed(n_dp, n_tensor, normed2, grad_rows, hidden1, gate_full, up_full, down_full, smalls)
    input_grad, block_out, qkv_blocks, out_grad, gate_grad, up_grad, down_grad = backward(
        n_dp, n_tensor, grad_own, hidden1_grad, block_in, hidden1, mlp_part, normed1, queries,
        keyvals, log_total, attended, cosine, sine, qkv_full, out_full, smalls, down_part, gate_part, up_part, down_got, mlp_row,
        fixed,
    )
    quarter = qkv_full.shape[1]

    def row_of(index, gain):
        return jnp.sum(qkv_blocks[:, quarter + index].astype(f32), axis=0) / gain.astype(f32)

    blocks = qkv_blocks[:, :quarter]
    qkv_grad = blocks.reshape(-1, blocks.shape[2]).T.astype(f32)
    gains = [row_of(0, attn_gain), row_of(1, mlp_gain)]
    return (
        block_out,
        input_grad,
        gains[0],
        qkv_grad,
        out_grad.astype(f32),
        gains[1],
        gate_grad.astype(f32),
        up_grad.astype(f32),
        down_grad.T.astype(f32),
    )


def solution(mesh):
    in_specs = (
        P(("dp", "tensor"), None),
        P(("dp", "tensor"), None),
        P("dp", None),
        P("dp"),
        P("dp", "tensor"),
        P("tensor", "dp"),
        P("dp"),
        P("dp", "tensor"),
        P("dp", "tensor"),
        P("tensor", "dp"),
    )
    out_specs = (
        P(("dp", "tensor"), None),
        P(("dp", "tensor"), None),
        P("dp"),
        P("dp", "tensor"),
        P("tensor", "dp"),
        P("dp"),
        P("dp", "tensor"),
        P("dp", "tensor"),
        P("tensor", "dp"),
    )
    n_dp, n_tensor = mesh.shape["dp"], mesh.shape["tensor"]

    def body(*arrays):
        rows = arrays[0].shape[0]
        groups = arrays[4].shape[1] // (4 * HEAD_SIZE)
        if n_dp == 2 * GROUP and groups == 2 and rows >= WINDOW and rows % TILE == 0:
            return fast_local(n_dp, n_tensor, *arrays)
        return local(*arrays)

    return jax.shard_map(body, mesh=mesh, in_specs=in_specs, out_specs=out_specs, check_vma=False)
```

```python
import functools

import jax
import jax.numpy as jnp
import numpy as np
from jax import lax
from jax.experimental import pallas as pl
from jax.experimental.pallas import tpu as pltpu
from jax.sharding import PartitionSpec as P

QUERY_HEADS = 16
KEY_VALUE_HEADS = 8
HEAD_SIZE = 96


EPS = 1e-05
ROPE_BASE = 100000.0
NEG_FILL = -1e30


def doc_positions(segments):
    length = segments.shape[1]
    position_index = jnp.broadcast_to(jnp.arange(length, dtype=jnp.int32)[None, :], segments.shape)
    change = jnp.concatenate(
        [jnp.ones((segments.shape[0], 1), dtype=bool), segments[:, 1:] != segments[:, :-1]], axis=1
    )
    starts = lax.cummax(jnp.where(change, position_index, jnp.zeros_like(position_index)), axis=1)
    return position_index - starts


def rotary_tables(segments):
    half_dim = HEAD_SIZE // 2
    frequency = jnp.power(ROPE_BASE, -(2.0 * jnp.arange(half_dim, dtype=jnp.float32)) / HEAD_SIZE)
    angles = doc_positions(segments).astype(jnp.float32)[..., None] * frequency
    cosine_table = jnp.concatenate([jnp.cos(angles), jnp.cos(angles)], axis=-1)
    sine_table = jnp.concatenate([jnp.sin(angles), jnp.sin(angles)], axis=-1)
    return (cosine_table, sine_table)


def rotate(vector, cosine_table, sine_table):
    half_dim = vector.shape[-1] // 2
    turned = jnp.concatenate([-vector[..., half_dim:], vector[..., :half_dim]], axis=-1)
    return vector * cosine_table + turned * sine_table


def unrotate(vector, cosine_table, sine_table):
    half_dim = vector.shape[-1] // 2
    shifted = vector * sine_table
    returned = jnp.concatenate([shifted[..., half_dim:], -shifted[..., :half_dim]], axis=-1)
    return vector * cosine_table + returned


def allowed_pairs(segments):
    length = segments.shape[1]
    offsets = jnp.arange(length)
    causal = offsets[None, :] <= offsets[:, None]
    same_doc = segments[:, :, None] == segments[:, None, :]
    return (causal[None] & same_doc)[:, None, None]


def score_block(queries, key_heads, segments):
    scores = jnp.einsum(
        "sqgrd,skgd->sgrqk", queries, key_heads, preferred_element_type=jnp.float32
    ) * HEAD_SIZE ** (-0.5)
    return jnp.where(allowed_pairs(segments), scores, NEG_FILL)


def rms_scale(features):
    return lax.rsqrt(jnp.mean(features * features, axis=-1, keepdims=True) + EPS)


def norm_back(features, inverse, gain_vector, upstream):
    scaled = gain_vector * upstream
    return inverse * scaled - features * (inverse * inverse * inverse) * jnp.mean(
        scaled * features, axis=-1, keepdims=True
    )


def widen(shard_rows):
    return lax.all_gather(shard_rows, "tensor", axis=0, tiled=True)


def narrow(partial_value):
    return lax.psum_scatter(
        partial_value.astype(jnp.bfloat16), "tensor", scatter_dimension=0, tiled=True
    ).astype(jnp.float32)


def local(
    block_in,
    cotangent,
    segment_ids,
    attn_gain,
    qkv_weight,
    out_weight,
    mlp_gain,
    gate_weight,
    up_weight,
    down_weight,
):
    qkv_full, gate_full, up_full, gain_attn_raw, gain_mlp_raw = (
        lax.all_gather(qkv_weight, "dp", axis=0, tiled=True),
        lax.all_gather(gate_weight, "dp", axis=0, tiled=True),
        lax.all_gather(up_weight, "dp", axis=0, tiled=True),
        lax.all_gather(attn_gain, "dp", axis=0, tiled=True),
        lax.all_gather(mlp_gain, "dp", axis=0, tiled=True),
    )
    out_cols, down_cols = (
        lax.all_gather(out_weight, "dp", axis=1, tiled=True),
        lax.all_gather(down_weight, "dp", axis=1, tiled=True),
    )
    seq_count, length = segment_ids.shape
    repeat_factor = QUERY_HEADS // KEY_VALUE_HEADS
    groups = qkv_full.shape[1] // ((repeat_factor + 2) * HEAD_SIZE)
    gain_attn = gain_attn_raw.astype(jnp.float32)
    gain_mlp = gain_mlp_raw.astype(jnp.float32)
    residual = block_in.astype(jnp.float32)
    scale_attn = rms_scale(residual)
    normed1 = widen((residual * scale_attn * gain_attn).astype(jnp.bfloat16))
    projected = jnp.dot(normed1, qkv_full, preferred_element_type=jnp.float32).reshape(
        seq_count, length, groups, repeat_factor + 2, HEAD_SIZE
    )
    cosine_table, sine_table = rotary_tables(segment_ids)
    cos_query = cosine_table[:, :, None, None, :]
    sin_query = sine_table[:, :, None, None, :]
    cos_key = cosine_table[:, :, None, :]
    sin_key = sine_table[:, :, None, :]
    queries = rotate(projected[:, :, :, :repeat_factor], cos_query, sin_query).astype(jnp.bfloat16)
    key_heads = rotate(projected[:, :, :, repeat_factor], cos_key, sin_key).astype(jnp.bfloat16)
    values = projected[:, :, :, repeat_factor + 1].astype(jnp.bfloat16)
    scores = score_block(queries, key_heads, segment_ids)
    highest = jnp.max(scores, axis=-1, keepdims=True)
    log_total = highest + jnp.log(jnp.sum(jnp.exp(scores - highest), axis=-1, keepdims=True))
    probability = jnp.exp(scores - log_total).astype(jnp.bfloat16)
    attended = jnp.einsum(
        "sgrqk,skgd->sqgrd", probability, values, preferred_element_type=jnp.float32
    ).astype(jnp.bfloat16)
    attn_flat = attended.reshape(seq_count * length, groups * repeat_factor * HEAD_SIZE)
    attn_delta = lax.psum_scatter(
        jnp.dot(attn_flat, out_cols, preferred_element_type=jnp.float32).astype(jnp.bfloat16),
        "tensor",
        scatter_dimension=0,
        tiled=True,
    ).astype(jnp.float32)
    hidden1 = residual + attn_delta
    scale_mlp = rms_scale(hidden1)
    normed2 = widen((hidden1 * scale_mlp * gain_mlp).astype(jnp.bfloat16))
    gate = jnp.dot(normed2, gate_full, preferred_element_type=jnp.float32)
    up_value = jnp.dot(normed2, up_full, preferred_element_type=jnp.float32)
    sigmoid_gate = jax.nn.sigmoid(gate)
    activated = (gate * sigmoid_gate * up_value).astype(jnp.bfloat16)
    mlp_delta = narrow(jnp.dot(activated, down_cols, preferred_element_type=jnp.float32))
    block_out = (hidden1 + mlp_delta).astype(jnp.bfloat16)
    grad_rows = widen(cotangent)
    down_part = jnp.einsum("tf,td->fd", activated, grad_rows, preferred_element_type=jnp.float32)
    act_grad = jnp.einsum("td,fd->tf", grad_rows, down_cols, preferred_element_type=jnp.float32)
    gate_delta = (act_grad * up_value * sigmoid_gate * (1.0 + gate * (1.0 - sigmoid_gate))).astype(
        jnp.bfloat16
    )
    up_delta = (act_grad * gate * sigmoid_gate).astype(jnp.bfloat16)
    gate_part = jnp.einsum("td,tf->df", normed2, gate_delta, preferred_element_type=jnp.float32)
    up_part = jnp.einsum("td,tf->df", normed2, up_delta, preferred_element_type=jnp.float32)
    normed2_term = jnp.einsum(
        "tf,df->td", gate_delta, gate_full, preferred_element_type=jnp.float32
    ) + jnp.einsum("tf,df->td", up_delta, up_full, preferred_element_type=jnp.float32)
    normed2_grad = narrow(normed2_term)
    mlp_gain_part = jnp.sum(normed2_grad * hidden1 * scale_mlp, axis=0)
    hidden1_grad = cotangent.astype(jnp.float32) + norm_back(
        hidden1, scale_mlp, gain_mlp, normed2_grad
    )
    hidden1_rounded = hidden1_grad.astype(jnp.bfloat16)
    grad_full = lax.all_gather(hidden1_rounded, "tensor", axis=0, tiled=True)
    attended_grad = jnp.einsum(
        "td,hd->th", grad_full, out_cols, preferred_element_type=jnp.float32
    ).astype(jnp.bfloat16)
    out_part = jnp.einsum("th,td->hd", attn_flat, grad_full, preferred_element_type=jnp.float32)
    attended_grad = attended_grad.reshape(seq_count, length, groups, repeat_factor, HEAD_SIZE)
    prob_full = jnp.exp(score_block(queries, key_heads, segment_ids) - log_total)
    prob_grad = jnp.einsum(
        "sqgrd,skgd->sgrqk", attended_grad, values, preferred_element_type=jnp.float32
    )
    inner_sum = jnp.sum(prob_full * prob_grad, axis=-1, keepdims=True)
    score_grad = (prob_full * (prob_grad - inner_sum) * HEAD_SIZE ** (-0.5)).astype(jnp.bfloat16)
    query_grad = jnp.einsum(
        "sgrqk,skgd->sqgrd", score_grad, key_heads, preferred_element_type=jnp.float32
    )
    key_grad = jnp.einsum(
        "sgrqk,sqgrd->skgd", score_grad, queries, preferred_element_type=jnp.float32
    )
    value_grad = jnp.einsum(
        "sgrqk,sqgrd->skgd",
        prob_full.astype(jnp.bfloat16),
        attended_grad,
        preferred_element_type=jnp.float32,
    )
    projected_grad = jnp.concatenate(
        [
            unrotate(query_grad, cos_query, sin_query),
            unrotate(key_grad, cos_key, sin_key)[:, :, :, None],
            value_grad[:, :, :, None],
        ],
        axis=3,
    )
    projected_grad = projected_grad.astype(jnp.bfloat16).reshape(
        seq_count * length, groups * (repeat_factor + 2) * HEAD_SIZE
    )
    qkv_part = jnp.einsum("td,tc->dc", normed1, projected_grad, preferred_element_type=jnp.float32)
    normed1_grad = narrow(
        jnp.einsum("tc,dc->td", projected_grad, qkv_full, preferred_element_type=jnp.float32)
    )
    attn_gain_part = jnp.sum(normed1_grad * residual * scale_attn, axis=0)
    input_grad = (hidden1_grad + norm_back(residual, scale_attn, gain_attn, normed1_grad)).astype(
        jnp.bfloat16
    )
    attn_gain_total, mlp_gain_total = lax.psum((attn_gain_part, mlp_gain_part), "tensor")
    attn_gain_grad, qkv_grad, gate_grad, up_grad, mlp_gain_grad = (
        lax.psum_scatter(
            attn_gain_total.astype(jnp.bfloat16), "dp", scatter_dimension=0, tiled=True
        ).astype(jnp.float32),
        lax.psum_scatter(
            qkv_part.astype(jnp.bfloat16), "dp", scatter_dimension=0, tiled=True
        ).astype(jnp.float32),
        lax.psum_scatter(
            gate_part.astype(jnp.bfloat16), "dp", scatter_dimension=0, tiled=True
        ).astype(jnp.float32),
        lax.psum_scatter(
            up_part.astype(jnp.bfloat16), "dp", scatter_dimension=0, tiled=True
        ).astype(jnp.float32),
        lax.psum_scatter(
            mlp_gain_total.astype(jnp.bfloat16), "dp", scatter_dimension=0, tiled=True
        ).astype(jnp.float32),
    )
    out_grad, down_grad = (
        lax.psum_scatter(
            out_part.astype(jnp.bfloat16), "dp", scatter_dimension=1, tiled=True
        ).astype(jnp.float32),
        lax.psum_scatter(
            down_part.astype(jnp.bfloat16), "dp", scatter_dimension=1, tiled=True
        ).astype(jnp.float32),
    )
    return (
        block_out,
        input_grad,
        attn_gain_grad,
        qkv_grad,
        out_grad,
        mlp_gain_grad,
        gate_grad,
        up_grad,
        down_grad,
    )


GROUP = 4
WINDOW = 256
LANES = 384
TILE = 128


MESH = pl.DeviceIdType.MESH


class Transfer:
    def __init__(self, copy, sends=None, receives=None):
        self.copy, self.sends, self.receives = copy, sends, receives

    def _when(self, condition, action):
        if condition is None:
            action()
        else:
            pl.when(condition)(action)

    def start(self):
        self._when(self.sends, self.copy.start)
        return self

    def wait_recv(self):
        self._when(self.receives, self.copy.wait_recv)

    def wait_send(self):
        self._when(self.sends, self.copy.wait_send)


class Links:
    def __init__(self, n_dp, n_tensor, out_sems, in_sems, local_sems):
        self.n_dp, self.n_tensor = n_dp, n_tensor
        self.out_sems, self.in_sems, self.local_sems = out_sems, in_sems, local_sems
        self.d_at, self.z_at = lax.axis_index("dp"), lax.axis_index("tensor")
        self.used, self.used_local = 0, 0
        self.sent, self.saved = [], []

    def barrier(self):
        barrier = pltpu.get_barrier_semaphore()
        for k in range(1, self.n_dp):
            pl.semaphore_signal(
                barrier,
                inc=1,
                device_id={"dp": self.d_at ^ k, "tensor": self.z_at},
                device_id_type=MESH,
            )
        for s in range(1, self.n_tensor):
            pl.semaphore_signal(
                barrier,
                inc=1,
                device_id={"dp": self.d_at, "tensor": lax.rem(self.z_at + s, self.n_tensor)},
                device_id_type=MESH,
            )
        pl.semaphore_wait(barrier, self.n_dp - 1 + self.n_tensor - 1)

    def plan(self, source, target, bit=0, shift=0, sends=None, receives=None):
        slot = self.used
        self.used += 1
        copy = pltpu.make_async_remote_copy(
            src_ref=source,
            dst_ref=target,
            send_sem=self.out_sems.at[slot],
            recv_sem=self.in_sems.at[slot],
            device_id={
                "dp": self.d_at ^ bit,
                "tensor": lax.rem(self.z_at + self.n_tensor + shift, self.n_tensor),
            },
            device_id_type=MESH,
        )
        transfer = Transfer(copy, sends, receives)
        self.sent.append(transfer)
        return transfer

    def send(self, source, target, bit=0, shift=0):
        return self.plan(source, target, bit, shift).start()

    def move(self, source, target):
        copy = pltpu.make_async_copy(source, target, self.local_sems.at[self.used_local])
        self.used_local += 1
        copy.start()
        return copy

    def save(self, source, target):
        self.saved.append(self.move(source, target))

    def finish(self):
        for transfer in self.sent:
            transfer.wait_send()
        for copy in self.saved:
            copy.wait()


class Spread:
    def __init__(self, links, own_piece, target, columns):
        self.links, self.own_piece, self.target, self.columns = links, own_piece, target, columns
        self.ahead, self.back, self.swaps = [], [], []

    def _slot(self, index):
        n = self.links.n_tensor
        return self.target.at[lax.rem(index + n, n), :, self.columns]

    def issue(self):
        links, n, z = self.links, self.links.n_tensor, self.links.z_at
        own = self._slot(z)
        for s in range(1, n):
            up_from, down_from = z - (s - 1), z + (s - 1)
            up_source = self.own_piece if s == 1 else self._slot(up_from)
            down_source = self.own_piece if s == 1 else self._slot(down_from)
            self.ahead.append(
                links.plan(
                    up_source, self._slot(up_from), shift=1,
                    sends=(z < n - 1) & (up_from >= 0), receives=z >= s,
                )
            )
            self.back.append(
                links.plan(
                    down_source, self._slot(down_from), shift=-1,
                    sends=(z > 0) & (down_from < n), receives=z + s < n,
                )
            )
        self.ahead[0].start()
        self.back[0].start()
        self.swaps.append(links.plan(self.own_piece, own, bit=GROUP).start())

    def step(self, s):
        links, n, z = self.links, self.links.n_tensor, self.links.z_at
        for arrivals, piece, here in (
            (self.ahead, z - s, z >= s),
            (self.back, z + s, z + s < n),
        ):
            arrivals[s - 1].wait_recv()
            if s < n - 1:
                arrivals[s].start()
            slot = self._slot(piece)
            self.swaps.append(
                links.plan(slot, slot, bit=GROUP, sends=here, receives=here).start()
            )

    def wait(self):
        for swap in self.swaps:
            swap.wait_recv()


def kernel_forward(
    n_dp, n_tensor,
    tokens, cot, gate_w, up_w, down_w, out_w, qkv_w, segments, gain_rows, fixed,
    normed1_out, normed2_out, hidden_out, query_out, keyval_out, log_out, att_out,
    cos_out, sin_out, qkv_out, out_out, small_out, cot_out, gate_out, up_out, down_out,
    x_all, n1_all, first, dealt, first_piece, qkv, out_parcel, obuf, gbuf, ubuf, dbuf, piece, outw,
    small, small_all, stream, parts, recv, queries, keyvals,
    att, by_repeat, logs, cosine, sine, low_col, to_core, from_core, to_across, from_across,
    hidden, n2_all, stage, out_sems, in_sems, local_sems,
):
    f32, bf16 = jnp.float32, jnp.bfloat16
    links = Links(n_dp, n_tensor, out_sems, in_sems, local_sems)
    send, move, save = links.send, links.move, links.save
    d_at, z_at = links.d_at, links.z_at
    member = d_at % GROUP
    core = d_at % 2
    upper = d_at // GROUP
    rows, width = tokens.shape
    half = width // 2
    chunk = qkv_w.shape[0]
    contract = (((1,), (1,)), ((), ()))
    columns = pl.ds(pl.multiple_of(upper * half, half), half)

    turned = qkv_w[...].T
    quarter = turned.shape[0] // GROUP
    for i in range(GROUP):
        first[i] = turned[i * quarter : (i + 1) * quarter]
    turned = out_w[...].T
    out_quarter = turned.shape[0] // GROUP
    for i in range(GROUP):
        out_parcel[i] = turned[i * out_quarter : (i + 1) * out_quarter]
    ids = segments[...]
    seqs, length = ids.shape
    begin = jnp.zeros_like(ids)
    for value in range(3):
        count = jnp.sum((ids == value).astype(jnp.int32), axis=1, keepdims=True)
        begin = begin + jnp.where(ids > value, count, 0)
    begin = begin.astype(f32)
    for i in range(seqs):
        stream[:, i * length : (i + 1) * length] = jnp.broadcast_to(
            begin[i : i + 1] + float(i * length), (stream.shape[0], length)
        )
    window = stream[:, pl.ds(pl.multiple_of(z_at * rows, TILE), rows)]
    here = lax.broadcasted_iota(jnp.int32, window.shape, 1) + z_at * rows
    small[...] = window
    small[0:1] = here.astype(f32)[0:1] - window[0:1]
    small[2:4, :chunk] = gain_rows[...].astype(f32)

    @pl.when(z_at == 0)
    def _():
        keyvals[:, :WINDOW, :] = jnp.zeros_like(keyvals[:, :WINDOW, :])

    links.barrier()

    deals = [send(first.at[member ^ k], dealt.at[member], bit=k) for k in range(1, GROUP)]
    beside = send(tokens, x_all.at[2], bit=1)
    smalls = [send(small, small_all.at[d_at], bit=k) for k in range(1, n_dp)]
    def columns_of(ref, at):
        size = ref.shape[1] // GROUP
        return ref.at[:, pl.ds(pl.multiple_of(at * size, TILE), size)]

    def parcel_of(ref, at):
        return ref.at[at]

    pairs = [
        (out_parcel, obuf, parcel_of), (gate_w, gbuf, columns_of), (up_w, ubuf, columns_of),
        (down_w, dbuf, columns_of),
    ]

    def deal(group):
        return [
            send(take(ref, member ^ k), buffer.at[member], bit=k)
            for ref, buffer, take in group
            for k in range(1, GROUP)
        ]

    rests = deal(pairs[:2])
    across = send(tokens, x_all.at[1], bit=2)
    late_rests = deal(pairs[2:])
    own = [move(tokens, x_all.at[0])]
    for ref, buffer, take in pairs:
        own.append(move(take(ref, member), buffer.at[member]))
    cot_stage = move(cot, stage)
    small_all[d_at] = small[...]
    dealt[member] = first[member]

    entries = lax.broadcasted_iota(jnp.int32, (WINDOW, LANES), 0).astype(f32)
    angles = entries * fixed[0:1]

    def split(table):
        pieces = []
        for _ in range(3):
            pieces.append(table.astype(bf16))
            table = table - pieces[-1].astype(f32)
        return pieces

    cos_parts, sin_parts = split(jnp.cos(angles)), split(jnp.sin(angles))
    second = fixed[1:2]
    own_turns = jnp.where(core == 0, jnp.ones_like(second), fixed[2:3])

    for copy in deals:
        copy.wait_recv()
    for i in range(GROUP):
        first_piece[:, i * chunk : (i + 1) * chunk] = dealt[i]
    spread_first = Spread(links, first_piece, qkv, columns)
    spread_first.issue()
    save(first_piece, qkv.at[z_at, :, columns])
    own_qkv = links.saved.pop()
    for copy in own:
        copy.wait()
    cot_stage.wait()
    save(stage, cot_out.at[0])
    spread_first.step(1)
    for copy in smalls:
        copy.wait_recv()
    spread_first.step(2)
    gains = []
    for row in (2, 3):
        gains.append(
            jnp.concatenate([small_all[i, row : row + 1, :chunk] for i in range(n_dp)], axis=1)
        )
    for copy in rests:
        copy.wait_recv()
    sizes = [obuf.shape[1], gbuf.shape[2], ubuf.shape[2], dbuf.shape[2]]
    starts = [sum(sizes[:i]) for i in range(len(sizes))]
    saves = []

    def prepare(index, target, buffer):
        at = slice(starts[index], starts[index] + sizes[index])
        for i in range(GROUP):
            piece[at, i * chunk : (i + 1) * chunk] = buffer[i] if index == 0 else buffer[i].T
        own_piece = piece.at[pl.ds(starts[index], sizes[index])]
        saves.append(move(own_piece, target.at[z_at, :, columns]))
        return Spread(links, own_piece, target, columns)

    out_spread = prepare(0, outw, obuf)
    gate_spread = prepare(1, gate_out, gbuf)
    out_spread.issue()
    spread_first.step(3)
    gate_spread.issue()
    beside.wait_recv()
    own_qkv.wait()
    spread_first.wait()

    def project_block(m, k):
        features = x_all[m].astype(f32)
        scale = lax.rsqrt(jnp.mean(features * features, axis=1, keepdims=True) + EPS)
        normal = (features * scale * gains[0]).astype(bf16)
        n1_all[m] = normal
        units = qkv.shape[0] * qkv.shape[1]
        product = lax.dot_general(
            normal, qkv[...].reshape(units, width), contract, preferred_element_type=f32
        )
        info = small_all[d_at ^ k].T
        key = lax.broadcasted_iota(jnp.int32, (rows, WINDOW), 1)
        chosen = (info[:, 0:1].astype(jnp.int32) == key).astype(bf16)

        def pick(table):
            total = jnp.dot(chosen, table[0], preferred_element_type=f32)
            for part in table[1:]:
                total += jnp.dot(chosen, part, preferred_element_type=f32)
            return total

        cos_here, sin_here = pick(cos_parts), pick(sin_parts)
        parts[m] = turn(product, cos_here, sin_here, second, own_turns, 1.0).astype(bf16)
        if m < 2:
            cosine[m] = cos_here
            sine[m] = sin_here
            low_col[m] = info[:, 1:2].astype(jnp.int32) - z_at * rows + WINDOW

    is_first = core == 0
    halos = [
        links.plan(
            keyvals.at[m, pl.ds(rows, WINDOW)], keyvals.at[m, pl.ds(0, WINDOW)], shift=1,
            sends=z_at < n_tensor - 1, receives=z_at > 0,
        )
        for m in range(2)
    ]

    def take_block(m, swap):
        swap.wait_recv()
        mine, other = parts[m], recv[m]
        queries[m] = jnp.where(is_first, mine, other)
        keyvals[m, WINDOW:, :] = jnp.where(is_first, other, mine)
        halos[m].start()

    project_block(2, 1)
    part_swap = send(parts.at[2], recv.at[0], bit=1)
    project_block(0, 0)
    take_block(0, part_swap)
    out_spread.step(1)
    across.wait_recv()
    both = send(x_all.at[1], x_all.at[3], bit=1)
    cot_across = send(cot, cot_out.at[1], bit=2)
    cot_beside = send(cot, cot_out.at[2], bit=1)
    project_block(1, 2)
    both.wait_recv()
    project_block(3, 3)
    part_swap = send(parts.at[3], recv.at[1], bit=1)
    save(n1_all, normed1_out)
    save(cosine, cos_out)
    save(sine, sin_out)
    take_block(1, part_swap)
    out_spread.step(2)
    gate_spread.step(1)
    for copy in late_rests:
        copy.wait_recv()
    up_spread = prepare(2, up_out, ubuf)
    down_spread = prepare(3, down_out, dbuf)
    save(queries, query_out)
    heads = queries.shape[2] // HEAD_SIZE
    repeat = QUERY_HEADS // KEY_VALUE_HEADS
    span = TILE + WINDOW

    def attend_tile(m, start):
        key = lax.broadcasted_iota(jnp.int32, (TILE, span), 1)
        query = lax.broadcasted_iota(jnp.int32, (TILE, span), 0)
        lowest = low_col[m, pl.ds(start, TILE), :] - start
        allowed = (key >= lowest) & (key <= query + WINDOW)
        for head in range(heads):
            group, r = head // repeat, head % repeat
            base = group * 2 * HEAD_SIZE
            q = queries[m, pl.ds(start, TILE), head * HEAD_SIZE : (head + 1) * HEAD_SIZE]
            k = keyvals[m, pl.ds(start, span), base : base + HEAD_SIZE]
            v = keyvals[m, pl.ds(start, span), base + HEAD_SIZE : base + 2 * HEAD_SIZE]
            s = lax.dot_general(q, k, contract, preferred_element_type=f32) * HEAD_SIZE ** (-0.5)
            s = jnp.where(allowed, s, NEG_FILL)
            highest = jnp.max(s, axis=1, keepdims=True)
            e = jnp.exp(s - highest)
            whole = jnp.sum(e, axis=1, keepdims=True)
            p = (e * (1.0 / whole)).astype(bf16)
            o = jnp.dot(p, v, preferred_element_type=f32).astype(bf16)
            logs[m, pl.ds(start, TILE), head : head + 1] = highest + jnp.log(whole)
            by_repeat[r, m, pl.ds(start, TILE), group * HEAD_SIZE : (group + 1) * HEAD_SIZE] = o

    tiles = rows // TILE
    free = -(-WINDOW // TILE)

    def attend_tiles(blocks, first_tile, last_tile):
        count = last_tile - first_tile

        def body(i, carry):
            m = blocks[0] + (i // count) * (blocks[-1] - blocks[0])
            attend_tile(m, pl.multiple_of((first_tile + i % count) * TILE, TILE))
            return carry

        lax.fori_loop(0, count * len(blocks), body, 0)

    attend_tiles((1, 0), free, tiles)
    out_spread.step(3)
    up_spread.issue()
    halos[0].wait_recv()
    halos[1].wait_recv()
    attend_tiles((1,), 0, free)
    att_swap1 = send(by_repeat.at[1 - core, 1], att.at[3], bit=1)
    gate_spread.step(2)
    attend_tiles((0,), 0, free)
    att_swap0 = send(by_repeat.at[1 - core, 0], att.at[2], bit=1)
    save(keyvals, keyval_out)
    save(logs, log_out)
    att[0] = by_repeat[core, 0]
    att[1] = by_repeat[core, 1]
    down_spread.issue()
    cot_across.wait_recv()
    cot_both = send(cot_out.at[1], cot_out.at[3], bit=1)

    saves[0].wait()
    out_spread.wait()

    def project_out(b):
        units = outw.shape[0] * outw.shape[1]
        return jnp.dot(att[b], outw[...].reshape(units, width), preferred_element_type=f32)

    att_swap1.wait_recv()
    to_core[1] = project_out(3).astype(bf16)
    core_send1 = send(to_core.at[1], from_core.at[1], bit=1)
    hidden[...] = project_out(1)
    att_swap0.wait_recv()
    to_core[0] = project_out(2).astype(bf16)
    core_send0 = send(to_core.at[0], from_core.at[0], bit=1)
    core_send1.wait_recv()
    across_sends = []
    for i in range(tiles):
        at = pl.ds(i * TILE, TILE)
        to_across[at] = (hidden[at, :] + from_core[1, at, :].astype(f32)).astype(bf16)
        across_sends.append(send(to_across.at[at], from_across.at[at], bit=2))
    hidden[...] = project_out(0) + x_all[0].astype(f32)
    core_send0.wait_recv()
    hidden[...] += from_core[0].astype(f32)
    save(att, att_out)
    gate_spread.step(3)
    up_spread.step(1)
    steps = [
        (up_spread, 2), (up_spread, 3), (down_spread, 1), (down_spread, 2), (down_spread, 3),
    ]
    last = []
    for i in range(tiles):
        at = pl.ds(i * TILE, TILE)
        across_sends[i].wait_recv()
        value = hidden[at, :] + from_across[at, :].astype(f32)
        hidden[at, :] = value
        scale = lax.rsqrt(jnp.mean(value * value, axis=1, keepdims=True) + EPS)
        n2_all[0, at, :] = (value * scale * gains[1]).astype(bf16)
        last.append(send(n2_all.at[0, at], n2_all.at[1, at], bit=2))
        last.append(send(n2_all.at[0, at], n2_all.at[2, at], bit=1))
        if i < 3:
            spread, s = steps.pop(0)
            spread.step(s)
    save(hidden, hidden_out)
    save(qkv, qkv_out)
    save(outw, out_out)
    save(small_all, small_out)
    ends = []
    for i in range(tiles):
        at = pl.ds(i * TILE, TILE)
        last[2 * i].wait_recv()
        ends.append(send(n2_all.at[1, at], n2_all.at[3, at], bit=1))
        if i < 2:
            spread, s = steps.pop(0)
            spread.step(s)
    for copy in ends + last[1::2]:
        copy.wait_recv()
    save(n2_all, normed2_out)
    for copy in saves[1:]:
        copy.wait()
    for spread in (gate_spread, up_spread, down_spread):
        spread.wait()
    for copy in (cot_beside, cot_both):
        copy.wait_recv()
    links.finish()


def forward(
    n_dp, n_tensor, tokens, cot, segments, gain_rows, qkv_w, out_w, gate_w, up_w, down_w
):
    out_w, down_w = out_w.T, down_w.T
    rows, width = tokens.shape
    f32, bf16 = jnp.float32, jnp.bfloat16
    vmem = pl.BlockSpec(memory_space=pltpu.VMEM)
    hbm = pl.BlockSpec(memory_space=pl.ANY)
    chunk = qkv_w.shape[0]
    quarter = qkv_w.shape[1] // GROUP
    sizes = [
        out_w.shape[1] // GROUP, gate_w.shape[1] // GROUP, up_w.shape[1] // GROUP,
        down_w.shape[1] // GROUP,
    ]
    units = quarter * n_tensor
    heads = units // HEAD_SIZE
    lane = np.arange(LANES)
    within = lane % HEAD_SIZE
    fixed = np.zeros((8, LANES), np.float32)
    fixed[0] = np.power(ROPE_BASE, -(2.0 * (within % (HEAD_SIZE // 2))) / HEAD_SIZE)
    fixed[1] = within >= HEAD_SIZE // 2
    fixed[2] = lane % (2 * HEAD_SIZE) < HEAD_SIZE
    fixed[3] = 1.0

    def shape(dims, dtype=bf16):
        return jax.ShapeDtypeStruct(tuple(dims), dtype)

    full = (GROUP, rows, width)
    qkv_shape = (n_tensor, quarter, width)
    out_shape = (n_tensor, sizes[0], width)
    att_shape = (GROUP, rows, units // 2)
    small_shape = (n_dp, 8, rows)
    table = (2, rows, LANES)
    outs = [
        shape(full),
        shape(full),
        shape((rows, width), f32),
        shape((2, rows, units)),
        shape((2, rows + WINDOW, units)),
        shape((2, rows, heads), f32),
        shape(att_shape),
        shape(table, f32),
        shape(table, f32),
        shape(qkv_shape),
        shape(out_shape),
        shape(small_shape, f32),
        shape(full),
    ] + [shape((n_tensor, size, width)) for size in sizes[1:]]
    scratch = [
        pltpu.VMEM(full, bf16),
        pltpu.VMEM(full, bf16),
        pltpu.VMEM((GROUP, quarter, chunk), bf16),
        pltpu.VMEM((GROUP, quarter, chunk), bf16),
        pltpu.VMEM((quarter, width // 2), bf16),
        pltpu.VMEM(qkv_shape, bf16),
        pltpu.VMEM((GROUP, sizes[0], chunk), bf16),
        pltpu.VMEM((GROUP, sizes[0], chunk), bf16),
        pltpu.VMEM((GROUP, chunk, sizes[1]), bf16),
        pltpu.VMEM((GROUP, chunk, sizes[2]), bf16),
        pltpu.VMEM((GROUP, chunk, sizes[3]), bf16),
        pltpu.VMEM((sum(sizes), width // 2), bf16),
        pltpu.VMEM(out_shape, bf16),
        pltpu.VMEM((8, rows), f32),
        pltpu.VMEM(small_shape, f32),
        pltpu.VMEM((8, n_tensor * rows), f32),
        pltpu.VMEM((GROUP, rows, units), bf16),
        pltpu.VMEM((2, rows, units), bf16),
        pltpu.VMEM((2, rows, units), bf16),
        pltpu.VMEM((2, rows + WINDOW, units), bf16),
        pltpu.VMEM(att_shape, bf16),
        pltpu.VMEM((2, 2, rows, units // 2), bf16),
        pltpu.VMEM((2, rows, heads), f32),
        pltpu.VMEM(table, f32),
        pltpu.VMEM(table, f32),
        pltpu.VMEM((2, rows, 1), jnp.int32),
        pltpu.VMEM((2, rows, width), bf16),
        pltpu.VMEM((2, rows, width), bf16),
        pltpu.VMEM((rows, width), bf16),
        pltpu.VMEM((rows, width), bf16),
        pltpu.VMEM((rows, width), f32),
        pltpu.VMEM(full, bf16),
        pltpu.VMEM((rows, width), bf16),
        pltpu.SemaphoreType.DMA((128,)),
        pltpu.SemaphoreType.DMA((128,)),
        pltpu.SemaphoreType.DMA((40,)),
    ]
    results = pl.pallas_call(
        functools.partial(kernel_forward, n_dp, n_tensor),
        in_specs=[hbm] * 5 + [vmem] * 5,
        out_specs=[hbm] * len(outs),
        out_shape=outs,
        scratch_shapes=scratch,
        compiler_params=pltpu.CompilerParams(
            collective_id=0, has_side_effects=True, vmem_limit_bytes=60 * 1024 * 1024
        ),
        name="forward",
    )(
        tokens, cot, gate_w, up_w, down_w, out_w, qkv_w, segments, gain_rows, jnp.asarray(fixed)
    )
    return results, jnp.asarray(fixed)


def turn(value, cosine, sine, second, turns, sign):
    width = value.shape[1]
    half = HEAD_SIZE // 2
    c = turns * cosine + (1.0 - turns)
    u = (sign * turns * second) * sine
    d = (sign * turns * (second - 1.0)) * sine
    pieces = []
    up = pltpu.roll(value, half, 1)
    down = pltpu.roll(value, width - half, 1)
    for i in range(width // LANES):
        at = slice(i * LANES, (i + 1) * LANES)
        pieces.append(value[:, at] * c + up[:, at] * u + down[:, at] * d)
    return jnp.concatenate(pieces, axis=1)


def kernel_feed(
    n_dp, n_tensor,
    n2_in, cot_in, hidden_in, gate_in, up_in, down_in, smalls,
    grad_out, grad_own_out, mlp_out, down_out, gate_out, up_out, down_got, row_out,
    n2_all, cot_all, gate_w, up_w, down_w, active, gate_delta, up_delta,
    down_part, gate_part, up_part, to_core, from_core, to_across, from_across, hidden, total,
    rounded, row, out_sems, in_sems, local_sems,
):
    f32, bf16 = jnp.float32, jnp.bfloat16
    links = Links(n_dp, n_tensor, out_sems, in_sems, local_sems)
    send, move, save = links.send, links.move, links.save
    upper = links.d_at // GROUP
    rows, width = hidden.shape
    half = width // 2
    chunk = width // n_dp
    size = gate_w.shape[1]
    units = n_tensor * size
    contract = (((1,), (1,)), ((), ()))
    over_rows = (((0,), (0,)), ((), ()))
    other = pl.ds(pl.multiple_of((1 - upper) * half, half), half)
    tiles = rows // TILE

    first_sem = links.used_local
    links.used_local += 3 * n_tensor + 2 * GROUP
    weights = ((gate_in, gate_w), (up_in, up_w), (down_in, down_w))
    tokens = ((n2_in, n2_all), (cot_in, cot_all))

    def weight_loads(p):
        return [
            pltpu.make_async_copy(
                source.at[p], target.at[p], local_sems.at[first_sem + i * n_tensor + p]
            )
            for i, (source, target) in enumerate(weights)
        ]

    def token_loads(m):
        start = first_sem + 3 * n_tensor
        return [
            pltpu.make_async_copy(source.at[m], target.at[m], local_sems.at[start + i * GROUP + m])
            for i, (source, target) in enumerate(tokens)
        ]

    for copy in token_loads(3):
        copy.start()
    for p in range(n_tensor):
        for copy in weight_loads(p):
            copy.start()
    for m in (1, 2, 0):
        for copy in token_loads(m):
            copy.start()
    hidden_load = move(hidden_in, hidden)
    links.barrier()

    def inner(i, carry):
        turn_at, p = i // n_tensor, i % n_tensor
        m = 3 - 2 * (turn_at % 2) - turn_at // 2

        @pl.when(p == 0)
        def _():
            for copy in token_loads(m):
                copy.wait()

        @pl.when(turn_at == 0)
        def _():
            for copy in weight_loads(p):
                copy.wait()

        at = pl.ds(pl.multiple_of(p * size, TILE), size)
        gate = lax.dot_general(n2_all[m], gate_w[p], contract, preferred_element_type=f32)
        up_value = lax.dot_general(n2_all[m], up_w[p], contract, preferred_element_type=f32)
        act_grad = lax.dot_general(cot_all[m], down_w[p], contract, preferred_element_type=f32)
        sigmoid = jax.nn.sigmoid(gate)
        silu = gate * sigmoid
        active[m, :, at] = (silu * up_value).astype(bf16)
        gate_delta[m, :, at] = (
            act_grad * up_value * sigmoid * (1.0 + gate * (1.0 - sigmoid))
        ).astype(bf16)
        up_delta[m, :, at] = (act_grad * silu).astype(bf16)
        return carry

    lax.fori_loop(0, 2 * n_tensor, inner, 0)

    def back(m):
        return jnp.dot(
            gate_delta[m], gate_w[...].reshape(units, width), preferred_element_type=f32
        ) + jnp.dot(up_delta[m], up_w[...].reshape(units, width), preferred_element_type=f32)

    to_core[1] = back(3).astype(bf16)
    core_send1 = send(to_core.at[1], from_core.at[1], bit=1)
    total[...] = back(1)
    core_send1.wait_recv()
    across = []
    for i in range(tiles):
        at = pl.ds(i * TILE, TILE)
        to_across[at] = (total[at, :] + from_core[1, at, :].astype(f32)).astype(bf16)
        across.append(send(to_across.at[at], from_across.at[at], bit=2))
    lax.fori_loop(2 * n_tensor, GROUP * n_tensor, inner, 0)

    order = []
    for i in range((n_tensor + 1) // 2):
        order.extend(dict.fromkeys((n_tensor - 1 - i, i)))

    def grads(left, right, part, target, weight=None):
        def one(p, carry):
            at = pl.ds(pl.multiple_of(p * size, TILE), size)
            grad = lax.dot_general(
                left[:, :, at].reshape(GROUP * rows, size),
                right[...].reshape(GROUP * rows, width),
                over_rows,
                preferred_element_type=f32,
            )
            part[p] = grad.astype(bf16)
            if weight is not None:
                row[...] += jnp.sum(grad * weight[p].astype(f32), axis=0, keepdims=True)
            return carry

        lax.fori_loop(0, n_tensor, one, 0)
        save(part, target)

    row[...] = jnp.zeros_like(row)
    grads(active, cot_all, down_part, down_out)
    swaps = [
        send(down_part.at[p, :, other], down_got.at[p], bit=GROUP) for p in order[: n_tensor // 2]
    ]
    to_core[0] = back(2).astype(bf16)
    core_send0 = send(to_core.at[0], from_core.at[0], bit=1)
    total[...] = back(0)
    core_send0.wait_recv()
    total[...] += from_core[0].astype(f32)
    grads(gate_delta, n2_all, gate_part, gate_out, gate_w)
    grads(up_delta, n2_all, up_part, up_out, up_w)
    save(row, row_out)

    def feed_out(m, carry):
        n2_all[m] = jnp.dot(
            active[m], down_w[...].reshape(units, width), preferred_element_type=f32
        ).astype(bf16)
        return carry

    lax.fori_loop(0, GROUP, feed_out, 0)
    save(n2_all, mlp_out)
    gain = jnp.concatenate([smalls[i, 3:4, :chunk] for i in range(n_dp)], axis=1)
    hidden_load.wait()
    for i in range(tiles):
        at = pl.ds(i * TILE, TILE)
        across[i].wait_recv()
        upstream = total[at, :] + from_across[at, :].astype(f32)
        features = hidden[at, :]
        inverse = lax.rsqrt(jnp.mean(features * features, axis=1, keepdims=True) + EPS)
        scaled = gain * upstream
        mean = jnp.mean(scaled * features, axis=1, keepdims=True)
        result = cot_all[0, at, :].astype(f32) + (
            inverse * scaled - features * (inverse * inverse * inverse) * mean
        )
        total[at, :] = result
        rounded[at, :] = result.astype(bf16)
    save(total, grad_out)
    save(rounded, grad_own_out)
    for copy in swaps:
        copy.wait_recv()
    links.finish()


def feed(n_dp, n_tensor, normed2, grad_rows, hidden1, gate_w, up_w, down_w, smalls):
    f32, bf16 = jnp.float32, jnp.bfloat16
    rows, width = hidden1.shape
    half = width // 2
    vmem = pl.BlockSpec(memory_space=pltpu.VMEM)
    hbm = pl.BlockSpec(memory_space=pl.ANY)
    weight = gate_w.shape
    inner = (GROUP, rows, n_tensor * weight[1])

    def shape(dims, dtype=bf16):
        return jax.ShapeDtypeStruct(tuple(dims), dtype)

    outs = [
        shape((rows, width), f32), shape((rows, width)), shape(normed2.shape),
        shape(weight), shape(weight), shape(weight), shape((n_tensor, weight[1], half)),
        shape((1, width), f32),
    ]
    scratch = [
        pltpu.VMEM(normed2.shape, bf16),
        pltpu.VMEM(normed2.shape, bf16),
        pltpu.VMEM(weight, bf16),
        pltpu.VMEM(weight, bf16),
        pltpu.VMEM(weight, bf16),
        pltpu.VMEM(inner, bf16),
        pltpu.VMEM(inner, bf16),
        pltpu.VMEM(inner, bf16),
        pltpu.VMEM(weight, bf16),
        pltpu.VMEM(weight, bf16),
        pltpu.VMEM(weight, bf16),
        pltpu.VMEM((2, rows, width), bf16),
        pltpu.VMEM((2, rows, width), bf16),
        pltpu.VMEM((rows, width), bf16),
        pltpu.VMEM((rows, width), bf16),
        pltpu.VMEM((rows, width), f32),
        pltpu.VMEM((rows, width), f32),
        pltpu.VMEM((rows, width), bf16),
        pltpu.VMEM((1, width), f32),
        pltpu.SemaphoreType.DMA((16,)),
        pltpu.SemaphoreType.DMA((16,)),
        pltpu.SemaphoreType.DMA((40,)),
    ]
    return pl.pallas_call(
        functools.partial(kernel_feed, n_dp, n_tensor),
        in_specs=[hbm] * 6 + [vmem],
        out_specs=[hbm] * len(outs),
        out_shape=outs,
        scratch_shapes=scratch,
        compiler_params=pltpu.CompilerParams(
            collective_id=2, has_side_effects=True, vmem_limit_bytes=67043328
        ),
        name="feed",
    )(normed2, grad_rows, hidden1, gate_w, up_w, down_w, smalls)


class Collect:
    def __init__(
        self, links, part, swapped, stage, arrived, late, blocks, target, mine, other, turned=False
    ):
        self.turned = turned
        self.links, self.part, self.swapped, self.stage = links, part, swapped, stage
        self.arrived, self.late, self.blocks, self.target = arrived, late, blocks, target
        self.mine, self.other = mine, other
        self.swaps, self.loads, self.deals = {}, [], []

    def issue(self, order, load=True):
        links = self.links
        for p in order:
            self.swaps[p] = links.send(
                self.part.at[p, :, self.other], self.swapped.at[p], bit=GROUP
            )
        if self.stage is not None and load:
            self.loads = [links.move(self.part.at[:, :, self.mine], self.stage)]

    def load(self, received, order):
        links = self.links
        count = links.n_tensor // 2
        self.loads = [links.move(received.at[p], self.swapped.at[p]) for p in order[:count]]
        self.loads.append(links.move(self.part.at[:, :, self.mine], self.stage))

    def step(self, p):
        links, n, z = self.links, self.links.n_tensor, self.links.z_at
        f32, bf16 = jnp.float32, jnp.bfloat16
        while self.loads:
            self.loads.pop().wait()
        if p in self.swaps:
            self.swaps[p].wait_recv()
        own = self.stage[p] if self.stage is not None else self.part[p, :, self.mine]
        self.swapped[p] = (own.astype(f32) + self.swapped[p].astype(f32)).astype(bf16)
        if not hasattr(self, "ahead"):
            self.ahead, self.back, self.back_last = [None] * n, [None] * n, [None] * n
        source = self.swapped.at[p]
        self.ahead[p] = links.plan(
            source, self.arrived.at[p], shift=1, sends=z < p, receives=(z > 0) & (z <= p)
        )
        self.back[p] = links.plan(
            source, self.arrived.at[p], shift=-1, sends=z > p + 1,
            receives=(z > p) & (z < n - 1),
        )
        self.back_last[p] = links.plan(
            source, self.late, shift=-1, sends=z == p + 1, receives=(z == p) & (z < n - 1)
        )

        @pl.when((z == 0) & (z < p))
        def _():
            self.ahead[p].copy.start()

        @pl.when((z == n - 1) & (z > p + 1))
        def _():
            self.back[p].copy.start()

        @pl.when((z == n - 1) & (z == p + 1))
        def _():
            self.back_last[p].copy.start()

    def relay(self, i):
        links, n, z = self.links, self.links.n_tensor, self.links.z_at
        f32, bf16 = jnp.float32, jnp.bfloat16

        def add(p):
            self.swapped[p] = (
                self.swapped[p].astype(f32) + self.arrived[p].astype(f32)
            ).astype(bf16)

        for p in range(n):
            at = i - (n - 1) + p
            if 0 < at < n - 1 and at < p:

                @pl.when(z == at)
                def _(p=p):
                    self.ahead[p].copy.wait_recv()
                    add(p)
                    self.ahead[p].copy.start()

            at = n - 1 - i + p
            if 0 < at < n - 1 and at > p:

                @pl.when(z == at)
                def _(p=p, at=at):
                    self.back[p].copy.wait_recv()
                    add(p)
                    (self.back_last if at == p + 1 else self.back)[p].copy.start()

    def finish(self):
        links, n, z = self.links, self.links.n_tensor, self.links.z_at
        f32, bf16 = jnp.float32, jnp.bfloat16
        member = links.d_at % GROUP
        for p in range(n):

            @pl.when((z == p) & (z > 0))
            def _(p=p):
                self.ahead[p].copy.wait_recv()

            @pl.when((z == p) & (z < n - 1))
            def _(p=p):
                self.back_last[p].copy.wait_recv()

        below = jnp.where(z > 0, self.arrived[z].astype(f32), 0.0)
        above = jnp.where(z < n - 1, self.late[...].astype(f32), 0.0)
        total = (self.swapped[z].astype(f32) + below + above).astype(bf16)
        chunk = total.shape[1] // GROUP
        size = self.blocks.shape[2 if self.turned else 1]
        place = pl.ds(pl.multiple_of(member * size, 16), size)
        if self.turned:
            place = pl.ds(pl.multiple_of(member * size, TILE), size)
        for i in range(GROUP):
            block = total[:, i * chunk : (i + 1) * chunk]
            self.blocks[i] = block.T if self.turned else block
        if self.turned:
            target = self.target.at[:, place]
        elif len(self.target.shape) == 2:
            target = self.target.at[place, :]
        else:
            target = self.target.at[member]
        for k in range(1, GROUP):
            self.deals.append(links.send(self.blocks.at[member ^ k], target, bit=k))
        links.save(self.blocks.at[member], target)

    def wait(self):
        for deal in self.deals:
            deal.wait_recv()


def kernel_backward(
    n_dp, n_tensor,
    grad_own, hidden_grad, tokens, hidden1, mlp_part, n1_in, query_in, keyval_in, log_in, att_in,
    cos_in, sin_in, qkv_in, out_in, small_in, down_in, gate_in, up_in, down_got,
    mlp_row, fixed,
    input_out, block_out, qkv_out, out_out, gate_out, up_out, down_out,
    g_all, n1_all, qkv, outw, queries, keyvals, logs, att, cosine, sine, gains, low_col,
    att_grad, other_grad, totals, query_total, pass_on, delta, halo_send, halo_recv,
    to_core, from_core, to_across, from_across, mlp_across, hidden, stage, gate_stage,
    down_swap, gate_swap, up_swap, out_swap, qkv_swap,
    down_come, gate_come, up_come, out_come, qkv_come,
    down_late, gate_late, up_late, out_late, qkv_late,
    down_block, gate_block, up_block, out_block, qkv_block,
    out_sems, in_sems, local_sems,
):
    f32, bf16 = jnp.float32, jnp.bfloat16
    links = Links(n_dp, n_tensor, out_sems, in_sems, local_sems)
    send, move, save = links.send, links.move, links.save
    d_at, z_at = links.d_at, links.z_at
    core = d_at % 2
    upper = d_at // GROUP
    rows, width = grad_own.shape
    half = width // 2
    contract = (((1,), (1,)), ((), ()))
    over_rows = (((0,), (0,)), ((), ()))
    mine = pl.ds(pl.multiple_of(upper * half, half), half)
    other = pl.ds(pl.multiple_of((1 - upper) * half, half), half)
    tiles = rows // TILE
    span = TILE + WINDOW
    quarter = qkv.shape[1]
    out_quarter = outw.shape[1]
    extra = qkv_swap.shape[1] - quarter

    order = []
    for i in range((n_tensor + 1) // 2):
        order.extend(dict.fromkeys((n_tensor - 1 - i, i)))

    down = Collect(
        links, down_in, down_swap, stage, down_come, down_late, down_block, down_out, mine, other,
        turned=True,
    )
    gate = Collect(
        links, gate_in, gate_swap, gate_stage, gate_come, gate_late, gate_block, gate_out, mine, other,
        turned=True,
    )
    up = Collect(
        links, up_in, up_swap, stage, up_come, up_late, up_block, up_out, mine, other, turned=True
    )
    out_part = g_all.at[:, pl.ds(quarter + extra, out_quarter), :]
    qkv_part = g_all.at[:, pl.ds(0, quarter + extra), :]
    out_collect = Collect(
        links, out_part, out_swap, None, out_come, out_late, out_block, out_out, mine, other
    )
    qkv_collect = Collect(
        links, qkv_part, qkv_swap, None, qkv_come, qkv_late, qkv_block, qkv_out, mine, other
    )
    small = move(small_in, gains)
    loads = [
        move(grad_own, g_all.at[0]), move(out_in, outw),
    ]
    down.load(down_got, order)
    loads += [
        move(query_in, queries),
        move(keyval_in, keyvals), move(log_in, logs), move(cos_in, cosine), move(sin_in, sine),
        move(mlp_part.at[pl.ds(0, 2)], to_core), move(hidden1, hidden), move(att_in, att),
        move(qkv_in, qkv), move(n1_in, n1_all),
    ]
    links.barrier()
    across = send(grad_own, g_all.at[1], bit=2)
    beside = send(grad_own, g_all.at[2], bit=1)
    mlp_core = send(mlp_part.at[pl.ds(2, 2)], from_core, bit=1)
    down.issue(order[n_tensor // 2 :], load=False)
    gate.issue(order)
    small.wait()
    for m, k in ((0, 0), (1, 2)):
        info = gains[d_at ^ k].T
        low_col[m] = info[:, 1:2].astype(jnp.int32) - z_at * rows + WINDOW
    loads[0].wait()
    loads[1].wait()

    def attended_back(b):
        units = outw.shape[0] * outw.shape[1]
        att_grad[b] = lax.dot_general(
            g_all[b], outw[...].reshape(units, width), contract, preferred_element_type=f32
        ).astype(bf16)

    attended_back(0)
    beside.wait_recv()
    attended_back(2)
    grad_swap = send(att_grad.at[2], other_grad.at[0], bit=1)
    for p in order[: n_tensor // 2]:
        down.step(p)
    for copy in loads[2:]:
        copy.wait()
    mlp_core.wait_recv()
    heads = queries.shape[2] // HEAD_SIZE
    repeat = QUERY_HEADS // KEY_VALUE_HEADS
    scale = HEAD_SIZE ** (-0.5)
    is_first = core == 0
    second, keys_turn, all_turn = fixed[1:2], fixed[2:3], fixed[3:4]

    def back_tile(m, tile):
        start = tile * TILE
        at = slice(start, start + TILE)
        reach = slice(start, start + span)
        key = lax.broadcasted_iota(jnp.int32, (TILE, span), 1)
        query = lax.broadcasted_iota(jnp.int32, (TILE, span), 0)
        allowed = (key >= low_col[m, at, :] - start) & (key <= query + WINDOW)
        own, others = att_grad[m, at, :], other_grad[m, at, :]
        by_repeat = (jnp.where(is_first, own, others), jnp.where(is_first, others, own))
        for group in range(heads // repeat):
            base = group * 2 * HEAD_SIZE
            k = keyvals[m, reach, base : base + HEAD_SIZE]
            v = keyvals[m, reach, base + HEAD_SIZE : base + 2 * HEAD_SIZE]
            key_sum = None
            for r in range(repeat):
                head = group * repeat + r
                q = queries[m, at, head * HEAD_SIZE : (head + 1) * HEAD_SIZE]
                g = by_repeat[r][:, group * HEAD_SIZE : (group + 1) * HEAD_SIZE]
                s = lax.dot_general(q, k, contract, preferred_element_type=f32) * scale
                total = logs[m, at, head : head + 1]
                p = jnp.exp(jnp.where(allowed, s, NEG_FILL) - total)
                pg = lax.dot_general(g, v, contract, preferred_element_type=f32)
                inner = jnp.sum(p * pg, axis=1, keepdims=True)
                sg = (p * (pg - inner) * scale).astype(bf16)
                query_total[:, head * HEAD_SIZE : (head + 1) * HEAD_SIZE] = jnp.dot(
                    sg, k, preferred_element_type=f32
                )
                dk = lax.dot_general(sg, q, over_rows, preferred_element_type=f32)
                dv = lax.dot_general(p.astype(bf16), g, over_rows, preferred_element_type=f32)
                both = jnp.concatenate([dk, dv], axis=1)
                key_sum = both if key_sum is None else key_sum + both
            totals[m, reach, base : base + 2 * HEAD_SIZE] += key_sum
        turned = turn(
            query_total[...], cosine[m, at, :], sine[m, at, :], second, all_turn, -1.0
        ).astype(bf16)

        @pl.when(is_first)
        def _():
            delta[m, at, :] = turned

        @pl.when(core != 0)
        def _():
            pass_on[m, at, :] = turned

    halos = [
        links.plan(
            halo_send.at[m], halo_recv.at[m], shift=-1, sends=z_at > 0,
            receives=z_at < n_tensor - 1,
        )
        for m in range(2)
    ]

    def back_tiles(m, first_tile, last_tile):
        for tile in range(first_tile, last_tile):
            back_tile(m, tile)

    def send_halo(m):
        halo_send[m] = totals[m, :WINDOW].astype(bf16)
        halos[m].start()

    def finish_block(m):
        halos[m].wait_recv()
        full = totals[m, WINDOW:]
        tail = full[rows - WINDOW :] + jnp.where(
            z_at < n_tensor - 1, halo_recv[m].astype(f32), 0.0
        )
        full = jnp.concatenate([full[: rows - WINDOW], tail], axis=0)
        turned = turn(full, cosine[m], sine[m], second, keys_turn, -1.0).astype(bf16)

        @pl.when(is_first)
        def _():
            pass_on[m] = turned

        @pl.when(core != 0)
        def _():
            delta[m] = turned

        return send(pass_on.at[m], delta.at[2 + m], bit=1)

    free = -(-WINDOW // TILE)
    totals[...] = jnp.zeros_like(totals)
    grad_swap.wait_recv()
    back_tiles(0, 0, free)
    down.relay(1)
    send_halo(0)
    for p in order[n_tensor // 2 : n_tensor - 1]:
        down.step(p)
    back_tiles(0, free, tiles)
    for p in order[n_tensor - 1 :]:
        down.step(p)
    up.issue(order)
    across.wait_recv()
    both = send(g_all.at[1], g_all.at[3], bit=1)
    to_across[...] = (to_core[1].astype(f32) + from_core[1].astype(f32)).astype(bf16)
    mlp_send = send(to_across, mlp_across, bit=2)
    hidden[...] += to_core[0].astype(f32) + from_core[0].astype(f32)
    attended_back(1)
    both.wait_recv()
    attended_back(3)
    grad_swap = send(att_grad.at[3], other_grad.at[1], bit=1)
    gate.step(order[0])

    def weight_grad(left, right, at):
        total = None
        for b in range(GROUP):
            term = lax.dot_general(
                left[b, :, at], right[b], over_rows, preferred_element_type=f32
            )
            total = term if total is None else total + term
        return total

    out_grad = weight_grad(att, g_all, slice(0, n_tensor * out_quarter)).astype(bf16)
    both.wait_send()
    links.sent.remove(both)
    out_part[...] = out_grad.reshape(n_tensor, out_quarter, width)
    grad_swap.wait_recv()
    back_tiles(1, 0, free)
    for i in range(2, n_tensor - 1):
        down.relay(i)
    send_halo(1)
    gate.step(order[1])
    back_tiles(1, free, tiles)
    for p in order[2 : n_tensor - 1]:
        gate.step(p)
    swap0 = finish_block(0)
    gate.relay(1)
    swap1 = finish_block(1)
    grad_loads = [
        move(hidden_grad.at[:, pl.ds(i * half, half)], totals.at[i, pl.ds(0, rows)])
        for i in range(2)
    ]
    down.finish()
    for p in order[n_tensor - 1 :]:
        gate.step(p)

    def project_back(b):
        units = qkv.shape[0] * quarter
        return jnp.dot(delta[b], qkv[...].reshape(units, width), preferred_element_type=f32)

    mlp_send.wait_recv()
    mlp_across[...] = (hidden[...] + mlp_across[...].astype(f32)).astype(bf16)
    save(mlp_across, block_out)
    mlp_send.wait_send()
    links.sent.remove(mlp_send)
    swap1.wait_recv()
    to_core[1] = project_back(3).astype(bf16)
    core_send1 = send(to_core.at[1], from_core.at[1], bit=1)
    hidden[...] = project_back(1)
    swap0.wait_recv()
    to_core[0] = project_back(2).astype(bf16)
    core_send0 = send(to_core.at[0], from_core.at[0], bit=1)
    core_send1.wait_recv()
    across_sends = []
    for i in range(tiles):
        at = pl.ds(i * TILE, TILE)
        to_across[at] = (hidden[at, :] + from_core[1, at, :].astype(f32)).astype(bf16)
        across_sends.append(send(to_across.at[at], from_across.at[at], bit=2))
    hidden[...] = project_back(0)
    core_send0.wait_recv()
    hidden[...] += from_core[0].astype(f32)
    up.step(order[0])
    attn_row = None
    for p in range(n_tensor):
        at = slice(p * quarter, (p + 1) * quarter)
        grad = weight_grad(delta, n1_all, at)
        row = jnp.sum(grad * qkv[p].astype(f32), axis=0, keepdims=True)
        attn_row = row if attn_row is None else attn_row + row
        qkv_part[p, :quarter, :] = grad.astype(bf16)
    ending = jnp.concatenate(
        [attn_row, mlp_row[...], jnp.zeros((extra - 2, width), f32)], axis=0
    ).astype(bf16)
    for p in range(n_tensor):
        qkv_part[p, quarter:, :] = ending
    qkv_collect.issue(order)
    out_collect.issue(order)
    token_load = move(tokens, n1_all.at[0])
    up.step(order[1])
    gain = jnp.concatenate([gains[i, 2:3, : width // n_dp] for i in range(n_dp)], axis=1)
    for i in range(tiles):
        at = pl.ds(i * TILE, TILE)
        across_sends[i].wait_recv()
        if i == 0:
            for copy in grad_loads + [token_load]:
                copy.wait()
        upstream = hidden[at, :] + from_across[at, :].astype(f32)
        features = n1_all[0, at, :].astype(f32)
        inverse = lax.rsqrt(jnp.mean(features * features, axis=1, keepdims=True) + EPS)
        scaled = gain * upstream
        mean = jnp.mean(scaled * features, axis=1, keepdims=True)
        change = inverse * scaled - features * (inverse * inverse * inverse) * mean
        n1_all[1, at, :half] = (totals[0, at, :] + change[:, :half]).astype(bf16)
        n1_all[1, at, half:] = (totals[1, at, :] + change[:, half:]).astype(bf16)
        if i == 0:
            for j in range(2, n_tensor - 1):
                gate.relay(j)
        if i == 1:
            for p in order[2 : n_tensor - 1]:
                up.step(p)
    save(n1_all.at[1], input_out)
    gate.finish()
    for p in order[n_tensor - 1 :]:
        up.step(p)
    up.relay(1)
    for p in order[:2]:
        qkv_collect.step(p)
    for i in range(2, n_tensor - 1):
        up.relay(i)
    for p in order[2 : n_tensor - 1]:
        qkv_collect.step(p)
    up.finish()
    for p in order[n_tensor - 1 :]:
        qkv_collect.step(p)
    qkv_collect.relay(1)
    for p in order[:2]:
        out_collect.step(p)
    for i in range(2, n_tensor - 1):
        qkv_collect.relay(i)
    for p in order[2:]:
        out_collect.step(p)
    out_collect.relay(1)
    qkv_collect.finish()
    for i in range(2, n_tensor - 1):
        out_collect.relay(i)
    out_collect.finish()
    for collect in (down, gate, up, out_collect, qkv_collect):
        collect.wait()
    links.finish()


def backward(
    n_dp, n_tensor, grad_own, hidden_grad, tokens, hidden1, mlp_part, normed1, queries, keyvals, logs, attended,
    cosine, sine, qkv_full, out_full, smalls, down_part, gate_part, up_part, down_got,
    mlp_row, fixed,
):
    f32, bf16 = jnp.float32, jnp.bfloat16
    rows, width = grad_own.shape
    half = width // 2
    chunk = width // n_dp
    units = queries.shape[2]
    vmem = pl.BlockSpec(memory_space=pltpu.VMEM)
    hbm = pl.BlockSpec(memory_space=pl.ANY)
    extra = 16
    quarters = [
        down_part.shape[1], gate_part.shape[1], up_part.shape[1], out_full.shape[1],
        qkv_full.shape[1] + extra,
    ]

    def shape(dims, dtype=bf16):
        return jax.ShapeDtypeStruct(tuple(dims), dtype)

    def finals(index):
        return shape((GROUP, quarters[index], chunk))

    outs = [
        shape((rows, width)), shape((rows, width)), finals(4), shape((GROUP * quarters[3], chunk)),
        shape((chunk, GROUP * quarters[1])), shape((chunk, GROUP * quarters[2])),
        shape((chunk, GROUP * quarters[0])),
    ]
    full = (GROUP, rows, width)
    scratch = [
        pltpu.VMEM(full, bf16),
        pltpu.VMEM(full, bf16),
        pltpu.VMEM(qkv_full.shape, bf16),
        pltpu.VMEM(out_full.shape, bf16),
        pltpu.VMEM(queries.shape, bf16),
        pltpu.VMEM(keyvals.shape, bf16),
        pltpu.VMEM(logs.shape, f32),
        pltpu.VMEM(attended.shape, bf16),
        pltpu.VMEM(cosine.shape, f32),
        pltpu.VMEM(sine.shape, f32),
        pltpu.VMEM(smalls.shape, f32),
        pltpu.VMEM((2, rows, 1), jnp.int32),
        pltpu.VMEM(attended.shape, bf16),
        pltpu.VMEM((2,) + attended.shape[1:], bf16),
        pltpu.VMEM((2, rows + WINDOW, units), f32),
        pltpu.VMEM((TILE, units), f32),
        pltpu.VMEM((2, rows, units), bf16),
        pltpu.VMEM((GROUP, rows, units), bf16),
        pltpu.VMEM((2, WINDOW, units), bf16),
        pltpu.VMEM((2, WINDOW, units), bf16),
        pltpu.VMEM((2, rows, width), bf16),
        pltpu.VMEM((2, rows, width), bf16),
        pltpu.VMEM((rows, width), bf16),
        pltpu.VMEM((rows, width), bf16),
        pltpu.VMEM((rows, width), bf16),
        pltpu.VMEM((rows, width), f32),
        pltpu.VMEM((n_tensor, quarters[0], half), bf16),
        pltpu.VMEM((n_tensor, quarters[1], half), bf16),
    ]
    scratch += [pltpu.VMEM((n_tensor, q, half), bf16) for q in quarters]
    scratch += [pltpu.VMEM((n_tensor, q, half), bf16) for q in quarters]
    scratch += [pltpu.VMEM((q, half), bf16) for q in quarters]
    scratch += [
        pltpu.VMEM((GROUP, chunk, q) if turned else (GROUP, q, chunk), bf16)
        for q, turned in zip(quarters, (True, True, True, False, False))
    ]
    scratch += [
        pltpu.SemaphoreType.DMA((160,)),
        pltpu.SemaphoreType.DMA((160,)),
        pltpu.SemaphoreType.DMA((40,)),
    ]
    return pl.pallas_call(
        functools.partial(kernel_backward, n_dp, n_tensor),
        in_specs=[hbm] * 19 + [vmem] * 2,
        out_specs=[hbm] * len(outs),
        out_shape=outs,
        scratch_shapes=scratch,
        compiler_params=pltpu.CompilerParams(
            collective_id=1, has_side_effects=True, vmem_limit_bytes=67043328
        ),
        name="backward",
    )(
        grad_own, hidden_grad, tokens, hidden1, mlp_part, normed1, queries, keyvals, logs, attended, cosine, sine,
        qkv_full, out_full, smalls, down_part, gate_part, up_part, down_got, mlp_row, fixed,
    )


def fast_local(
    n_dp,
    n_tensor,
    block_in,
    cotangent,
    segment_ids,
    attn_gain,
    qkv_weight,
    out_weight,
    mlp_gain,
    gate_weight,
    up_weight,
    down_weight,
):
    bf16, f32 = jnp.bfloat16, jnp.float32
    rows, width = block_in.shape
    part = attn_gain.shape[0]
    (
        normed1, normed2, hidden1, queries, keyvals, log_total, attended, cosine, sine, qkv_full,
        out_full, smalls, grad_rows, gate_full, up_full, down_full,
    ), fixed = forward(
        n_dp, n_tensor, block_in, cotangent, segment_ids, jnp.stack([attn_gain, mlp_gain]),
        qkv_weight, out_weight, gate_weight, up_weight, down_weight,
    )
    (
        hidden1_grad, grad_own, mlp_part, down_part, gate_part, up_part, down_got, mlp_row,
    ) = feed(n_dp, n_tensor, normed2, grad_rows, hidden1, gate_full, up_full, down_full, smalls)
    input_grad, block_out, qkv_blocks, out_grad, gate_grad, up_grad, down_grad = backward(
        n_dp, n_tensor, grad_own, hidden1_grad, block_in, hidden1, mlp_part, normed1, queries,
        keyvals, log_total, attended, cosine, sine, qkv_full, out_full, smalls, down_part, gate_part, up_part, down_got, mlp_row,
        fixed,
    )
    quarter = qkv_full.shape[1]

    def row_of(index, gain):
        return jnp.sum(qkv_blocks[:, quarter + index].astype(f32), axis=0) / gain.astype(f32)

    blocks = qkv_blocks[:, :quarter]
    qkv_grad = blocks.reshape(-1, blocks.shape[2]).T.astype(f32)
    gains = [row_of(0, attn_gain), row_of(1, mlp_gain)]
    return (
        block_out,
        input_grad,
        gains[0],
        qkv_grad,
        out_grad.astype(f32),
        gains[1],
        gate_grad.astype(f32),
        up_grad.astype(f32),
        down_grad.T.astype(f32),
    )


def solution(mesh):
    in_specs = (
        P(("dp", "tensor"), None),
        P(("dp", "tensor"), None),
        P("dp", None),
        P("dp"),
        P("dp", "tensor"),
        P("tensor", "dp"),
        P("dp"),
        P("dp", "tensor"),
        P("dp", "tensor"),
        P("tensor", "dp"),
    )
    out_specs = (
        P(("dp", "tensor"), None),
        P(("dp", "tensor"), None),
        P("dp"),
        P("dp", "tensor"),
        P("tensor", "dp"),
        P("dp"),
        P("dp", "tensor"),
        P("dp", "tensor"),
        P("tensor", "dp"),
    )
    n_dp, n_tensor = mesh.shape["dp"], mesh.shape["tensor"]

    def body(*arrays):
        rows = arrays[0].shape[0]
        groups = arrays[4].shape[1] // (4 * HEAD_SIZE)
        if n_dp == 2 * GROUP and groups == 2 and rows >= WINDOW and rows % TILE == 0:
            return fast_local(n_dp, n_tensor, *arrays)
        return local(*arrays)

    return jax.shard_map(body, mesh=mesh, in_specs=in_specs, out_specs=out_specs, check_vma=False)
```

```python
import functools

import jax
import jax.numpy as jnp
import numpy as np
from jax import lax
from jax.experimental import pallas as pl
from jax.experimental.pallas import tpu as pltpu
from jax.sharding import PartitionSpec as P

QUERY_HEADS = 16
KEY_VALUE_HEADS = 8
HEAD_SIZE = 96


EPS = 1e-05
ROPE_BASE = 100000.0
NEG_FILL = -1e30


def doc_positions(segments):
    length = segments.shape[1]
    position_index = jnp.broadcast_to(jnp.arange(length, dtype=jnp.int32)[None, :], segments.shape)
    change = jnp.concatenate(
        [jnp.ones((segments.shape[0], 1), dtype=bool), segments[:, 1:] != segments[:, :-1]], axis=1
    )
    starts = lax.cummax(jnp.where(change, position_index, jnp.zeros_like(position_index)), axis=1)
    return position_index - starts


def rotary_tables(segments):
    half_dim = HEAD_SIZE // 2
    frequency = jnp.power(ROPE_BASE, -(2.0 * jnp.arange(half_dim, dtype=jnp.float32)) / HEAD_SIZE)
    angles = doc_positions(segments).astype(jnp.float32)[..., None] * frequency
    cosine_table = jnp.concatenate([jnp.cos(angles), jnp.cos(angles)], axis=-1)
    sine_table = jnp.concatenate([jnp.sin(angles), jnp.sin(angles)], axis=-1)
    return (cosine_table, sine_table)


def rotate(vector, cosine_table, sine_table):
    half_dim = vector.shape[-1] // 2
    turned = jnp.concatenate([-vector[..., half_dim:], vector[..., :half_dim]], axis=-1)
    return vector * cosine_table + turned * sine_table


def unrotate(vector, cosine_table, sine_table):
    half_dim = vector.shape[-1] // 2
    shifted = vector * sine_table
    returned = jnp.concatenate([shifted[..., half_dim:], -shifted[..., :half_dim]], axis=-1)
    return vector * cosine_table + returned


def allowed_pairs(segments):
    length = segments.shape[1]
    offsets = jnp.arange(length)
    causal = offsets[None, :] <= offsets[:, None]
    same_doc = segments[:, :, None] == segments[:, None, :]
    return (causal[None] & same_doc)[:, None, None]


def score_block(queries, key_heads, segments):
    scores = jnp.einsum(
        "sqgrd,skgd->sgrqk", queries, key_heads, preferred_element_type=jnp.float32
    ) * HEAD_SIZE ** (-0.5)
    return jnp.where(allowed_pairs(segments), scores, NEG_FILL)


def rms_scale(features):
    return lax.rsqrt(jnp.mean(features * features, axis=-1, keepdims=True) + EPS)


def norm_back(features, inverse, gain_vector, upstream):
    scaled = gain_vector * upstream
    return inverse * scaled - features * (inverse * inverse * inverse) * jnp.mean(
        scaled * features, axis=-1, keepdims=True
    )


def widen(shard_rows):
    return lax.all_gather(shard_rows, "tensor", axis=0, tiled=True)


def narrow(partial_value):
    return lax.psum_scatter(
        partial_value.astype(jnp.bfloat16), "tensor", scatter_dimension=0, tiled=True
    ).astype(jnp.float32)


def local(
    block_in,
    cotangent,
    segment_ids,
    attn_gain,
    qkv_weight,
    out_weight,
    mlp_gain,
    gate_weight,
    up_weight,
    down_weight,
):
    qkv_full, gate_full, up_full, gain_attn_raw, gain_mlp_raw = (
        lax.all_gather(qkv_weight, "dp", axis=0, tiled=True),
        lax.all_gather(gate_weight, "dp", axis=0, tiled=True),
        lax.all_gather(up_weight, "dp", axis=0, tiled=True),
        lax.all_gather(attn_gain, "dp", axis=0, tiled=True),
        lax.all_gather(mlp_gain, "dp", axis=0, tiled=True),
    )
    out_cols, down_cols = (
        lax.all_gather(out_weight, "dp", axis=1, tiled=True),
        lax.all_gather(down_weight, "dp", axis=1, tiled=True),
    )
    seq_count, length = segment_ids.shape
    repeat_factor = QUERY_HEADS // KEY_VALUE_HEADS
    groups = qkv_full.shape[1] // ((repeat_factor + 2) * HEAD_SIZE)
    gain_attn = gain_attn_raw.astype(jnp.float32)
    gain_mlp = gain_mlp_raw.astype(jnp.float32)
    residual = block_in.astype(jnp.float32)
    scale_attn = rms_scale(residual)
    normed1 = widen((residual * scale_attn * gain_attn).astype(jnp.bfloat16))
    projected = jnp.dot(normed1, qkv_full, preferred_element_type=jnp.float32).reshape(
        seq_count, length, groups, repeat_factor + 2, HEAD_SIZE
    )
    cosine_table, sine_table = rotary_tables(segment_ids)
    cos_query = cosine_table[:, :, None, None, :]
    sin_query = sine_table[:, :, None, None, :]
    cos_key = cosine_table[:, :, None, :]
    sin_key = sine_table[:, :, None, :]
    queries = rotate(projected[:, :, :, :repeat_factor], cos_query, sin_query).astype(jnp.bfloat16)
    key_heads = rotate(projected[:, :, :, repeat_factor], cos_key, sin_key).astype(jnp.bfloat16)
    values = projected[:, :, :, repeat_factor + 1].astype(jnp.bfloat16)
    scores = score_block(queries, key_heads, segment_ids)
    highest = jnp.max(scores, axis=-1, keepdims=True)
    log_total = highest + jnp.log(jnp.sum(jnp.exp(scores - highest), axis=-1, keepdims=True))
    probability = jnp.exp(scores - log_total).astype(jnp.bfloat16)
    attended = jnp.einsum(
        "sgrqk,skgd->sqgrd", probability, values, preferred_element_type=jnp.float32
    ).astype(jnp.bfloat16)
    attn_flat = attended.reshape(seq_count * length, groups * repeat_factor * HEAD_SIZE)
    attn_delta = lax.psum_scatter(
        jnp.dot(attn_flat, out_cols, preferred_element_type=jnp.float32).astype(jnp.bfloat16),
        "tensor",
        scatter_dimension=0,
        tiled=True,
    ).astype(jnp.float32)
    hidden1 = residual + attn_delta
    scale_mlp = rms_scale(hidden1)
    normed2 = widen((hidden1 * scale_mlp * gain_mlp).astype(jnp.bfloat16))
    gate = jnp.dot(normed2, gate_full, preferred_element_type=jnp.float32)
    up_value = jnp.dot(normed2, up_full, preferred_element_type=jnp.float32)
    sigmoid_gate = jax.nn.sigmoid(gate)
    activated = (gate * sigmoid_gate * up_value).astype(jnp.bfloat16)
    mlp_delta = narrow(jnp.dot(activated, down_cols, preferred_element_type=jnp.float32))
    block_out = (hidden1 + mlp_delta).astype(jnp.bfloat16)
    grad_rows = widen(cotangent)
    down_part = jnp.einsum("tf,td->fd", activated, grad_rows, preferred_element_type=jnp.float32)
    act_grad = jnp.einsum("td,fd->tf", grad_rows, down_cols, preferred_element_type=jnp.float32)
    gate_delta = (act_grad * up_value * sigmoid_gate * (1.0 + gate * (1.0 - sigmoid_gate))).astype(
        jnp.bfloat16
    )
    up_delta = (act_grad * gate * sigmoid_gate).astype(jnp.bfloat16)
    gate_part = jnp.einsum("td,tf->df", normed2, gate_delta, preferred_element_type=jnp.float32)
    up_part = jnp.einsum("td,tf->df", normed2, up_delta, preferred_element_type=jnp.float32)
    normed2_term = jnp.einsum(
        "tf,df->td", gate_delta, gate_full, preferred_element_type=jnp.float32
    ) + jnp.einsum("tf,df->td", up_delta, up_full, preferred_element_type=jnp.float32)
    normed2_grad = narrow(normed2_term)
    mlp_gain_part = jnp.sum(normed2_grad * hidden1 * scale_mlp, axis=0)
    hidden1_grad = cotangent.astype(jnp.float32) + norm_back(
        hidden1, scale_mlp, gain_mlp, normed2_grad
    )
    hidden1_rounded = hidden1_grad.astype(jnp.bfloat16)
    grad_full = lax.all_gather(hidden1_rounded, "tensor", axis=0, tiled=True)
    attended_grad = jnp.einsum(
        "td,hd->th", grad_full, out_cols, preferred_element_type=jnp.float32
    ).astype(jnp.bfloat16)
    out_part = jnp.einsum("th,td->hd", attn_flat, grad_full, preferred_element_type=jnp.float32)
    attended_grad = attended_grad.reshape(seq_count, length, groups, repeat_factor, HEAD_SIZE)
    prob_full = jnp.exp(score_block(queries, key_heads, segment_ids) - log_total)
    prob_grad = jnp.einsum(
        "sqgrd,skgd->sgrqk", attended_grad, values, preferred_element_type=jnp.float32
    )
    inner_sum = jnp.sum(prob_full * prob_grad, axis=-1, keepdims=True)
    score_grad = (prob_full * (prob_grad - inner_sum) * HEAD_SIZE ** (-0.5)).astype(jnp.bfloat16)
    query_grad = jnp.einsum(
        "sgrqk,skgd->sqgrd", score_grad, key_heads, preferred_element_type=jnp.float32
    )
    key_grad = jnp.einsum(
        "sgrqk,sqgrd->skgd", score_grad, queries, preferred_element_type=jnp.float32
    )
    value_grad = jnp.einsum(
        "sgrqk,sqgrd->skgd",
        prob_full.astype(jnp.bfloat16),
        attended_grad,
        preferred_element_type=jnp.float32,
    )
    projected_grad = jnp.concatenate(
        [
            unrotate(query_grad, cos_query, sin_query),
            unrotate(key_grad, cos_key, sin_key)[:, :, :, None],
            value_grad[:, :, :, None],
        ],
        axis=3,
    )
    projected_grad = projected_grad.astype(jnp.bfloat16).reshape(
        seq_count * length, groups * (repeat_factor + 2) * HEAD_SIZE
    )
    qkv_part = jnp.einsum("td,tc->dc", normed1, projected_grad, preferred_element_type=jnp.float32)
    normed1_grad = narrow(
        jnp.einsum("tc,dc->td", projected_grad, qkv_full, preferred_element_type=jnp.float32)
    )
    attn_gain_part = jnp.sum(normed1_grad * residual * scale_attn, axis=0)
    input_grad = (hidden1_grad + norm_back(residual, scale_attn, gain_attn, normed1_grad)).astype(
        jnp.bfloat16
    )
    attn_gain_total, mlp_gain_total = lax.psum((attn_gain_part, mlp_gain_part), "tensor")
    attn_gain_grad, qkv_grad, gate_grad, up_grad, mlp_gain_grad = (
        lax.psum_scatter(
            attn_gain_total.astype(jnp.bfloat16), "dp", scatter_dimension=0, tiled=True
        ).astype(jnp.float32),
        lax.psum_scatter(
            qkv_part.astype(jnp.bfloat16), "dp", scatter_dimension=0, tiled=True
        ).astype(jnp.float32),
        lax.psum_scatter(
            gate_part.astype(jnp.bfloat16), "dp", scatter_dimension=0, tiled=True
        ).astype(jnp.float32),
        lax.psum_scatter(
            up_part.astype(jnp.bfloat16), "dp", scatter_dimension=0, tiled=True
        ).astype(jnp.float32),
        lax.psum_scatter(
            mlp_gain_total.astype(jnp.bfloat16), "dp", scatter_dimension=0, tiled=True
        ).astype(jnp.float32),
    )
    out_grad, down_grad = (
        lax.psum_scatter(
            out_part.astype(jnp.bfloat16), "dp", scatter_dimension=1, tiled=True
        ).astype(jnp.float32),
        lax.psum_scatter(
            down_part.astype(jnp.bfloat16), "dp", scatter_dimension=1, tiled=True
        ).astype(jnp.float32),
    )
    return (
        block_out,
        input_grad,
        attn_gain_grad,
        qkv_grad,
        out_grad,
        mlp_gain_grad,
        gate_grad,
        up_grad,
        down_grad,
    )


GROUP = 4
WINDOW = 256
LANES = 384
TILE = 128


MESH = pl.DeviceIdType.MESH


class Transfer:
    def __init__(self, copy, sends=None, receives=None):
        self.copy, self.sends, self.receives = copy, sends, receives

    def _when(self, condition, action):
        if condition is None:
            action()
        else:
            pl.when(condition)(action)

    def start(self):
        self._when(self.sends, self.copy.start)
        return self

    def wait_recv(self):
        self._when(self.receives, self.copy.wait_recv)

    def wait_send(self):
        self._when(self.sends, self.copy.wait_send)


class Links:
    def __init__(self, n_dp, n_tensor, out_sems, in_sems, local_sems):
        self.n_dp, self.n_tensor = n_dp, n_tensor
        self.out_sems, self.in_sems, self.local_sems = out_sems, in_sems, local_sems
        self.d_at, self.z_at = lax.axis_index("dp"), lax.axis_index("tensor")
        self.used, self.used_local = 0, 0
        self.sent, self.saved = [], []

    def barrier(self):
        barrier = pltpu.get_barrier_semaphore()
        for k in range(1, self.n_dp):
            pl.semaphore_signal(
                barrier,
                inc=1,
                device_id={"dp": self.d_at ^ k, "tensor": self.z_at},
                device_id_type=MESH,
            )
        for s in range(1, self.n_tensor):
            pl.semaphore_signal(
                barrier,
                inc=1,
                device_id={"dp": self.d_at, "tensor": lax.rem(self.z_at + s, self.n_tensor)},
                device_id_type=MESH,
            )
        pl.semaphore_wait(barrier, self.n_dp - 1 + self.n_tensor - 1)

    def plan(self, source, target, bit=0, shift=0, sends=None, receives=None):
        slot = self.used
        self.used += 1
        copy = pltpu.make_async_remote_copy(
            src_ref=source,
            dst_ref=target,
            send_sem=self.out_sems.at[slot],
            recv_sem=self.in_sems.at[slot],
            device_id={
                "dp": self.d_at ^ bit,
                "tensor": lax.rem(self.z_at + self.n_tensor + shift, self.n_tensor),
            },
            device_id_type=MESH,
        )
        transfer = Transfer(copy, sends, receives)
        self.sent.append(transfer)
        return transfer

    def send(self, source, target, bit=0, shift=0):
        return self.plan(source, target, bit, shift).start()

    def move(self, source, target):
        copy = pltpu.make_async_copy(source, target, self.local_sems.at[self.used_local])
        self.used_local += 1
        copy.start()
        return copy

    def save(self, source, target):
        self.saved.append(self.move(source, target))

    def finish(self):
        for transfer in self.sent:
            transfer.wait_send()
        for copy in self.saved:
            copy.wait()


class Spread:
    def __init__(self, links, own_piece, target, columns):
        self.links, self.own_piece, self.target, self.columns = links, own_piece, target, columns
        self.ahead, self.back, self.swaps = [], [], []

    def _slot(self, index):
        n = self.links.n_tensor
        return self.target.at[lax.rem(index + n, n), :, self.columns]

    def issue(self):
        links, n, z = self.links, self.links.n_tensor, self.links.z_at
        own = self._slot(z)
        for s in range(1, n):
            up_from, down_from = z - (s - 1), z + (s - 1)
            up_source = self.own_piece if s == 1 else self._slot(up_from)
            down_source = self.own_piece if s == 1 else self._slot(down_from)
            self.ahead.append(
                links.plan(
                    up_source, self._slot(up_from), shift=1,
                    sends=(z < n - 1) & (up_from >= 0), receives=z >= s,
                )
            )
            self.back.append(
                links.plan(
                    down_source, self._slot(down_from), shift=-1,
                    sends=(z > 0) & (down_from < n), receives=z + s < n,
                )
            )
        self.ahead[0].start()
        self.back[0].start()
        self.swaps.append(links.plan(self.own_piece, own, bit=GROUP).start())

    def step(self, s):
        links, n, z = self.links, self.links.n_tensor, self.links.z_at
        for arrivals, piece, here in (
            (self.ahead, z - s, z >= s),
            (self.back, z + s, z + s < n),
        ):
            arrivals[s - 1].wait_recv()
            if s < n - 1:
                arrivals[s].start()
            slot = self._slot(piece)
            self.swaps.append(
                links.plan(slot, slot, bit=GROUP, sends=here, receives=here).start()
            )

    def wait(self):
        for swap in self.swaps:
            swap.wait_recv()


def kernel_forward(
    n_dp, n_tensor,
    tokens, cot, gate_w, up_w, down_w, out_w, qkv_w, segments, gain_rows, fixed,
    normed1_out, normed2_out, hidden_out, query_out, keyval_out, log_out, att_out,
    cos_out, sin_out, qkv_out, out_out, small_out, cot_out, gate_out, up_out, down_out,
    x_all, n1_all, first, dealt, first_piece, qkv, out_parcel, obuf, gbuf, ubuf, dbuf, piece, outw,
    small, small_all, stream, parts, recv, queries, keyvals,
    att, by_repeat, logs, cosine, sine, low_col, to_core, from_core, to_across, from_across,
    hidden, n2_all, stage, out_sems, in_sems, local_sems,
):
    f32, bf16 = jnp.float32, jnp.bfloat16
    links = Links(n_dp, n_tensor, out_sems, in_sems, local_sems)
    send, move, save = links.send, links.move, links.save
    d_at, z_at = links.d_at, links.z_at
    member = d_at % GROUP
    core = d_at % 2
    upper = d_at // GROUP
    rows, width = tokens.shape
    half = width // 2
    chunk = qkv_w.shape[0]
    contract = (((1,), (1,)), ((), ()))
    columns = pl.ds(pl.multiple_of(upper * half, half), half)

    turned = qkv_w[...].T
    quarter = turned.shape[0] // GROUP
    for i in range(GROUP):
        first[i] = turned[i * quarter : (i + 1) * quarter]
    turned = out_w[...].T
    out_quarter = turned.shape[0] // GROUP
    for i in range(GROUP):
        out_parcel[i] = turned[i * out_quarter : (i + 1) * out_quarter]
    ids = segments[...]
    seqs, length = ids.shape
    begin = jnp.zeros_like(ids)
    for value in range(3):
        count = jnp.sum((ids == value).astype(jnp.int32), axis=1, keepdims=True)
        begin = begin + jnp.where(ids > value, count, 0)
    begin = begin.astype(f32)
    for i in range(seqs):
        stream[:, i * length : (i + 1) * length] = jnp.broadcast_to(
            begin[i : i + 1] + float(i * length), (stream.shape[0], length)
        )
    window = stream[:, pl.ds(pl.multiple_of(z_at * rows, TILE), rows)]
    here = lax.broadcasted_iota(jnp.int32, window.shape, 1) + z_at * rows
    small[...] = window
    small[0:1] = here.astype(f32)[0:1] - window[0:1]
    small[2:4, :chunk] = gain_rows[...].astype(f32)

    @pl.when(z_at == 0)
    def _():
        keyvals[:, :WINDOW, :] = jnp.zeros_like(keyvals[:, :WINDOW, :])

    links.barrier()

    deals = [send(first.at[member ^ k], dealt.at[member], bit=k) for k in range(1, GROUP)]
    beside = send(tokens, x_all.at[2], bit=1)
    smalls = [send(small, small_all.at[d_at], bit=k) for k in range(1, n_dp)]
    def columns_of(ref, at):
        size = ref.shape[1] // GROUP
        return ref.at[:, pl.ds(pl.multiple_of(at * size, TILE), size)]

    def parcel_of(ref, at):
        return ref.at[at]

    pairs = [
        (out_parcel, obuf, parcel_of), (gate_w, gbuf, columns_of), (up_w, ubuf, columns_of),
        (down_w, dbuf, columns_of),
    ]

    def deal(group):
        return [
            send(take(ref, member ^ k), buffer.at[member], bit=k)
            for ref, buffer, take in group
            for k in range(1, GROUP)
        ]

    rests = deal(pairs[:2])
    across = send(tokens, x_all.at[1], bit=2)
    late_rests = deal(pairs[2:])
    own = [move(tokens, x_all.at[0])]
    for ref, buffer, take in pairs:
        own.append(move(take(ref, member), buffer.at[member]))
    cot_stage = move(cot, stage)
    small_all[d_at] = small[...]
    dealt[member] = first[member]

    entries = lax.broadcasted_iota(jnp.int32, (WINDOW, LANES), 0).astype(f32)
    angles = entries * fixed[0:1]

    def split(table):
        pieces = []
        for _ in range(3):
            pieces.append(table.astype(bf16))
            table = table - pieces[-1].astype(f32)
        return pieces

    cos_parts, sin_parts = split(jnp.cos(angles)), split(jnp.sin(angles))
    second = fixed[1:2]
    own_turns = jnp.where(core == 0, jnp.ones_like(second), fixed[2:3])

    for copy in deals:
        copy.wait_recv()
    for i in range(GROUP):
        first_piece[:, i * chunk : (i + 1) * chunk] = dealt[i]
    spread_first = Spread(links, first_piece, qkv, columns)
    spread_first.issue()
    save(first_piece, qkv.at[z_at, :, columns])
    own_qkv = links.saved.pop()
    for copy in own:
        copy.wait()
    cot_stage.wait()
    save(stage, cot_out.at[0])
    spread_first.step(1)
    for copy in smalls:
        copy.wait_recv()
    spread_first.step(2)
    gains = []
    for row in (2, 3):
        gains.append(
            jnp.concatenate([small_all[i, row : row + 1, :chunk] for i in range(n_dp)], axis=1)
        )
    for copy in rests:
        copy.wait_recv()
    sizes = [obuf.shape[1], gbuf.shape[2], ubuf.shape[2], dbuf.shape[2]]
    starts = [sum(sizes[:i]) for i in range(len(sizes))]
    saves = []

    def prepare(index, target, buffer):
        at = slice(starts[index], starts[index] + sizes[index])
        for i in range(GROUP):
            piece[at, i * chunk : (i + 1) * chunk] = buffer[i] if index == 0 else buffer[i].T
        own_piece = piece.at[pl.ds(starts[index], sizes[index])]
        saves.append(move(own_piece, target.at[z_at, :, columns]))
        return Spread(links, own_piece, target, columns)

    out_spread = prepare(0, outw, obuf)
    gate_spread = prepare(1, gate_out, gbuf)
    out_spread.issue()
    spread_first.step(3)
    gate_spread.issue()
    beside.wait_recv()
    own_qkv.wait()
    spread_first.wait()

    def project_block(m, k):
        features = x_all[m].astype(f32)
        scale = lax.rsqrt(jnp.mean(features * features, axis=1, keepdims=True) + EPS)
        normal = (features * scale * gains[0]).astype(bf16)
        n1_all[m] = normal
        units = qkv.shape[0] * qkv.shape[1]
        product = lax.dot_general(
            normal, qkv[...].reshape(units, width), contract, preferred_element_type=f32
        )
        info = small_all[d_at ^ k].T
        key = lax.broadcasted_iota(jnp.int32, (rows, WINDOW), 1)
        chosen = (info[:, 0:1].astype(jnp.int32) == key).astype(bf16)

        def pick(table):
            total = jnp.dot(chosen, table[0], preferred_element_type=f32)
            for part in table[1:]:
                total += jnp.dot(chosen, part, preferred_element_type=f32)
            return total

        cos_here, sin_here = pick(cos_parts), pick(sin_parts)
        parts[m] = turn(product, cos_here, sin_here, second, own_turns, 1.0).astype(bf16)
        if m < 2:
            cosine[m] = cos_here
            sine[m] = sin_here
            low_col[m] = info[:, 1:2].astype(jnp.int32) - z_at * rows + WINDOW

    is_first = core == 0
    halos = [
        links.plan(
            keyvals.at[m, pl.ds(rows, WINDOW)], keyvals.at[m, pl.ds(0, WINDOW)], shift=1,
            sends=z_at < n_tensor - 1, receives=z_at > 0,
        )
        for m in range(2)
    ]

    def take_block(m, swap):
        swap.wait_recv()
        mine, other = parts[m], recv[m]
        queries[m] = jnp.where(is_first, mine, other)
        keyvals[m, WINDOW:, :] = jnp.where(is_first, other, mine)
        halos[m].start()

    project_block(2, 1)
    part_swap = send(parts.at[2], recv.at[0], bit=1)
    project_block(0, 0)
    take_block(0, part_swap)
    out_spread.step(1)
    across.wait_recv()
    both = send(x_all.at[1], x_all.at[3], bit=1)
    cot_across = send(cot, cot_out.at[1], bit=2)
    cot_beside = send(cot, cot_out.at[2], bit=1)
    project_block(1, 2)
    both.wait_recv()
    project_block(3, 3)
    part_swap = send(parts.at[3], recv.at[1], bit=1)
    save(n1_all, normed1_out)
    save(cosine, cos_out)
    save(sine, sin_out)
    take_block(1, part_swap)
    out_spread.step(2)
    gate_spread.step(1)
    for copy in late_rests:
        copy.wait_recv()
    up_spread = prepare(2, up_out, ubuf)
    down_spread = prepare(3, down_out, dbuf)
    save(queries, query_out)
    heads = queries.shape[2] // HEAD_SIZE
    repeat = QUERY_HEADS // KEY_VALUE_HEADS
    span = TILE + WINDOW

    def attend_tile(m, start):
        key = lax.broadcasted_iota(jnp.int32, (TILE, span), 1)
        query = lax.broadcasted_iota(jnp.int32, (TILE, span), 0)
        lowest = low_col[m, pl.ds(start, TILE), :] - start
        allowed = (key >= lowest) & (key <= query + WINDOW)
        for head in range(heads):
            group, r = head // repeat, head % repeat
            base = group * 2 * HEAD_SIZE
            q = queries[m, pl.ds(start, TILE), head * HEAD_SIZE : (head + 1) * HEAD_SIZE]
            k = keyvals[m, pl.ds(start, span), base : base + HEAD_SIZE]
            v = keyvals[m, pl.ds(start, span), base + HEAD_SIZE : base + 2 * HEAD_SIZE]
            s = lax.dot_general(q, k, contract, preferred_element_type=f32) * HEAD_SIZE ** (-0.5)
            s = jnp.where(allowed, s, NEG_FILL)
            highest = jnp.max(s, axis=1, keepdims=True)
            e = jnp.exp(s - highest)
            whole = jnp.sum(e, axis=1, keepdims=True)
            p = (e * (1.0 / whole)).astype(bf16)
            o = jnp.dot(p, v, preferred_element_type=f32).astype(bf16)
            logs[m, pl.ds(start, TILE), head : head + 1] = highest + jnp.log(whole)
            by_repeat[r, m, pl.ds(start, TILE), group * HEAD_SIZE : (group + 1) * HEAD_SIZE] = o

    tiles = rows // TILE
    free = -(-WINDOW // TILE)

    def attend_tiles(blocks, first_tile, last_tile):
        for m in blocks:
            for tile in range(first_tile, last_tile):
                attend_tile(m, tile * TILE)

    attend_tiles((1, 0), free, tiles)
    out_spread.step(3)
    up_spread.issue()
    halos[0].wait_recv()
    halos[1].wait_recv()
    attend_tiles((1,), 0, free)
    att_swap1 = send(by_repeat.at[1 - core, 1], att.at[3], bit=1)
    gate_spread.step(2)
    attend_tiles((0,), 0, free)
    att_swap0 = send(by_repeat.at[1 - core, 0], att.at[2], bit=1)
    save(keyvals, keyval_out)
    save(logs, log_out)
    att[0] = by_repeat[core, 0]
    att[1] = by_repeat[core, 1]
    down_spread.issue()
    cot_across.wait_recv()
    cot_both = send(cot_out.at[1], cot_out.at[3], bit=1)

    saves[0].wait()
    out_spread.wait()

    def project_out(b):
        units = outw.shape[0] * outw.shape[1]
        return jnp.dot(att[b], outw[...].reshape(units, width), preferred_element_type=f32)

    att_swap1.wait_recv()
    to_core[1] = project_out(3).astype(bf16)
    core_send1 = send(to_core.at[1], from_core.at[1], bit=1)
    hidden[...] = project_out(1)
    att_swap0.wait_recv()
    to_core[0] = project_out(2).astype(bf16)
    core_send0 = send(to_core.at[0], from_core.at[0], bit=1)
    core_send1.wait_recv()
    across_sends = []
    for i in range(tiles):
        at = pl.ds(i * TILE, TILE)
        to_across[at] = (hidden[at, :] + from_core[1, at, :].astype(f32)).astype(bf16)
        across_sends.append(send(to_across.at[at], from_across.at[at], bit=2))
    hidden[...] = project_out(0) + x_all[0].astype(f32)
    core_send0.wait_recv()
    hidden[...] += from_core[0].astype(f32)
    save(att, att_out)
    gate_spread.step(3)
    up_spread.step(1)
    steps = [
        (up_spread, 2), (up_spread, 3), (down_spread, 1), (down_spread, 2), (down_spread, 3),
    ]
    last = []
    for i in range(tiles):
        at = pl.ds(i * TILE, TILE)
        across_sends[i].wait_recv()
        value = hidden[at, :] + from_across[at, :].astype(f32)
        hidden[at, :] = value
        scale = lax.rsqrt(jnp.mean(value * value, axis=1, keepdims=True) + EPS)
        n2_all[0, at, :] = (value * scale * gains[1]).astype(bf16)
        last.append(send(n2_all.at[0, at], n2_all.at[1, at], bit=2))
        last.append(send(n2_all.at[0, at], n2_all.at[2, at], bit=1))
        if i < 3:
            spread, s = steps.pop(0)
            spread.step(s)
    save(hidden, hidden_out)
    save(qkv, qkv_out)
    save(outw, out_out)
    save(small_all, small_out)
    ends = []
    for i in range(tiles):
        at = pl.ds(i * TILE, TILE)
        last[2 * i].wait_recv()
        ends.append(send(n2_all.at[1, at], n2_all.at[3, at], bit=1))
        if i < 2:
            spread, s = steps.pop(0)
            spread.step(s)
    for copy in ends + last[1::2]:
        copy.wait_recv()
    save(n2_all, normed2_out)
    for copy in saves[1:]:
        copy.wait()
    for spread in (gate_spread, up_spread, down_spread):
        spread.wait()
    for copy in (cot_beside, cot_both):
        copy.wait_recv()
    links.finish()


def forward(
    n_dp, n_tensor, tokens, cot, segments, gain_rows, qkv_w, out_w, gate_w, up_w, down_w
):
    out_w, down_w = out_w.T, down_w.T
    rows, width = tokens.shape
    f32, bf16 = jnp.float32, jnp.bfloat16
    vmem = pl.BlockSpec(memory_space=pltpu.VMEM)
    hbm = pl.BlockSpec(memory_space=pl.ANY)
    chunk = qkv_w.shape[0]
    quarter = qkv_w.shape[1] // GROUP
    sizes = [
        out_w.shape[1] // GROUP, gate_w.shape[1] // GROUP, up_w.shape[1] // GROUP,
        down_w.shape[1] // GROUP,
    ]
    units = quarter * n_tensor
    heads = units // HEAD_SIZE
    lane = np.arange(LANES)
    within = lane % HEAD_SIZE
    fixed = np.zeros((8, LANES), np.float32)
    fixed[0] = np.power(ROPE_BASE, -(2.0 * (within % (HEAD_SIZE // 2))) / HEAD_SIZE)
    fixed[1] = within >= HEAD_SIZE // 2
    fixed[2] = lane % (2 * HEAD_SIZE) < HEAD_SIZE
    fixed[3] = 1.0

    def shape(dims, dtype=bf16):
        return jax.ShapeDtypeStruct(tuple(dims), dtype)

    full = (GROUP, rows, width)
    qkv_shape = (n_tensor, quarter, width)
    out_shape = (n_tensor, sizes[0], width)
    att_shape = (GROUP, rows, units // 2)
    small_shape = (n_dp, 8, rows)
    table = (2, rows, LANES)
    outs = [
        shape(full),
        shape(full),
        shape((rows, width), f32),
        shape((2, rows, units)),
        shape((2, rows + WINDOW, units)),
        shape((2, rows, heads), f32),
        shape(att_shape),
        shape(table, f32),
        shape(table, f32),
        shape(qkv_shape),
        shape(out_shape),
        shape(small_shape, f32),
        shape(full),
    ] + [shape((n_tensor, size, width)) for size in sizes[1:]]
    scratch = [
        pltpu.VMEM(full, bf16),
        pltpu.VMEM(full, bf16),
        pltpu.VMEM((GROUP, quarter, chunk), bf16),
        pltpu.VMEM((GROUP, quarter, chunk), bf16),
        pltpu.VMEM((quarter, width // 2), bf16),
        pltpu.VMEM(qkv_shape, bf16),
        pltpu.VMEM((GROUP, sizes[0], chunk), bf16),
        pltpu.VMEM((GROUP, sizes[0], chunk), bf16),
        pltpu.VMEM((GROUP, chunk, sizes[1]), bf16),
        pltpu.VMEM((GROUP, chunk, sizes[2]), bf16),
        pltpu.VMEM((GROUP, chunk, sizes[3]), bf16),
        pltpu.VMEM((sum(sizes), width // 2), bf16),
        pltpu.VMEM(out_shape, bf16),
        pltpu.VMEM((8, rows), f32),
        pltpu.VMEM(small_shape, f32),
        pltpu.VMEM((8, n_tensor * rows), f32),
        pltpu.VMEM((GROUP, rows, units), bf16),
        pltpu.VMEM((2, rows, units), bf16),
        pltpu.VMEM((2, rows, units), bf16),
        pltpu.VMEM((2, rows + WINDOW, units), bf16),
        pltpu.VMEM(att_shape, bf16),
        pltpu.VMEM((2, 2, rows, units // 2), bf16),
        pltpu.VMEM((2, rows, heads), f32),
        pltpu.VMEM(table, f32),
        pltpu.VMEM(table, f32),
        pltpu.VMEM((2, rows, 1), jnp.int32),
        pltpu.VMEM((2, rows, width), bf16),
        pltpu.VMEM((2, rows, width), bf16),
        pltpu.VMEM((rows, width), bf16),
        pltpu.VMEM((rows, width), bf16),
        pltpu.VMEM((rows, width), f32),
        pltpu.VMEM(full, bf16),
        pltpu.VMEM((rows, width), bf16),
        pltpu.SemaphoreType.DMA((128,)),
        pltpu.SemaphoreType.DMA((128,)),
        pltpu.SemaphoreType.DMA((40,)),
    ]
    results = pl.pallas_call(
        functools.partial(kernel_forward, n_dp, n_tensor),
        in_specs=[hbm] * 5 + [vmem] * 5,
        out_specs=[hbm] * len(outs),
        out_shape=outs,
        scratch_shapes=scratch,
        compiler_params=pltpu.CompilerParams(
            collective_id=0, has_side_effects=True, vmem_limit_bytes=60 * 1024 * 1024
        ),
        name="forward",
    )(
        tokens, cot, gate_w, up_w, down_w, out_w, qkv_w, segments, gain_rows, jnp.asarray(fixed)
    )
    return results, jnp.asarray(fixed)


def turn(value, cosine, sine, second, turns, sign):
    width = value.shape[1]
    half = HEAD_SIZE // 2
    c = turns * cosine + (1.0 - turns)
    u = (sign * turns * second) * sine
    d = (sign * turns * (second - 1.0)) * sine
    pieces = []
    up = pltpu.roll(value, half, 1)
    down = pltpu.roll(value, width - half, 1)
    for i in range(width // LANES):
        at = slice(i * LANES, (i + 1) * LANES)
        pieces.append(value[:, at] * c + up[:, at] * u + down[:, at] * d)
    return jnp.concatenate(pieces, axis=1)


def kernel_feed(
    n_dp, n_tensor,
    n2_in, cot_in, hidden_in, gate_in, up_in, down_in, smalls,
    grad_out, grad_own_out, mlp_out, down_out, gate_out, up_out, down_got, row_out,
    n2_all, cot_all, gate_w, up_w, down_w, active, gate_delta, up_delta,
    down_part, gate_part, up_part, to_core, from_core, to_across, from_across, hidden, total,
    rounded, row, out_sems, in_sems, local_sems,
):
    f32, bf16 = jnp.float32, jnp.bfloat16
    links = Links(n_dp, n_tensor, out_sems, in_sems, local_sems)
    send, move, save = links.send, links.move, links.save
    upper = links.d_at // GROUP
    rows, width = hidden.shape
    half = width // 2
    chunk = width // n_dp
    size = gate_w.shape[1]
    units = n_tensor * size
    contract = (((1,), (1,)), ((), ()))
    over_rows = (((0,), (0,)), ((), ()))
    other = pl.ds(pl.multiple_of((1 - upper) * half, half), half)
    tiles = rows // TILE

    first_sem = links.used_local
    links.used_local += 3 * n_tensor + 2 * GROUP
    weights = ((gate_in, gate_w), (up_in, up_w), (down_in, down_w))
    tokens = ((n2_in, n2_all), (cot_in, cot_all))

    def weight_loads(p):
        return [
            pltpu.make_async_copy(
                source.at[p], target.at[p], local_sems.at[first_sem + i * n_tensor + p]
            )
            for i, (source, target) in enumerate(weights)
        ]

    def token_loads(m):
        start = first_sem + 3 * n_tensor
        return [
            pltpu.make_async_copy(source.at[m], target.at[m], local_sems.at[start + i * GROUP + m])
            for i, (source, target) in enumerate(tokens)
        ]

    for copy in token_loads(3):
        copy.start()
    for p in range(n_tensor):
        for copy in weight_loads(p):
            copy.start()
    for m in (1, 2, 0):
        for copy in token_loads(m):
            copy.start()
    hidden_load = move(hidden_in, hidden)
    links.barrier()

    def inner(i, carry):
        turn_at, p = i // n_tensor, i % n_tensor
        m = 3 - 2 * (turn_at % 2) - turn_at // 2

        @pl.when(p == 0)
        def _():
            for copy in token_loads(m):
                copy.wait()

        @pl.when(turn_at == 0)
        def _():
            for copy in weight_loads(p):
                copy.wait()

        at = pl.ds(pl.multiple_of(p * size, TILE), size)
        gate = lax.dot_general(n2_all[m], gate_w[p], contract, preferred_element_type=f32)
        up_value = lax.dot_general(n2_all[m], up_w[p], contract, preferred_element_type=f32)
        act_grad = lax.dot_general(cot_all[m], down_w[p], contract, preferred_element_type=f32)
        sigmoid = jax.nn.sigmoid(gate)
        silu = gate * sigmoid
        active[m, :, at] = (silu * up_value).astype(bf16)
        gate_delta[m, :, at] = (
            act_grad * up_value * sigmoid * (1.0 + gate * (1.0 - sigmoid))
        ).astype(bf16)
        up_delta[m, :, at] = (act_grad * silu).astype(bf16)
        return carry

    lax.fori_loop(0, 2 * n_tensor, inner, 0)

    def back(m):
        return jnp.dot(
            gate_delta[m], gate_w[...].reshape(units, width), preferred_element_type=f32
        ) + jnp.dot(up_delta[m], up_w[...].reshape(units, width), preferred_element_type=f32)

    to_core[1] = back(3).astype(bf16)
    core_send1 = send(to_core.at[1], from_core.at[1], bit=1)
    total[...] = back(1)
    core_send1.wait_recv()
    across = []
    for i in range(tiles):
        at = pl.ds(i * TILE, TILE)
        to_across[at] = (total[at, :] + from_core[1, at, :].astype(f32)).astype(bf16)
        across.append(send(to_across.at[at], from_across.at[at], bit=2))
    lax.fori_loop(2 * n_tensor, GROUP * n_tensor, inner, 0)

    order = []
    for i in range((n_tensor + 1) // 2):
        order.extend(dict.fromkeys((n_tensor - 1 - i, i)))

    swaps = []

    def grads(left, right, part, target, weight=None):
        for p in order:
            at = slice(p * size, (p + 1) * size)
            grad = lax.dot_general(
                left[...].reshape(GROUP * rows, units)[:, at],
                right[...].reshape(GROUP * rows, width),
                over_rows,
                preferred_element_type=f32,
            )
            part[p] = grad.astype(bf16)
            if weight is not None:
                row[...] += jnp.sum(grad * weight[p].astype(f32), axis=0, keepdims=True)
            elif p in order[: n_tensor // 2]:
                swaps.append(send(part.at[p, :, other], down_got.at[p], bit=GROUP))
            save(part.at[p], target.at[p])

    row[...] = jnp.zeros_like(row)
    grads(active, cot_all, down_part, down_out)
    to_core[0] = back(2).astype(bf16)
    core_send0 = send(to_core.at[0], from_core.at[0], bit=1)
    total[...] = back(0)
    core_send0.wait_recv()
    total[...] += from_core[0].astype(f32)
    grads(gate_delta, n2_all, gate_part, gate_out, gate_w)
    grads(up_delta, n2_all, up_part, up_out, up_w)
    save(row, row_out)

    for m in range(GROUP):
        n2_all[m] = jnp.dot(
            active[m], down_w[...].reshape(units, width), preferred_element_type=f32
        ).astype(bf16)
        save(n2_all.at[m], mlp_out.at[m])
    gain = jnp.concatenate([smalls[i, 3:4, :chunk] for i in range(n_dp)], axis=1)
    hidden_load.wait()
    for i in range(tiles):
        at = pl.ds(i * TILE, TILE)
        across[i].wait_recv()
        upstream = total[at, :] + from_across[at, :].astype(f32)
        features = hidden[at, :]
        inverse = lax.rsqrt(jnp.mean(features * features, axis=1, keepdims=True) + EPS)
        scaled = gain * upstream
        mean = jnp.mean(scaled * features, axis=1, keepdims=True)
        result = cot_all[0, at, :].astype(f32) + (
            inverse * scaled - features * (inverse * inverse * inverse) * mean
        )
        total[at, :] = result
        rounded[at, :] = result.astype(bf16)
    save(total, grad_out)
    save(rounded, grad_own_out)
    for copy in swaps:
        copy.wait_recv()
    links.finish()


def feed(n_dp, n_tensor, normed2, grad_rows, hidden1, gate_w, up_w, down_w, smalls):
    f32, bf16 = jnp.float32, jnp.bfloat16
    rows, width = hidden1.shape
    half = width // 2
    vmem = pl.BlockSpec(memory_space=pltpu.VMEM)
    hbm = pl.BlockSpec(memory_space=pl.ANY)
    weight = gate_w.shape
    inner = (GROUP, rows, n_tensor * weight[1])

    def shape(dims, dtype=bf16):
        return jax.ShapeDtypeStruct(tuple(dims), dtype)

    outs = [
        shape((rows, width), f32), shape((rows, width)), shape(normed2.shape),
        shape(weight), shape(weight), shape(weight), shape((n_tensor, weight[1], half)),
        shape((1, width), f32),
    ]
    scratch = [
        pltpu.VMEM(normed2.shape, bf16),
        pltpu.VMEM(normed2.shape, bf16),
        pltpu.VMEM(weight, bf16),
        pltpu.VMEM(weight, bf16),
        pltpu.VMEM(weight, bf16),
        pltpu.VMEM(inner, bf16),
        pltpu.VMEM(inner, bf16),
        pltpu.VMEM(inner, bf16),
        pltpu.VMEM(weight, bf16),
        pltpu.VMEM(weight, bf16),
        pltpu.VMEM(weight, bf16),
        pltpu.VMEM((2, rows, width), bf16),
        pltpu.VMEM((2, rows, width), bf16),
        pltpu.VMEM((rows, width), bf16),
        pltpu.VMEM((rows, width), bf16),
        pltpu.VMEM((rows, width), f32),
        pltpu.VMEM((rows, width), f32),
        pltpu.VMEM((rows, width), bf16),
        pltpu.VMEM((1, width), f32),
        pltpu.SemaphoreType.DMA((16,)),
        pltpu.SemaphoreType.DMA((16,)),
        pltpu.SemaphoreType.DMA((40,)),
    ]
    return pl.pallas_call(
        functools.partial(kernel_feed, n_dp, n_tensor),
        in_specs=[hbm] * 6 + [vmem],
        out_specs=[hbm] * len(outs),
        out_shape=outs,
        scratch_shapes=scratch,
        compiler_params=pltpu.CompilerParams(
            collective_id=2, has_side_effects=True, vmem_limit_bytes=67043328
        ),
        name="feed",
    )(normed2, grad_rows, hidden1, gate_w, up_w, down_w, smalls)


class Collect:
    def __init__(
        self, links, part, swapped, stage, arrived, late, blocks, target, mine, other, turned=False
    ):
        self.turned = turned
        self.links, self.part, self.swapped, self.stage = links, part, swapped, stage
        self.arrived, self.late, self.blocks, self.target = arrived, late, blocks, target
        self.mine, self.other = mine, other
        self.swaps, self.loads, self.deals = {}, [], []

    def issue(self, order, load=True):
        links = self.links
        for p in order:
            self.swaps[p] = links.send(
                self.part.at[p, :, self.other], self.swapped.at[p], bit=GROUP
            )
        if self.stage is not None and load:
            self.loads = [links.move(self.part.at[:, :, self.mine], self.stage)]

    def load(self, received, order):
        links = self.links
        count = links.n_tensor // 2
        self.loads = [links.move(received.at[p], self.swapped.at[p]) for p in order[:count]]
        self.loads.append(links.move(self.part.at[:, :, self.mine], self.stage))

    def step(self, p):
        links, n, z = self.links, self.links.n_tensor, self.links.z_at
        f32, bf16 = jnp.float32, jnp.bfloat16
        while self.loads:
            self.loads.pop().wait()
        if p in self.swaps:
            self.swaps[p].wait_recv()
        own = self.stage[p] if self.stage is not None else self.part[p, :, self.mine]
        self.swapped[p] = (own.astype(f32) + self.swapped[p].astype(f32)).astype(bf16)
        if not hasattr(self, "ahead"):
            self.ahead, self.back, self.back_last = [None] * n, [None] * n, [None] * n
        source = self.swapped.at[p]
        self.ahead[p] = links.plan(
            source, self.arrived.at[p], shift=1, sends=z < p, receives=(z > 0) & (z <= p)
        )
        self.back[p] = links.plan(
            source, self.arrived.at[p], shift=-1, sends=z > p + 1,
            receives=(z > p) & (z < n - 1),
        )
        self.back_last[p] = links.plan(
            source, self.late, shift=-1, sends=z == p + 1, receives=(z == p) & (z < n - 1)
        )

        @pl.when((z == 0) & (z < p))
        def _():
            self.ahead[p].copy.start()

        @pl.when((z == n - 1) & (z > p + 1))
        def _():
            self.back[p].copy.start()

        @pl.when((z == n - 1) & (z == p + 1))
        def _():
            self.back_last[p].copy.start()

    def relay(self, i):
        links, n, z = self.links, self.links.n_tensor, self.links.z_at
        f32, bf16 = jnp.float32, jnp.bfloat16

        def add(p):
            self.swapped[p] = (
                self.swapped[p].astype(f32) + self.arrived[p].astype(f32)
            ).astype(bf16)

        for p in range(n):
            at = i - (n - 1) + p
            if 0 < at < n - 1 and at < p:

                @pl.when(z == at)
                def _(p=p):
                    self.ahead[p].copy.wait_recv()
                    add(p)
                    self.ahead[p].copy.start()

            at = n - 1 - i + p
            if 0 < at < n - 1 and at > p:

                @pl.when(z == at)
                def _(p=p, at=at):
                    self.back[p].copy.wait_recv()
                    add(p)
                    (self.back_last if at == p + 1 else self.back)[p].copy.start()

    def finish(self):
        links, n, z = self.links, self.links.n_tensor, self.links.z_at
        f32, bf16 = jnp.float32, jnp.bfloat16
        member = links.d_at % GROUP
        for p in range(n):

            @pl.when((z == p) & (z > 0))
            def _(p=p):
                self.ahead[p].copy.wait_recv()

            @pl.when((z == p) & (z < n - 1))
            def _(p=p):
                self.back_last[p].copy.wait_recv()

        below = jnp.where(z > 0, self.arrived[z].astype(f32), 0.0)
        above = jnp.where(z < n - 1, self.late[...].astype(f32), 0.0)
        total = (self.swapped[z].astype(f32) + below + above).astype(bf16)
        chunk = total.shape[1] // GROUP
        size = self.blocks.shape[2 if self.turned else 1]
        place = pl.ds(pl.multiple_of(member * size, 16), size)
        if self.turned:
            place = pl.ds(pl.multiple_of(member * size, TILE), size)
        for i in range(GROUP):
            block = total[:, i * chunk : (i + 1) * chunk]
            self.blocks[i] = block.T if self.turned else block
        if self.turned:
            target = self.target.at[:, place]
        elif len(self.target.shape) == 2:
            target = self.target.at[place, :]
        else:
            target = self.target.at[member]
        for k in range(1, GROUP):
            self.deals.append(links.send(self.blocks.at[member ^ k], target, bit=k))
        links.save(self.blocks.at[member], target)

    def wait(self):
        for deal in self.deals:
            deal.wait_recv()


def kernel_backward(
    n_dp, n_tensor,
    grad_own, hidden_grad, tokens, hidden1, mlp_part, n1_in, query_in, keyval_in, log_in, att_in,
    cos_in, sin_in, qkv_in, out_in, small_in, down_in, gate_in, up_in, down_got,
    mlp_row, fixed,
    input_out, block_out, qkv_out, out_out, gate_out, up_out, down_out,
    g_all, n1_all, qkv, outw, queries, keyvals, logs, att, cosine, sine, gains, low_col,
    att_grad, other_grad, totals, query_total, pass_on, delta, halo_send, halo_recv,
    to_core, from_core, to_across, from_across, mlp_across, hidden, stage, gate_stage,
    down_swap, gate_swap, up_swap, out_swap, qkv_swap,
    down_come, gate_come, up_come, out_come, qkv_come,
    down_late, gate_late, up_late, out_late, qkv_late,
    down_block, gate_block, up_block, out_block, qkv_block,
    out_sems, in_sems, local_sems,
):
    f32, bf16 = jnp.float32, jnp.bfloat16
    links = Links(n_dp, n_tensor, out_sems, in_sems, local_sems)
    send, move, save = links.send, links.move, links.save
    d_at, z_at = links.d_at, links.z_at
    core = d_at % 2
    upper = d_at // GROUP
    rows, width = grad_own.shape
    half = width // 2
    contract = (((1,), (1,)), ((), ()))
    over_rows = (((0,), (0,)), ((), ()))
    mine = pl.ds(pl.multiple_of(upper * half, half), half)
    other = pl.ds(pl.multiple_of((1 - upper) * half, half), half)
    tiles = rows // TILE
    span = TILE + WINDOW
    quarter = qkv.shape[1]
    out_quarter = outw.shape[1]
    extra = qkv_swap.shape[1] - quarter

    order = []
    for i in range((n_tensor + 1) // 2):
        order.extend(dict.fromkeys((n_tensor - 1 - i, i)))

    down = Collect(
        links, down_in, down_swap, stage, down_come, down_late, down_block, down_out, mine, other,
        turned=True,
    )
    gate = Collect(
        links, gate_in, gate_swap, gate_stage, gate_come, gate_late, gate_block, gate_out, mine, other,
        turned=True,
    )
    up = Collect(
        links, up_in, up_swap, stage, up_come, up_late, up_block, up_out, mine, other, turned=True
    )
    out_part = g_all.at[:, pl.ds(quarter + extra, out_quarter), :]
    qkv_part = g_all.at[:, pl.ds(0, quarter + extra), :]
    out_collect = Collect(
        links, out_part, out_swap, None, out_come, out_late, out_block, out_out, mine, other
    )
    qkv_collect = Collect(
        links, qkv_part, qkv_swap, None, qkv_come, qkv_late, qkv_block, qkv_out, mine, other
    )
    small = move(small_in, gains)
    loads = [
        move(grad_own, g_all.at[0]), move(out_in, outw),
    ]
    down.load(down_got, order)
    loads += [
        move(query_in, queries),
        move(keyval_in, keyvals), move(log_in, logs), move(cos_in, cosine), move(sin_in, sine),
        move(mlp_part.at[pl.ds(0, 2)], to_core), move(hidden1, hidden), move(att_in, att),
        move(qkv_in, qkv), move(n1_in, n1_all),
    ]
    links.barrier()
    across = send(grad_own, g_all.at[1], bit=2)
    beside = send(grad_own, g_all.at[2], bit=1)
    mlp_core = send(mlp_part.at[pl.ds(2, 2)], from_core, bit=1)
    down.issue(order[n_tensor // 2 :], load=False)
    gate.issue(order)
    small.wait()
    for m, k in ((0, 0), (1, 2)):
        info = gains[d_at ^ k].T
        low_col[m] = info[:, 1:2].astype(jnp.int32) - z_at * rows + WINDOW
    loads[0].wait()
    loads[1].wait()

    def attended_back(b):
        units = outw.shape[0] * outw.shape[1]
        att_grad[b] = lax.dot_general(
            g_all[b], outw[...].reshape(units, width), contract, preferred_element_type=f32
        ).astype(bf16)

    attended_back(0)
    beside.wait_recv()
    attended_back(2)
    grad_swap = send(att_grad.at[2], other_grad.at[0], bit=1)
    for p in order[: n_tensor // 2]:
        down.step(p)
    for copy in loads[2:]:
        copy.wait()
    mlp_core.wait_recv()
    heads = queries.shape[2] // HEAD_SIZE
    repeat = QUERY_HEADS // KEY_VALUE_HEADS
    scale = HEAD_SIZE ** (-0.5)
    is_first = core == 0
    second, keys_turn, all_turn = fixed[1:2], fixed[2:3], fixed[3:4]

    def back_tile(m, tile):
        start = tile * TILE
        at = slice(start, start + TILE)
        reach = slice(start, start + span)
        key = lax.broadcasted_iota(jnp.int32, (TILE, span), 1)
        query = lax.broadcasted_iota(jnp.int32, (TILE, span), 0)
        allowed = (key >= low_col[m, at, :] - start) & (key <= query + WINDOW)
        own, others = att_grad[m, at, :], other_grad[m, at, :]
        by_repeat = (jnp.where(is_first, own, others), jnp.where(is_first, others, own))
        for group in range(heads // repeat):
            base = group * 2 * HEAD_SIZE
            k = keyvals[m, reach, base : base + HEAD_SIZE]
            v = keyvals[m, reach, base + HEAD_SIZE : base + 2 * HEAD_SIZE]
            key_sum = None
            for r in range(repeat):
                head = group * repeat + r
                q = queries[m, at, head * HEAD_SIZE : (head + 1) * HEAD_SIZE]
                g = by_repeat[r][:, group * HEAD_SIZE : (group + 1) * HEAD_SIZE]
                s = lax.dot_general(q, k, contract, preferred_element_type=f32) * scale
                total = logs[m, at, head : head + 1]
                p = jnp.exp(jnp.where(allowed, s, NEG_FILL) - total)
                pg = lax.dot_general(g, v, contract, preferred_element_type=f32)
                inner = jnp.sum(p * pg, axis=1, keepdims=True)
                sg = (p * (pg - inner) * scale).astype(bf16)
                query_total[:, head * HEAD_SIZE : (head + 1) * HEAD_SIZE] = jnp.dot(
                    sg, k, preferred_element_type=f32
                )
                dk = lax.dot_general(sg, q, over_rows, preferred_element_type=f32)
                dv = lax.dot_general(p.astype(bf16), g, over_rows, preferred_element_type=f32)
                both = jnp.concatenate([dk, dv], axis=1)
                key_sum = both if key_sum is None else key_sum + both
            totals[m, reach, base : base + 2 * HEAD_SIZE] += key_sum
        turned = turn(
            query_total[...], cosine[m, at, :], sine[m, at, :], second, all_turn, -1.0
        ).astype(bf16)

        @pl.when(is_first)
        def _():
            delta[m, at, :] = turned

        @pl.when(core != 0)
        def _():
            pass_on[m, at, :] = turned

    halos = [
        links.plan(
            halo_send.at[m], halo_recv.at[m], shift=-1, sends=z_at > 0,
            receives=z_at < n_tensor - 1,
        )
        for m in range(2)
    ]

    def back_tiles(m, first_tile, last_tile):
        for tile in range(first_tile, last_tile):
            back_tile(m, tile)

    def send_halo(m):
        halo_send[m] = totals[m, :WINDOW].astype(bf16)
        halos[m].start()

    def finish_block(m):
        halos[m].wait_recv()
        full = totals[m, WINDOW:]
        tail = full[rows - WINDOW :] + jnp.where(
            z_at < n_tensor - 1, halo_recv[m].astype(f32), 0.0
        )
        full = jnp.concatenate([full[: rows - WINDOW], tail], axis=0)
        turned = turn(full, cosine[m], sine[m], second, keys_turn, -1.0).astype(bf16)

        @pl.when(is_first)
        def _():
            pass_on[m] = turned

        @pl.when(core != 0)
        def _():
            delta[m] = turned

        return send(pass_on.at[m], delta.at[2 + m], bit=1)

    free = -(-WINDOW // TILE)
    totals[...] = jnp.zeros_like(totals)
    grad_swap.wait_recv()
    back_tiles(0, 0, free)
    down.relay(1)
    send_halo(0)
    for p in order[n_tensor // 2 : n_tensor - 1]:
        down.step(p)
    back_tiles(0, free, tiles)
    for p in order[n_tensor - 1 :]:
        down.step(p)
    up.issue(order)
    across.wait_recv()
    both = send(g_all.at[1], g_all.at[3], bit=1)
    to_across[...] = (to_core[1].astype(f32) + from_core[1].astype(f32)).astype(bf16)
    mlp_send = send(to_across, mlp_across, bit=2)
    hidden[...] += to_core[0].astype(f32) + from_core[0].astype(f32)
    attended_back(1)
    both.wait_recv()
    attended_back(3)
    grad_swap = send(att_grad.at[3], other_grad.at[1], bit=1)
    gate.step(order[0])

    def weight_grad(left, right, at):
        total = None
        for b in range(GROUP):
            term = lax.dot_general(
                left[b, :, at], right[b], over_rows, preferred_element_type=f32
            )
            total = term if total is None else total + term
        return total

    out_grad = weight_grad(att, g_all, slice(0, n_tensor * out_quarter)).astype(bf16)
    both.wait_send()
    links.sent.remove(both)
    out_part[...] = out_grad.reshape(n_tensor, out_quarter, width)
    grad_swap.wait_recv()
    back_tiles(1, 0, free)
    for i in range(2, n_tensor - 1):
        down.relay(i)
    send_halo(1)
    gate.step(order[1])
    back_tiles(1, free, tiles)
    for p in order[2 : n_tensor - 1]:
        gate.step(p)
    swap0 = finish_block(0)
    gate.relay(1)
    swap1 = finish_block(1)
    grad_loads = [
        move(hidden_grad.at[:, pl.ds(i * half, half)], totals.at[i, pl.ds(0, rows)])
        for i in range(2)
    ]
    down.finish()
    for p in order[n_tensor - 1 :]:
        gate.step(p)

    def project_back(b):
        units = qkv.shape[0] * quarter
        return jnp.dot(delta[b], qkv[...].reshape(units, width), preferred_element_type=f32)

    mlp_send.wait_recv()
    mlp_across[...] = (hidden[...] + mlp_across[...].astype(f32)).astype(bf16)
    save(mlp_across, block_out)
    mlp_send.wait_send()
    links.sent.remove(mlp_send)
    swap1.wait_recv()
    to_core[1] = project_back(3).astype(bf16)
    core_send1 = send(to_core.at[1], from_core.at[1], bit=1)
    hidden[...] = project_back(1)
    swap0.wait_recv()
    to_core[0] = project_back(2).astype(bf16)
    core_send0 = send(to_core.at[0], from_core.at[0], bit=1)
    core_send1.wait_recv()
    across_sends = []
    for i in range(tiles):
        at = pl.ds(i * TILE, TILE)
        to_across[at] = (hidden[at, :] + from_core[1, at, :].astype(f32)).astype(bf16)
        across_sends.append(send(to_across.at[at], from_across.at[at], bit=2))
    hidden[...] = project_back(0)
    core_send0.wait_recv()
    hidden[...] += from_core[0].astype(f32)
    up.step(order[0])
    attn_row = None
    for p in range(n_tensor):
        at = slice(p * quarter, (p + 1) * quarter)
        grad = weight_grad(delta, n1_all, at)
        row = jnp.sum(grad * qkv[p].astype(f32), axis=0, keepdims=True)
        attn_row = row if attn_row is None else attn_row + row
        qkv_part[p, :quarter, :] = grad.astype(bf16)
    ending = jnp.concatenate(
        [attn_row, mlp_row[...], jnp.zeros((extra - 2, width), f32)], axis=0
    ).astype(bf16)
    for p in range(n_tensor):
        qkv_part[p, quarter:, :] = ending
    qkv_collect.issue(order)
    out_collect.issue(order)
    token_load = move(tokens, n1_all.at[0])
    up.step(order[1])
    gain = jnp.concatenate([gains[i, 2:3, : width // n_dp] for i in range(n_dp)], axis=1)
    for i in range(tiles):
        at = pl.ds(i * TILE, TILE)
        across_sends[i].wait_recv()
        if i == 0:
            for copy in grad_loads + [token_load]:
                copy.wait()
        upstream = hidden[at, :] + from_across[at, :].astype(f32)
        features = n1_all[0, at, :].astype(f32)
        inverse = lax.rsqrt(jnp.mean(features * features, axis=1, keepdims=True) + EPS)
        scaled = gain * upstream
        mean = jnp.mean(scaled * features, axis=1, keepdims=True)
        change = inverse * scaled - features * (inverse * inverse * inverse) * mean
        n1_all[1, at, :half] = (totals[0, at, :] + change[:, :half]).astype(bf16)
        n1_all[1, at, half:] = (totals[1, at, :] + change[:, half:]).astype(bf16)
        if i == 0:
            for j in range(2, n_tensor - 1):
                gate.relay(j)
        if i == 1:
            for p in order[2 : n_tensor - 1]:
                up.step(p)
    save(n1_all.at[1], input_out)
    gate.finish()
    for p in order[n_tensor - 1 :]:
        up.step(p)
    up.relay(1)
    for p in order[:2]:
        qkv_collect.step(p)
    for i in range(2, n_tensor - 1):
        up.relay(i)
    for p in order[2 : n_tensor - 1]:
        qkv_collect.step(p)
    up.finish()
    for p in order[n_tensor - 1 :]:
        qkv_collect.step(p)
    qkv_collect.relay(1)
    for p in order[:2]:
        out_collect.step(p)
    for i in range(2, n_tensor - 1):
        qkv_collect.relay(i)
    for p in order[2:]:
        out_collect.step(p)
    out_collect.relay(1)
    qkv_collect.finish()
    for i in range(2, n_tensor - 1):
        out_collect.relay(i)
    out_collect.finish()
    for collect in (down, gate, up, out_collect, qkv_collect):
        collect.wait()
    links.finish()


def backward(
    n_dp, n_tensor, grad_own, hidden_grad, tokens, hidden1, mlp_part, normed1, queries, keyvals, logs, attended,
    cosine, sine, qkv_full, out_full, smalls, down_part, gate_part, up_part, down_got,
    mlp_row, fixed,
):
    f32, bf16 = jnp.float32, jnp.bfloat16
    rows, width = grad_own.shape
    half = width // 2
    chunk = width // n_dp
    units = queries.shape[2]
    vmem = pl.BlockSpec(memory_space=pltpu.VMEM)
    hbm = pl.BlockSpec(memory_space=pl.ANY)
    extra = 16
    quarters = [
        down_part.shape[1], gate_part.shape[1], up_part.shape[1], out_full.shape[1],
        qkv_full.shape[1] + extra,
    ]

    def shape(dims, dtype=bf16):
        return jax.ShapeDtypeStruct(tuple(dims), dtype)

    def finals(index):
        return shape((GROUP, quarters[index], chunk))

    outs = [
        shape((rows, width)), shape((rows, width)), finals(4), shape((GROUP * quarters[3], chunk)),
        shape((chunk, GROUP * quarters[1])), shape((chunk, GROUP * quarters[2])),
        shape((chunk, GROUP * quarters[0])),
    ]
    full = (GROUP, rows, width)
    scratch = [
        pltpu.VMEM(full, bf16),
        pltpu.VMEM(full, bf16),
        pltpu.VMEM(qkv_full.shape, bf16),
        pltpu.VMEM(out_full.shape, bf16),
        pltpu.VMEM(queries.shape, bf16),
        pltpu.VMEM(keyvals.shape, bf16),
        pltpu.VMEM(logs.shape, f32),
        pltpu.VMEM(attended.shape, bf16),
        pltpu.VMEM(cosine.shape, f32),
        pltpu.VMEM(sine.shape, f32),
        pltpu.VMEM(smalls.shape, f32),
        pltpu.VMEM((2, rows, 1), jnp.int32),
        pltpu.VMEM(attended.shape, bf16),
        pltpu.VMEM((2,) + attended.shape[1:], bf16),
        pltpu.VMEM((2, rows + WINDOW, units), f32),
        pltpu.VMEM((TILE, units), f32),
        pltpu.VMEM((2, rows, units), bf16),
        pltpu.VMEM((GROUP, rows, units), bf16),
        pltpu.VMEM((2, WINDOW, units), bf16),
        pltpu.VMEM((2, WINDOW, units), bf16),
        pltpu.VMEM((2, rows, width), bf16),
        pltpu.VMEM((2, rows, width), bf16),
        pltpu.VMEM((rows, width), bf16),
        pltpu.VMEM((rows, width), bf16),
        pltpu.VMEM((rows, width), bf16),
        pltpu.VMEM((rows, width), f32),
        pltpu.VMEM((n_tensor, quarters[0], half), bf16),
        pltpu.VMEM((n_tensor, quarters[1], half), bf16),
    ]
    scratch += [pltpu.VMEM((n_tensor, q, half), bf16) for q in quarters]
    scratch += [pltpu.VMEM((n_tensor, q, half), bf16) for q in quarters]
    scratch += [pltpu.VMEM((q, half), bf16) for q in quarters]
    scratch += [
        pltpu.VMEM((GROUP, chunk, q) if turned else (GROUP, q, chunk), bf16)
        for q, turned in zip(quarters, (True, True, True, False, False))
    ]
    scratch += [
        pltpu.SemaphoreType.DMA((160,)),
        pltpu.SemaphoreType.DMA((160,)),
        pltpu.SemaphoreType.DMA((40,)),
    ]
    return pl.pallas_call(
        functools.partial(kernel_backward, n_dp, n_tensor),
        in_specs=[hbm] * 19 + [vmem] * 2,
        out_specs=[hbm] * len(outs),
        out_shape=outs,
        scratch_shapes=scratch,
        compiler_params=pltpu.CompilerParams(
            collective_id=1, has_side_effects=True, vmem_limit_bytes=67043328
        ),
        name="backward",
    )(
        grad_own, hidden_grad, tokens, hidden1, mlp_part, normed1, queries, keyvals, logs, attended, cosine, sine,
        qkv_full, out_full, smalls, down_part, gate_part, up_part, down_got, mlp_row, fixed,
    )


def fast_local(
    n_dp,
    n_tensor,
    block_in,
    cotangent,
    segment_ids,
    attn_gain,
    qkv_weight,
    out_weight,
    mlp_gain,
    gate_weight,
    up_weight,
    down_weight,
):
    bf16, f32 = jnp.bfloat16, jnp.float32
    rows, width = block_in.shape
    part = attn_gain.shape[0]
    (
        normed1, normed2, hidden1, queries, keyvals, log_total, attended, cosine, sine, qkv_full,
        out_full, smalls, grad_rows, gate_full, up_full, down_full,
    ), fixed = forward(
        n_dp, n_tensor, block_in, cotangent, segment_ids, jnp.stack([attn_gain, mlp_gain]),
        qkv_weight, out_weight, gate_weight, up_weight, down_weight,
    )
    (
        hidden1_grad, grad_own, mlp_part, down_part, gate_part, up_part, down_got, mlp_row,
    ) = feed(n_dp, n_tensor, normed2, grad_rows, hidden1, gate_full, up_full, down_full, smalls)
    input_grad, block_out, qkv_blocks, out_grad, gate_grad, up_grad, down_grad = backward(
        n_dp, n_tensor, grad_own, hidden1_grad, block_in, hidden1, mlp_part, normed1, queries,
        keyvals, log_total, attended, cosine, sine, qkv_full, out_full, smalls, down_part, gate_part, up_part, down_got, mlp_row,
        fixed,
    )
    quarter = qkv_full.shape[1]

    def row_of(index, gain):
        return jnp.sum(qkv_blocks[:, quarter + index].astype(f32), axis=0) / gain.astype(f32)

    blocks = qkv_blocks[:, :quarter]
    qkv_grad = blocks.reshape(-1, blocks.shape[2]).T.astype(f32)
    gains = [row_of(0, attn_gain), row_of(1, mlp_gain)]
    return (
        block_out,
        input_grad,
        gains[0],
        qkv_grad,
        out_grad.astype(f32),
        gains[1],
        gate_grad.astype(f32),
        up_grad.astype(f32),
        down_grad.T.astype(f32),
    )


def solution(mesh):
    in_specs = (
        P(("dp", "tensor"), None),
        P(("dp", "tensor"), None),
        P("dp", None),
        P("dp"),
        P("dp", "tensor"),
        P("tensor", "dp"),
        P("dp"),
        P("dp", "tensor"),
        P("dp", "tensor"),
        P("tensor", "dp"),
    )
    out_specs = (
        P(("dp", "tensor"), None),
        P(("dp", "tensor"), None),
        P("dp"),
        P("dp", "tensor"),
        P("tensor", "dp"),
        P("dp"),
        P("dp", "tensor"),
        P("dp", "tensor"),
        P("tensor", "dp"),
    )
    n_dp, n_tensor = mesh.shape["dp"], mesh.shape["tensor"]

    def body(*arrays):
        rows = arrays[0].shape[0]
        groups = arrays[4].shape[1] // (4 * HEAD_SIZE)
        if n_dp == 2 * GROUP and groups == 2 and rows >= WINDOW and rows % TILE == 0:
            return fast_local(n_dp, n_tensor, *arrays)
        return local(*arrays)

    return jax.shard_map(body, mesh=mesh, in_specs=in_specs, out_specs=out_specs, check_vma=False)
```

```python
import functools

import jax
import jax.numpy as jnp
import numpy as np
from jax import lax
from jax.experimental import pallas as pl
from jax.experimental.pallas import tpu as pltpu
from jax.sharding import PartitionSpec as P

QUERY_HEADS = 16
KEY_VALUE_HEADS = 8
HEAD_SIZE = 96


EPS = 1e-05
ROPE_BASE = 100000.0
NEG_FILL = -1e30


def doc_positions(segments):
    length = segments.shape[1]
    position_index = jnp.broadcast_to(jnp.arange(length, dtype=jnp.int32)[None, :], segments.shape)
    change = jnp.concatenate(
        [jnp.ones((segments.shape[0], 1), dtype=bool), segments[:, 1:] != segments[:, :-1]], axis=1
    )
    starts = lax.cummax(jnp.where(change, position_index, jnp.zeros_like(position_index)), axis=1)
    return position_index - starts


def rotary_tables(segments):
    half_dim = HEAD_SIZE // 2
    frequency = jnp.power(ROPE_BASE, -(2.0 * jnp.arange(half_dim, dtype=jnp.float32)) / HEAD_SIZE)
    angles = doc_positions(segments).astype(jnp.float32)[..., None] * frequency
    cosine_table = jnp.concatenate([jnp.cos(angles), jnp.cos(angles)], axis=-1)
    sine_table = jnp.concatenate([jnp.sin(angles), jnp.sin(angles)], axis=-1)
    return (cosine_table, sine_table)


def rotate(vector, cosine_table, sine_table):
    half_dim = vector.shape[-1] // 2
    turned = jnp.concatenate([-vector[..., half_dim:], vector[..., :half_dim]], axis=-1)
    return vector * cosine_table + turned * sine_table


def unrotate(vector, cosine_table, sine_table):
    half_dim = vector.shape[-1] // 2
    shifted = vector * sine_table
    returned = jnp.concatenate([shifted[..., half_dim:], -shifted[..., :half_dim]], axis=-1)
    return vector * cosine_table + returned


def allowed_pairs(segments):
    length = segments.shape[1]
    offsets = jnp.arange(length)
    causal = offsets[None, :] <= offsets[:, None]
    same_doc = segments[:, :, None] == segments[:, None, :]
    return (causal[None] & same_doc)[:, None, None]


def score_block(queries, key_heads, segments):
    scores = jnp.einsum(
        "sqgrd,skgd->sgrqk", queries, key_heads, preferred_element_type=jnp.float32
    ) * HEAD_SIZE ** (-0.5)
    return jnp.where(allowed_pairs(segments), scores, NEG_FILL)


def rms_scale(features):
    return lax.rsqrt(jnp.mean(features * features, axis=-1, keepdims=True) + EPS)


def norm_back(features, inverse, gain_vector, upstream):
    scaled = gain_vector * upstream
    return inverse * scaled - features * (inverse * inverse * inverse) * jnp.mean(
        scaled * features, axis=-1, keepdims=True
    )


def widen(shard_rows):
    return lax.all_gather(shard_rows, "tensor", axis=0, tiled=True)


def narrow(partial_value):
    return lax.psum_scatter(
        partial_value.astype(jnp.bfloat16), "tensor", scatter_dimension=0, tiled=True
    ).astype(jnp.float32)


def local(
    block_in,
    cotangent,
    segment_ids,
    attn_gain,
    qkv_weight,
    out_weight,
    mlp_gain,
    gate_weight,
    up_weight,
    down_weight,
):
    qkv_full, gate_full, up_full, gain_attn_raw, gain_mlp_raw = (
        lax.all_gather(qkv_weight, "dp", axis=0, tiled=True),
        lax.all_gather(gate_weight, "dp", axis=0, tiled=True),
        lax.all_gather(up_weight, "dp", axis=0, tiled=True),
        lax.all_gather(attn_gain, "dp", axis=0, tiled=True),
        lax.all_gather(mlp_gain, "dp", axis=0, tiled=True),
    )
    out_cols, down_cols = (
        lax.all_gather(out_weight, "dp", axis=1, tiled=True),
        lax.all_gather(down_weight, "dp", axis=1, tiled=True),
    )
    seq_count, length = segment_ids.shape
    repeat_factor = QUERY_HEADS // KEY_VALUE_HEADS
    groups = qkv_full.shape[1] // ((repeat_factor + 2) * HEAD_SIZE)
    gain_attn = gain_attn_raw.astype(jnp.float32)
    gain_mlp = gain_mlp_raw.astype(jnp.float32)
    residual = block_in.astype(jnp.float32)
    scale_attn = rms_scale(residual)
    normed1 = widen((residual * scale_attn * gain_attn).astype(jnp.bfloat16))
    projected = jnp.dot(normed1, qkv_full, preferred_element_type=jnp.float32).reshape(
        seq_count, length, groups, repeat_factor + 2, HEAD_SIZE
    )
    cosine_table, sine_table = rotary_tables(segment_ids)
    cos_query = cosine_table[:, :, None, None, :]
    sin_query = sine_table[:, :, None, None, :]
    cos_key = cosine_table[:, :, None, :]
    sin_key = sine_table[:, :, None, :]
    queries = rotate(projected[:, :, :, :repeat_factor], cos_query, sin_query).astype(jnp.bfloat16)
    key_heads = rotate(projected[:, :, :, repeat_factor], cos_key, sin_key).astype(jnp.bfloat16)
    values = projected[:, :, :, repeat_factor + 1].astype(jnp.bfloat16)
    scores = score_block(queries, key_heads, segment_ids)
    highest = jnp.max(scores, axis=-1, keepdims=True)
    log_total = highest + jnp.log(jnp.sum(jnp.exp(scores - highest), axis=-1, keepdims=True))
    probability = jnp.exp(scores - log_total).astype(jnp.bfloat16)
    attended = jnp.einsum(
        "sgrqk,skgd->sqgrd", probability, values, preferred_element_type=jnp.float32
    ).astype(jnp.bfloat16)
    attn_flat = attended.reshape(seq_count * length, groups * repeat_factor * HEAD_SIZE)
    attn_delta = lax.psum_scatter(
        jnp.dot(attn_flat, out_cols, preferred_element_type=jnp.float32).astype(jnp.bfloat16),
        "tensor",
        scatter_dimension=0,
        tiled=True,
    ).astype(jnp.float32)
    hidden1 = residual + attn_delta
    scale_mlp = rms_scale(hidden1)
    normed2 = widen((hidden1 * scale_mlp * gain_mlp).astype(jnp.bfloat16))
    gate = jnp.dot(normed2, gate_full, preferred_element_type=jnp.float32)
    up_value = jnp.dot(normed2, up_full, preferred_element_type=jnp.float32)
    sigmoid_gate = jax.nn.sigmoid(gate)
    activated = (gate * sigmoid_gate * up_value).astype(jnp.bfloat16)
    mlp_delta = narrow(jnp.dot(activated, down_cols, preferred_element_type=jnp.float32))
    block_out = (hidden1 + mlp_delta).astype(jnp.bfloat16)
    grad_rows = widen(cotangent)
    down_part = jnp.einsum("tf,td->fd", activated, grad_rows, preferred_element_type=jnp.float32)
    act_grad = jnp.einsum("td,fd->tf", grad_rows, down_cols, preferred_element_type=jnp.float32)
    gate_delta = (act_grad * up_value * sigmoid_gate * (1.0 + gate * (1.0 - sigmoid_gate))).astype(
        jnp.bfloat16
    )
    up_delta = (act_grad * gate * sigmoid_gate).astype(jnp.bfloat16)
    gate_part = jnp.einsum("td,tf->df", normed2, gate_delta, preferred_element_type=jnp.float32)
    up_part = jnp.einsum("td,tf->df", normed2, up_delta, preferred_element_type=jnp.float32)
    normed2_term = jnp.einsum(
        "tf,df->td", gate_delta, gate_full, preferred_element_type=jnp.float32
    ) + jnp.einsum("tf,df->td", up_delta, up_full, preferred_element_type=jnp.float32)
    normed2_grad = narrow(normed2_term)
    mlp_gain_part = jnp.sum(normed2_grad * hidden1 * scale_mlp, axis=0)
    hidden1_grad = cotangent.astype(jnp.float32) + norm_back(
        hidden1, scale_mlp, gain_mlp, normed2_grad
    )
    hidden1_rounded = hidden1_grad.astype(jnp.bfloat16)
    grad_full = lax.all_gather(hidden1_rounded, "tensor", axis=0, tiled=True)
    attended_grad = jnp.einsum(
        "td,hd->th", grad_full, out_cols, preferred_element_type=jnp.float32
    ).astype(jnp.bfloat16)
    out_part = jnp.einsum("th,td->hd", attn_flat, grad_full, preferred_element_type=jnp.float32)
    attended_grad = attended_grad.reshape(seq_count, length, groups, repeat_factor, HEAD_SIZE)
    prob_full = jnp.exp(score_block(queries, key_heads, segment_ids) - log_total)
    prob_grad = jnp.einsum(
        "sqgrd,skgd->sgrqk", attended_grad, values, preferred_element_type=jnp.float32
    )
    inner_sum = jnp.sum(prob_full * prob_grad, axis=-1, keepdims=True)
    score_grad = (prob_full * (prob_grad - inner_sum) * HEAD_SIZE ** (-0.5)).astype(jnp.bfloat16)
    query_grad = jnp.einsum(
        "sgrqk,skgd->sqgrd", score_grad, key_heads, preferred_element_type=jnp.float32
    )
    key_grad = jnp.einsum(
        "sgrqk,sqgrd->skgd", score_grad, queries, preferred_element_type=jnp.float32
    )
    value_grad = jnp.einsum(
        "sgrqk,sqgrd->skgd",
        prob_full.astype(jnp.bfloat16),
        attended_grad,
        preferred_element_type=jnp.float32,
    )
    projected_grad = jnp.concatenate(
        [
            unrotate(query_grad, cos_query, sin_query),
            unrotate(key_grad, cos_key, sin_key)[:, :, :, None],
            value_grad[:, :, :, None],
        ],
        axis=3,
    )
    projected_grad = projected_grad.astype(jnp.bfloat16).reshape(
        seq_count * length, groups * (repeat_factor + 2) * HEAD_SIZE
    )
    qkv_part = jnp.einsum("td,tc->dc", normed1, projected_grad, preferred_element_type=jnp.float32)
    normed1_grad = narrow(
        jnp.einsum("tc,dc->td", projected_grad, qkv_full, preferred_element_type=jnp.float32)
    )
    attn_gain_part = jnp.sum(normed1_grad * residual * scale_attn, axis=0)
    input_grad = (hidden1_grad + norm_back(residual, scale_attn, gain_attn, normed1_grad)).astype(
        jnp.bfloat16
    )
    attn_gain_total, mlp_gain_total = lax.psum((attn_gain_part, mlp_gain_part), "tensor")
    attn_gain_grad, qkv_grad, gate_grad, up_grad, mlp_gain_grad = (
        lax.psum_scatter(
            attn_gain_total.astype(jnp.bfloat16), "dp", scatter_dimension=0, tiled=True
        ).astype(jnp.float32),
        lax.psum_scatter(
            qkv_part.astype(jnp.bfloat16), "dp", scatter_dimension=0, tiled=True
        ).astype(jnp.float32),
        lax.psum_scatter(
            gate_part.astype(jnp.bfloat16), "dp", scatter_dimension=0, tiled=True
        ).astype(jnp.float32),
        lax.psum_scatter(
            up_part.astype(jnp.bfloat16), "dp", scatter_dimension=0, tiled=True
        ).astype(jnp.float32),
        lax.psum_scatter(
            mlp_gain_total.astype(jnp.bfloat16), "dp", scatter_dimension=0, tiled=True
        ).astype(jnp.float32),
    )
    out_grad, down_grad = (
        lax.psum_scatter(
            out_part.astype(jnp.bfloat16), "dp", scatter_dimension=1, tiled=True
        ).astype(jnp.float32),
        lax.psum_scatter(
            down_part.astype(jnp.bfloat16), "dp", scatter_dimension=1, tiled=True
        ).astype(jnp.float32),
    )
    return (
        block_out,
        input_grad,
        attn_gain_grad,
        qkv_grad,
        out_grad,
        mlp_gain_grad,
        gate_grad,
        up_grad,
        down_grad,
    )


GROUP = 4
WINDOW = 256
LANES = 384
TILE = 128


MESH = pl.DeviceIdType.MESH


class Transfer:
    def __init__(self, copy, sends=None, receives=None):
        self.copy, self.sends, self.receives = copy, sends, receives

    def _when(self, condition, action):
        if condition is None:
            action()
        else:
            pl.when(condition)(action)

    def start(self):
        self._when(self.sends, self.copy.start)
        return self

    def wait_recv(self):
        self._when(self.receives, self.copy.wait_recv)

    def wait_send(self):
        self._when(self.sends, self.copy.wait_send)


class Links:
    def __init__(self, n_dp, n_tensor, out_sems, in_sems, local_sems):
        self.n_dp, self.n_tensor = n_dp, n_tensor
        self.out_sems, self.in_sems, self.local_sems = out_sems, in_sems, local_sems
        self.d_at, self.z_at = lax.axis_index("dp"), lax.axis_index("tensor")
        self.used, self.used_local = 0, 0
        self.sent, self.saved = [], []

    def barrier(self):
        barrier = pltpu.get_barrier_semaphore()
        for k in range(1, self.n_dp):
            pl.semaphore_signal(
                barrier,
                inc=1,
                device_id={"dp": self.d_at ^ k, "tensor": self.z_at},
                device_id_type=MESH,
            )
        for s in range(1, self.n_tensor):
            pl.semaphore_signal(
                barrier,
                inc=1,
                device_id={"dp": self.d_at, "tensor": lax.rem(self.z_at + s, self.n_tensor)},
                device_id_type=MESH,
            )
        pl.semaphore_wait(barrier, self.n_dp - 1 + self.n_tensor - 1)

    def plan(self, source, target, bit=0, shift=0, sends=None, receives=None):
        slot = self.used
        self.used += 1
        copy = pltpu.make_async_remote_copy(
            src_ref=source,
            dst_ref=target,
            send_sem=self.out_sems.at[slot],
            recv_sem=self.in_sems.at[slot],
            device_id={
                "dp": self.d_at ^ bit,
                "tensor": lax.rem(self.z_at + self.n_tensor + shift, self.n_tensor),
            },
            device_id_type=MESH,
        )
        transfer = Transfer(copy, sends, receives)
        self.sent.append(transfer)
        return transfer

    def send(self, source, target, bit=0, shift=0):
        return self.plan(source, target, bit, shift).start()

    def move(self, source, target):
        copy = pltpu.make_async_copy(source, target, self.local_sems.at[self.used_local])
        self.used_local += 1
        copy.start()
        return copy

    def save(self, source, target):
        self.saved.append(self.move(source, target))

    def finish(self):
        for transfer in self.sent:
            transfer.wait_send()
        for copy in self.saved:
            copy.wait()


class Spread:
    def __init__(self, links, own_piece, target, columns):
        self.links, self.own_piece, self.target, self.columns = links, own_piece, target, columns
        self.ahead, self.back, self.swaps = [], [], []

    def _slot(self, index):
        n = self.links.n_tensor
        return self.target.at[lax.rem(index + n, n), :, self.columns]

    def issue(self):
        links, n, z = self.links, self.links.n_tensor, self.links.z_at
        own = self._slot(z)
        for s in range(1, n):
            up_from, down_from = z - (s - 1), z + (s - 1)
            up_source = self.own_piece if s == 1 else self._slot(up_from)
            down_source = self.own_piece if s == 1 else self._slot(down_from)
            self.ahead.append(
                links.plan(
                    up_source, self._slot(up_from), shift=1,
                    sends=(z < n - 1) & (up_from >= 0), receives=z >= s,
                )
            )
            self.back.append(
                links.plan(
                    down_source, self._slot(down_from), shift=-1,
                    sends=(z > 0) & (down_from < n), receives=z + s < n,
                )
            )
        self.ahead[0].start()
        self.back[0].start()
        self.swaps.append(links.plan(self.own_piece, own, bit=GROUP).start())

    def step(self, s):
        links, n, z = self.links, self.links.n_tensor, self.links.z_at
        for arrivals, piece, here in (
            (self.ahead, z - s, z >= s),
            (self.back, z + s, z + s < n),
        ):
            arrivals[s - 1].wait_recv()
            if s < n - 1:
                arrivals[s].start()
            slot = self._slot(piece)
            self.swaps.append(
                links.plan(slot, slot, bit=GROUP, sends=here, receives=here).start()
            )

    def wait(self):
        for swap in self.swaps:
            swap.wait_recv()


def kernel_forward(
    n_dp, n_tensor,
    tokens, cot, gate_w, up_w, down_w, out_w, qkv_w, segments, gain1, gain2, fixed,
    normed1_out, normed2_out, hidden_out, query_out, keyval_out, log_out, att_out,
    cos_out, sin_out, qkv_out, out_out, small_out, cot_out, gate_out, up_out, down_out,
    x_all, n1_all, first, dealt, first_piece, qkv, out_parcel, obuf, gbuf, ubuf, dbuf, piece, outw,
    small, small_all, stream, parts, recv, queries, keyvals,
    att, by_repeat, logs, cosine, sine, low_col, to_core, from_core, to_across, from_across,
    hidden, n2_all, stage, out_sems, in_sems, local_sems,
):
    f32, bf16 = jnp.float32, jnp.bfloat16
    links = Links(n_dp, n_tensor, out_sems, in_sems, local_sems)
    send, move, save = links.send, links.move, links.save
    d_at, z_at = links.d_at, links.z_at
    member = d_at % GROUP
    core = d_at % 2
    upper = d_at // GROUP
    rows, width = tokens.shape
    half = width // 2
    chunk = qkv_w.shape[0]
    contract = (((1,), (1,)), ((), ()))
    columns = pl.ds(pl.multiple_of(upper * half, half), half)

    turned = qkv_w[...].T
    quarter = turned.shape[0] // GROUP
    for i in range(GROUP):
        first[i] = turned[i * quarter : (i + 1) * quarter]
    turned = out_w[...].T
    out_quarter = turned.shape[0] // GROUP
    for i in range(GROUP):
        out_parcel[i] = turned[i * out_quarter : (i + 1) * out_quarter]
    ids = segments[...]
    seqs, length = ids.shape
    begin = jnp.zeros_like(ids)
    for value in range(3):
        count = jnp.sum((ids == value).astype(jnp.int32), axis=1, keepdims=True)
        begin = begin + jnp.where(ids > value, count, 0)
    begin = begin.astype(f32)
    for i in range(seqs):
        stream[:, i * length : (i + 1) * length] = jnp.broadcast_to(
            begin[i : i + 1] + float(i * length), (stream.shape[0], length)
        )
    window = stream[:, pl.ds(pl.multiple_of(z_at * rows, TILE), rows)]
    here = lax.broadcasted_iota(jnp.int32, window.shape, 1) + z_at * rows
    small[...] = window
    small[0:1] = here.astype(f32)[0:1] - window[0:1]
    small[2:3, :chunk] = gain1[...].astype(f32)
    small[3:4, :chunk] = gain2[...].astype(f32)

    @pl.when(z_at == 0)
    def _():
        keyvals[:, :WINDOW, :] = jnp.zeros_like(keyvals[:, :WINDOW, :])

    links.barrier()

    deals = [send(first.at[member ^ k], dealt.at[member], bit=k) for k in range(1, GROUP)]
    beside = send(tokens, x_all.at[2], bit=1)
    smalls = [send(small, small_all.at[d_at], bit=k) for k in range(1, n_dp)]
    def columns_of(ref, at):
        size = ref.shape[1] // GROUP
        return ref.at[:, pl.ds(pl.multiple_of(at * size, TILE), size)]

    def parcel_of(ref, at):
        return ref.at[at]

    pairs = [
        (out_parcel, obuf, parcel_of), (gate_w, gbuf, columns_of), (up_w, ubuf, columns_of),
        (down_w, dbuf, columns_of),
    ]

    def deal(group):
        return [
            send(take(ref, member ^ k), buffer.at[member], bit=k)
            for ref, buffer, take in group
            for k in range(1, GROUP)
        ]

    rests = deal(pairs[:2])
    across = send(tokens, x_all.at[1], bit=2)
    late_rests = deal(pairs[2:])
    own = [move(tokens, x_all.at[0])]
    for ref, buffer, take in pairs:
        own.append(move(take(ref, member), buffer.at[member]))
    cot_stage = move(cot, stage)
    small_all[d_at] = small[...]
    dealt[member] = first[member]

    entries = lax.broadcasted_iota(jnp.int32, (WINDOW, LANES), 0).astype(f32)
    angles = entries * fixed[0:1]

    def split(table):
        pieces = []
        for _ in range(3):
            pieces.append(table.astype(bf16))
            table = table - pieces[-1].astype(f32)
        return pieces

    cos_parts, sin_parts = split(jnp.cos(angles)), split(jnp.sin(angles))
    second = fixed[1:2]
    own_turns = jnp.where(core == 0, jnp.ones_like(second), fixed[2:3])

    for copy in deals:
        copy.wait_recv()
    for i in range(GROUP):
        first_piece[:, i * chunk : (i + 1) * chunk] = dealt[i]
    spread_first = Spread(links, first_piece, qkv, columns)
    spread_first.issue()
    save(first_piece, qkv.at[z_at, :, columns])
    own_qkv = links.saved.pop()
    for copy in own:
        copy.wait()
    cot_stage.wait()
    save(stage, cot_out.at[0])
    spread_first.step(1)
    for copy in smalls:
        copy.wait_recv()
    spread_first.step(2)
    gains = []
    for row in (2, 3):
        gains.append(
            jnp.concatenate([small_all[i, row : row + 1, :chunk] for i in range(n_dp)], axis=1)
        )
    for copy in rests:
        copy.wait_recv()
    sizes = [obuf.shape[1], gbuf.shape[2], ubuf.shape[2], dbuf.shape[2]]
    starts = [sum(sizes[:i]) for i in range(len(sizes))]
    saves = []

    def prepare(index, target, buffer):
        at = slice(starts[index], starts[index] + sizes[index])
        for i in range(GROUP):
            piece[at, i * chunk : (i + 1) * chunk] = buffer[i] if index == 0 else buffer[i].T
        own_piece = piece.at[pl.ds(starts[index], sizes[index])]
        saves.append(move(own_piece, target.at[z_at, :, columns]))
        return Spread(links, own_piece, target, columns)

    out_spread = prepare(0, outw, obuf)
    gate_spread = prepare(1, gate_out, gbuf)
    out_spread.issue()
    spread_first.step(3)
    gate_spread.issue()
    beside.wait_recv()
    own_qkv.wait()
    spread_first.wait()

    def project_block(m, k):
        features = x_all[m].astype(f32)
        scale = lax.rsqrt(jnp.mean(features * features, axis=1, keepdims=True) + EPS)
        normal = (features * scale * gains[0]).astype(bf16)
        n1_all[m] = normal
        units = qkv.shape[0] * qkv.shape[1]
        product = lax.dot_general(
            normal, qkv[...].reshape(units, width), contract, preferred_element_type=f32
        )
        info = small_all[d_at ^ k].T
        key = lax.broadcasted_iota(jnp.int32, (rows, WINDOW), 1)
        chosen = (info[:, 0:1].astype(jnp.int32) == key).astype(bf16)

        def pick(table):
            total = jnp.dot(chosen, table[0], preferred_element_type=f32)
            for part in table[1:]:
                total += jnp.dot(chosen, part, preferred_element_type=f32)
            return total

        cos_here, sin_here = pick(cos_parts), pick(sin_parts)
        parts[m] = turn(product, cos_here, sin_here, second, own_turns, 1.0).astype(bf16)
        if m < 2:
            cosine[m] = cos_here
            sine[m] = sin_here
            low_col[m] = info[:, 1:2].astype(jnp.int32) - z_at * rows + WINDOW

    is_first = core == 0
    halos = [
        links.plan(
            keyvals.at[m, pl.ds(rows, WINDOW)], keyvals.at[m, pl.ds(0, WINDOW)], shift=1,
            sends=z_at < n_tensor - 1, receives=z_at > 0,
        )
        for m in range(2)
    ]

    def take_block(m, swap):
        swap.wait_recv()
        mine, other = parts[m], recv[m]
        queries[m] = jnp.where(is_first, mine, other)
        keyvals[m, WINDOW:, :] = jnp.where(is_first, other, mine)
        halos[m].start()

    project_block(2, 1)
    part_swap = send(parts.at[2], recv.at[0], bit=1)
    project_block(0, 0)
    take_block(0, part_swap)
    out_spread.step(1)
    across.wait_recv()
    both = send(x_all.at[1], x_all.at[3], bit=1)
    cot_across = send(cot, cot_out.at[1], bit=2)
    cot_beside = send(cot, cot_out.at[2], bit=1)
    project_block(1, 2)
    both.wait_recv()
    project_block(3, 3)
    part_swap = send(parts.at[3], recv.at[1], bit=1)
    save(n1_all, normed1_out)
    save(cosine, cos_out)
    save(sine, sin_out)
    take_block(1, part_swap)
    out_spread.step(2)
    gate_spread.step(1)
    for copy in late_rests:
        copy.wait_recv()
    up_spread = prepare(2, up_out, ubuf)
    down_spread = prepare(3, down_out, dbuf)
    save(queries, query_out)
    heads = queries.shape[2] // HEAD_SIZE
    repeat = QUERY_HEADS // KEY_VALUE_HEADS
    span = TILE + WINDOW

    def attend_tile(m, start):
        key = lax.broadcasted_iota(jnp.int32, (TILE, span), 1)
        query = lax.broadcasted_iota(jnp.int32, (TILE, span), 0)
        lowest = low_col[m, pl.ds(start, TILE), :] - start
        allowed = (key >= lowest) & (key <= query + WINDOW)
        for head in range(heads):
            group, r = head // repeat, head % repeat
            base = group * 2 * HEAD_SIZE
            q = queries[m, pl.ds(start, TILE), head * HEAD_SIZE : (head + 1) * HEAD_SIZE]
            k = keyvals[m, pl.ds(start, span), base : base + HEAD_SIZE]
            v = keyvals[m, pl.ds(start, span), base + HEAD_SIZE : base + 2 * HEAD_SIZE]
            s = lax.dot_general(q, k, contract, preferred_element_type=f32) * HEAD_SIZE ** (-0.5)
            s = jnp.where(allowed, s, NEG_FILL)
            highest = jnp.max(s, axis=1, keepdims=True)
            e = jnp.exp(s - highest)
            whole = jnp.sum(e, axis=1, keepdims=True)
            p = (e * (1.0 / whole)).astype(bf16)
            o = jnp.dot(p, v, preferred_element_type=f32).astype(bf16)
            logs[m, pl.ds(start, TILE), head : head + 1] = highest + jnp.log(whole)
            by_repeat[r, m, pl.ds(start, TILE), group * HEAD_SIZE : (group + 1) * HEAD_SIZE] = o

    tiles = rows // TILE
    free = -(-WINDOW // TILE)

    def attend_tiles(blocks, first_tile, last_tile):
        for m in blocks:
            for tile in range(first_tile, last_tile):
                attend_tile(m, tile * TILE)

    attend_tiles((1, 0), free, tiles)
    out_spread.step(3)
    up_spread.issue()
    halos[0].wait_recv()
    halos[1].wait_recv()
    attend_tiles((1,), 0, free)
    att_swap1 = send(by_repeat.at[1 - core, 1], att.at[3], bit=1)
    gate_spread.step(2)
    attend_tiles((0,), 0, free)
    att_swap0 = send(by_repeat.at[1 - core, 0], att.at[2], bit=1)
    save(keyvals, keyval_out)
    save(logs, log_out)
    att[0] = by_repeat[core, 0]
    att[1] = by_repeat[core, 1]
    down_spread.issue()
    cot_across.wait_recv()
    cot_both = send(cot_out.at[1], cot_out.at[3], bit=1)

    saves[0].wait()
    out_spread.wait()

    def project_out(b):
        units = outw.shape[0] * outw.shape[1]
        return jnp.dot(att[b], outw[...].reshape(units, width), preferred_element_type=f32)

    att_swap1.wait_recv()
    to_core[1] = project_out(3).astype(bf16)
    core_send1 = send(to_core.at[1], from_core.at[1], bit=1)
    hidden[...] = project_out(1)
    att_swap0.wait_recv()
    to_core[0] = project_out(2).astype(bf16)
    core_send0 = send(to_core.at[0], from_core.at[0], bit=1)
    core_send1.wait_recv()
    across_sends = []
    for i in range(tiles):
        at = pl.ds(i * TILE, TILE)
        to_across[at] = (hidden[at, :] + from_core[1, at, :].astype(f32)).astype(bf16)
        across_sends.append(send(to_across.at[at], from_across.at[at], bit=2))
    hidden[...] = project_out(0) + x_all[0].astype(f32)
    core_send0.wait_recv()
    hidden[...] += from_core[0].astype(f32)
    save(att, att_out)
    gate_spread.step(3)
    up_spread.step(1)
    steps = [
        (up_spread, 2), (up_spread, 3), (down_spread, 1), (down_spread, 2), (down_spread, 3),
    ]
    last = []
    for i in range(tiles):
        at = pl.ds(i * TILE, TILE)
        across_sends[i].wait_recv()
        value = hidden[at, :] + from_across[at, :].astype(f32)
        hidden[at, :] = value
        scale = lax.rsqrt(jnp.mean(value * value, axis=1, keepdims=True) + EPS)
        n2_all[0, at, :] = (value * scale * gains[1]).astype(bf16)
        last.append(send(n2_all.at[0, at], n2_all.at[1, at], bit=2))
        last.append(send(n2_all.at[0, at], n2_all.at[2, at], bit=1))
        if i < 3:
            spread, s = steps.pop(0)
            spread.step(s)
    save(hidden, hidden_out)
    save(qkv, qkv_out)
    save(outw, out_out)
    save(small_all, small_out)
    ends = []
    for i in range(tiles):
        at = pl.ds(i * TILE, TILE)
        last[2 * i].wait_recv()
        ends.append(send(n2_all.at[1, at], n2_all.at[3, at], bit=1))
        if i < 2:
            spread, s = steps.pop(0)
            spread.step(s)
    for copy in ends + last[1::2]:
        copy.wait_recv()
    save(n2_all, normed2_out)
    for copy in saves[1:]:
        copy.wait()
    for spread in (gate_spread, up_spread, down_spread):
        spread.wait()
    for copy in (cot_beside, cot_both):
        copy.wait_recv()
    links.finish()


def forward(
    n_dp, n_tensor, tokens, cot, segments, gain1, gain2, qkv_w, out_w, gate_w, up_w, down_w
):
    out_w, down_w = out_w.T, down_w.T
    rows, width = tokens.shape
    f32, bf16 = jnp.float32, jnp.bfloat16
    vmem = pl.BlockSpec(memory_space=pltpu.VMEM)
    hbm = pl.BlockSpec(memory_space=pl.ANY)
    chunk = qkv_w.shape[0]
    quarter = qkv_w.shape[1] // GROUP
    sizes = [
        out_w.shape[1] // GROUP, gate_w.shape[1] // GROUP, up_w.shape[1] // GROUP,
        down_w.shape[1] // GROUP,
    ]
    units = quarter * n_tensor
    heads = units // HEAD_SIZE
    lane = np.arange(LANES)
    within = lane % HEAD_SIZE
    fixed = np.zeros((8, LANES), np.float32)
    fixed[0] = np.power(ROPE_BASE, -(2.0 * (within % (HEAD_SIZE // 2))) / HEAD_SIZE)
    fixed[1] = within >= HEAD_SIZE // 2
    fixed[2] = lane % (2 * HEAD_SIZE) < HEAD_SIZE
    fixed[3] = 1.0

    def shape(dims, dtype=bf16):
        return jax.ShapeDtypeStruct(tuple(dims), dtype)

    full = (GROUP, rows, width)
    qkv_shape = (n_tensor, quarter, width)
    out_shape = (n_tensor, sizes[0], width)
    att_shape = (GROUP, rows, units // 2)
    small_shape = (n_dp, 8, rows)
    table = (2, rows, LANES)
    outs = [
        shape(full),
        shape(full),
        shape((rows, width), f32),
        shape((2, rows, units)),
        shape((2, rows + WINDOW, units)),
        shape((2, rows, heads), f32),
        shape(att_shape),
        shape(table, f32),
        shape(table, f32),
        shape(qkv_shape),
        shape(out_shape),
        shape(small_shape, f32),
        shape(full),
    ] + [shape((n_tensor, size, width)) for size in sizes[1:]]
    scratch = [
        pltpu.VMEM(full, bf16),
        pltpu.VMEM(full, bf16),
        pltpu.VMEM((GROUP, quarter, chunk), bf16),
        pltpu.VMEM((GROUP, quarter, chunk), bf16),
        pltpu.VMEM((quarter, width // 2), bf16),
        pltpu.VMEM(qkv_shape, bf16),
        pltpu.VMEM((GROUP, sizes[0], chunk), bf16),
        pltpu.VMEM((GROUP, sizes[0], chunk), bf16),
        pltpu.VMEM((GROUP, chunk, sizes[1]), bf16),
        pltpu.VMEM((GROUP, chunk, sizes[2]), bf16),
        pltpu.VMEM((GROUP, chunk, sizes[3]), bf16),
        pltpu.VMEM((sum(sizes), width // 2), bf16),
        pltpu.VMEM(out_shape, bf16),
        pltpu.VMEM((8, rows), f32),
        pltpu.VMEM(small_shape, f32),
        pltpu.VMEM((8, n_tensor * rows), f32),
        pltpu.VMEM((GROUP, rows, units), bf16),
        pltpu.VMEM((2, rows, units), bf16),
        pltpu.VMEM((2, rows, units), bf16),
        pltpu.VMEM((2, rows + WINDOW, units), bf16),
        pltpu.VMEM(att_shape, bf16),
        pltpu.VMEM((2, 2, rows, units // 2), bf16),
        pltpu.VMEM((2, rows, heads), f32),
        pltpu.VMEM(table, f32),
        pltpu.VMEM(table, f32),
        pltpu.VMEM((2, rows, 1), jnp.int32),
        pltpu.VMEM((2, rows, width), bf16),
        pltpu.VMEM((2, rows, width), bf16),
        pltpu.VMEM((rows, width), bf16),
        pltpu.VMEM((rows, width), bf16),
        pltpu.VMEM((rows, width), f32),
        pltpu.VMEM(full, bf16),
        pltpu.VMEM((rows, width), bf16),
        pltpu.SemaphoreType.DMA((128,)),
        pltpu.SemaphoreType.DMA((128,)),
        pltpu.SemaphoreType.DMA((40,)),
    ]
    results = pl.pallas_call(
        functools.partial(kernel_forward, n_dp, n_tensor),
        in_specs=[hbm] * 5 + [vmem] * 6,
        out_specs=[hbm] * len(outs),
        out_shape=outs,
        scratch_shapes=scratch,
        compiler_params=pltpu.CompilerParams(
            collective_id=0, has_side_effects=True, vmem_limit_bytes=60 * 1024 * 1024
        ),
        name="forward",
    )(
        tokens, cot, gate_w, up_w, down_w, out_w, qkv_w, segments, gain1, gain2,
        jnp.asarray(fixed),
    )
    return results, jnp.asarray(fixed)


def turn(value, cosine, sine, second, turns, sign):
    width = value.shape[1]
    half = HEAD_SIZE // 2
    c = turns * cosine + (1.0 - turns)
    u = (sign * turns * second) * sine
    d = (sign * turns * (second - 1.0)) * sine
    pieces = []
    up = pltpu.roll(value, half, 1)
    down = pltpu.roll(value, width - half, 1)
    for i in range(width // LANES):
        at = slice(i * LANES, (i + 1) * LANES)
        pieces.append(value[:, at] * c + up[:, at] * u + down[:, at] * d)
    return jnp.concatenate(pieces, axis=1)


def kernel_feed(
    n_dp, n_tensor,
    n2_in, cot_in, hidden_in, gate_in, up_in, down_in, smalls,
    grad_out, grad_own_out, mlp_out, down_out, gate_out, up_out, down_got, row_out,
    n2_all, cot_all, gate_w, up_w, down_w, active, gate_delta, up_delta,
    down_part, gate_part, up_part, to_core, from_core, to_across, from_across, hidden, total,
    rounded, row, out_sems, in_sems, local_sems,
):
    f32, bf16 = jnp.float32, jnp.bfloat16
    links = Links(n_dp, n_tensor, out_sems, in_sems, local_sems)
    send, move, save = links.send, links.move, links.save
    upper = links.d_at // GROUP
    rows, width = hidden.shape
    half = width // 2
    chunk = width // n_dp
    size = gate_w.shape[1]
    units = n_tensor * size
    contract = (((1,), (1,)), ((), ()))
    over_rows = (((0,), (0,)), ((), ()))
    other = pl.ds(pl.multiple_of((1 - upper) * half, half), half)
    tiles = rows // TILE

    first_sem = links.used_local
    links.used_local += 3 * n_tensor + 2 * GROUP
    weights = ((gate_in, gate_w), (up_in, up_w), (down_in, down_w))
    tokens = ((n2_in, n2_all), (cot_in, cot_all))

    def weight_loads(p):
        return [
            pltpu.make_async_copy(
                source.at[p], target.at[p], local_sems.at[first_sem + i * n_tensor + p]
            )
            for i, (source, target) in enumerate(weights)
        ]

    def token_loads(m):
        start = first_sem + 3 * n_tensor
        return [
            pltpu.make_async_copy(source.at[m], target.at[m], local_sems.at[start + i * GROUP + m])
            for i, (source, target) in enumerate(tokens)
        ]

    for copy in token_loads(3):
        copy.start()
    for p in range(n_tensor):
        for copy in weight_loads(p):
            copy.start()
    for m in (1, 2, 0):
        for copy in token_loads(m):
            copy.start()
    hidden_load = move(hidden_in, hidden)
    links.barrier()

    def inner(i, carry):
        turn_at, p = i // n_tensor, i % n_tensor
        m = 3 - 2 * (turn_at % 2) - turn_at // 2

        @pl.when(p == 0)
        def _():
            for copy in token_loads(m):
                copy.wait()

        @pl.when(turn_at == 0)
        def _():
            for copy in weight_loads(p):
                copy.wait()

        at = pl.ds(pl.multiple_of(p * size, TILE), size)
        gate = lax.dot_general(n2_all[m], gate_w[p], contract, preferred_element_type=f32)
        up_value = lax.dot_general(n2_all[m], up_w[p], contract, preferred_element_type=f32)
        act_grad = lax.dot_general(cot_all[m], down_w[p], contract, preferred_element_type=f32)
        sigmoid = jax.nn.sigmoid(gate)
        silu = gate * sigmoid
        active[m, :, at] = (silu * up_value).astype(bf16)
        gate_delta[m, :, at] = (
            act_grad * up_value * sigmoid * (1.0 + gate * (1.0 - sigmoid))
        ).astype(bf16)
        up_delta[m, :, at] = (act_grad * silu).astype(bf16)
        return carry

    lax.fori_loop(0, 2 * n_tensor, inner, 0)

    def back(m):
        return jnp.dot(
            gate_delta[m], gate_w[...].reshape(units, width), preferred_element_type=f32
        ) + jnp.dot(up_delta[m], up_w[...].reshape(units, width), preferred_element_type=f32)

    to_core[1] = back(3).astype(bf16)
    core_send1 = send(to_core.at[1], from_core.at[1], bit=1)
    total[...] = back(1)
    core_send1.wait_recv()
    across = []
    for i in range(tiles):
        at = pl.ds(i * TILE, TILE)
        to_across[at] = (total[at, :] + from_core[1, at, :].astype(f32)).astype(bf16)
        across.append(send(to_across.at[at], from_across.at[at], bit=2))
    lax.fori_loop(2 * n_tensor, GROUP * n_tensor, inner, 0)

    order = []
    for i in range((n_tensor + 1) // 2):
        order.extend(dict.fromkeys((n_tensor - 1 - i, i)))

    swaps = []

    def grads(left, right, part, target, weight=None):
        for p in order:
            at = slice(p * size, (p + 1) * size)
            grad = lax.dot_general(
                left[...].reshape(GROUP * rows, units)[:, at],
                right[...].reshape(GROUP * rows, width),
                over_rows,
                preferred_element_type=f32,
            )
            part[p] = grad.astype(bf16)
            if weight is not None:
                row[...] += jnp.sum(grad * weight[p].astype(f32), axis=0, keepdims=True)
            elif p in order[: n_tensor // 2]:
                swaps.append(send(part.at[p, :, other], down_got.at[p], bit=GROUP))
            save(part.at[p], target.at[p])

    row[...] = jnp.zeros_like(row)
    grads(active, cot_all, down_part, down_out)
    to_core[0] = back(2).astype(bf16)
    core_send0 = send(to_core.at[0], from_core.at[0], bit=1)
    total[...] = back(0)
    core_send0.wait_recv()
    total[...] += from_core[0].astype(f32)
    grads(gate_delta, n2_all, gate_part, gate_out, gate_w)
    grads(up_delta, n2_all, up_part, up_out, up_w)
    save(row, row_out)

    for m in range(GROUP):
        n2_all[m] = jnp.dot(
            active[m], down_w[...].reshape(units, width), preferred_element_type=f32
        ).astype(bf16)
        save(n2_all.at[m], mlp_out.at[m])
    gain = jnp.concatenate([smalls[i, 3:4, :chunk] for i in range(n_dp)], axis=1)
    hidden_load.wait()
    for i in range(tiles):
        at = pl.ds(i * TILE, TILE)
        across[i].wait_recv()
        upstream = total[at, :] + from_across[at, :].astype(f32)
        features = hidden[at, :]
        inverse = lax.rsqrt(jnp.mean(features * features, axis=1, keepdims=True) + EPS)
        scaled = gain * upstream
        mean = jnp.mean(scaled * features, axis=1, keepdims=True)
        result = cot_all[0, at, :].astype(f32) + (
            inverse * scaled - features * (inverse * inverse * inverse) * mean
        )
        total[at, :] = result
        rounded[at, :] = result.astype(bf16)
    save(total, grad_out)
    save(rounded, grad_own_out)
    for copy in swaps:
        copy.wait_recv()
    links.finish()


def feed(n_dp, n_tensor, normed2, grad_rows, hidden1, gate_w, up_w, down_w, smalls):
    f32, bf16 = jnp.float32, jnp.bfloat16
    rows, width = hidden1.shape
    half = width // 2
    vmem = pl.BlockSpec(memory_space=pltpu.VMEM)
    hbm = pl.BlockSpec(memory_space=pl.ANY)
    weight = gate_w.shape
    inner = (GROUP, rows, n_tensor * weight[1])

    def shape(dims, dtype=bf16):
        return jax.ShapeDtypeStruct(tuple(dims), dtype)

    outs = [
        shape((rows, width), f32), shape((rows, width)), shape(normed2.shape),
        shape(weight), shape(weight), shape(weight), shape((n_tensor, weight[1], half)),
        shape((1, width), f32),
    ]
    scratch = [
        pltpu.VMEM(normed2.shape, bf16),
        pltpu.VMEM(normed2.shape, bf16),
        pltpu.VMEM(weight, bf16),
        pltpu.VMEM(weight, bf16),
        pltpu.VMEM(weight, bf16),
        pltpu.VMEM(inner, bf16),
        pltpu.VMEM(inner, bf16),
        pltpu.VMEM(inner, bf16),
        pltpu.VMEM(weight, bf16),
        pltpu.VMEM(weight, bf16),
        pltpu.VMEM(weight, bf16),
        pltpu.VMEM((2, rows, width), bf16),
        pltpu.VMEM((2, rows, width), bf16),
        pltpu.VMEM((rows, width), bf16),
        pltpu.VMEM((rows, width), bf16),
        pltpu.VMEM((rows, width), f32),
        pltpu.VMEM((rows, width), f32),
        pltpu.VMEM((rows, width), bf16),
        pltpu.VMEM((1, width), f32),
        pltpu.SemaphoreType.DMA((16,)),
        pltpu.SemaphoreType.DMA((16,)),
        pltpu.SemaphoreType.DMA((40,)),
    ]
    return pl.pallas_call(
        functools.partial(kernel_feed, n_dp, n_tensor),
        in_specs=[hbm] * 6 + [vmem],
        out_specs=[hbm] * len(outs),
        out_shape=outs,
        scratch_shapes=scratch,
        compiler_params=pltpu.CompilerParams(
            collective_id=2, has_side_effects=True, vmem_limit_bytes=67043328
        ),
        name="feed",
    )(normed2, grad_rows, hidden1, gate_w, up_w, down_w, smalls)


class Collect:
    def __init__(
        self, links, part, swapped, stage, arrived, late, blocks, target, mine, other, turned=False
    ):
        self.turned = turned
        self.links, self.part, self.swapped, self.stage = links, part, swapped, stage
        self.arrived, self.late, self.blocks, self.target = arrived, late, blocks, target
        self.mine, self.other = mine, other
        self.swaps, self.loads, self.deals = {}, [], []

    def issue(self, order, load=True):
        links = self.links
        for p in order:
            self.swaps[p] = links.send(
                self.part.at[p, :, self.other], self.swapped.at[p], bit=GROUP
            )
        if self.stage is not None and load:
            self.loads = [links.move(self.part.at[:, :, self.mine], self.stage)]

    def load(self, received, order):
        links = self.links
        count = links.n_tensor // 2
        self.loads = [links.move(received.at[p], self.swapped.at[p]) for p in order[:count]]
        self.loads.append(links.move(self.part.at[:, :, self.mine], self.stage))

    def step(self, p):
        links, n, z = self.links, self.links.n_tensor, self.links.z_at
        f32, bf16 = jnp.float32, jnp.bfloat16
        while self.loads:
            self.loads.pop().wait()
        if p in self.swaps:
            self.swaps[p].wait_recv()
        own = self.stage[p] if self.stage is not None else self.part[p, :, self.mine]
        self.swapped[p] = (own.astype(f32) + self.swapped[p].astype(f32)).astype(bf16)
        if not hasattr(self, "ahead"):
            self.ahead, self.back, self.back_last = [None] * n, [None] * n, [None] * n
        source = self.swapped.at[p]
        self.ahead[p] = links.plan(
            source, self.arrived.at[p], shift=1, sends=z < p, receives=(z > 0) & (z <= p)
        )
        self.back[p] = links.plan(
            source, self.arrived.at[p], shift=-1, sends=z > p + 1,
            receives=(z > p) & (z < n - 1),
        )
        self.back_last[p] = links.plan(
            source, self.late, shift=-1, sends=z == p + 1, receives=(z == p) & (z < n - 1)
        )

        @pl.when((z == 0) & (z < p))
        def _():
            self.ahead[p].copy.start()

        @pl.when((z == n - 1) & (z > p + 1))
        def _():
            self.back[p].copy.start()

        @pl.when((z == n - 1) & (z == p + 1))
        def _():
            self.back_last[p].copy.start()

    def relay(self, i):
        links, n, z = self.links, self.links.n_tensor, self.links.z_at
        f32, bf16 = jnp.float32, jnp.bfloat16

        def add(p):
            self.swapped[p] = (
                self.swapped[p].astype(f32) + self.arrived[p].astype(f32)
            ).astype(bf16)

        for p in range(n):
            at = i - (n - 1) + p
            if 0 < at < n - 1 and at < p:

                @pl.when(z == at)
                def _(p=p):
                    self.ahead[p].copy.wait_recv()
                    add(p)
                    self.ahead[p].copy.start()

            at = n - 1 - i + p
            if 0 < at < n - 1 and at > p:

                @pl.when(z == at)
                def _(p=p, at=at):
                    self.back[p].copy.wait_recv()
                    add(p)
                    (self.back_last if at == p + 1 else self.back)[p].copy.start()

    def finish(self):
        links, n, z = self.links, self.links.n_tensor, self.links.z_at
        f32, bf16 = jnp.float32, jnp.bfloat16
        member = links.d_at % GROUP
        for p in range(n):

            @pl.when((z == p) & (z > 0))
            def _(p=p):
                self.ahead[p].copy.wait_recv()

            @pl.when((z == p) & (z < n - 1))
            def _(p=p):
                self.back_last[p].copy.wait_recv()

        below = jnp.where(z > 0, self.arrived[z].astype(f32), 0.0)
        above = jnp.where(z < n - 1, self.late[...].astype(f32), 0.0)
        total = (self.swapped[z].astype(f32) + below + above).astype(bf16)
        chunk = total.shape[1] // GROUP
        size = self.blocks.shape[2 if self.turned else 1]
        place = pl.ds(pl.multiple_of(member * size, 16), size)
        if self.turned:
            place = pl.ds(pl.multiple_of(member * size, TILE), size)
        for i in range(GROUP):
            block = total[:, i * chunk : (i + 1) * chunk]
            self.blocks[i] = block.T if self.turned else block
        if self.turned:
            target = self.target.at[:, place]
        elif len(self.target.shape) == 2:
            target = self.target.at[place, :]
        else:
            target = self.target.at[member]
        for k in range(1, GROUP):
            self.deals.append(links.send(self.blocks.at[member ^ k], target, bit=k))
        links.save(self.blocks.at[member], target)

    def wait(self):
        for deal in self.deals:
            deal.wait_recv()


def kernel_backward(
    n_dp, n_tensor,
    grad_own, hidden_grad, tokens, hidden1, mlp_part, n1_in, query_in, keyval_in, log_in, att_in,
    cos_in, sin_in, qkv_in, out_in, small_in, down_in, gate_in, up_in, down_got,
    mlp_row, fixed,
    input_out, block_out, qkv_out, out_out, gate_out, up_out, down_out,
    g_all, n1_all, qkv, outw, queries, keyvals, logs, att, cosine, sine, gains, low_col,
    att_grad, other_grad, totals, query_total, pass_on, delta, halo_send, halo_recv,
    to_core, from_core, to_across, from_across, mlp_across, hidden, stage, gate_stage,
    down_swap, gate_swap, up_swap, out_swap, qkv_swap,
    down_come, gate_come, up_come, out_come, qkv_come,
    down_late, gate_late, up_late, out_late, qkv_late,
    down_block, gate_block, up_block, out_block, qkv_block,
    out_sems, in_sems, local_sems,
):
    f32, bf16 = jnp.float32, jnp.bfloat16
    links = Links(n_dp, n_tensor, out_sems, in_sems, local_sems)
    send, move, save = links.send, links.move, links.save
    d_at, z_at = links.d_at, links.z_at
    core = d_at % 2
    upper = d_at // GROUP
    rows, width = grad_own.shape
    half = width // 2
    contract = (((1,), (1,)), ((), ()))
    over_rows = (((0,), (0,)), ((), ()))
    mine = pl.ds(pl.multiple_of(upper * half, half), half)
    other = pl.ds(pl.multiple_of((1 - upper) * half, half), half)
    tiles = rows // TILE
    span = TILE + WINDOW
    quarter = qkv.shape[1]
    out_quarter = outw.shape[1]
    extra = qkv_swap.shape[1] - quarter

    order = []
    for i in range((n_tensor + 1) // 2):
        order.extend(dict.fromkeys((n_tensor - 1 - i, i)))

    down = Collect(
        links, down_in, down_swap, stage, down_come, down_late, down_block, down_out, mine, other,
        turned=True,
    )
    gate = Collect(
        links, gate_in, gate_swap, gate_stage, gate_come, gate_late, gate_block, gate_out, mine, other,
        turned=True,
    )
    up = Collect(
        links, up_in, up_swap, stage, up_come, up_late, up_block, up_out, mine, other, turned=True
    )
    out_part = g_all.at[:, pl.ds(quarter + extra, out_quarter), :]
    qkv_part = g_all.at[:, pl.ds(0, quarter + extra), :]
    out_collect = Collect(
        links, out_part, out_swap, None, out_come, out_late, out_block, out_out, mine, other
    )
    qkv_collect = Collect(
        links, qkv_part, qkv_swap, None, qkv_come, qkv_late, qkv_block, qkv_out, mine, other
    )
    small = move(small_in, gains)
    loads = [
        move(grad_own, g_all.at[0]), move(out_in, outw),
    ]
    down.load(down_got, order)
    loads += [
        move(query_in, queries),
        move(keyval_in, keyvals), move(log_in, logs), move(cos_in, cosine), move(sin_in, sine),
        move(mlp_part.at[pl.ds(0, 2)], to_core), move(hidden1, hidden), move(att_in, att),
        move(qkv_in, qkv), move(n1_in, n1_all),
    ]
    links.barrier()
    across = send(grad_own, g_all.at[1], bit=2)
    beside = send(grad_own, g_all.at[2], bit=1)
    mlp_core = send(mlp_part.at[pl.ds(2, 2)], from_core, bit=1)
    down.issue(order[n_tensor // 2 :], load=False)
    gate.issue(order)
    for p in order[: n_tensor // 2]:
        down.step(p)
    small.wait()
    for m, k in ((0, 0), (1, 2)):
        info = gains[d_at ^ k].T
        low_col[m] = info[:, 1:2].astype(jnp.int32) - z_at * rows + WINDOW
    loads[0].wait()
    loads[1].wait()

    def attended_back(b):
        units = outw.shape[0] * outw.shape[1]
        att_grad[b] = lax.dot_general(
            g_all[b], outw[...].reshape(units, width), contract, preferred_element_type=f32
        ).astype(bf16)

    attended_back(0)
    beside.wait_recv()
    attended_back(2)
    grad_swap = send(att_grad.at[2], other_grad.at[0], bit=1)
    for copy in loads[2:]:
        copy.wait()
    mlp_core.wait_recv()
    heads = queries.shape[2] // HEAD_SIZE
    repeat = QUERY_HEADS // KEY_VALUE_HEADS
    scale = HEAD_SIZE ** (-0.5)
    is_first = core == 0
    second, keys_turn, all_turn = fixed[1:2], fixed[2:3], fixed[3:4]

    def back_tile(m, tile):
        start = tile * TILE
        at = slice(start, start + TILE)
        reach = slice(start, start + span)
        key = lax.broadcasted_iota(jnp.int32, (TILE, span), 1)
        query = lax.broadcasted_iota(jnp.int32, (TILE, span), 0)
        allowed = (key >= low_col[m, at, :] - start) & (key <= query + WINDOW)
        own, others = att_grad[m, at, :], other_grad[m, at, :]
        by_repeat = (jnp.where(is_first, own, others), jnp.where(is_first, others, own))
        for group in range(heads // repeat):
            base = group * 2 * HEAD_SIZE
            k = keyvals[m, reach, base : base + HEAD_SIZE]
            v = keyvals[m, reach, base + HEAD_SIZE : base + 2 * HEAD_SIZE]
            key_sum = None
            for r in range(repeat):
                head = group * repeat + r
                q = queries[m, at, head * HEAD_SIZE : (head + 1) * HEAD_SIZE]
                g = by_repeat[r][:, group * HEAD_SIZE : (group + 1) * HEAD_SIZE]
                s = lax.dot_general(q, k, contract, preferred_element_type=f32) * scale
                total = logs[m, at, head : head + 1]
                p = jnp.exp(jnp.where(allowed, s, NEG_FILL) - total)
                pg = lax.dot_general(g, v, contract, preferred_element_type=f32)
                inner = jnp.sum(p * pg, axis=1, keepdims=True)
                sg = (p * (pg - inner) * scale).astype(bf16)
                query_total[:, head * HEAD_SIZE : (head + 1) * HEAD_SIZE] = jnp.dot(
                    sg, k, preferred_element_type=f32
                )
                dk = lax.dot_general(sg, q, over_rows, preferred_element_type=f32)
                dv = lax.dot_general(p.astype(bf16), g, over_rows, preferred_element_type=f32)
                both = jnp.concatenate([dk, dv], axis=1)
                key_sum = both if key_sum is None else key_sum + both
            totals[m, reach, base : base + 2 * HEAD_SIZE] += key_sum
        turned = turn(
            query_total[...], cosine[m, at, :], sine[m, at, :], second, all_turn, -1.0
        ).astype(bf16)

        @pl.when(is_first)
        def _():
            delta[m, at, :] = turned

        @pl.when(core != 0)
        def _():
            pass_on[m, at, :] = turned

    halos = [
        links.plan(
            halo_send.at[m], halo_recv.at[m], shift=-1, sends=z_at > 0,
            receives=z_at < n_tensor - 1,
        )
        for m in range(2)
    ]

    def back_tiles(m, first_tile, last_tile):
        for tile in range(first_tile, last_tile):
            back_tile(m, tile)

    def send_halo(m):
        halo_send[m] = totals[m, :WINDOW].astype(bf16)
        halos[m].start()

    def finish_block(m):
        halos[m].wait_recv()
        full = totals[m, WINDOW:]
        tail = full[rows - WINDOW :] + jnp.where(
            z_at < n_tensor - 1, halo_recv[m].astype(f32), 0.0
        )
        full = jnp.concatenate([full[: rows - WINDOW], tail], axis=0)
        turned = turn(full, cosine[m], sine[m], second, keys_turn, -1.0).astype(bf16)

        @pl.when(is_first)
        def _():
            pass_on[m] = turned

        @pl.when(core != 0)
        def _():
            delta[m] = turned

        return send(pass_on.at[m], delta.at[2 + m], bit=1)

    free = -(-WINDOW // TILE)
    totals[...] = jnp.zeros_like(totals)
    grad_swap.wait_recv()
    back_tiles(0, 0, free)
    down.relay(1)
    send_halo(0)
    for p in order[n_tensor // 2 : n_tensor - 1]:
        down.step(p)
    back_tiles(0, free, tiles)
    for p in order[n_tensor - 1 :]:
        down.step(p)
    up.issue(order)
    across.wait_recv()
    both = send(g_all.at[1], g_all.at[3], bit=1)
    to_across[...] = (to_core[1].astype(f32) + from_core[1].astype(f32)).astype(bf16)
    mlp_send = send(to_across, mlp_across, bit=2)
    hidden[...] += to_core[0].astype(f32) + from_core[0].astype(f32)
    attended_back(1)
    both.wait_recv()
    attended_back(3)
    grad_swap = send(att_grad.at[3], other_grad.at[1], bit=1)
    gate.step(order[0])

    def weight_grad(left, right, at):
        total = None
        for b in range(GROUP):
            term = lax.dot_general(
                left[b, :, at], right[b], over_rows, preferred_element_type=f32
            )
            total = term if total is None else total + term
        return total

    out_grad = weight_grad(att, g_all, slice(0, n_tensor * out_quarter)).astype(bf16)
    both.wait_send()
    links.sent.remove(both)
    out_part[...] = out_grad.reshape(n_tensor, out_quarter, width)
    grad_swap.wait_recv()
    back_tiles(1, 0, 1)
    gate.step(order[1])
    back_tiles(1, 1, free)
    for i in range(2, n_tensor - 1):
        down.relay(i)
    send_halo(1)
    back_tiles(1, free, tiles)
    for p in order[2 : n_tensor - 1]:
        gate.step(p)
    swap0 = finish_block(0)
    gate.relay(1)
    swap1 = finish_block(1)
    grad_loads = [
        move(hidden_grad.at[:, pl.ds(i * half, half)], totals.at[i, pl.ds(0, rows)])
        for i in range(2)
    ]
    down.finish()
    for p in order[n_tensor - 1 :]:
        gate.step(p)

    def project_back(b):
        units = qkv.shape[0] * quarter
        return jnp.dot(delta[b], qkv[...].reshape(units, width), preferred_element_type=f32)

    mlp_send.wait_recv()
    mlp_across[...] = (hidden[...] + mlp_across[...].astype(f32)).astype(bf16)
    save(mlp_across, block_out)
    mlp_send.wait_send()
    links.sent.remove(mlp_send)
    swap1.wait_recv()
    to_core[1] = project_back(3).astype(bf16)
    core_send1 = send(to_core.at[1], from_core.at[1], bit=1)
    hidden[...] = project_back(1)
    swap0.wait_recv()
    to_core[0] = project_back(2).astype(bf16)
    core_send0 = send(to_core.at[0], from_core.at[0], bit=1)
    core_send1.wait_recv()
    across_sends = []
    for i in range(tiles):
        at = pl.ds(i * TILE, TILE)
        to_across[at] = (hidden[at, :] + from_core[1, at, :].astype(f32)).astype(bf16)
        across_sends.append(send(to_across.at[at], from_across.at[at], bit=2))
    hidden[...] = project_back(0)
    core_send0.wait_recv()
    hidden[...] += from_core[0].astype(f32)
    up.step(order[0])
    attn_row = None
    for p in range(n_tensor):
        at = slice(p * quarter, (p + 1) * quarter)
        grad = weight_grad(delta, n1_all, at)
        row = jnp.sum(grad * qkv[p].astype(f32), axis=0, keepdims=True)
        attn_row = row if attn_row is None else attn_row + row
        qkv_part[p, :quarter, :] = grad.astype(bf16)
    ending = jnp.concatenate(
        [attn_row, mlp_row[...], jnp.zeros((extra - 2, width), f32)], axis=0
    ).astype(bf16)
    for p in range(n_tensor):
        qkv_part[p, quarter:, :] = ending
    qkv_collect.issue(order)
    out_collect.issue(order)
    token_load = move(tokens, n1_all.at[0])
    up.step(order[1])
    gain = jnp.concatenate([gains[i, 2:3, : width // n_dp] for i in range(n_dp)], axis=1)
    for i in range(tiles):
        at = pl.ds(i * TILE, TILE)
        across_sends[i].wait_recv()
        if i == 0:
            for copy in grad_loads + [token_load]:
                copy.wait()
        upstream = hidden[at, :] + from_across[at, :].astype(f32)
        features = n1_all[0, at, :].astype(f32)
        inverse = lax.rsqrt(jnp.mean(features * features, axis=1, keepdims=True) + EPS)
        scaled = gain * upstream
        mean = jnp.mean(scaled * features, axis=1, keepdims=True)
        change = inverse * scaled - features * (inverse * inverse * inverse) * mean
        n1_all[1, at, :half] = (totals[0, at, :] + change[:, :half]).astype(bf16)
        n1_all[1, at, half:] = (totals[1, at, :] + change[:, half:]).astype(bf16)
        if i == 0:
            for j in range(2, n_tensor - 1):
                gate.relay(j)
        if i == 1:
            for p in order[2 : n_tensor - 1]:
                up.step(p)
    save(n1_all.at[1], input_out)
    gate.finish()
    for p in order[n_tensor - 1 :]:
        up.step(p)
    up.relay(1)
    for p in order[:2]:
        qkv_collect.step(p)
    for i in range(2, n_tensor - 1):
        up.relay(i)
    for p in order[2 : n_tensor - 1]:
        qkv_collect.step(p)
    up.finish()
    for p in order[n_tensor - 1 :]:
        qkv_collect.step(p)
    qkv_collect.relay(1)
    for p in order[:2]:
        out_collect.step(p)
    for i in range(2, n_tensor - 1):
        qkv_collect.relay(i)
    for p in order[2:]:
        out_collect.step(p)
    out_collect.relay(1)
    qkv_collect.finish()
    for i in range(2, n_tensor - 1):
        out_collect.relay(i)
    out_collect.finish()
    for collect in (down, gate, up, out_collect, qkv_collect):
        collect.wait()
    links.finish()


def backward(
    n_dp, n_tensor, grad_own, hidden_grad, tokens, hidden1, mlp_part, normed1, queries, keyvals, logs, attended,
    cosine, sine, qkv_full, out_full, smalls, down_part, gate_part, up_part, down_got,
    mlp_row, fixed,
):
    f32, bf16 = jnp.float32, jnp.bfloat16
    rows, width = grad_own.shape
    half = width // 2
    chunk = width // n_dp
    units = queries.shape[2]
    vmem = pl.BlockSpec(memory_space=pltpu.VMEM)
    hbm = pl.BlockSpec(memory_space=pl.ANY)
    extra = 16
    quarters = [
        down_part.shape[1], gate_part.shape[1], up_part.shape[1], out_full.shape[1],
        qkv_full.shape[1] + extra,
    ]

    def shape(dims, dtype=bf16):
        return jax.ShapeDtypeStruct(tuple(dims), dtype)

    def finals(index):
        return shape((GROUP, quarters[index], chunk))

    outs = [
        shape((rows, width)), shape((rows, width)), finals(4), shape((GROUP * quarters[3], chunk)),
        shape((chunk, GROUP * quarters[1])), shape((chunk, GROUP * quarters[2])),
        shape((chunk, GROUP * quarters[0])),
    ]
    full = (GROUP, rows, width)
    scratch = [
        pltpu.VMEM(full, bf16),
        pltpu.VMEM(full, bf16),
        pltpu.VMEM(qkv_full.shape, bf16),
        pltpu.VMEM(out_full.shape, bf16),
        pltpu.VMEM(queries.shape, bf16),
        pltpu.VMEM(keyvals.shape, bf16),
        pltpu.VMEM(logs.shape, f32),
        pltpu.VMEM(attended.shape, bf16),
        pltpu.VMEM(cosine.shape, f32),
        pltpu.VMEM(sine.shape, f32),
        pltpu.VMEM(smalls.shape, f32),
        pltpu.VMEM((2, rows, 1), jnp.int32),
        pltpu.VMEM(attended.shape, bf16),
        pltpu.VMEM((2,) + attended.shape[1:], bf16),
        pltpu.VMEM((2, rows + WINDOW, units), f32),
        pltpu.VMEM((TILE, units), f32),
        pltpu.VMEM((2, rows, units), bf16),
        pltpu.VMEM((GROUP, rows, units), bf16),
        pltpu.VMEM((2, WINDOW, units), bf16),
        pltpu.VMEM((2, WINDOW, units), bf16),
        pltpu.VMEM((2, rows, width), bf16),
        pltpu.VMEM((2, rows, width), bf16),
        pltpu.VMEM((rows, width), bf16),
        pltpu.VMEM((rows, width), bf16),
        pltpu.VMEM((rows, width), bf16),
        pltpu.VMEM((rows, width), f32),
        pltpu.VMEM((n_tensor, quarters[0], half), bf16),
        pltpu.VMEM((n_tensor, quarters[1], half), bf16),
    ]
    scratch += [pltpu.VMEM((n_tensor, q, half), bf16) for q in quarters]
    scratch += [pltpu.VMEM((n_tensor, q, half), bf16) for q in quarters]
    scratch += [pltpu.VMEM((q, half), bf16) for q in quarters]
    scratch += [
        pltpu.VMEM((GROUP, chunk, q) if turned else (GROUP, q, chunk), bf16)
        for q, turned in zip(quarters, (True, True, True, False, False))
    ]
    scratch += [
        pltpu.SemaphoreType.DMA((160,)),
        pltpu.SemaphoreType.DMA((160,)),
        pltpu.SemaphoreType.DMA((40,)),
    ]
    return pl.pallas_call(
        functools.partial(kernel_backward, n_dp, n_tensor),
        in_specs=[hbm] * 19 + [vmem] * 2,
        out_specs=[hbm] * len(outs),
        out_shape=outs,
        scratch_shapes=scratch,
        compiler_params=pltpu.CompilerParams(
            collective_id=1, has_side_effects=True, vmem_limit_bytes=67043328
        ),
        name="backward",
    )(
        grad_own, hidden_grad, tokens, hidden1, mlp_part, normed1, queries, keyvals, logs, attended, cosine, sine,
        qkv_full, out_full, smalls, down_part, gate_part, up_part, down_got, mlp_row, fixed,
    )


def fast_local(
    n_dp,
    n_tensor,
    block_in,
    cotangent,
    segment_ids,
    attn_gain,
    qkv_weight,
    out_weight,
    mlp_gain,
    gate_weight,
    up_weight,
    down_weight,
):
    bf16, f32 = jnp.bfloat16, jnp.float32
    rows, width = block_in.shape
    part = attn_gain.shape[0]
    (
        normed1, normed2, hidden1, queries, keyvals, log_total, attended, cosine, sine, qkv_full,
        out_full, smalls, grad_rows, gate_full, up_full, down_full,
    ), fixed = forward(
        n_dp, n_tensor, block_in, cotangent, segment_ids, attn_gain[None], mlp_gain[None],
        qkv_weight, out_weight, gate_weight, up_weight, down_weight,
    )
    (
        hidden1_grad, grad_own, mlp_part, down_part, gate_part, up_part, down_got, mlp_row,
    ) = feed(n_dp, n_tensor, normed2, grad_rows, hidden1, gate_full, up_full, down_full, smalls)
    input_grad, block_out, qkv_blocks, out_grad, gate_grad, up_grad, down_grad = backward(
        n_dp, n_tensor, grad_own, hidden1_grad, block_in, hidden1, mlp_part, normed1, queries,
        keyvals, log_total, attended, cosine, sine, qkv_full, out_full, smalls, down_part, gate_part, up_part, down_got, mlp_row,
        fixed,
    )
    quarter = qkv_full.shape[1]

    def row_of(index, gain):
        return jnp.sum(qkv_blocks[:, quarter + index].astype(f32), axis=0) / gain.astype(f32)

    blocks = qkv_blocks[:, :quarter]
    qkv_grad = blocks.reshape(-1, blocks.shape[2]).T.astype(f32)
    gains = [row_of(0, attn_gain), row_of(1, mlp_gain)]
    return (
        block_out,
        input_grad,
        gains[0],
        qkv_grad,
        out_grad.astype(f32),
        gains[1],
        gate_grad.astype(f32),
        up_grad.astype(f32),
        down_grad.T.astype(f32),
    )


def solution(mesh):
    in_specs = (
        P(("dp", "tensor"), None),
        P(("dp", "tensor"), None),
        P("dp", None),
        P("dp"),
        P("dp", "tensor"),
        P("tensor", "dp"),
        P("dp"),
        P("dp", "tensor"),
        P("dp", "tensor"),
        P("tensor", "dp"),
    )
    out_specs = (
        P(("dp", "tensor"), None),
        P(("dp", "tensor"), None),
        P("dp"),
        P("dp", "tensor"),
        P("tensor", "dp"),
        P("dp"),
        P("dp", "tensor"),
        P("dp", "tensor"),
        P("tensor", "dp"),
    )
    n_dp, n_tensor = mesh.shape["dp"], mesh.shape["tensor"]

    def body(*arrays):
        rows = arrays[0].shape[0]
        groups = arrays[4].shape[1] // (4 * HEAD_SIZE)
        if n_dp == 2 * GROUP and groups == 2 and rows >= WINDOW and rows % TILE == 0:
            return fast_local(n_dp, n_tensor, *arrays)
        return local(*arrays)

    return jax.shard_map(body, mesh=mesh, in_specs=in_specs, out_specs=out_specs, check_vma=False)
```

```python
import functools

import jax
import jax.numpy as jnp
import numpy as np
from jax import lax
from jax.experimental import pallas as pl
from jax.experimental.pallas import tpu as pltpu
from jax.sharding import PartitionSpec as P

QUERY_HEADS = 16
KEY_VALUE_HEADS = 8
HEAD_SIZE = 96


EPS = 1e-05
ROPE_BASE = 100000.0
NEG_FILL = -1e30


def doc_positions(segments):
    length = segments.shape[1]
    position_index = jnp.broadcast_to(jnp.arange(length, dtype=jnp.int32)[None, :], segments.shape)
    change = jnp.concatenate(
        [jnp.ones((segments.shape[0], 1), dtype=bool), segments[:, 1:] != segments[:, :-1]], axis=1
    )
    starts = lax.cummax(jnp.where(change, position_index, jnp.zeros_like(position_index)), axis=1)
    return position_index - starts


def rotary_tables(segments):
    half_dim = HEAD_SIZE // 2
    frequency = jnp.power(ROPE_BASE, -(2.0 * jnp.arange(half_dim, dtype=jnp.float32)) / HEAD_SIZE)
    angles = doc_positions(segments).astype(jnp.float32)[..., None] * frequency
    cosine_table = jnp.concatenate([jnp.cos(angles), jnp.cos(angles)], axis=-1)
    sine_table = jnp.concatenate([jnp.sin(angles), jnp.sin(angles)], axis=-1)
    return (cosine_table, sine_table)


def rotate(vector, cosine_table, sine_table):
    half_dim = vector.shape[-1] // 2
    turned = jnp.concatenate([-vector[..., half_dim:], vector[..., :half_dim]], axis=-1)
    return vector * cosine_table + turned * sine_table


def unrotate(vector, cosine_table, sine_table):
    half_dim = vector.shape[-1] // 2
    shifted = vector * sine_table
    returned = jnp.concatenate([shifted[..., half_dim:], -shifted[..., :half_dim]], axis=-1)
    return vector * cosine_table + returned


def allowed_pairs(segments):
    length = segments.shape[1]
    offsets = jnp.arange(length)
    causal = offsets[None, :] <= offsets[:, None]
    same_doc = segments[:, :, None] == segments[:, None, :]
    return (causal[None] & same_doc)[:, None, None]


def score_block(queries, key_heads, segments):
    scores = jnp.einsum(
        "sqgrd,skgd->sgrqk", queries, key_heads, preferred_element_type=jnp.float32
    ) * HEAD_SIZE ** (-0.5)
    return jnp.where(allowed_pairs(segments), scores, NEG_FILL)


def rms_scale(features):
    return lax.rsqrt(jnp.mean(features * features, axis=-1, keepdims=True) + EPS)


def norm_back(features, inverse, gain_vector, upstream):
    scaled = gain_vector * upstream
    return inverse * scaled - features * (inverse * inverse * inverse) * jnp.mean(
        scaled * features, axis=-1, keepdims=True
    )


def widen(shard_rows):
    return lax.all_gather(shard_rows, "tensor", axis=0, tiled=True)


def narrow(partial_value):
    return lax.psum_scatter(
        partial_value.astype(jnp.bfloat16), "tensor", scatter_dimension=0, tiled=True
    ).astype(jnp.float32)


def local(
    block_in,
    cotangent,
    segment_ids,
    attn_gain,
    qkv_weight,
    out_weight,
    mlp_gain,
    gate_weight,
    up_weight,
    down_weight,
):
    qkv_full, gate_full, up_full, gain_attn_raw, gain_mlp_raw = (
        lax.all_gather(qkv_weight, "dp", axis=0, tiled=True),
        lax.all_gather(gate_weight, "dp", axis=0, tiled=True),
        lax.all_gather(up_weight, "dp", axis=0, tiled=True),
        lax.all_gather(attn_gain, "dp", axis=0, tiled=True),
        lax.all_gather(mlp_gain, "dp", axis=0, tiled=True),
    )
    out_cols, down_cols = (
        lax.all_gather(out_weight, "dp", axis=1, tiled=True),
        lax.all_gather(down_weight, "dp", axis=1, tiled=True),
    )
    seq_count, length = segment_ids.shape
    repeat_factor = QUERY_HEADS // KEY_VALUE_HEADS
    groups = qkv_full.shape[1] // ((repeat_factor + 2) * HEAD_SIZE)
    gain_attn = gain_attn_raw.astype(jnp.float32)
    gain_mlp = gain_mlp_raw.astype(jnp.float32)
    residual = block_in.astype(jnp.float32)
    scale_attn = rms_scale(residual)
    normed1 = widen((residual * scale_attn * gain_attn).astype(jnp.bfloat16))
    projected = jnp.dot(normed1, qkv_full, preferred_element_type=jnp.float32).reshape(
        seq_count, length, groups, repeat_factor + 2, HEAD_SIZE
    )
    cosine_table, sine_table = rotary_tables(segment_ids)
    cos_query = cosine_table[:, :, None, None, :]
    sin_query = sine_table[:, :, None, None, :]
    cos_key = cosine_table[:, :, None, :]
    sin_key = sine_table[:, :, None, :]
    queries = rotate(projected[:, :, :, :repeat_factor], cos_query, sin_query).astype(jnp.bfloat16)
    key_heads = rotate(projected[:, :, :, repeat_factor], cos_key, sin_key).astype(jnp.bfloat16)
    values = projected[:, :, :, repeat_factor + 1].astype(jnp.bfloat16)
    scores = score_block(queries, key_heads, segment_ids)
    highest = jnp.max(scores, axis=-1, keepdims=True)
    log_total = highest + jnp.log(jnp.sum(jnp.exp(scores - highest), axis=-1, keepdims=True))
    probability = jnp.exp(scores - log_total).astype(jnp.bfloat16)
    attended = jnp.einsum(
        "sgrqk,skgd->sqgrd", probability, values, preferred_element_type=jnp.float32
    ).astype(jnp.bfloat16)
    attn_flat = attended.reshape(seq_count * length, groups * repeat_factor * HEAD_SIZE)
    attn_delta = lax.psum_scatter(
        jnp.dot(attn_flat, out_cols, preferred_element_type=jnp.float32).astype(jnp.bfloat16),
        "tensor",
        scatter_dimension=0,
        tiled=True,
    ).astype(jnp.float32)
    hidden1 = residual + attn_delta
    scale_mlp = rms_scale(hidden1)
    normed2 = widen((hidden1 * scale_mlp * gain_mlp).astype(jnp.bfloat16))
    gate = jnp.dot(normed2, gate_full, preferred_element_type=jnp.float32)
    up_value = jnp.dot(normed2, up_full, preferred_element_type=jnp.float32)
    sigmoid_gate = jax.nn.sigmoid(gate)
    activated = (gate * sigmoid_gate * up_value).astype(jnp.bfloat16)
    mlp_delta = narrow(jnp.dot(activated, down_cols, preferred_element_type=jnp.float32))
    block_out = (hidden1 + mlp_delta).astype(jnp.bfloat16)
    grad_rows = widen(cotangent)
    down_part = jnp.einsum("tf,td->fd", activated, grad_rows, preferred_element_type=jnp.float32)
    act_grad = jnp.einsum("td,fd->tf", grad_rows, down_cols, preferred_element_type=jnp.float32)
    gate_delta = (act_grad * up_value * sigmoid_gate * (1.0 + gate * (1.0 - sigmoid_gate))).astype(
        jnp.bfloat16
    )
    up_delta = (act_grad * gate * sigmoid_gate).astype(jnp.bfloat16)
    gate_part = jnp.einsum("td,tf->df", normed2, gate_delta, preferred_element_type=jnp.float32)
    up_part = jnp.einsum("td,tf->df", normed2, up_delta, preferred_element_type=jnp.float32)
    normed2_term = jnp.einsum(
        "tf,df->td", gate_delta, gate_full, preferred_element_type=jnp.float32
    ) + jnp.einsum("tf,df->td", up_delta, up_full, preferred_element_type=jnp.float32)
    normed2_grad = narrow(normed2_term)
    mlp_gain_part = jnp.sum(normed2_grad * hidden1 * scale_mlp, axis=0)
    hidden1_grad = cotangent.astype(jnp.float32) + norm_back(
        hidden1, scale_mlp, gain_mlp, normed2_grad
    )
    hidden1_rounded = hidden1_grad.astype(jnp.bfloat16)
    grad_full = lax.all_gather(hidden1_rounded, "tensor", axis=0, tiled=True)
    attended_grad = jnp.einsum(
        "td,hd->th", grad_full, out_cols, preferred_element_type=jnp.float32
    ).astype(jnp.bfloat16)
    out_part = jnp.einsum("th,td->hd", attn_flat, grad_full, preferred_element_type=jnp.float32)
    attended_grad = attended_grad.reshape(seq_count, length, groups, repeat_factor, HEAD_SIZE)
    prob_full = jnp.exp(score_block(queries, key_heads, segment_ids) - log_total)
    prob_grad = jnp.einsum(
        "sqgrd,skgd->sgrqk", attended_grad, values, preferred_element_type=jnp.float32
    )
    inner_sum = jnp.sum(prob_full * prob_grad, axis=-1, keepdims=True)
    score_grad = (prob_full * (prob_grad - inner_sum) * HEAD_SIZE ** (-0.5)).astype(jnp.bfloat16)
    query_grad = jnp.einsum(
        "sgrqk,skgd->sqgrd", score_grad, key_heads, preferred_element_type=jnp.float32
    )
    key_grad = jnp.einsum(
        "sgrqk,sqgrd->skgd", score_grad, queries, preferred_element_type=jnp.float32
    )
    value_grad = jnp.einsum(
        "sgrqk,sqgrd->skgd",
        prob_full.astype(jnp.bfloat16),
        attended_grad,
        preferred_element_type=jnp.float32,
    )
    projected_grad = jnp.concatenate(
        [
            unrotate(query_grad, cos_query, sin_query),
            unrotate(key_grad, cos_key, sin_key)[:, :, :, None],
            value_grad[:, :, :, None],
        ],
        axis=3,
    )
    projected_grad = projected_grad.astype(jnp.bfloat16).reshape(
        seq_count * length, groups * (repeat_factor + 2) * HEAD_SIZE
    )
    qkv_part = jnp.einsum("td,tc->dc", normed1, projected_grad, preferred_element_type=jnp.float32)
    normed1_grad = narrow(
        jnp.einsum("tc,dc->td", projected_grad, qkv_full, preferred_element_type=jnp.float32)
    )
    attn_gain_part = jnp.sum(normed1_grad * residual * scale_attn, axis=0)
    input_grad = (hidden1_grad + norm_back(residual, scale_attn, gain_attn, normed1_grad)).astype(
        jnp.bfloat16
    )
    attn_gain_total, mlp_gain_total = lax.psum((attn_gain_part, mlp_gain_part), "tensor")
    attn_gain_grad, qkv_grad, gate_grad, up_grad, mlp_gain_grad = (
        lax.psum_scatter(
            attn_gain_total.astype(jnp.bfloat16), "dp", scatter_dimension=0, tiled=True
        ).astype(jnp.float32),
        lax.psum_scatter(
            qkv_part.astype(jnp.bfloat16), "dp", scatter_dimension=0, tiled=True
        ).astype(jnp.float32),
        lax.psum_scatter(
            gate_part.astype(jnp.bfloat16), "dp", scatter_dimension=0, tiled=True
        ).astype(jnp.float32),
        lax.psum_scatter(
            up_part.astype(jnp.bfloat16), "dp", scatter_dimension=0, tiled=True
        ).astype(jnp.float32),
        lax.psum_scatter(
            mlp_gain_total.astype(jnp.bfloat16), "dp", scatter_dimension=0, tiled=True
        ).astype(jnp.float32),
    )
    out_grad, down_grad = (
        lax.psum_scatter(
            out_part.astype(jnp.bfloat16), "dp", scatter_dimension=1, tiled=True
        ).astype(jnp.float32),
        lax.psum_scatter(
            down_part.astype(jnp.bfloat16), "dp", scatter_dimension=1, tiled=True
        ).astype(jnp.float32),
    )
    return (
        block_out,
        input_grad,
        attn_gain_grad,
        qkv_grad,
        out_grad,
        mlp_gain_grad,
        gate_grad,
        up_grad,
        down_grad,
    )


GROUP = 4
WINDOW = 256
LANES = 384
TILE = 128


MESH = pl.DeviceIdType.MESH


class Transfer:
    def __init__(self, copy, sends=None, receives=None):
        self.copy, self.sends, self.receives = copy, sends, receives

    def _when(self, condition, action):
        if condition is None:
            action()
        else:
            pl.when(condition)(action)

    def start(self):
        self._when(self.sends, self.copy.start)
        return self

    def wait_recv(self):
        self._when(self.receives, self.copy.wait_recv)

    def wait_send(self):
        self._when(self.sends, self.copy.wait_send)


class Links:
    def __init__(self, n_dp, n_tensor, out_sems, in_sems, local_sems):
        self.n_dp, self.n_tensor = n_dp, n_tensor
        self.out_sems, self.in_sems, self.local_sems = out_sems, in_sems, local_sems
        self.d_at, self.z_at = lax.axis_index("dp"), lax.axis_index("tensor")
        self.used, self.used_local = 0, 0
        self.sent, self.saved = [], []

    def barrier(self):
        barrier = pltpu.get_barrier_semaphore()
        for k in range(1, self.n_dp):
            pl.semaphore_signal(
                barrier,
                inc=1,
                device_id={"dp": self.d_at ^ k, "tensor": self.z_at},
                device_id_type=MESH,
            )
        for s in range(1, self.n_tensor):
            pl.semaphore_signal(
                barrier,
                inc=1,
                device_id={"dp": self.d_at, "tensor": lax.rem(self.z_at + s, self.n_tensor)},
                device_id_type=MESH,
            )
        pl.semaphore_wait(barrier, self.n_dp - 1 + self.n_tensor - 1)

    def plan(self, source, target, bit=0, shift=0, sends=None, receives=None):
        slot = self.used
        self.used += 1
        copy = pltpu.make_async_remote_copy(
            src_ref=source,
            dst_ref=target,
            send_sem=self.out_sems.at[slot],
            recv_sem=self.in_sems.at[slot],
            device_id={
                "dp": self.d_at ^ bit,
                "tensor": lax.rem(self.z_at + self.n_tensor + shift, self.n_tensor),
            },
            device_id_type=MESH,
        )
        transfer = Transfer(copy, sends, receives)
        self.sent.append(transfer)
        return transfer

    def send(self, source, target, bit=0, shift=0):
        return self.plan(source, target, bit, shift).start()

    def move(self, source, target):
        copy = pltpu.make_async_copy(source, target, self.local_sems.at[self.used_local])
        self.used_local += 1
        copy.start()
        return copy

    def save(self, source, target):
        self.saved.append(self.move(source, target))

    def finish(self):
        for transfer in self.sent:
            transfer.wait_send()
        for copy in self.saved:
            copy.wait()


class Spread:
    def __init__(self, links, own_piece, target, columns):
        self.links, self.own_piece, self.target, self.columns = links, own_piece, target, columns
        self.ahead, self.back, self.swaps = [], [], []

    def _slot(self, index):
        n = self.links.n_tensor
        return self.target.at[lax.rem(index + n, n), :, self.columns]

    def issue(self):
        links, n, z = self.links, self.links.n_tensor, self.links.z_at
        own = self._slot(z)
        for s in range(1, n):
            up_from, down_from = z - (s - 1), z + (s - 1)
            up_source = self.own_piece if s == 1 else self._slot(up_from)
            down_source = self.own_piece if s == 1 else self._slot(down_from)
            self.ahead.append(
                links.plan(
                    up_source, self._slot(up_from), shift=1,
                    sends=(z < n - 1) & (up_from >= 0), receives=z >= s,
                )
            )
            self.back.append(
                links.plan(
                    down_source, self._slot(down_from), shift=-1,
                    sends=(z > 0) & (down_from < n), receives=z + s < n,
                )
            )
        self.ahead[0].start()
        self.back[0].start()
        self.swaps.append(links.plan(self.own_piece, own, bit=GROUP).start())

    def step(self, s):
        links, n, z = self.links, self.links.n_tensor, self.links.z_at
        for arrivals, piece, here in (
            (self.ahead, z - s, z >= s),
            (self.back, z + s, z + s < n),
        ):
            arrivals[s - 1].wait_recv()
            if s < n - 1:
                arrivals[s].start()
            slot = self._slot(piece)
            self.swaps.append(
                links.plan(slot, slot, bit=GROUP, sends=here, receives=here).start()
            )

    def wait(self):
        for swap in self.swaps:
            swap.wait_recv()


def kernel_forward(
    n_dp, n_tensor,
    tokens, cot, gate_w, up_w, down_w, out_w, qkv_w, segments, gain1, gain2, fixed,
    normed1_out, normed2_out, hidden_out, query_out, keyval_out, log_out, att_out,
    cos_out, sin_out, qkv_out, out_out, small_out, cot_out, gate_out, up_out, down_out,
    x_all, n1_all, first, dealt, first_piece, qkv, out_parcel, obuf, gbuf, ubuf, dbuf, piece, outw,
    small, small_all, stream, parts, recv, queries, keyvals,
    att, by_repeat, logs, cosine, sine, low_col, to_core, from_core, to_across, from_across,
    hidden, n2_all, stage, out_sems, in_sems, local_sems,
):
    f32, bf16 = jnp.float32, jnp.bfloat16
    links = Links(n_dp, n_tensor, out_sems, in_sems, local_sems)
    send, move, save = links.send, links.move, links.save
    d_at, z_at = links.d_at, links.z_at
    member = d_at % GROUP
    core = d_at % 2
    upper = d_at // GROUP
    rows, width = tokens.shape
    half = width // 2
    chunk = qkv_w.shape[0]
    contract = (((1,), (1,)), ((), ()))
    columns = pl.ds(pl.multiple_of(upper * half, half), half)

    turned = qkv_w[...].T
    quarter = turned.shape[0] // GROUP
    for i in range(GROUP):
        first[i] = turned[i * quarter : (i + 1) * quarter]
    turned = out_w[...].T
    out_quarter = turned.shape[0] // GROUP
    for i in range(GROUP):
        out_parcel[i] = turned[i * out_quarter : (i + 1) * out_quarter]
    ids = segments[...]
    seqs, length = ids.shape
    begin = jnp.zeros_like(ids)
    for value in range(3):
        count = jnp.sum((ids == value).astype(jnp.int32), axis=1, keepdims=True)
        begin = begin + jnp.where(ids > value, count, 0)
    begin = begin.astype(f32)
    for i in range(seqs):
        stream[:, i * length : (i + 1) * length] = jnp.broadcast_to(
            begin[i : i + 1] + float(i * length), (stream.shape[0], length)
        )
    window = stream[:, pl.ds(pl.multiple_of(z_at * rows, TILE), rows)]
    here = lax.broadcasted_iota(jnp.int32, window.shape, 1) + z_at * rows
    small[...] = window
    small[0:1] = here.astype(f32)[0:1] - window[0:1]
    small[2:3, :chunk] = gain1[...].astype(f32)
    small[3:4, :chunk] = gain2[...].astype(f32)

    @pl.when(z_at == 0)
    def _():
        keyvals[:, :WINDOW, :] = jnp.zeros_like(keyvals[:, :WINDOW, :])

    links.barrier()

    deals = [send(first.at[member ^ k], dealt.at[member], bit=k) for k in range(1, GROUP)]
    beside = send(tokens, x_all.at[2], bit=1)
    smalls = [send(small, small_all.at[d_at], bit=k) for k in range(1, n_dp)]
    def columns_of(ref, at):
        size = ref.shape[1] // GROUP
        return ref.at[:, pl.ds(pl.multiple_of(at * size, TILE), size)]

    def parcel_of(ref, at):
        return ref.at[at]

    pairs = [
        (out_parcel, obuf, parcel_of), (gate_w, gbuf, columns_of), (up_w, ubuf, columns_of),
        (down_w, dbuf, columns_of),
    ]

    def deal(group):
        return [
            send(take(ref, member ^ k), buffer.at[member], bit=k)
            for ref, buffer, take in group
            for k in range(1, GROUP)
        ]

    rests = deal(pairs[:2])
    across = send(tokens, x_all.at[1], bit=2)
    late_rests = deal(pairs[2:])
    own = [move(tokens, x_all.at[0])]
    for ref, buffer, take in pairs:
        own.append(move(take(ref, member), buffer.at[member]))
    cot_stage = move(cot, stage)
    small_all[d_at] = small[...]
    dealt[member] = first[member]

    entries = lax.broadcasted_iota(jnp.int32, (WINDOW, LANES), 0).astype(f32)
    angles = entries * fixed[0:1]

    def split(table):
        pieces = []
        for _ in range(3):
            pieces.append(table.astype(bf16))
            table = table - pieces[-1].astype(f32)
        return pieces

    cos_parts, sin_parts = split(jnp.cos(angles)), split(jnp.sin(angles))
    second = fixed[1:2]
    own_turns = jnp.where(core == 0, jnp.ones_like(second), fixed[2:3])

    for copy in deals:
        copy.wait_recv()
    for i in range(GROUP):
        first_piece[:, i * chunk : (i + 1) * chunk] = dealt[i]
    spread_first = Spread(links, first_piece, qkv, columns)
    spread_first.issue()
    save(first_piece, qkv.at[z_at, :, columns])
    own_qkv = links.saved.pop()
    for copy in own:
        copy.wait()
    cot_stage.wait()
    save(stage, cot_out.at[0])
    spread_first.step(1)
    for copy in smalls:
        copy.wait_recv()
    spread_first.step(2)
    gains = []
    for row in (2, 3):
        gains.append(
            jnp.concatenate([small_all[i, row : row + 1, :chunk] for i in range(n_dp)], axis=1)
        )
    for copy in rests:
        copy.wait_recv()
    sizes = [obuf.shape[1], gbuf.shape[2], ubuf.shape[2], dbuf.shape[2]]
    starts = [sum(sizes[:i]) for i in range(len(sizes))]
    saves = []

    def prepare(index, target, buffer):
        at = slice(starts[index], starts[index] + sizes[index])
        for i in range(GROUP):
            piece[at, i * chunk : (i + 1) * chunk] = buffer[i] if index == 0 else buffer[i].T
        own_piece = piece.at[pl.ds(starts[index], sizes[index])]
        saves.append(move(own_piece, target.at[z_at, :, columns]))
        return Spread(links, own_piece, target, columns)

    out_spread = prepare(0, outw, obuf)
    gate_spread = prepare(1, gate_out, gbuf)
    out_spread.issue()
    spread_first.step(3)
    gate_spread.issue()
    beside.wait_recv()
    own_qkv.wait()
    spread_first.wait()

    def project_block(m, k):
        features = x_all[m].astype(f32)
        scale = lax.rsqrt(jnp.mean(features * features, axis=1, keepdims=True) + EPS)
        normal = (features * scale * gains[0]).astype(bf16)
        n1_all[m] = normal
        units = qkv.shape[0] * qkv.shape[1]
        product = lax.dot_general(
            normal, qkv[...].reshape(units, width), contract, preferred_element_type=f32
        )
        info = small_all[d_at ^ k].T
        key = lax.broadcasted_iota(jnp.int32, (rows, WINDOW), 1)
        chosen = (info[:, 0:1].astype(jnp.int32) == key).astype(bf16)

        def pick(table):
            total = jnp.dot(chosen, table[0], preferred_element_type=f32)
            for part in table[1:]:
                total += jnp.dot(chosen, part, preferred_element_type=f32)
            return total

        cos_here, sin_here = pick(cos_parts), pick(sin_parts)
        parts[m] = turn(product, cos_here, sin_here, second, own_turns, 1.0).astype(bf16)
        if m < 2:
            cosine[m] = cos_here
            sine[m] = sin_here
            low_col[m] = info[:, 1:2].astype(jnp.int32) - z_at * rows + WINDOW

    is_first = core == 0
    halos = [
        links.plan(
            keyvals.at[m, pl.ds(rows, WINDOW)], keyvals.at[m, pl.ds(0, WINDOW)], shift=1,
            sends=z_at < n_tensor - 1, receives=z_at > 0,
        )
        for m in range(2)
    ]

    def take_block(m, swap):
        swap.wait_recv()
        mine, other = parts[m], recv[m]
        queries[m] = jnp.where(is_first, mine, other)
        keyvals[m, WINDOW:, :] = jnp.where(is_first, other, mine)
        halos[m].start()

    project_block(2, 1)
    part_swap = send(parts.at[2], recv.at[0], bit=1)
    project_block(0, 0)
    take_block(0, part_swap)
    out_spread.step(1)
    across.wait_recv()
    both = send(x_all.at[1], x_all.at[3], bit=1)
    cot_across = send(cot, cot_out.at[1], bit=2)
    cot_beside = send(cot, cot_out.at[2], bit=1)
    project_block(1, 2)
    both.wait_recv()
    project_block(3, 3)
    part_swap = send(parts.at[3], recv.at[1], bit=1)
    save(n1_all, normed1_out)
    save(cosine, cos_out)
    save(sine, sin_out)
    take_block(1, part_swap)
    out_spread.step(2)
    gate_spread.step(1)
    for copy in late_rests:
        copy.wait_recv()
    up_spread = prepare(2, up_out, ubuf)
    down_spread = prepare(3, down_out, dbuf)
    save(queries, query_out)
    heads = queries.shape[2] // HEAD_SIZE
    repeat = QUERY_HEADS // KEY_VALUE_HEADS
    span = TILE + WINDOW

    def attend_tile(m, start):
        key = lax.broadcasted_iota(jnp.int32, (TILE, span), 1)
        query = lax.broadcasted_iota(jnp.int32, (TILE, span), 0)
        lowest = low_col[m, pl.ds(start, TILE), :] - start
        allowed = (key >= lowest) & (key <= query + WINDOW)
        for head in range(heads):
            group, r = head // repeat, head % repeat
            base = group * 2 * HEAD_SIZE
            q = queries[m, pl.ds(start, TILE), head * HEAD_SIZE : (head + 1) * HEAD_SIZE]
            k = keyvals[m, pl.ds(start, span), base : base + HEAD_SIZE]
            v = keyvals[m, pl.ds(start, span), base + HEAD_SIZE : base + 2 * HEAD_SIZE]
            s = lax.dot_general(q, k, contract, preferred_element_type=f32) * HEAD_SIZE ** (-0.5)
            s = jnp.where(allowed, s, NEG_FILL)
            highest = jnp.max(s, axis=1, keepdims=True)
            e = jnp.exp(s - highest)
            whole = jnp.sum(e, axis=1, keepdims=True)
            p = (e * (1.0 / whole)).astype(bf16)
            o = jnp.dot(p, v, preferred_element_type=f32).astype(bf16)
            logs[m, pl.ds(start, TILE), head : head + 1] = highest + jnp.log(whole)
            by_repeat[r, m, pl.ds(start, TILE), group * HEAD_SIZE : (group + 1) * HEAD_SIZE] = o

    tiles = rows // TILE
    free = -(-WINDOW // TILE)

    def attend_tiles(blocks, first_tile, last_tile):
        for m in blocks:
            for tile in range(first_tile, last_tile):
                attend_tile(m, tile * TILE)

    attend_tiles((1, 0), free, tiles)
    out_spread.step(3)
    up_spread.issue()
    halos[0].wait_recv()
    halos[1].wait_recv()
    attend_tiles((1,), 0, free)
    att_swap1 = send(by_repeat.at[1 - core, 1], att.at[3], bit=1)
    gate_spread.step(2)
    attend_tiles((0,), 0, free)
    att_swap0 = send(by_repeat.at[1 - core, 0], att.at[2], bit=1)
    save(keyvals, keyval_out)
    save(logs, log_out)
    att[0] = by_repeat[core, 0]
    att[1] = by_repeat[core, 1]
    down_spread.issue()
    cot_across.wait_recv()
    cot_both = send(cot_out.at[1], cot_out.at[3], bit=1)

    saves[0].wait()
    out_spread.wait()

    def project_out(b):
        units = outw.shape[0] * outw.shape[1]
        return jnp.dot(att[b], outw[...].reshape(units, width), preferred_element_type=f32)

    att_swap1.wait_recv()
    to_core[1] = project_out(3).astype(bf16)
    core_send1 = send(to_core.at[1], from_core.at[1], bit=1)
    hidden[...] = project_out(1)
    att_swap0.wait_recv()
    to_core[0] = project_out(2).astype(bf16)
    core_send0 = send(to_core.at[0], from_core.at[0], bit=1)
    core_send1.wait_recv()
    across_sends = []
    for i in range(tiles):
        at = pl.ds(i * TILE, TILE)
        to_across[at] = (hidden[at, :] + from_core[1, at, :].astype(f32)).astype(bf16)
        across_sends.append(send(to_across.at[at], from_across.at[at], bit=2))
    hidden[...] = project_out(0) + x_all[0].astype(f32)
    core_send0.wait_recv()
    hidden[...] += from_core[0].astype(f32)
    save(att, att_out)
    gate_spread.step(3)
    up_spread.step(1)
    steps = [
        (up_spread, 2), (up_spread, 3), (down_spread, 1), (down_spread, 2), (down_spread, 3),
    ]
    last = []
    for i in range(tiles):
        at = pl.ds(i * TILE, TILE)
        across_sends[i].wait_recv()
        value = hidden[at, :] + from_across[at, :].astype(f32)
        hidden[at, :] = value
        scale = lax.rsqrt(jnp.mean(value * value, axis=1, keepdims=True) + EPS)
        n2_all[0, at, :] = (value * scale * gains[1]).astype(bf16)
        last.append(send(n2_all.at[0, at], n2_all.at[1, at], bit=2))
        last.append(send(n2_all.at[0, at], n2_all.at[2, at], bit=1))
        if i < 3:
            spread, s = steps.pop(0)
            spread.step(s)
    save(hidden, hidden_out)
    save(qkv, qkv_out)
    save(outw, out_out)
    save(small_all, small_out)
    ends = []
    for i in range(tiles):
        at = pl.ds(i * TILE, TILE)
        last[2 * i].wait_recv()
        ends.append(send(n2_all.at[1, at], n2_all.at[3, at], bit=1))
        if i < 2:
            spread, s = steps.pop(0)
            spread.step(s)
    for copy in ends + last[1::2]:
        copy.wait_recv()
    save(n2_all, normed2_out)
    for copy in saves[1:]:
        copy.wait()
    for spread in (gate_spread, up_spread, down_spread):
        spread.wait()
    for copy in (cot_beside, cot_both):
        copy.wait_recv()
    links.finish()


def forward(
    n_dp, n_tensor, tokens, cot, segments, gain1, gain2, qkv_w, out_w, gate_w, up_w, down_w
):
    out_w, down_w = out_w.T, down_w.T
    rows, width = tokens.shape
    f32, bf16 = jnp.float32, jnp.bfloat16
    vmem = pl.BlockSpec(memory_space=pltpu.VMEM)
    hbm = pl.BlockSpec(memory_space=pl.ANY)
    chunk = qkv_w.shape[0]
    quarter = qkv_w.shape[1] // GROUP
    sizes = [
        out_w.shape[1] // GROUP, gate_w.shape[1] // GROUP, up_w.shape[1] // GROUP,
        down_w.shape[1] // GROUP,
    ]
    units = quarter * n_tensor
    heads = units // HEAD_SIZE
    lane = np.arange(LANES)
    within = lane % HEAD_SIZE
    fixed = np.zeros((8, LANES), np.float32)
    fixed[0] = np.power(ROPE_BASE, -(2.0 * (within % (HEAD_SIZE // 2))) / HEAD_SIZE)
    fixed[1] = within >= HEAD_SIZE // 2
    fixed[2] = lane % (2 * HEAD_SIZE) < HEAD_SIZE
    fixed[3] = 1.0

    def shape(dims, dtype=bf16):
        return jax.ShapeDtypeStruct(tuple(dims), dtype)

    full = (GROUP, rows, width)
    qkv_shape = (n_tensor, quarter, width)
    out_shape = (n_tensor, sizes[0], width)
    att_shape = (GROUP, rows, units // 2)
    small_shape = (n_dp, 8, rows)
    table = (2, rows, LANES)
    outs = [
        shape(full),
        shape(full),
        shape((rows, width), f32),
        shape((2, rows, units)),
        shape((2, rows + WINDOW, units)),
        shape((2, rows, heads), f32),
        shape(att_shape),
        shape(table, f32),
        shape(table, f32),
        shape(qkv_shape),
        shape(out_shape),
        shape(small_shape, f32),
        shape(full),
    ] + [shape((n_tensor, size, width)) for size in sizes[1:]]
    scratch = [
        pltpu.VMEM(full, bf16),
        pltpu.VMEM(full, bf16),
        pltpu.VMEM((GROUP, quarter, chunk), bf16),
        pltpu.VMEM((GROUP, quarter, chunk), bf16),
        pltpu.VMEM((quarter, width // 2), bf16),
        pltpu.VMEM(qkv_shape, bf16),
        pltpu.VMEM((GROUP, sizes[0], chunk), bf16),
        pltpu.VMEM((GROUP, sizes[0], chunk), bf16),
        pltpu.VMEM((GROUP, chunk, sizes[1]), bf16),
        pltpu.VMEM((GROUP, chunk, sizes[2]), bf16),
        pltpu.VMEM((GROUP, chunk, sizes[3]), bf16),
        pltpu.VMEM((sum(sizes), width // 2), bf16),
        pltpu.VMEM(out_shape, bf16),
        pltpu.VMEM((8, rows), f32),
        pltpu.VMEM(small_shape, f32),
        pltpu.VMEM((8, n_tensor * rows), f32),
        pltpu.VMEM((GROUP, rows, units), bf16),
        pltpu.VMEM((2, rows, units), bf16),
        pltpu.VMEM((2, rows, units), bf16),
        pltpu.VMEM((2, rows + WINDOW, units), bf16),
        pltpu.VMEM(att_shape, bf16),
        pltpu.VMEM((2, 2, rows, units // 2), bf16),
        pltpu.VMEM((2, rows, heads), f32),
        pltpu.VMEM(table, f32),
        pltpu.VMEM(table, f32),
        pltpu.VMEM((2, rows, 1), jnp.int32),
        pltpu.VMEM((2, rows, width), bf16),
        pltpu.VMEM((2, rows, width), bf16),
        pltpu.VMEM((rows, width), bf16),
        pltpu.VMEM((rows, width), bf16),
        pltpu.VMEM((rows, width), f32),
        pltpu.VMEM(full, bf16),
        pltpu.VMEM((rows, width), bf16),
        pltpu.SemaphoreType.DMA((128,)),
        pltpu.SemaphoreType.DMA((128,)),
        pltpu.SemaphoreType.DMA((40,)),
    ]
    results = pl.pallas_call(
        functools.partial(kernel_forward, n_dp, n_tensor),
        in_specs=[hbm] * 5 + [vmem] * 6,
        out_specs=[hbm] * len(outs),
        out_shape=outs,
        scratch_shapes=scratch,
        compiler_params=pltpu.CompilerParams(
            collective_id=0, has_side_effects=True, vmem_limit_bytes=60 * 1024 * 1024
        ),
        name="forward",
    )(
        tokens, cot, gate_w, up_w, down_w, out_w, qkv_w, segments, gain1, gain2,
        jnp.asarray(fixed),
    )
    return results, jnp.asarray(fixed)


def turn(value, cosine, sine, second, turns, sign):
    width = value.shape[1]
    half = HEAD_SIZE // 2
    c = turns * cosine + (1.0 - turns)
    u = (sign * turns * second) * sine
    d = (sign * turns * (second - 1.0)) * sine
    pieces = []
    up = pltpu.roll(value, half, 1)
    down = pltpu.roll(value, width - half, 1)
    for i in range(width // LANES):
        at = slice(i * LANES, (i + 1) * LANES)
        pieces.append(value[:, at] * c + up[:, at] * u + down[:, at] * d)
    return jnp.concatenate(pieces, axis=1)


def kernel_feed(
    n_dp, n_tensor,
    n2_in, cot_in, hidden_in, gate_in, up_in, down_in, smalls,
    grad_out, grad_own_out, mlp_out, down_out, gate_out, up_out, down_got, row_out,
    n2_all, cot_all, gate_w, up_w, down_w, active, gate_delta, up_delta,
    down_part, gate_part, up_part, to_core, from_core, to_across, from_across, hidden, total,
    rounded, row, out_sems, in_sems, local_sems,
):
    f32, bf16 = jnp.float32, jnp.bfloat16
    links = Links(n_dp, n_tensor, out_sems, in_sems, local_sems)
    send, move, save = links.send, links.move, links.save
    upper = links.d_at // GROUP
    rows, width = hidden.shape
    half = width // 2
    chunk = width // n_dp
    size = gate_w.shape[1]
    units = n_tensor * size
    contract = (((1,), (1,)), ((), ()))
    over_rows = (((0,), (0,)), ((), ()))
    other = pl.ds(pl.multiple_of((1 - upper) * half, half), half)
    tiles = rows // TILE

    first_sem = links.used_local
    links.used_local += 3 * n_tensor + 2 * GROUP
    weights = ((gate_in, gate_w), (up_in, up_w), (down_in, down_w))
    tokens = ((n2_in, n2_all), (cot_in, cot_all))

    def weight_loads(p):
        return [
            pltpu.make_async_copy(
                source.at[p], target.at[p], local_sems.at[first_sem + i * n_tensor + p]
            )
            for i, (source, target) in enumerate(weights)
        ]

    def token_loads(m):
        start = first_sem + 3 * n_tensor
        return [
            pltpu.make_async_copy(source.at[m], target.at[m], local_sems.at[start + i * GROUP + m])
            for i, (source, target) in enumerate(tokens)
        ]

    for copy in token_loads(3):
        copy.start()
    for p in range(n_tensor):
        for copy in weight_loads(p):
            copy.start()
    for m in (1, 2, 0):
        for copy in token_loads(m):
            copy.start()
    hidden_load = move(hidden_in, hidden)
    links.barrier()

    def inner(i, carry):
        turn_at, p = i // n_tensor, i % n_tensor
        m = 3 - 2 * (turn_at % 2) - turn_at // 2

        @pl.when(p == 0)
        def _():
            for copy in token_loads(m):
                copy.wait()

        @pl.when(turn_at == 0)
        def _():
            for copy in weight_loads(p):
                copy.wait()

        at = pl.ds(pl.multiple_of(p * size, TILE), size)
        gate = lax.dot_general(n2_all[m], gate_w[p], contract, preferred_element_type=f32)
        up_value = lax.dot_general(n2_all[m], up_w[p], contract, preferred_element_type=f32)
        act_grad = lax.dot_general(cot_all[m], down_w[p], contract, preferred_element_type=f32)
        sigmoid = jax.nn.sigmoid(gate)
        silu = gate * sigmoid
        active[m, :, at] = (silu * up_value).astype(bf16)
        gate_delta[m, :, at] = (
            act_grad * up_value * sigmoid * (1.0 + gate * (1.0 - sigmoid))
        ).astype(bf16)
        up_delta[m, :, at] = (act_grad * silu).astype(bf16)
        return carry

    lax.fori_loop(0, 2 * n_tensor, inner, 0)

    def back(m):
        return jnp.dot(
            gate_delta[m], gate_w[...].reshape(units, width), preferred_element_type=f32
        ) + jnp.dot(up_delta[m], up_w[...].reshape(units, width), preferred_element_type=f32)

    to_core[1] = back(3).astype(bf16)
    core_send1 = send(to_core.at[1], from_core.at[1], bit=1)
    total[...] = back(1)
    core_send1.wait_recv()
    across = []
    for i in range(tiles):
        at = pl.ds(i * TILE, TILE)
        to_across[at] = (total[at, :] + from_core[1, at, :].astype(f32)).astype(bf16)
        across.append(send(to_across.at[at], from_across.at[at], bit=2))
    lax.fori_loop(2 * n_tensor, GROUP * n_tensor, inner, 0)

    order = []
    for i in range((n_tensor + 1) // 2):
        order.extend(dict.fromkeys((n_tensor - 1 - i, i)))

    swaps = []

    def grads(left, right, part, target, weight=None):
        for p in order:
            at = slice(p * size, (p + 1) * size)
            grad = lax.dot_general(
                left[...].reshape(GROUP * rows, units)[:, at],
                right[...].reshape(GROUP * rows, width),
                over_rows,
                preferred_element_type=f32,
            )
            part[p] = grad.astype(bf16)
            if weight is not None:
                row[...] += jnp.sum(grad * weight[p].astype(f32), axis=0, keepdims=True)
            elif p in order[: n_tensor - 1]:
                swaps.append(send(part.at[p, :, other], down_got.at[p], bit=GROUP))
            save(part.at[p], target.at[p])

    row[...] = jnp.zeros_like(row)
    grads(active, cot_all, down_part, down_out)
    to_core[0] = back(2).astype(bf16)
    core_send0 = send(to_core.at[0], from_core.at[0], bit=1)
    total[...] = back(0)
    core_send0.wait_recv()
    total[...] += from_core[0].astype(f32)
    grads(gate_delta, n2_all, gate_part, gate_out, gate_w)
    grads(up_delta, n2_all, up_part, up_out, up_w)
    save(row, row_out)

    for m in range(GROUP):
        n2_all[m] = jnp.dot(
            active[m], down_w[...].reshape(units, width), preferred_element_type=f32
        ).astype(bf16)
        save(n2_all.at[m], mlp_out.at[m])
    gain = jnp.concatenate([smalls[i, 3:4, :chunk] for i in range(n_dp)], axis=1)
    hidden_load.wait()
    for i in range(tiles):
        at = pl.ds(i * TILE, TILE)
        across[i].wait_recv()
        upstream = total[at, :] + from_across[at, :].astype(f32)
        features = hidden[at, :]
        inverse = lax.rsqrt(jnp.mean(features * features, axis=1, keepdims=True) + EPS)
        scaled = gain * upstream
        mean = jnp.mean(scaled * features, axis=1, keepdims=True)
        result = cot_all[0, at, :].astype(f32) + (
            inverse * scaled - features * (inverse * inverse * inverse) * mean
        )
        total[at, :] = result
        rounded[at, :] = result.astype(bf16)
    save(total, grad_out)
    save(rounded, grad_own_out)
    for copy in swaps:
        copy.wait_recv()
    links.finish()


def feed(n_dp, n_tensor, normed2, grad_rows, hidden1, gate_w, up_w, down_w, smalls):
    f32, bf16 = jnp.float32, jnp.bfloat16
    rows, width = hidden1.shape
    half = width // 2
    vmem = pl.BlockSpec(memory_space=pltpu.VMEM)
    hbm = pl.BlockSpec(memory_space=pl.ANY)
    weight = gate_w.shape
    inner = (GROUP, rows, n_tensor * weight[1])

    def shape(dims, dtype=bf16):
        return jax.ShapeDtypeStruct(tuple(dims), dtype)

    outs = [
        shape((rows, width), f32), shape((rows, width)), shape(normed2.shape),
        shape(weight), shape(weight), shape(weight), shape((n_tensor, weight[1], half)),
        shape((1, width), f32),
    ]
    scratch = [
        pltpu.VMEM(normed2.shape, bf16),
        pltpu.VMEM(normed2.shape, bf16),
        pltpu.VMEM(weight, bf16),
        pltpu.VMEM(weight, bf16),
        pltpu.VMEM(weight, bf16),
        pltpu.VMEM(inner, bf16),
        pltpu.VMEM(inner, bf16),
        pltpu.VMEM(inner, bf16),
        pltpu.VMEM(weight, bf16),
        pltpu.VMEM(weight, bf16),
        pltpu.VMEM(weight, bf16),
        pltpu.VMEM((2, rows, width), bf16),
        pltpu.VMEM((2, rows, width), bf16),
        pltpu.VMEM((rows, width), bf16),
        pltpu.VMEM((rows, width), bf16),
        pltpu.VMEM((rows, width), f32),
        pltpu.VMEM((rows, width), f32),
        pltpu.VMEM((rows, width), bf16),
        pltpu.VMEM((1, width), f32),
        pltpu.SemaphoreType.DMA((16,)),
        pltpu.SemaphoreType.DMA((16,)),
        pltpu.SemaphoreType.DMA((40,)),
    ]
    return pl.pallas_call(
        functools.partial(kernel_feed, n_dp, n_tensor),
        in_specs=[hbm] * 6 + [vmem],
        out_specs=[hbm] * len(outs),
        out_shape=outs,
        scratch_shapes=scratch,
        compiler_params=pltpu.CompilerParams(
            collective_id=2, has_side_effects=True, vmem_limit_bytes=67043328
        ),
        name="feed",
    )(normed2, grad_rows, hidden1, gate_w, up_w, down_w, smalls)


class Collect:
    def __init__(
        self, links, part, swapped, stage, arrived, late, blocks, target, mine, other, turned=False
    ):
        self.turned = turned
        self.links, self.part, self.swapped, self.stage = links, part, swapped, stage
        self.arrived, self.late, self.blocks, self.target = arrived, late, blocks, target
        self.mine, self.other = mine, other
        self.swaps, self.loads, self.deals = {}, [], []

    def issue(self, order, load=True):
        links = self.links
        for p in order:
            self.swaps[p] = links.send(
                self.part.at[p, :, self.other], self.swapped.at[p], bit=GROUP
            )
        if self.stage is not None and load:
            self.loads = [links.move(self.part.at[:, :, self.mine], self.stage)]

    def load(self, received, order):
        links = self.links
        count = links.n_tensor - 1
        self.loads = [links.move(received.at[p], self.swapped.at[p]) for p in order[:count]]
        self.loads.append(links.move(self.part.at[:, :, self.mine], self.stage))

    def step(self, p):
        links, n, z = self.links, self.links.n_tensor, self.links.z_at
        f32, bf16 = jnp.float32, jnp.bfloat16
        while self.loads:
            self.loads.pop().wait()
        if p in self.swaps:
            self.swaps[p].wait_recv()
        own = self.stage[p] if self.stage is not None else self.part[p, :, self.mine]
        self.swapped[p] = (own.astype(f32) + self.swapped[p].astype(f32)).astype(bf16)
        if not hasattr(self, "ahead"):
            self.ahead, self.back, self.back_last = [None] * n, [None] * n, [None] * n
        source = self.swapped.at[p]
        self.ahead[p] = links.plan(
            source, self.arrived.at[p], shift=1, sends=z < p, receives=(z > 0) & (z <= p)
        )
        self.back[p] = links.plan(
            source, self.arrived.at[p], shift=-1, sends=z > p + 1,
            receives=(z > p) & (z < n - 1),
        )
        self.back_last[p] = links.plan(
            source, self.late, shift=-1, sends=z == p + 1, receives=(z == p) & (z < n - 1)
        )

        @pl.when((z == 0) & (z < p))
        def _():
            self.ahead[p].copy.start()

        @pl.when((z == n - 1) & (z > p + 1))
        def _():
            self.back[p].copy.start()

        @pl.when((z == n - 1) & (z == p + 1))
        def _():
            self.back_last[p].copy.start()

    def relay(self, i):
        links, n, z = self.links, self.links.n_tensor, self.links.z_at
        f32, bf16 = jnp.float32, jnp.bfloat16

        def add(p):
            self.swapped[p] = (
                self.swapped[p].astype(f32) + self.arrived[p].astype(f32)
            ).astype(bf16)

        for p in range(n):
            at = i - (n - 1) + p
            if 0 < at < n - 1 and at < p:

                @pl.when(z == at)
                def _(p=p):
                    self.ahead[p].copy.wait_recv()
                    add(p)
                    self.ahead[p].copy.start()

            at = n - 1 - i + p
            if 0 < at < n - 1 and at > p:

                @pl.when(z == at)
                def _(p=p, at=at):
                    self.back[p].copy.wait_recv()
                    add(p)
                    (self.back_last if at == p + 1 else self.back)[p].copy.start()

    def finish(self):
        links, n, z = self.links, self.links.n_tensor, self.links.z_at
        f32, bf16 = jnp.float32, jnp.bfloat16
        member = links.d_at % GROUP
        for p in range(n):

            @pl.when((z == p) & (z > 0))
            def _(p=p):
                self.ahead[p].copy.wait_recv()

            @pl.when((z == p) & (z < n - 1))
            def _(p=p):
                self.back_last[p].copy.wait_recv()

        below = jnp.where(z > 0, self.arrived[z].astype(f32), 0.0)
        above = jnp.where(z < n - 1, self.late[...].astype(f32), 0.0)
        total = (self.swapped[z].astype(f32) + below + above).astype(bf16)
        chunk = total.shape[1] // GROUP
        size = self.blocks.shape[2 if self.turned else 1]
        place = pl.ds(pl.multiple_of(member * size, 16), size)
        if self.turned:
            place = pl.ds(pl.multiple_of(member * size, TILE), size)
        for i in range(GROUP):
            block = total[:, i * chunk : (i + 1) * chunk]
            self.blocks[i] = block.T if self.turned else block
        if self.turned:
            target = self.target.at[:, place]
        elif len(self.target.shape) == 2:
            target = self.target.at[place, :]
        else:
            target = self.target.at[member]
        for k in range(1, GROUP):
            self.deals.append(links.send(self.blocks.at[member ^ k], target, bit=k))
        links.save(self.blocks.at[member], target)

    def wait(self):
        for deal in self.deals:
            deal.wait_recv()


def kernel_backward(
    n_dp, n_tensor,
    grad_own, hidden_grad, tokens, hidden1, mlp_part, n1_in, query_in, keyval_in, log_in, att_in,
    cos_in, sin_in, qkv_in, out_in, small_in, down_in, gate_in, up_in, down_got,
    mlp_row, fixed,
    input_out, block_out, qkv_out, out_out, gate_out, up_out, down_out,
    g_all, n1_all, qkv, outw, queries, keyvals, logs, att, cosine, sine, gains, low_col,
    att_grad, other_grad, totals, query_total, pass_on, delta, halo_send, halo_recv,
    to_core, from_core, to_across, from_across, mlp_across, hidden, stage, gate_stage,
    down_swap, gate_swap, up_swap, out_swap, qkv_swap,
    down_come, gate_come, up_come, out_come, qkv_come,
    down_late, gate_late, up_late, out_late, qkv_late,
    down_block, gate_block, up_block, out_block, qkv_block,
    out_sems, in_sems, local_sems,
):
    f32, bf16 = jnp.float32, jnp.bfloat16
    links = Links(n_dp, n_tensor, out_sems, in_sems, local_sems)
    send, move, save = links.send, links.move, links.save
    d_at, z_at = links.d_at, links.z_at
    core = d_at % 2
    upper = d_at // GROUP
    rows, width = grad_own.shape
    half = width // 2
    contract = (((1,), (1,)), ((), ()))
    over_rows = (((0,), (0,)), ((), ()))
    mine = pl.ds(pl.multiple_of(upper * half, half), half)
    other = pl.ds(pl.multiple_of((1 - upper) * half, half), half)
    tiles = rows // TILE
    span = TILE + WINDOW
    quarter = qkv.shape[1]
    out_quarter = outw.shape[1]
    extra = qkv_swap.shape[1] - quarter

    order = []
    for i in range((n_tensor + 1) // 2):
        order.extend(dict.fromkeys((n_tensor - 1 - i, i)))

    down = Collect(
        links, down_in, down_swap, stage, down_come, down_late, down_block, down_out, mine, other,
        turned=True,
    )
    gate = Collect(
        links, gate_in, gate_swap, gate_stage, gate_come, gate_late, gate_block, gate_out, mine, other,
        turned=True,
    )
    up = Collect(
        links, up_in, up_swap, stage, up_come, up_late, up_block, up_out, mine, other, turned=True
    )
    out_part = g_all.at[:, pl.ds(quarter + extra, out_quarter), :]
    qkv_part = g_all.at[:, pl.ds(0, quarter + extra), :]
    out_collect = Collect(
        links, out_part, out_swap, None, out_come, out_late, out_block, out_out, mine, other
    )
    qkv_collect = Collect(
        links, qkv_part, qkv_swap, None, qkv_come, qkv_late, qkv_block, qkv_out, mine, other
    )
    small = move(small_in, gains)
    loads = [
        move(grad_own, g_all.at[0]), move(out_in, outw),
    ]
    down.load(down_got, order)
    loads += [
        move(query_in, queries),
        move(keyval_in, keyvals), move(log_in, logs), move(cos_in, cosine), move(sin_in, sine),
        move(mlp_part.at[pl.ds(0, 2)], to_core), move(hidden1, hidden), move(att_in, att),
        move(qkv_in, qkv), move(n1_in, n1_all),
    ]
    links.barrier()
    across = send(grad_own, g_all.at[1], bit=2)
    beside = send(grad_own, g_all.at[2], bit=1)
    mlp_core = send(mlp_part.at[pl.ds(2, 2)], from_core, bit=1)
    down.issue(order[n_tensor - 1 :], load=False)
    gate.issue(order)
    for p in order[: n_tensor - 1]:
        down.step(p)
    small.wait()
    for m, k in ((0, 0), (1, 2)):
        info = gains[d_at ^ k].T
        low_col[m] = info[:, 1:2].astype(jnp.int32) - z_at * rows + WINDOW
    loads[0].wait()
    loads[1].wait()

    def attended_back(b):
        units = outw.shape[0] * outw.shape[1]
        att_grad[b] = lax.dot_general(
            g_all[b], outw[...].reshape(units, width), contract, preferred_element_type=f32
        ).astype(bf16)

    attended_back(0)
    beside.wait_recv()
    attended_back(2)
    grad_swap = send(att_grad.at[2], other_grad.at[0], bit=1)
    for copy in loads[2:]:
        copy.wait()
    mlp_core.wait_recv()
    heads = queries.shape[2] // HEAD_SIZE
    repeat = QUERY_HEADS // KEY_VALUE_HEADS
    scale = HEAD_SIZE ** (-0.5)
    is_first = core == 0
    second, keys_turn, all_turn = fixed[1:2], fixed[2:3], fixed[3:4]

    def back_tile(m, tile):
        start = tile * TILE
        at = slice(start, start + TILE)
        reach = slice(start, start + span)
        key = lax.broadcasted_iota(jnp.int32, (TILE, span), 1)
        query = lax.broadcasted_iota(jnp.int32, (TILE, span), 0)
        allowed = (key >= low_col[m, at, :] - start) & (key <= query + WINDOW)
        own, others = att_grad[m, at, :], other_grad[m, at, :]
        by_repeat = (jnp.where(is_first, own, others), jnp.where(is_first, others, own))
        for group in range(heads // repeat):
            base = group * 2 * HEAD_SIZE
            k = keyvals[m, reach, base : base + HEAD_SIZE]
            v = keyvals[m, reach, base + HEAD_SIZE : base + 2 * HEAD_SIZE]
            key_sum = None
            for r in range(repeat):
                head = group * repeat + r
                q = queries[m, at, head * HEAD_SIZE : (head + 1) * HEAD_SIZE]
                g = by_repeat[r][:, group * HEAD_SIZE : (group + 1) * HEAD_SIZE]
                s = lax.dot_general(q, k, contract, preferred_element_type=f32) * scale
                total = logs[m, at, head : head + 1]
                p = jnp.exp(jnp.where(allowed, s, NEG_FILL) - total)
                pg = lax.dot_general(g, v, contract, preferred_element_type=f32)
                inner = jnp.sum(p * pg, axis=1, keepdims=True)
                sg = (p * (pg - inner) * scale).astype(bf16)
                query_total[:, head * HEAD_SIZE : (head + 1) * HEAD_SIZE] = jnp.dot(
                    sg, k, preferred_element_type=f32
                )
                dk = lax.dot_general(sg, q, over_rows, preferred_element_type=f32)
                dv = lax.dot_general(p.astype(bf16), g, over_rows, preferred_element_type=f32)
                both = jnp.concatenate([dk, dv], axis=1)
                key_sum = both if key_sum is None else key_sum + both
            totals[m, reach, base : base + 2 * HEAD_SIZE] += key_sum
        turned = turn(
            query_total[...], cosine[m, at, :], sine[m, at, :], second, all_turn, -1.0
        ).astype(bf16)

        @pl.when(is_first)
        def _():
            delta[m, at, :] = turned

        @pl.when(core != 0)
        def _():
            pass_on[m, at, :] = turned

    halos = [
        links.plan(
            halo_send.at[m], halo_recv.at[m], shift=-1, sends=z_at > 0,
            receives=z_at < n_tensor - 1,
        )
        for m in range(2)
    ]

    def back_tiles(m, first_tile, last_tile):
        for tile in range(first_tile, last_tile):
            back_tile(m, tile)

    def send_halo(m):
        halo_send[m] = totals[m, :WINDOW].astype(bf16)
        halos[m].start()

    def finish_block(m):
        halos[m].wait_recv()
        full = totals[m, WINDOW:]
        tail = full[rows - WINDOW :] + jnp.where(
            z_at < n_tensor - 1, halo_recv[m].astype(f32), 0.0
        )
        full = jnp.concatenate([full[: rows - WINDOW], tail], axis=0)
        turned = turn(full, cosine[m], sine[m], second, keys_turn, -1.0).astype(bf16)

        @pl.when(is_first)
        def _():
            pass_on[m] = turned

        @pl.when(core != 0)
        def _():
            delta[m] = turned

        return send(pass_on.at[m], delta.at[2 + m], bit=1)

    free = -(-WINDOW // TILE)
    totals[...] = jnp.zeros_like(totals)
    grad_swap.wait_recv()
    back_tiles(0, 0, free)
    down.relay(1)
    send_halo(0)
    for p in order[n_tensor - 1 : n_tensor - 1]:
        down.step(p)
    back_tiles(0, free, tiles)
    for p in order[n_tensor - 1 :]:
        down.step(p)
    up.issue(order)
    across.wait_recv()
    both = send(g_all.at[1], g_all.at[3], bit=1)
    to_across[...] = (to_core[1].astype(f32) + from_core[1].astype(f32)).astype(bf16)
    mlp_send = send(to_across, mlp_across, bit=2)
    hidden[...] += to_core[0].astype(f32) + from_core[0].astype(f32)
    attended_back(1)
    both.wait_recv()
    attended_back(3)
    grad_swap = send(att_grad.at[3], other_grad.at[1], bit=1)
    gate.step(order[0])

    def weight_grad(left, right, at):
        total = None
        for b in range(GROUP):
            term = lax.dot_general(
                left[b, :, at], right[b], over_rows, preferred_element_type=f32
            )
            total = term if total is None else total + term
        return total

    out_grad = weight_grad(att, g_all, slice(0, n_tensor * out_quarter)).astype(bf16)
    both.wait_send()
    links.sent.remove(both)
    out_part[...] = out_grad.reshape(n_tensor, out_quarter, width)
    grad_swap.wait_recv()
    back_tiles(1, 0, 1)
    gate.step(order[1])
    back_tiles(1, 1, free)
    for i in range(2, n_tensor - 1):
        down.relay(i)
    send_halo(1)
    back_tiles(1, free, tiles)
    for p in order[2 : n_tensor - 1]:
        gate.step(p)
    swap0 = finish_block(0)
    gate.relay(1)
    swap1 = finish_block(1)
    grad_loads = [
        move(hidden_grad.at[:, pl.ds(i * half, half)], totals.at[i, pl.ds(0, rows)])
        for i in range(2)
    ]
    down.finish()
    for p in order[n_tensor - 1 :]:
        gate.step(p)

    def project_back(b):
        units = qkv.shape[0] * quarter
        return jnp.dot(delta[b], qkv[...].reshape(units, width), preferred_element_type=f32)

    mlp_send.wait_recv()
    mlp_across[...] = (hidden[...] + mlp_across[...].astype(f32)).astype(bf16)
    save(mlp_across, block_out)
    mlp_send.wait_send()
    links.sent.remove(mlp_send)
    swap1.wait_recv()
    to_core[1] = project_back(3).astype(bf16)
    core_send1 = send(to_core.at[1], from_core.at[1], bit=1)
    hidden[...] = project_back(1)
    swap0.wait_recv()
    to_core[0] = project_back(2).astype(bf16)
    core_send0 = send(to_core.at[0], from_core.at[0], bit=1)
    core_send1.wait_recv()
    across_sends = []
    for i in range(tiles):
        at = pl.ds(i * TILE, TILE)
        to_across[at] = (hidden[at, :] + from_core[1, at, :].astype(f32)).astype(bf16)
        across_sends.append(send(to_across.at[at], from_across.at[at], bit=2))
    hidden[...] = project_back(0)
    core_send0.wait_recv()
    hidden[...] += from_core[0].astype(f32)
    up.step(order[0])
    attn_row = None
    for p in range(n_tensor):
        at = slice(p * quarter, (p + 1) * quarter)
        grad = weight_grad(delta, n1_all, at)
        row = jnp.sum(grad * qkv[p].astype(f32), axis=0, keepdims=True)
        attn_row = row if attn_row is None else attn_row + row
        qkv_part[p, :quarter, :] = grad.astype(bf16)
    ending = jnp.concatenate(
        [attn_row, mlp_row[...], jnp.zeros((extra - 2, width), f32)], axis=0
    ).astype(bf16)
    for p in range(n_tensor):
        qkv_part[p, quarter:, :] = ending
    qkv_collect.issue(order)
    out_collect.issue(order)
    token_load = move(tokens, n1_all.at[0])
    up.step(order[1])
    gain = jnp.concatenate([gains[i, 2:3, : width // n_dp] for i in range(n_dp)], axis=1)
    for i in range(tiles):
        at = pl.ds(i * TILE, TILE)
        across_sends[i].wait_recv()
        if i == 0:
            for copy in grad_loads + [token_load]:
                copy.wait()
        upstream = hidden[at, :] + from_across[at, :].astype(f32)
        features = n1_all[0, at, :].astype(f32)
        inverse = lax.rsqrt(jnp.mean(features * features, axis=1, keepdims=True) + EPS)
        scaled = gain * upstream
        mean = jnp.mean(scaled * features, axis=1, keepdims=True)
        change = inverse * scaled - features * (inverse * inverse * inverse) * mean
        n1_all[1, at, :half] = (totals[0, at, :] + change[:, :half]).astype(bf16)
        n1_all[1, at, half:] = (totals[1, at, :] + change[:, half:]).astype(bf16)
        if i == 0:
            for j in range(2, n_tensor - 1):
                gate.relay(j)
        if i == 1:
            for p in order[2 : n_tensor - 1]:
                up.step(p)
    save(n1_all.at[1], input_out)
    gate.finish()
    for p in order[n_tensor - 1 :]:
        up.step(p)
    up.relay(1)
    for p in order[:2]:
        qkv_collect.step(p)
    for i in range(2, n_tensor - 1):
        up.relay(i)
    for p in order[2 : n_tensor - 1]:
        qkv_collect.step(p)
    up.finish()
    for p in order[n_tensor - 1 :]:
        qkv_collect.step(p)
    qkv_collect.relay(1)
    for p in order[:2]:
        out_collect.step(p)
    for i in range(2, n_tensor - 1):
        qkv_collect.relay(i)
    for p in order[2:]:
        out_collect.step(p)
    out_collect.relay(1)
    qkv_collect.finish()
    for i in range(2, n_tensor - 1):
        out_collect.relay(i)
    out_collect.finish()
    for collect in (down, gate, up, out_collect, qkv_collect):
        collect.wait()
    links.finish()


def backward(
    n_dp, n_tensor, grad_own, hidden_grad, tokens, hidden1, mlp_part, normed1, queries, keyvals, logs, attended,
    cosine, sine, qkv_full, out_full, smalls, down_part, gate_part, up_part, down_got,
    mlp_row, fixed,
):
    f32, bf16 = jnp.float32, jnp.bfloat16
    rows, width = grad_own.shape
    half = width // 2
    chunk = width // n_dp
    units = queries.shape[2]
    vmem = pl.BlockSpec(memory_space=pltpu.VMEM)
    hbm = pl.BlockSpec(memory_space=pl.ANY)
    extra = 16
    quarters = [
        down_part.shape[1], gate_part.shape[1], up_part.shape[1], out_full.shape[1],
        qkv_full.shape[1] + extra,
    ]

    def shape(dims, dtype=bf16):
        return jax.ShapeDtypeStruct(tuple(dims), dtype)

    def finals(index):
        return shape((GROUP, quarters[index], chunk))

    outs = [
        shape((rows, width)), shape((rows, width)), finals(4), shape((GROUP * quarters[3], chunk)),
        shape((chunk, GROUP * quarters[1])), shape((chunk, GROUP * quarters[2])),
        shape((chunk, GROUP * quarters[0])),
    ]
    full = (GROUP, rows, width)
    scratch = [
        pltpu.VMEM(full, bf16),
        pltpu.VMEM(full, bf16),
        pltpu.VMEM(qkv_full.shape, bf16),
        pltpu.VMEM(out_full.shape, bf16),
        pltpu.VMEM(queries.shape, bf16),
        pltpu.VMEM(keyvals.shape, bf16),
        pltpu.VMEM(logs.shape, f32),
        pltpu.VMEM(attended.shape, bf16),
        pltpu.VMEM(cosine.shape, f32),
        pltpu.VMEM(sine.shape, f32),
        pltpu.VMEM(smalls.shape, f32),
        pltpu.VMEM((2, rows, 1), jnp.int32),
        pltpu.VMEM(attended.shape, bf16),
        pltpu.VMEM((2,) + attended.shape[1:], bf16),
        pltpu.VMEM((2, rows + WINDOW, units), f32),
        pltpu.VMEM((TILE, units), f32),
        pltpu.VMEM((2, rows, units), bf16),
        pltpu.VMEM((GROUP, rows, units), bf16),
        pltpu.VMEM((2, WINDOW, units), bf16),
        pltpu.VMEM((2, WINDOW, units), bf16),
        pltpu.VMEM((2, rows, width), bf16),
        pltpu.VMEM((2, rows, width), bf16),
        pltpu.VMEM((rows, width), bf16),
        pltpu.VMEM((rows, width), bf16),
        pltpu.VMEM((rows, width), bf16),
        pltpu.VMEM((rows, width), f32),
        pltpu.VMEM((n_tensor, quarters[0], half), bf16),
        pltpu.VMEM((n_tensor, quarters[1], half), bf16),
    ]
    scratch += [pltpu.VMEM((n_tensor, q, half), bf16) for q in quarters]
    scratch += [pltpu.VMEM((n_tensor, q, half), bf16) for q in quarters]
    scratch += [pltpu.VMEM((q, half), bf16) for q in quarters]
    scratch += [
        pltpu.VMEM((GROUP, chunk, q) if turned else (GROUP, q, chunk), bf16)
        for q, turned in zip(quarters, (True, True, True, False, False))
    ]
    scratch += [
        pltpu.SemaphoreType.DMA((160,)),
        pltpu.SemaphoreType.DMA((160,)),
        pltpu.SemaphoreType.DMA((40,)),
    ]
    return pl.pallas_call(
        functools.partial(kernel_backward, n_dp, n_tensor),
        in_specs=[hbm] * 19 + [vmem] * 2,
        out_specs=[hbm] * len(outs),
        out_shape=outs,
        scratch_shapes=scratch,
        compiler_params=pltpu.CompilerParams(
            collective_id=1, has_side_effects=True, vmem_limit_bytes=67043328
        ),
        name="backward",
    )(
        grad_own, hidden_grad, tokens, hidden1, mlp_part, normed1, queries, keyvals, logs, attended, cosine, sine,
        qkv_full, out_full, smalls, down_part, gate_part, up_part, down_got, mlp_row, fixed,
    )


def fast_local(
    n_dp,
    n_tensor,
    block_in,
    cotangent,
    segment_ids,
    attn_gain,
    qkv_weight,
    out_weight,
    mlp_gain,
    gate_weight,
    up_weight,
    down_weight,
):
    bf16, f32 = jnp.bfloat16, jnp.float32
    rows, width = block_in.shape
    part = attn_gain.shape[0]
    (
        normed1, normed2, hidden1, queries, keyvals, log_total, attended, cosine, sine, qkv_full,
        out_full, smalls, grad_rows, gate_full, up_full, down_full,
    ), fixed = forward(
        n_dp, n_tensor, block_in, cotangent, segment_ids, attn_gain[None], mlp_gain[None],
        qkv_weight, out_weight, gate_weight, up_weight, down_weight,
    )
    (
        hidden1_grad, grad_own, mlp_part, down_part, gate_part, up_part, down_got, mlp_row,
    ) = feed(n_dp, n_tensor, normed2, grad_rows, hidden1, gate_full, up_full, down_full, smalls)
    input_grad, block_out, qkv_blocks, out_grad, gate_grad, up_grad, down_grad = backward(
        n_dp, n_tensor, grad_own, hidden1_grad, block_in, hidden1, mlp_part, normed1, queries,
        keyvals, log_total, attended, cosine, sine, qkv_full, out_full, smalls, down_part, gate_part, up_part, down_got, mlp_row,
        fixed,
    )
    quarter = qkv_full.shape[1]

    def row_of(index, gain):
        return jnp.sum(qkv_blocks[:, quarter + index].astype(f32), axis=0) / gain.astype(f32)

    blocks = qkv_blocks[:, :quarter]
    qkv_grad = blocks.reshape(-1, blocks.shape[2]).T.astype(f32)
    gains = [row_of(0, attn_gain), row_of(1, mlp_gain)]
    return (
        block_out,
        input_grad,
        gains[0],
        qkv_grad,
        out_grad.astype(f32),
        gains[1],
        gate_grad.astype(f32),
        up_grad.astype(f32),
        down_grad.T.astype(f32),
    )


def solution(mesh):
    in_specs = (
        P(("dp", "tensor"), None),
        P(("dp", "tensor"), None),
        P("dp", None),
        P("dp"),
        P("dp", "tensor"),
        P("tensor", "dp"),
        P("dp"),
        P("dp", "tensor"),
        P("dp", "tensor"),
        P("tensor", "dp"),
    )
    out_specs = (
        P(("dp", "tensor"), None),
        P(("dp", "tensor"), None),
        P("dp"),
        P("dp", "tensor"),
        P("tensor", "dp"),
        P("dp"),
        P("dp", "tensor"),
        P("dp", "tensor"),
        P("tensor", "dp"),
    )
    n_dp, n_tensor = mesh.shape["dp"], mesh.shape["tensor"]

    def body(*arrays):
        rows = arrays[0].shape[0]
        groups = arrays[4].shape[1] // (4 * HEAD_SIZE)
        if n_dp == 2 * GROUP and groups == 2 and rows >= WINDOW and rows % TILE == 0:
            return fast_local(n_dp, n_tensor, *arrays)
        return local(*arrays)

    return jax.shard_map(body, mesh=mesh, in_specs=in_specs, out_specs=out_specs, check_vma=False)
```
